8 devices in a mesh: dp: 2 (over z, y), sp: 4 (over x, core).
Axes of the slice: x: 2, y: 2, z: 1, core: 2. Of those that a mesh axis runs over, the one named last changes fastest.
Arguments:
- x: bfloat16 [8192, 3072], P(('dp', 'sp')), parts along dimension 0
- grad_out: bfloat16 [8192, 3072], P(('dp', 'sp')), parts along dimension 0
- positions: int32 [8192], P(('dp', 'sp')), parts along dimension 0
- gain: bfloat16 [3072], replicated
- w_q: bfloat16 [3072, 3072], replicated
- w_k: bfloat16 [3072, 1024], replicated
- w_v: bfloat16 [3072, 1024], replicated
- w_o: bfloat16 [3072, 3072], replicated
Outputs:
- output 1: bfloat16 [8192, 3072], P(('dp', 'sp')), parts along dimension 0
- output 2: bfloat16 [8192, 3072], P(('dp', 'sp')), parts along dimension 0
- output 3: float32 [6144, 3072], P('dp'), parts along dimension 0
- output 4: float32 [6144, 1024], P('dp'), parts along dimension 0
- output 5: float32 [6144, 1024], P('dp'), parts along dimension 0
- output 6: float32 [6144, 3072], P('dp'), parts along dimension 0
- output 7: float32 [6144], P('dp'), parts along dimension 0
There are 2 independent parts. The reference program is written for one: setup_inputs(seed, part) draws one part's arguments, and reference() takes and returns one part's arrays. A program takes and returns all parts, laid end to end along the dimension named above; an argument that names none is the same for every part.
All inputs are finite; a program needn't handle non-finite values.
Results may differ from the reference program's by a relative error of at most 0.0183931.
Values are sent between devices in bfloat16 or wider.
A program may use at most 1 GiB of HBM per device.

```python
import jax
import jax.numpy as jnp
from jax import lax

D = 3072
HEADS = 24
KV_HEADS = 8
HEAD = 128
SEQ = 4096
GROUP = HEADS // KV_HEADS
ROPE_THETA = 1000000.0
NORM_EPS = 1e-05
NEG_LARGE = -1e30


def block_rows(seq_len, row_cost):
    row_count = seq_len
    while row_count > 8 and row_count * row_cost > 2 ** 24:
        row_count = row_count // 2
    return row_count


def setup_inputs(seed: int = 0, part: int = 0) -> dict:
    base_key = jax.random.key(seed)
    part_key = jax.random.fold_in(base_key, part)
    key_x, key_dy, key_start, key_step = jax.random.split(part_key, 4)
    shared = jax.random.split(jax.random.key(seed + 1), 5)
    x = jax.random.normal(key_x, (SEQ, D), jnp.float32).astype(jnp.bfloat16)
    grad_out = jax.random.normal(key_dy, (SEQ, D), jnp.float32).astype(jnp.bfloat16)
    pos_start = jax.random.randint(key_start, (), 0, SEQ)
    pos_steps = jax.random.randint(key_step, (SEQ,), 1, 4)
    positions = (pos_start + jnp.cumsum(pos_steps) - pos_steps[0]).astype(jnp.int32)
    gain = (1.0 + 0.3 * jax.random.normal(shared[0], (D,), jnp.float32)).astype(jnp.bfloat16)
    w_q = (jax.random.normal(shared[1], (D, HEADS * HEAD), jnp.float32) * D ** -0.5).astype(jnp.bfloat16)
    w_k = (jax.random.normal(shared[2], (D, KV_HEADS * HEAD), jnp.float32) * D ** -0.5).astype(jnp.bfloat16)
    w_v = (jax.random.normal(shared[3], (D, KV_HEADS * HEAD), jnp.float32) * D ** -0.5).astype(jnp.bfloat16)
    w_o = (jax.random.normal(shared[4], (HEADS * HEAD, D), jnp.float32) * (HEADS * HEAD) ** -0.5).astype(jnp.bfloat16)
    return {'x': x, 'grad_out': grad_out, 'positions': positions, 'gain': gain, 'w_q': w_q, 'w_k': w_k, 'w_v': w_v, 'w_o': w_o}


def rope(values, cos_t, sin_t):
    half_dim = HEAD // 2
    lower_half = values[..., :half_dim]
    upper_half = values[..., half_dim:]
    return jnp.concatenate([lower_half * cos_t - upper_half * sin_t, upper_half * cos_t + lower_half * sin_t], axis=-1)


def attend(q_all, k_all, v_all):
    row_count = block_rows(SEQ, HEADS * SEQ)
    n_blocks = SEQ // row_count
    key_f = k_all.astype(jnp.float32)
    val_f = v_all.astype(jnp.float32)
    key_index = jnp.arange(SEQ)
    q_blocks = q_all.reshape(n_blocks, row_count, KV_HEADS, GROUP, HEAD)
    blk_starts = jnp.arange(n_blocks) * row_count

    def one_block(block_args):
        q_blk, blk_start = block_args
        scores = jnp.einsum('qhgd,khd->hgqk', q_blk.astype(jnp.float32), key_f) * HEAD ** -0.5
        causal = (blk_start + jnp.arange(row_count))[:, None] >= key_index[None, :]
        attn_prob = jax.nn.softmax(jnp.where(causal, scores, NEG_LARGE), axis=-1)
        blk_out = jnp.einsum('hgqk,khd->qhgd', attn_prob.astype(jnp.bfloat16).astype(jnp.float32), val_f)
        return blk_out.astype(jnp.bfloat16)

    outputs = lax.map(jax.checkpoint(one_block), (q_blocks, blk_starts))
    return outputs.reshape(SEQ, KV_HEADS, GROUP, HEAD)


def reference(x, grad_out, positions, gain, w_q, w_k, w_v, w_o):
    inv_freq = ROPE_THETA ** (-jnp.arange(0, HEAD, 2).astype(jnp.float32) / HEAD)
    angles = positions.astype(jnp.float32)[:, None] * inv_freq[None, :]
    cos_t = jnp.cos(angles)[:, None, :]
    sin_t = jnp.sin(angles)[:, None, :]

    def forward(x_f, gain_f, wq_f, wk_f, wv_f, wo_f):
        normed = x_f * lax.rsqrt(jnp.mean(x_f * x_f, axis=-1, keepdims=True) + NORM_EPS)
        hidden = (normed * gain_f).astype(jnp.bfloat16).astype(jnp.float32)
        q_proj = jnp.dot(hidden, wq_f, preferred_element_type=jnp.float32).reshape(SEQ, HEADS, HEAD)
        k_proj = jnp.dot(hidden, wk_f, preferred_element_type=jnp.float32).reshape(SEQ, KV_HEADS, HEAD)
        v_all = jnp.dot(hidden, wv_f, preferred_element_type=jnp.float32).astype(jnp.bfloat16).reshape(SEQ, KV_HEADS, HEAD)
        q_all = rope(q_proj, cos_t, sin_t).astype(jnp.bfloat16).reshape(SEQ, KV_HEADS, GROUP, HEAD)
        k_all = rope(k_proj, cos_t, sin_t).astype(jnp.bfloat16)
        attn = attend(q_all, k_all, v_all).reshape(SEQ, HEADS * HEAD)
        mixed = jnp.dot(attn.astype(jnp.float32), wo_f, preferred_element_type=jnp.float32)
        return (x_f + mixed).astype(jnp.bfloat16)

    result, pullback = jax.vjp(forward, x.astype(jnp.float32), gain.astype(jnp.float32), w_q.astype(jnp.float32), w_k.astype(jnp.float32), w_v.astype(jnp.float32), w_o.astype(jnp.float32))
    grad_xf, grad_gain, grad_wq, grad_wk, grad_wv, grad_wo = pullback(grad_out)
    return result, grad_xf.astype(jnp.bfloat16), grad_wq, grad_wk, grad_wv, grad_wo, grad_gain
```

```python
import functools
import math

import jax
import jax.numpy as jnp
from jax import lax
from jax.experimental import pallas as pl
from jax.experimental.pallas import tpu as pltpu
from jax.sharding import PartitionSpec as P

HEAD = 128
GROUP = 3
ROPE_THETA = 1000000.0
NORM_EPS = 1e-05
NEG_LARGE = -1e30
BF = jnp.bfloat16
F32 = jnp.float32
SCALE = HEAD ** -0.5
SCALE2 = SCALE * math.log2(math.e)
BLK = 512
VMEM_LIMIT = 62 * 1024 * 1024


def params(n_axes=1, limit=VMEM_LIMIT):
    return pltpu.CompilerParams(dimension_semantics=("arbitrary",) * n_axes, vmem_limit_bytes=limit)


def cost(flops, nbytes, trans=0):
    return pl.CostEstimate(flops=int(flops), bytes_accessed=int(nbytes), transcendentals=int(trans))


def mm(a, b):
    return jnp.dot(a, b, preferred_element_type=F32)


def mm_nt(a, b):
    return lax.dot_general(a, b, (((1,), (1,)), ((), ())), preferred_element_type=F32)


def rotate(val, cos_t, sin_t):
    return val * cos_t + pltpu.roll(val, HEAD // 2, 1) * sin_t


def proj_body(s_ref, x_ref, gain_ref, wq_ref, wk_ref, wv_ref, cos_ref, sin_ref, *rest):
    h_ref, q_ref, k_ref, v_ref = rest[-4:]
    xf = x_ref[...].astype(F32)
    inv = lax.rsqrt(jnp.mean(xf * xf, axis=-1, keepdims=True) + NORM_EPS)
    h_ref[...] = ((xf * inv) * gain_ref[...]).astype(BF)
    h = h_ref[...]
    cos_t, sin_t = cos_ref[...], sin_ref[...]
    for c in range(wq_ref.shape[1] // 256):
        out = mm(h, wq_ref[:, c * 256:(c + 1) * 256])
        for b in range(2):
            part = rotate(out[:, b * HEAD:(b + 1) * HEAD], cos_t, sin_t)
            q_ref[:, c * 256 + b * HEAD:c * 256 + (b + 1) * HEAD] = part.astype(BF)
    out = mm(h, wk_ref[...])
    for b in range(2):
        k_ref[:, b * HEAD:(b + 1) * HEAD] = rotate(out[:, b * HEAD:(b + 1) * HEAD], cos_t, sin_t).astype(BF)
    v_ref[...] = mm(h, wv_ref[...]).astype(BF)


def project(idx, x, gain, w_q, w_k, w_v, cos_t, sin_t, bufs, seq):
    rows, d = x.shape
    bm = min(512, rows)
    nb = rows // bm
    qc, kc = w_q.shape[1] // 4, w_k.shape[1] // 4
    row_map = lambda i, s: (s[0] * nb + i, 0)
    w_map = lambda i, s: (0, s[1])
    in_specs = [pl.BlockSpec((bm, d), lambda i, s: (i, 0)),
                pl.BlockSpec((1, d), lambda i, s: (0, 0)),
                pl.BlockSpec((d, qc), w_map), pl.BlockSpec((d, kc), w_map), pl.BlockSpec((d, kc), w_map),
                pl.BlockSpec((bm, HEAD), row_map), pl.BlockSpec((bm, HEAD), row_map)]
    args = [idx, x, gain, w_q, w_k, w_v, cos_t, sin_t]
    aliases = {}
    if bufs is not None:
        in_specs += [pl.BlockSpec(memory_space=pl.ANY)] * 4
        aliases = {len(args) + n: n for n in range(4)}
        args += list(bufs)
    widths = (d, qc, kc, kc)
    return pl.pallas_call(
        proj_body,
        grid_spec=pltpu.PrefetchScalarGridSpec(
            num_scalar_prefetch=1, grid=(nb,), in_specs=in_specs,
            out_specs=[pl.BlockSpec((bm, w), row_map) for w in widths]),
        out_shape=[jax.ShapeDtypeStruct((seq, w), BF) for w in widths],
        input_output_aliases=aliases,
        compiler_params=params(), name="proj",
        cost_estimate=cost(2 * rows * d * (qc + 2 * kc), rows * d * 4 + d * (qc + 2 * kc) * 2),
    )(*args)


def dout_body(s_ref, dy_ref, wo_ref, *rest):
    dy_out, do_out = rest[-2:]
    dy = dy_ref[...]
    dy_out[...] = dy
    for c in range(wo_ref.shape[0] // 256):
        do_out[:, c * 256:(c + 1) * 256] = mm_nt(dy, wo_ref[c * 256:(c + 1) * 256, :]).astype(BF)


def dout(idx, dy, w_o, bufs, seq):
    rows, d = dy.shape
    bm = min(512, rows)
    nb = rows // bm
    oc = w_o.shape[0] // 4
    row_map = lambda i, s: (s[0] * nb + i, 0)
    in_specs = [pl.BlockSpec((bm, d), lambda i, s: (i, 0)), pl.BlockSpec((oc, d), lambda i, s: (s[1], 0))]
    args = [idx, dy, w_o]
    aliases = {}
    if bufs is not None:
        in_specs += [pl.BlockSpec(memory_space=pl.ANY)] * 2
        aliases = {len(args) + n: n for n in range(2)}
        args += list(bufs)
    return pl.pallas_call(
        dout_body,
        grid_spec=pltpu.PrefetchScalarGridSpec(
            num_scalar_prefetch=1, grid=(nb,), in_specs=in_specs,
            out_specs=[pl.BlockSpec((bm, w), row_map) for w in (d, oc)]),
        out_shape=[jax.ShapeDtypeStruct((seq, w), BF) for w in (d, oc)],
        input_output_aliases=aliases,
        compiler_params=params(), name="dout",
        cost_estimate=cost(2 * rows * d * oc, rows * d * 4 + d * oc * 2),
    )(*args)


def fwd_body(q_ref, k_ref, v_ref, o_ref, lse_ref, qt, vt, s_scr, acc, stat):
    i = pl.program_id(1)
    seq = k_ref.shape[0]

    @pl.when(i == 0)
    def _():
        def tr(c, _):
            vt[:, pl.ds(c * BLK, BLK)] = v_ref[pl.ds(c * BLK, BLK), :].T
            return 0
        lax.fori_loop(0, seq // BLK, tr, 0)

    for h in range(GROUP):
        qt[h] = q_ref[:, h * HEAD:(h + 1) * HEAD].T
    acc[...] = jnp.zeros_like(acc)
    stat[0] = jnp.full(stat.shape[1:], NEG_LARGE, F32)
    stat[2] = jnp.zeros(stat.shape[1:], F32)

    def stage_a(h, j, masked):
        kj = k_ref[pl.ds(pl.multiple_of(j * BLK, BLK), BLK), :]
        s = mm(kj, qt[h])
        if masked:
            keep = lax.broadcasted_iota(jnp.int32, s.shape, 0) <= lax.broadcasted_iota(jnp.int32, s.shape, 1)
            s = jnp.where(keep, s, NEG_LARGE)
        s_scr[h] = s
        m_old = stat[0, h:h + 1]
        m_new = jnp.maximum(m_old, jnp.max(s, axis=0, keepdims=True))
        stat[1, h:h + 1] = jnp.exp2((m_old - m_new) * SCALE2)
        stat[0, h:h + 1] = m_new

    def stage_b(h, j):
        vj = vt[:, pl.ds(pl.multiple_of(j * BLK, BLK), BLK)]
        p = jnp.exp2(s_scr[h] * SCALE2 - stat[0, h:h + 1] * SCALE2)
        alpha = stat[1, h:h + 1]
        stat[2, h:h + 1] = stat[2, h:h + 1] * alpha + jnp.sum(p, axis=0, keepdims=True)
        acc[h] = acc[h] * alpha + mm(vj, p.astype(BF))

    @pl.when(i > 0)
    def _():
        for h in range(GROUP):
            stage_a(h, 0, False)

        def body(j, _):
            for h in range(GROUP):
                stage_b(h, j)
                stage_a(h, j + 1, False)
            return 0
        lax.fori_loop(0, i - 1, body, 0)
        for h in range(GROUP):
            stage_b(h, i - 1)
            stage_a(h, i, True)

    @pl.when(i == 0)
    def _():
        for h in range(GROUP):
            stage_a(h, 0, True)

    for h in range(GROUP):
        stage_b(h, i)
        den = stat[2, h:h + 1]
        o_ref[:, h * HEAD:(h + 1) * HEAD] = (acc[h] / den).T.astype(BF)
        lse_ref[0, h:h + 1, :] = stat[0, h:h + 1] * SCALE2 + jnp.log2(den)
    lse_ref[0, GROUP:, :] = jnp.zeros((8 - GROUP, BLK), F32)


def attn_fwd(q, k, v):
    seq = k.shape[0]
    nq = seq // BLK
    nkv = k.shape[1] // HEAD
    gw = GROUP * HEAD
    tiles = nkv * GROUP * nq * (nq + 1) // 2
    return pl.pallas_call(
        fwd_body, grid=(nkv, nq),
        in_specs=[pl.BlockSpec((BLK, gw), lambda g, i: (i, g)),
                  pl.BlockSpec((seq, HEAD), lambda g, i: (0, g)),
                  pl.BlockSpec((seq, HEAD), lambda g, i: (0, g))],
        out_specs=[pl.BlockSpec((BLK, gw), lambda g, i: (i, g)),
                   pl.BlockSpec((1, 8, BLK), lambda g, i: (g, 0, i))],
        out_shape=[jax.ShapeDtypeStruct(q.shape, BF), jax.ShapeDtypeStruct((nkv, 8, seq), F32)],
        scratch_shapes=[pltpu.VMEM((GROUP, HEAD, BLK), BF), pltpu.VMEM((HEAD, seq), BF),
                        pltpu.VMEM((GROUP, BLK, BLK), F32), pltpu.VMEM((GROUP, HEAD, BLK), F32),
                        pltpu.VMEM((3, 8, BLK), F32)],
        compiler_params=params(2), name="fwd",
        cost_estimate=cost(tiles * BLK * BLK * HEAD * 4, q.size * 4 + k.size * 4, tiles * BLK * BLK),
    )(q, k, v)


def bwd_body(q_ref, do_ref, o_ref, k_ref, v_ref, lse_ref, cos_ref, sin_ref, dq_ref, dk_ref, dv_ref,
             q3, do3, q3t, do3t, lse3, del3, dq3, dkt, dvt):
    i = pl.program_id(1)
    last = pl.num_programs(1) - 1
    seq = k_ref.shape[0]
    nc = BLK // HEAD

    @pl.when(i == 0)
    def _():
        dkt[...] = jnp.zeros_like(dkt)
        dvt[...] = jnp.zeros_like(dvt)

    for h in range(GROUP):
        cols = slice(h * HEAD, (h + 1) * HEAD)
        rows = slice(h * BLK, (h + 1) * BLK)
        qh, doh = q_ref[:, cols], do_ref[:, cols]
        q3[rows, :] = qh
        do3[rows, :] = doh
        q3t[:, rows] = qh.T
        do3t[:, rows] = doh.T
        delta = jnp.sum(doh.astype(F32) * o_ref[:, cols].astype(F32), axis=-1, keepdims=True)
        del3[rows, :] = jnp.broadcast_to(delta, (BLK, HEAD))
        for c in range(nc):
            row = lse_ref[0, h:h + 1, c * HEAD:(c + 1) * HEAD]
            lse3[h * BLK + c * HEAD:h * BLK + (c + 1) * HEAD, :] = jnp.broadcast_to(row, (HEAD, HEAD)).T
    dq3[...] = jnp.zeros_like(dq3)

    def step(j, masked):
        sl = pl.ds(pl.multiple_of(j * BLK, BLK), BLK)
        kj, vj = k_ref[sl, :], v_ref[sl, :]
        s = mm_nt(q3[...], kj)
        dp = mm_nt(do3[...], vj)
        p = jnp.exp2(s * SCALE2 - jnp.concatenate([lse3[...]] * nc, axis=1))
        if masked:
            keep = (lax.broadcasted_iota(jnp.int32, s.shape, 0) % BLK) >= lax.broadcasted_iota(jnp.int32, s.shape, 1)
            p = jnp.where(keep, p, 0.0)
        dvt[:, sl] += mm(do3t[...], p.astype(BF))
        ds = (p * (dp - jnp.concatenate([del3[...]] * nc, axis=1))).astype(BF)
        dkt[:, sl] += mm(q3t[...], ds)
        dq3[...] += mm(ds, kj)

    def body(j, _):
        step(j, False)
        return 0
    lax.fori_loop(0, i, body, 0)
    step(i, True)

    rsl = pl.ds(pl.multiple_of(i * BLK, BLK), BLK)
    for h in range(GROUP):
        val = dq3[h * BLK:(h + 1) * BLK, :] * SCALE
        dq_ref[:, h * HEAD:(h + 1) * HEAD] = rotate(val, cos_ref[rsl, :], -sin_ref[rsl, :]).astype(BF)

    @pl.when(i == last)
    def _():
        def fin(c, _):
            sl = pl.ds(pl.multiple_of(c * BLK, BLK), BLK)
            dk_ref[sl, :] = rotate(dkt[:, sl].T * SCALE, cos_ref[sl, :], -sin_ref[sl, :]).astype(BF)
            dv_ref[sl, :] = dvt[:, sl].T.astype(BF)
            return 0
        lax.fori_loop(0, seq // BLK, fin, 0)


def attn_bwd(q, do, o, k, v, lse, cos_t, sin_t):
    seq = k.shape[0]
    nq = seq // BLK
    nkv = k.shape[1] // HEAD
    gw = GROUP * HEAD
    tiles = nkv * GROUP * nq * (nq + 1) // 2
    qspec = pl.BlockSpec((BLK, gw), lambda g, i: (i, g))
    kspec = pl.BlockSpec((seq, HEAD), lambda g, i: (0, g))
    tspec = pl.BlockSpec((seq, HEAD), lambda g, i: (0, 0))
    m3 = GROUP * BLK
    return pl.pallas_call(
        bwd_body, grid=(nkv, nq),
        in_specs=[qspec, qspec, qspec, kspec, kspec, pl.BlockSpec((1, 8, BLK), lambda g, i: (g, 0, i)), tspec, tspec],
        out_specs=[qspec, kspec, kspec],
        out_shape=[jax.ShapeDtypeStruct(q.shape, BF), jax.ShapeDtypeStruct(k.shape, BF),
                   jax.ShapeDtypeStruct(k.shape, BF)],
        scratch_shapes=[pltpu.VMEM((m3, HEAD), BF), pltpu.VMEM((m3, HEAD), BF),
                        pltpu.VMEM((HEAD, m3), BF), pltpu.VMEM((HEAD, m3), BF),
                        pltpu.VMEM((m3, HEAD), F32), pltpu.VMEM((m3, HEAD), F32), pltpu.VMEM((m3, HEAD), F32),
                        pltpu.VMEM((HEAD, seq), F32), pltpu.VMEM((HEAD, seq), F32)],
        compiler_params=params(2), name="bwd",
        cost_estimate=cost(tiles * BLK * BLK * HEAD * 10, q.size * 8 + k.size * 8, tiles * BLK * BLK),
    )(q, do, o, k, v, lse, cos_t, sin_t)


def out_body(s_ref, x_ref, o0, o1, o2, o3, w_ref, out_ref):
    rows = o0.shape[1]
    acc = x_ref[...].astype(F32)
    for p, o_ref in enumerate((o0, o1, o2, o3)):
        start = pl.multiple_of(s_ref[1 + p] * rows, rows)
        acc = acc + mm(o_ref[...], w_ref[pl.ds(start, rows), :])
    out_ref[...] = acc.astype(BF)


def out_proj(idx, x, pieces, w_o):
    rows, d = x.shape
    hw = pieces[0].shape[1]
    bn = 512
    own = lambda n, s: (s[0], 0)
    loc = lambda n, s: (0, 0)
    return pl.pallas_call(
        out_body,
        grid_spec=pltpu.PrefetchScalarGridSpec(
            num_scalar_prefetch=1, grid=(d // bn,),
            in_specs=[pl.BlockSpec((rows, bn), lambda n, s: (0, n)),
                      pl.BlockSpec((rows, hw), own), pl.BlockSpec((rows, hw), loc),
                      pl.BlockSpec((rows, hw), own), pl.BlockSpec((rows, hw), loc),
                      pl.BlockSpec((w_o.shape[0], bn), lambda n, s: (0, n))],
            out_specs=pl.BlockSpec((rows, bn), lambda n, s: (0, n))),
        out_shape=jax.ShapeDtypeStruct((rows, d), BF),
        compiler_params=params(), name="outp",
        cost_estimate=cost(2 * rows * d * w_o.shape[0], rows * d * 6 + d * d * 2),
    )(idx, x, *pieces, w_o)


def dqkv_body(s_ref, h_ref, dq_ref, dk_ref, dv_ref, *rest):
    outs, ht = rest[-7:-1], rest[-1]
    ht[...] = h_ref[...].T
    for n, src in enumerate((dq_ref, dk_ref, dv_ref)):
        val = mm(ht[...], src[...])
        outs[n][...] = val
        outs[n + 3][...] = val


def dw_qkv(idx, h, dq, dk, dv, bufs):
    seq, d = h.shape
    bm = 256
    ws = (dq.shape[1], dk.shape[1], dv.shape[1])
    in_specs = [pl.BlockSpec((seq, bm), lambda i, s: (0, i))] + \
        [pl.BlockSpec((seq, w), lambda i, s: (0, 0)) for w in ws]
    args = [idx, h, dq, dk, dv]
    aliases = {}
    if bufs is not None:
        in_specs += [pl.BlockSpec(memory_space=pl.ANY)] * 3
        aliases = {len(args) + n: n for n in range(3)}
        args += list(bufs)
    return pl.pallas_call(
        dqkv_body,
        grid_spec=pltpu.PrefetchScalarGridSpec(
            num_scalar_prefetch=1, grid=(d // bm,), in_specs=in_specs,
            out_specs=[pl.BlockSpec((bm, w), lambda i, s: (i, s[0])) for w in ws]
            + [pl.BlockSpec((bm, w), lambda i, s: (i, 0)) for w in ws],
            scratch_shapes=[pltpu.VMEM((bm, seq), BF)]),
        out_shape=[jax.ShapeDtypeStruct((d, 4 * w), F32) for w in ws] + [jax.ShapeDtypeStruct((d, w), F32) for w in ws],
        input_output_aliases=aliases,
        compiler_params=params(), name="dwqkv",
        cost_estimate=cost(2 * seq * d * sum(ws), seq * (d + sum(ws)) * 2 + d * sum(ws) * 8),
    )(*args)


def dwo_body(s_ref, o_ref, dy_ref, *rest):
    fin, snd, ot = rest[-3:]

    @pl.when(pl.program_id(0) == 0)
    def _():
        def tr(c, _):
            sl = pl.ds(pl.multiple_of(c * BLK, BLK), BLK)
            ot[:, sl] = o_ref[sl, :].T
            return 0
        lax.fori_loop(0, o_ref.shape[0] // BLK, tr, 0)
    val = mm(ot[...], dy_ref[...])
    fin[...] = val
    snd[...] = val


def dw_o(idx, o, dy, buf):
    seq, d = dy.shape
    hw = o.shape[1]
    bn = 512
    in_specs = [pl.BlockSpec((seq, hw), lambda i, s: (0, 0)), pl.BlockSpec((seq, bn), lambda i, s: (0, i))]
    args = [idx, o, dy]
    aliases = {}
    if buf is not None:
        in_specs += [pl.BlockSpec(memory_space=pl.ANY)]
        aliases = {len(args): 0}
        args += [buf]
    return pl.pallas_call(
        dwo_body,
        grid_spec=pltpu.PrefetchScalarGridSpec(
            num_scalar_prefetch=1, grid=(d // bn,), in_specs=in_specs,
            out_specs=[pl.BlockSpec((hw, bn), lambda i, s: (s[0], i)), pl.BlockSpec((hw, bn), lambda i, s: (0, i))],
            scratch_shapes=[pltpu.VMEM((hw, seq), BF)]),
        out_shape=[jax.ShapeDtypeStruct((4 * hw, d), F32), jax.ShapeDtypeStruct((hw, d), F32)],
        input_output_aliases=aliases,
        compiler_params=params(), name="dwo",
        cost_estimate=cost(2 * seq * d * hw, seq * (d + hw) * 2 + d * hw * 8),
    )(*args)


def dx_body(s_ref, x_ref, dy_ref, gain_ref, *rest):
    pieces = rest[:12]
    wq_ref, wk_ref, wv_ref, dx_ref, dg_ref, acc = rest[12:]
    n = pl.program_id(0)
    bn = wq_ref.shape[0]
    val = None
    for p in range(4):
        dev = s_ref[1 + p]
        for src, w_ref in zip(pieces[3 * p:3 * p + 3], (wq_ref, wk_ref, wv_ref)):
            w = src.shape[1]
            part = mm_nt(src[...], w_ref[:, pl.ds(pl.multiple_of(dev * w, w), w)])
            val = part if val is None else val + part
    acc[:, pl.ds(pl.multiple_of(n * bn, bn), bn)] = val

    @pl.when(n == pl.num_programs(0) - 1)
    def _():
        step = 128
        gain = gain_ref[...]

        def epi(r, dg):
            sl = pl.ds(pl.multiple_of(r * step, step), step)
            xf = x_ref[sl, :].astype(F32)
            inv = lax.rsqrt(jnp.mean(xf * xf, axis=-1, keepdims=True) + NORM_EPS)
            normed = xf * inv
            dh = acc[sl, :]
            dn = dh * gain
            dxn = inv * (dn - normed * jnp.mean(dn * normed, axis=-1, keepdims=True))
            dx_ref[sl, :] = (dy_ref[sl, :].astype(F32) + dxn).astype(BF)
            return dg + jnp.sum(dh * normed, axis=0, keepdims=True)
        dg_ref[...] = lax.fori_loop(0, x_ref.shape[0] // step, epi, jnp.zeros(dg_ref.shape, F32))


def dx_call(idx, x, dy, gain, pieces, w_q, w_k, w_v):
    rows, d = x.shape
    bn = 512
    ws = (w_q.shape[1], w_k.shape[1], w_v.shape[1])
    own = lambda n, s: (s[0], 0)
    loc = lambda n, s: (0, 0)
    piece_specs = []
    for p in range(4):
        for w in ws:
            piece_specs.append(pl.BlockSpec((rows, w // 4), own if p % 2 == 0 else loc))
    return pl.pallas_call(
        dx_body,
        grid_spec=pltpu.PrefetchScalarGridSpec(
            num_scalar_prefetch=1, grid=(d // bn,),
            in_specs=[pl.BlockSpec((rows, d), loc), pl.BlockSpec((rows, d), loc), pl.BlockSpec((1, d), loc)]
            + piece_specs + [pl.BlockSpec((bn, w), lambda n, s: (n, 0)) for w in ws],
            out_specs=[pl.BlockSpec((rows, d), loc), pl.BlockSpec((1, d), loc)],
            scratch_shapes=[pltpu.VMEM((rows, d), F32)]),
        out_shape=[jax.ShapeDtypeStruct((rows, d), BF), jax.ShapeDtypeStruct((1, d), F32)],
        compiler_params=params(), name="dx",
        cost_estimate=cost(2 * rows * d * sum(ws), rows * d * 6 + d * sum(ws) * 2),
    )(idx, x, dy, gain, *[a for piece in pieces for a in piece], w_q, w_k, w_v)


def solution(mesh):
    sp = mesh.shape['sp']
    cross = [(a, a ^ 2) for a in range(sp)]
    pair = [(a, a ^ 1) for a in range(sp)]

    def over(val):
        return lax.ppermute(val, 'sp', cross)

    def near(val):
        return lax.ppermute(val, 'sp', pair)

    def after(val, *deps):
        return lax.optimization_barrier((val,) + deps)[0]

    def local_step(x, dy, positions, gain, w_q, w_k, w_v, w_o):
        j = lax.axis_index('sp').astype(jnp.int32)
        rows, d = x.shape
        seq = rows * sp
        dev = [j, j ^ 1, j ^ 2, j ^ 3]
        vec = lambda *vals: jnp.stack([jnp.asarray(v, jnp.int32) for v in vals])
        gain_f = gain.astype(F32).reshape(1, d)

        x2 = over(x)
        x1 = near(x)
        x3 = near(x2)
        dy2 = over(after(dy, x2))
        dy1 = near(after(dy, x1))
        dy3 = near(dy2)

        pos = lax.all_gather(positions, 'sp', tiled=True)
        inv_freq = ROPE_THETA ** (-jnp.arange(0, HEAD, 2).astype(F32) / HEAD)
        angles = pos.astype(F32)[:, None] * inv_freq[None, :]
        cos_h, sin_h = jnp.cos(angles), jnp.sin(angles)
        cos_t = jnp.concatenate([cos_h, cos_h], axis=1)
        sin_t = jnp.concatenate([-sin_h, sin_h], axis=1)

        bufs = None
        for p, xp in enumerate((x, x1, x2, x3)):
            bufs = project(vec(dev[p], j), xp, gain_f, w_q, w_k, w_v, cos_t, sin_t, bufs, seq)
        h_all, q, k, v = bufs
        o, lse = attn_fwd(q, k, v)

        dbufs = None
        for p, dyp in enumerate((dy, dy1, dy2, dy3)):
            dbufs = dout(vec(dev[p], j), dyp, w_o, dbufs, seq)
        dy_all, do = dbufs

        def rows_of(val, blk):
            return lax.dynamic_slice_in_dim(val, blk * rows, rows, 0)

        ox = over(after(o, dy2))
        o1 = near(rows_of(o, dev[1]))
        o3 = near(rows_of(ox, dev[1]))
        result = out_proj(vec(j, *dev), x, (o, o1, ox, o3), w_o)

        dq, dk, dv = attn_bwd(q, do, o, k, v, lse, cos_t, sin_t)
        grads = (dq, dk, dv)
        gx = tuple(over(g) for g in grads)
        g1 = tuple(near(rows_of(g, dev[1])) for g in grads)
        g3 = tuple(near(rows_of(g, dev[1])) for g in gx)

        wo_fin, wo_a = dw_o(vec(j), o, dy_all, None)
        wo_fin, wo_b = dw_o(vec(dev[2]), ox, dy_all, wo_fin)
        wo_1, wo_3 = near(wo_a), near(wo_b)
        wo_fin = lax.dynamic_update_slice(wo_fin, wo_1, (dev[1] * wo_1.shape[0], 0))
        wo_fin = lax.dynamic_update_slice(wo_fin, wo_3, (dev[3] * wo_3.shape[0], 0))

        res_a = dw_qkv(vec(j), h_all, *grads, None)
        res_b = dw_qkv(vec(dev[2]), h_all, *gx, res_a[:3])
        fins = []
        for n in range(3):
            fin = res_b[n]
            ra, rb = near(res_a[3 + n]), near(res_b[3 + n])
            fin = lax.dynamic_update_slice(fin, ra, (0, dev[1] * ra.shape[1]))
            fin = lax.dynamic_update_slice(fin, rb, (0, dev[3] * rb.shape[1]))
            fins.append(fin)

        grad_x, dg = dx_call(vec(j, *dev), x, dy, gain_f, (grads, g1, gx, g3), w_q, w_k, w_v)
        grad_gain = lax.psum(dg.reshape(d), 'sp')
        return result, grad_x, fins[0], fins[1], fins[2], wo_fin, grad_gain

    seq_spec = P(('dp', 'sp'), None)
    whole = P(None, None)
    part_rows = P('dp', None)
    return jax.shard_map(local_step, mesh=mesh,
                         in_specs=(seq_spec, seq_spec, P(('dp', 'sp')), P(None), whole, whole, whole, whole),
                         out_specs=(seq_spec, seq_spec, part_rows, part_rows, part_rows, part_rows, P('dp')),
                         check_vma=False)
```

```python
import math

import jax
import jax.numpy as jnp
from jax import lax
from jax.experimental import pallas as pl
from jax.experimental.pallas import tpu as pltpu
from jax.sharding import PartitionSpec as P


HEAD = 128
GROUP = 3
GW = GROUP * HEAD
QK = GW + HEAD
PW = QK + HEAD
PAIR = 2 * HEAD
ROPE_THETA = 1000000.0
NORM_EPS = 1e-05
NEG_LARGE = -1e30
BF = jnp.bfloat16
F32 = jnp.float32
SCALE = HEAD ** -0.5
SCALE2 = SCALE * math.log2(math.e)
BLK = 512
HB = BLK // 2
VMEM_LIMIT = 62 * 1024 * 1024
ANY = pl.BlockSpec(memory_space=pl.ANY)


def first_row(i, s):
    return (0, 0)


def row_map(i, s):
    return (i, 0)


def col_map(i, s):
    return (0, i)


def own_map(i, s):
    return (s[0], 0)


def sds(rows, cols, dtype=BF):
    return jax.ShapeDtypeStruct((rows, cols), dtype)


def call(body, grid, in_specs, out_specs, out_shape, args, flops, scratch=(), aliases=None):
    return pl.pallas_call(
        body,
        grid_spec=pltpu.PrefetchScalarGridSpec(
            num_scalar_prefetch=1, grid=grid, in_specs=in_specs, out_specs=out_specs, scratch_shapes=list(scratch)),
        out_shape=out_shape, input_output_aliases=aliases or {},
        compiler_params=pltpu.CompilerParams(dimension_semantics=("arbitrary",) * len(grid),
                                             vmem_limit_bytes=VMEM_LIMIT),
        cost_estimate=pl.CostEstimate(flops=int(flops), bytes_accessed=int(flops) // BLK,
                                      transcendentals=0))(*args)


def mm(a, b):
    return jnp.dot(a, b, preferred_element_type=F32)


def mm_nt(a, b):
    return lax.dot_general(a, b, (((1,), (1,)), ((), ())), preferred_element_type=F32)


def rotate(val, cos_t, sin_t):
    return val * cos_t + pltpu.roll(val, HEAD // 2, 1) * sin_t


def ds(start, size):
    return pl.ds(pl.multiple_of(start, size), size)


def split3(val):
    hi = val.astype(BF).astype(F32)
    mid = (val - hi).astype(BF).astype(F32)
    return hi, mid, val - hi - mid


def qkv_of(h, wq_ref, wk_ref, wv_ref, cos_ref, sin_ref, q_ref, k_ref, v_ref):
    cos_t, sin_t = cos_ref[...], sin_ref[...]
    out = mm(h, wq_ref[...])
    for c in range(wq_ref.shape[1] // HEAD):
        sl = slice(c * HEAD, c * HEAD + HEAD)
        q_ref[:, sl] = rotate(out[:, sl], cos_t, sin_t).astype(BF)
    out = mm(h, jnp.concatenate([wk_ref[...], wv_ref[...]], axis=1))
    for sl in (slice(0, HEAD), slice(HEAD, PAIR)):
        k_ref[:, sl] = rotate(out[:, sl], cos_t, sin_t).astype(BF)
    v_ref[...] = out[:, PAIR:].astype(BF)


def proj_body(s_ref, xa_ref, xb_ref, gain_ref, wq_ref, wk_ref, wv_ref, cos_ref, sin_ref, *rest):
    h_ref, q_ref, k_ref, v_ref, inv_scr = rest[-5:]
    half = pl.num_programs(0) // 2

    def norm(src):
        step = HEAD // 2

        def stats(c, _):
            sl = ds(c * step, step)
            xf = src[sl, :].astype(F32)
            inv = lax.rsqrt(jnp.mean(xf * xf, axis=-1, keepdims=True) + NORM_EPS)
            inv_scr[sl, :] = jnp.broadcast_to(inv, (step, HEAD))
            return 0

        def scale(c, _):
            sl = ds(c * step, step)
            inv, gain = inv_scr[sl, :], gain_ref[...]
            for n in range(src.shape[1] // HEAD):
                cols = slice(n * HEAD, n * HEAD + HEAD)
                h_ref[sl, cols] = (src[sl, cols].astype(F32) * inv * gain[:, cols]).astype(BF)
            return 0

        lax.fori_loop(0, src.shape[0] // step, stats, 0)
        lax.fori_loop(0, src.shape[0] // step, scale, 0)

    @pl.when(pl.program_id(0) < half)
    def _():
        norm(xa_ref)

    @pl.when(pl.program_id(0) >= half)
    def _():
        norm(xb_ref)

    qkv_of(h_ref[...], wq_ref, wk_ref, wv_ref, cos_ref, sin_ref, q_ref, k_ref, v_ref)


def two_source(rows):
    nb = rows // BLK

    def a_map(i, s):
        return (jnp.minimum(i, nb - 1), 0)

    def b_map(i, s):
        return (jnp.maximum(i - nb, 0), 0)

    def o_map(i, s):
        return (jnp.where(i < nb, s[0] + i, s[1] + i - nb), 0)

    return nb, a_map, b_map, o_map


def project(idx, xa, xb, gain, ws, tabs, bufs, seq):
    rows, d = xa.shape
    nb, a_map, b_map, o_map = two_source(rows)
    widths = [w.shape[1] // 4 for w in ws]
    in_specs = [pl.BlockSpec((BLK, d), a_map), pl.BlockSpec((BLK, d), b_map), pl.BlockSpec((1, d), first_row)]
    in_specs += [pl.BlockSpec((d, w), lambda i, s: (0, s[2])) for w in widths]
    in_specs += [pl.BlockSpec((BLK, HEAD), o_map)] * 2
    args = [idx, xa, xb, gain, *ws, *tabs]
    aliases = {}
    if bufs is not None:
        in_specs += [ANY] * 4
        aliases = {len(args) + n: n for n in range(4)}
        args += list(bufs)
    return call(proj_body, (2 * nb,), in_specs, [pl.BlockSpec((BLK, w), o_map) for w in (d, *widths)],
                [sds(seq, w) for w in (d, *widths)], args, 4 * rows * d * sum(widths),
                scratch=[pltpu.VMEM((BLK, HEAD), F32)], aliases=aliases)


def projc_body(s_ref, h_ref, *rest):
    qkv_of(h_ref[...], *rest)


def project_first(idx, h, ws, tabs, rows):
    d = h.shape[1]
    widths = [w.shape[1] // 4 for w in ws]
    return call(projc_body, (rows // BLK,),
                [pl.BlockSpec((BLK, d), row_map)] + [pl.BlockSpec((d, w), lambda i, s: (0, s[0])) for w in widths]
                + [pl.BlockSpec((BLK, HEAD), row_map)] * 2,
                [pl.BlockSpec((BLK, w), row_map) for w in widths], [sds(rows, w) for w in widths],
                [idx, h, *ws, *tabs], 2 * rows * d * sum(widths))


def dout_body(s_ref, da_ref, db_ref, wo_ref, *rest):
    dy_out, do_out = rest[-2:]
    half = pl.num_programs(0) // 2

    @pl.when(pl.program_id(0) < half)
    def _():
        dy_out[...] = da_ref[...]

    @pl.when(pl.program_id(0) >= half)
    def _():
        dy_out[...] = db_ref[...]

    do_out[...] = mm_nt(dy_out[...], wo_ref[...]).astype(BF)


def dout(idx, da, db, w_o, bufs, seq):
    rows, d = da.shape
    nb, a_map, b_map, o_map = two_source(rows)
    oc = w_o.shape[0] // 4
    in_specs = [pl.BlockSpec((BLK, d), a_map), pl.BlockSpec((BLK, d), b_map),
                pl.BlockSpec((oc, d), lambda i, s: (s[2], 0))]
    args = [idx, da, db, w_o]
    aliases = {}
    if bufs is not None:
        in_specs += [ANY] * 2
        aliases = {len(args) + n: n for n in range(2)}
        args += list(bufs)
    return call(dout_body, (2 * nb,), in_specs, [pl.BlockSpec((BLK, w), o_map) for w in (d, oc)],
                [sds(seq, w) for w in (d, oc)], args, 4 * rows * d * oc, aliases=aliases)


def fwd_body(s_ref, q_ref, k_ref, v_ref, o_ref, lse_ref, *rest):
    qt, kk, vt, s_scr, acc, stat = rest[-6:]
    seq = k_ref.shape[0]
    nq = seq // BLK

    def setup(c, _):
        sl = ds(c * BLK, BLK)
        vt[:, sl] = v_ref[sl, :].T
        kk[sl, :HEAD] = k_ref[sl, :]
        kk[sl, HEAD:] = k_ref[sl, :]
        for h in range(GROUP):
            qf = q_ref[sl, h * HEAD:(h + 1) * HEAD].astype(F32) * SCALE2
            hi = qf.astype(BF)
            qt[h, :HEAD, sl] = hi.T
            qt[h, HEAD:, sl] = (qf - hi.astype(F32)).astype(BF).T
        return 0

    lax.fori_loop(0, nq, setup, 0)
    acc[...] = jnp.zeros_like(acc)
    stat[...] = jnp.zeros_like(stat)
    cur, old, den_row = 0, 1, 2

    def stage_a(h, i, j, masked, first):
        row = slice(h, h + 1)
        s = mm(kk[ds(j * BLK, BLK), :], qt[h, :, ds(i * BLK, BLK)])
        if masked:
            keep = lax.broadcasted_iota(jnp.int32, s.shape, 0) <= lax.broadcasted_iota(jnp.int32, s.shape, 1)
            s = jnp.where(keep, s, NEG_LARGE)
        s_scr[h] = s
        m_new = jnp.max(s, axis=0, keepdims=True)
        if first:
            stat[old, row] = jnp.zeros((1, BLK), F32)
        else:
            m_old = stat[cur, row]
            m_new = jnp.maximum(m_old, m_new)
            stat[old, row] = jnp.exp2(m_old - m_new)
        stat[cur, row] = m_new

    def stage_b(h, j):
        row = slice(h, h + 1)
        p = jnp.exp2(s_scr[h] - stat[cur, row])
        alpha = stat[old, row]
        stat[den_row, row] = stat[den_row, row] * alpha + jnp.sum(p, axis=0, keepdims=True)
        acc[h] = acc[h] * alpha + mm(vt[:, ds(j * BLK, BLK)], p.astype(BF))

    def finish(h, i):
        row = slice(h, h + 1)
        den = stat[den_row, row]
        o_ref[ds(i * BLK, BLK), h * HEAD:(h + 1) * HEAD] = (acc[h] / den).T.astype(BF)
        lse_ref[0, row, ds(i * BLK, BLK)] = stat[cur, row] + jnp.log2(den)

    for h in range(GROUP):
        stage_a(h, 0, 0, True, True)

    def row(i, _):
        def inner(j, _):
            for h in range(GROUP):
                stage_b(h, j)
                stage_a(h, i, j + 1, False, False)
            return 0

        lax.fori_loop(0, i - 1, inner, 0)

        @pl.when(i > 0)
        def _():
            for h in range(GROUP):
                stage_b(h, i - 1)
                stage_a(h, i, i, True, False)

        nxt = jnp.minimum(i + 1, nq - 1)
        for h in range(GROUP):
            stage_b(h, i)
            finish(h, i)
            stage_a(h, nxt, 0, False, True)
        return 0

    lax.fori_loop(0, nq, row, 0)
    lse_ref[0, GROUP:, :] = jnp.zeros((8 - GROUP, seq), F32)
    if len(rest) > 6:
        hi_ref, pair_ref = rest[:2]
        hi_ref[...] = o_ref[seq // 2:, :]
        pair_ref[...] = o_ref[ds(s_ref[0] * pair_ref.shape[0], pair_ref.shape[0]), :]


def attn_fwd(idx, q, k, v, out_rows, rows):
    seq = k.shape[0]
    nq = seq // BLK
    nkv = k.shape[1] // HEAD
    extra = (seq // 2, rows) if rows else ()
    tiles = nkv * GROUP * nq * (nq + 1)
    qspec, kspec = pl.BlockSpec((seq, GW), col_map), pl.BlockSpec((seq, HEAD), col_map)
    return call(fwd_body, (nkv,), [qspec, kspec, kspec],
                [qspec, pl.BlockSpec((1, 8, seq), lambda g, s: (g, 0, 0))] + [pl.BlockSpec((r, GW), col_map) for r in extra],
                [sds(out_rows, q.shape[1]), jax.ShapeDtypeStruct((nkv, 8, seq), F32)] + [sds(r, q.shape[1]) for r in extra],
                [idx, q, k, v], tiles * BLK * BLK * PAIR,
                scratch=[pltpu.VMEM((GROUP, PAIR, seq), BF), pltpu.VMEM((seq, PAIR), BF),
                         pltpu.VMEM((HEAD, seq), BF), pltpu.VMEM((GROUP, BLK, BLK), F32),
                         pltpu.VMEM((GROUP, HEAD, BLK), F32), pltpu.VMEM((GROUP, 8, BLK), F32)])


def bwd_body(s_ref, q_ref, do_ref, o_ref, k_ref, v_ref, lse_ref, cos_ref, sin_ref, out_ref, pair_ref,
             qa, da, ka, va, q3t, do3t, dq3, dkt, dvt):
    i = pl.program_id(0)
    last = pl.num_programs(0) - 1
    seq = k_ref.shape[0]
    m3 = GROUP * HB

    @pl.when(i == 0)
    def _():
        dkt[...] = jnp.zeros_like(dkt)
        dvt[...] = jnp.zeros_like(dvt)

        def setup(c, _):
            sl = ds(c * BLK, BLK)
            minus = jnp.where(lax.broadcasted_iota(jnp.int32, (BLK, HEAD), 1) < 3, -1.0, 0.0).astype(BF)
            for src, dst in ((k_ref, ka), (v_ref, va)):
                dst[sl, :HEAD] = src[sl, :]
                dst[sl, HEAD:] = minus
            return 0

        lax.fori_loop(0, seq // BLK, setup, 0)

    srow = lax.broadcasted_iota(jnp.int32, (16, HB), 0)

    def augment(dst, rows, row):
        hi, mid, low = split3(row)
        parts = jnp.where(srow == 0, hi, jnp.where(srow == 1, mid, jnp.where(srow == 2, low, 0.0))).astype(BF)
        dst[rows, HEAD:] = jnp.concatenate([parts, jnp.zeros((HEAD - 16, HB), BF)], axis=0).T

    def spots():
        for b in range(2):
            for h in range(GROUP):
                start = (b * GROUP + h) * HB
                yield h, slice(b * HB, (b + 1) * HB), slice(h * HEAD, (h + 1) * HEAD), slice(start, start + HB)

    for h, src, cols, rows in spots():
        qh, doh = q_ref[src, cols], do_ref[src, cols]
        qa[rows, :HEAD] = qh
        da[rows, :HEAD] = doh
        q3t[:, rows] = qh.T
        dt = doh.T
        do3t[:, rows] = dt
        augment(da, rows, jnp.sum(dt.astype(F32) * o_ref[src, cols].T.astype(F32), axis=0, keepdims=True))
        augment(qa, rows, lse_ref[0, h:h + 1, src] * (1.0 / SCALE2))
    dq3[...] = jnp.zeros_like(dq3)

    def step(rows, start, width, masked):
        sl = pl.ds(pl.multiple_of(start, BLK), width)
        s = mm_nt(qa[rows, :], ka[sl, :])
        dp = mm_nt(da[rows, :], va[sl, :])
        p = jnp.exp2(s * SCALE2)
        if masked:
            off = width - HB
            tail = p[:, off:]
            keep = lax.broadcasted_iota(jnp.int32, tail.shape, 0) % HB >= lax.broadcasted_iota(jnp.int32, tail.shape, 1)
            tail = jnp.where(keep, tail, 0.0)
            p = jnp.concatenate([p[:, :off], tail], axis=1) if off else tail
        dvt[:, sl] += mm(do3t[:, rows], p.astype(BF))
        dsv = (p * dp).astype(BF)
        dkt[:, sl] += mm(q3t[:, rows], dsv)
        dq3[rows, :] += mm(dsv, ka[sl, :HEAD])

    def body(t, _):
        step(slice(0, 2 * m3), t * 2 * BLK, 2 * BLK, False)
        return 0

    lax.fori_loop(0, i // 2, body, 0)

    def tail_steps(start, width):
        step(slice(0, m3), start, width - HB, True)
        step(slice(m3, 2 * m3), start, width, True)

    @pl.when(i % 2 == 1)
    def _():
        tail_steps((i - 1) * BLK, 2 * BLK)

    @pl.when(i % 2 == 0)
    def _():
        tail_steps(i * BLK, BLK)

    for h, src, cols, rows in spots():
        rsl = ds(i * BLK + src.start, HB)
        out_ref[rsl, cols] = rotate(dq3[rows, :] * SCALE, cos_ref[rsl, :], -sin_ref[rsl, :]).astype(BF)

    @pl.when(i == last)
    def _():
        def fin(c, _):
            sl = ds(c * BLK, BLK)
            out_ref[sl, GW:QK] = rotate(dkt[:, sl].T * SCALE, cos_ref[sl, :], -sin_ref[sl, :]).astype(BF)
            out_ref[sl, QK:] = dvt[:, sl].T.astype(BF)
            return 0

        lax.fori_loop(0, seq // BLK, fin, 0)
        pair_ref[...] = out_ref[ds(s_ref[0] * pair_ref.shape[0], pair_ref.shape[0]), :]


def attn_bwd(idx, q, do, o, k, v, lse, tabs, rows):
    seq = k.shape[0]
    nq = seq // BLK
    qspec = pl.BlockSpec((BLK, GW), lambda i, s: (i, s[1]))
    kspec = pl.BlockSpec((seq, HEAD), lambda i, s: (0, s[1]))
    m3 = GROUP * BLK
    return call(bwd_body, (nq,),
                [qspec] * 3 + [kspec] * 2 + [pl.BlockSpec((1, 8, BLK), lambda i, s: (s[1], 0, i))]
                + [pl.BlockSpec((seq, HEAD), first_row)] * 2,
                [pl.BlockSpec((r, PW), first_row) for r in (seq, rows)], [sds(r, PW) for r in (seq, rows)],
                [idx, q, do, o, k, v, lse, *tabs], GROUP * nq * (nq + 1) * BLK * BLK * PW,
                scratch=[pltpu.VMEM((m3, PAIR), BF)] * 2 + [pltpu.VMEM((seq, PAIR), BF)] * 2
                + [pltpu.VMEM((HEAD, m3), BF)] * 2 + [pltpu.VMEM((m3, HEAD), F32)] + [pltpu.VMEM((HEAD, seq), F32)] * 2)


def out_body(s_ref, x_ref, *rest):
    ops, weights, out_ref = rest[:4], rest[4:8], rest[8]
    lhs = jnp.concatenate([r[...] for r in ops], axis=1)
    rhs = jnp.concatenate([r[...] for r in weights], axis=0)
    out_ref[...] = (x_ref[...].astype(F32) + mm(lhs, rhs)).astype(BF)


def out_proj(idx, x, pieces, w_o):
    rows, d = x.shape
    hw = pieces[0].shape[1]
    return call(out_body, (d // BLK,),
                [pl.BlockSpec((rows, BLK), col_map)]
                + [pl.BlockSpec((rows, hw), m) for m in (own_map, first_row, own_map, first_row)]
                + [pl.BlockSpec((hw, BLK), lambda n, s, p=p: (s[p], n)) for p in range(4)],
                pl.BlockSpec((rows, BLK), col_map), sds(rows, d), [idx, x, *pieces] + [w_o] * 4,
                2 * rows * d * d)


def dwo_body(s_ref, oa_ref, ob_ref, dy_ref, fin, snd, ot):
    hw = oa_ref.shape[1]

    @pl.when(jnp.logical_and(pl.program_id(0) == 0, pl.program_id(1) == 0))
    def _():
        def tr(c, _):
            sl = ds(c * BLK, BLK)
            ot[:hw, sl] = oa_ref[sl, :].T
            ot[hw:, sl] = ob_ref[sl, :].T
            return 0

        lax.fori_loop(0, oa_ref.shape[0] // BLK, tr, 0)

    val = mm(ot[ds(pl.program_id(1) * hw, hw), :], dy_ref[...])
    fin[...] = val
    snd[...] = val


def dw_o(idx, oa, ob, dy):
    seq, d = dy.shape
    hw = oa.shape[1]
    once = pl.BlockSpec((seq, hw), lambda i, p, s: (0, 0), pipeline_mode=pl.Buffered(1))
    return call(dwo_body, (d // BLK, 2),
                [once, once, pl.BlockSpec((seq, BLK), lambda i, p, s: (0, i))],
                [pl.BlockSpec((hw, BLK), lambda i, p, s: (s[p], i)), pl.BlockSpec((hw, BLK), lambda i, p, s: (p, i))],
                [sds(4 * hw, d, F32), sds(2 * hw, d, F32)], [idx, oa, ob, dy], 4 * seq * d * hw,
                scratch=[pltpu.VMEM((2 * hw, seq), BF)])


def dwown_body(s_ref, h_ref, ga_ref, gb_ref, wo_ref, _, fq, fk, fv, snd, wo_fin, ht, sem):
    i, rows = pl.program_id(0), wo_ref.shape[0]
    per = pl.num_programs(0) // 2
    start = jnp.where(i < per, s_ref[1] * per + i, s_ref[2] * per + i - per)
    copy = pltpu.make_async_copy(wo_ref, wo_fin.at[ds(start * rows, rows), :], sem)
    copy.start()
    ht[...] = h_ref[...].T
    lhs = ht[...]
    for n, g in enumerate((ga_ref, gb_ref)):
        val = mm(lhs, g[:, :QK])
        for ref, base in ((fq, 0), (snd, 0)):
            ref[:, base + n * GW:base + (n + 1) * GW] = val[:, :GW]
        fk[:, n * HEAD:(n + 1) * HEAD] = val[:, GW:]
        snd[:, 2 * GW + n * HEAD:2 * GW + (n + 1) * HEAD] = val[:, GW:]
    val = mm(lhs, jnp.concatenate([ga_ref[:, QK:], gb_ref[:, QK:]], axis=1))
    fv[...] = val
    snd[:, 2 * QK:] = val
    copy.wait()


def dw_own(idx, h, ga, gb, wo_rcv, wo_fin):
    seq, d = h.shape
    steps = d // HB
    gspec = pl.BlockSpec((seq, PW), first_row)
    widths = (2 * GW, PAIR, PAIR)
    return call(dwown_body, (steps,),
                [pl.BlockSpec((seq, HB), col_map), gspec, gspec, pl.BlockSpec((wo_rcv.shape[0] // steps, d), row_map), ANY],
                [pl.BlockSpec((HB, w), lambda i, s: (i, s[0])) for w in widths]
                + [pl.BlockSpec((HB, 2 * PW), row_map), ANY],
                [sds(d, 4 * w, F32) for w in widths] + [sds(d, 2 * PW, F32), sds(*wo_fin.shape, F32)],
                [idx, h, ga, gb, wo_rcv, wo_fin], 4 * seq * d * PW,
                scratch=[pltpu.VMEM((HB, seq), BF), pltpu.SemaphoreType.DMA], aliases={5: 4})


def dwgrp_body(with_v, s_ref, h_ref, ga_ref, gb_ref, *rest):
    ht, snd = rest[-1], rest[-2]
    outs = rest[-2 - (3 if with_v else 2):-2]
    ht[...] = h_ref[...].T
    lhs = ht[...]
    val = mm(lhs, (gb_ref if with_v else ga_ref)[:, :QK])
    outs[0][...] = val[:, :GW]
    outs[1][...] = val[:, GW:]
    snd[:, :QK] = val
    if with_v:
        val = mm(lhs, jnp.concatenate([ga_ref[:, QK:], gb_ref[:, QK:]], axis=1))
        outs[2][...] = val
        snd[:, QK:] = val


def group_specs(with_v):
    specs = [pl.BlockSpec((HB, w), lambda i, s: (i, 2 * s[0] + int(with_v))) for w in (GW, HEAD)]
    return specs + ([pl.BlockSpec((HB, PAIR), lambda i, s: (i, s[0]))] if with_v else [])


def dw_group(with_v, idx, h, ga, gb, bufs):
    seq, d = h.shape
    gspec = pl.BlockSpec((seq, PW), first_row)
    specs = group_specs(with_v)
    bufs = bufs[:len(specs)]
    sw = QK + (PAIR if with_v else 0)
    return call(lambda *refs: dwgrp_body(with_v, *refs), (d // HB,),
                [pl.BlockSpec((seq, HB), col_map), gspec, gspec] + [ANY] * len(specs),
                specs + [pl.BlockSpec((HB, sw), row_map)], [sds(*b.shape, F32) for b in bufs] + [sds(d, sw, F32)],
                [idx, h, ga, gb, *bufs], 2 * seq * d * sw, scratch=[pltpu.VMEM((HB, seq), BF)],
                aliases={4 + n: n for n in range(len(specs))})


def place_body(s_ref, rcv, *rest):
    q_out, k_out, v_out = rest[-3:]
    q_out[...] = rcv[:, :GW]
    k_out[...] = rcv[:, GW:QK]
    v_out[...] = rcv[:, QK:]


def place(idx, rcv, bufs):
    d, w = rcv.shape
    return call(place_body, (d // HB,), [pl.BlockSpec((HB, w), row_map)] + [ANY] * 3, group_specs(True),
                [sds(*b.shape, F32) for b in bufs], [idx, rcv, *bufs], d * w, aliases={2 + n: n for n in range(3)})


def pack_body(s_ref, q_ref, k_ref, v_ref, out_ref):
    out_ref[:, :GW] = q_ref[...]
    out_ref[:, GW:QK] = k_ref[...]
    out_ref[:, QK:] = v_ref[...]


def pack_weights(idx, ws):
    d, groups = ws[1].shape[0], ws[1].shape[1] // HEAD
    return call(pack_body, (groups,), [pl.BlockSpec((d, w), col_map) for w in (GW, HEAD, HEAD)],
                pl.BlockSpec((d, PW), col_map), sds(d, groups * PW), [idx, *ws], d * groups * PW)


def puts(rcv, outs, cols, widths, sem):
    rows, src, copies = ds(pl.program_id(0) * rcv.shape[0], rcv.shape[0]), 0, []
    for n, (out, col, w) in enumerate(zip(outs, cols, widths)):
        copies.append(pltpu.make_async_copy(rcv.at[:, src:src + w], out.at[rows, ds(col * w, w)], sem.at[n]))
        src += w
    for copy in copies:
        copy.start()
    return copies


def dxa_body(s_ref, *rest):
    pieces, weights, rcv = rest[:6], rest[6:10], rest[10]
    out_ref, fq, fk, fv, sem = rest[-5:]
    copies = puts(rcv, (fq, fk, fv), [s_ref[1]] * 3, (2 * GW, PAIR, PAIR), sem)
    lhs = jnp.concatenate([r[...] for r in pieces], axis=1)
    rhs = jnp.concatenate([r[...] for r in weights], axis=1)
    out_ref[...] = mm_nt(lhs, rhs)
    for copy in copies:
        copy.wait()


def dx_early(idx, pieces, w_p, rows, rcv, bufs):
    d = w_p.shape[0]
    maps = (own_map, own_map, first_row, first_row, own_map, first_row)
    wspecs = [pl.BlockSpec((BLK, 2 * PW), lambda n, s, p=p: (n, s[p])) for p in range(2)]
    wspecs += [pl.BlockSpec((BLK, PW), lambda n, s, p=p: (n, 2 * s[p])) for p in (2, 3)]
    return call(dxa_body, (d // BLK,),
                [pl.BlockSpec((rows, PW), m) for m in maps] + wspecs + [pl.BlockSpec((BLK, 2 * PW), row_map)] + [ANY] * 3,
                [pl.BlockSpec((rows, BLK), col_map)] + [ANY] * 3, [sds(rows, d, F32)] + [sds(*b.shape, F32) for b in bufs],
                [idx, *pieces] + [w_p] * 4 + [rcv, *bufs], 12 * rows * d * PW,
                scratch=[pltpu.SemaphoreType.DMA((3,))], aliases={12 + n: 1 + n for n in range(3)})


def dxb_body(s_ref, x_ref, dy_ref, gain_ref, early_ref, b2, b3, w2, w3, rcv, *rest):
    dx_ref, dg_ref, fq, fk, acc, inv_scr, sem = rest[-7:]
    n = pl.program_id(0)
    copies = puts(rcv, (fq, fk), [2 * s_ref[3]] * 2, (GW, HEAD), sem)
    lhs = jnp.concatenate([b2[...], b3[...]], axis=1)
    rhs = jnp.concatenate([w2[...], w3[...]], axis=1)
    acc[:, ds(n * BLK, BLK)] = early_ref[...] + mm_nt(lhs, rhs)

    @pl.when(n == pl.num_programs(0) - 1)
    def _():
        step = HEAD // 2
        rows, d = x_ref.shape
        tiles = [slice(c * HEAD, c * HEAD + HEAD) for c in range(d // HEAD)]

        def stats(r, _):
            sl = ds(r * step, step)
            sq = jnp.zeros((step, HEAD), F32)
            dot = jnp.zeros((step, HEAD), F32)
            for c in tiles:
                xf = x_ref[sl, c].astype(F32)
                sq += xf * xf
                dot += xf * acc[sl, c] * gain_ref[:, c]
            inv = lax.rsqrt(jnp.sum(sq, axis=-1, keepdims=True) / d + NORM_EPS)
            inv_scr[0, sl, :] = jnp.broadcast_to(inv, (step, HEAD))
            inv_scr[1, sl, :] = jnp.broadcast_to(jnp.sum(dot, axis=-1, keepdims=True) * inv * inv / d, (step, HEAD))
            return 0

        lax.fori_loop(0, rows // step, stats, 0)
        dg_ref[...] = jnp.zeros_like(dg_ref)

        def epi(r, _):
            sl = ds(r * step, step)
            inv, coef = inv_scr[0, sl, :], inv_scr[1, sl, :]
            for c in tiles:
                xf = x_ref[sl, c].astype(F32)
                dh = acc[sl, c]
                part = dh * (xf * inv)
                dx_ref[sl, c] = (dy_ref[sl, c].astype(F32) + inv * (dh * gain_ref[:, c] - xf * coef)).astype(BF)
                dg_ref[:, c] += jnp.sum(part.reshape(step // 8, 8, HEAD), axis=0)
            return 0

        lax.fori_loop(0, rows // step, epi, 0)

    for copy in copies:
        copy.wait()


def dx_late(idx, x, dy, gain, early, b2, b3, w_p, rcv, bufs):
    rows, d = x.shape
    wspecs = [pl.BlockSpec((BLK, PW), lambda n, s, p=p: (n, 2 * s[p] + 1)) for p in (2, 3)]
    whole = pl.BlockSpec((rows, d), first_row)
    return call(dxb_body, (d // BLK,),
                [whole, whole, pl.BlockSpec((1, d), first_row), pl.BlockSpec((rows, BLK), col_map),
                 pl.BlockSpec((rows, PW), own_map), pl.BlockSpec((rows, PW), first_row)] + wspecs
                + [pl.BlockSpec((BLK, QK), row_map)] + [ANY] * 2,
                [whole, pl.BlockSpec((8, d), first_row)] + [ANY] * 2,
                [sds(rows, d), sds(8, d, F32)] + [sds(*b.shape, F32) for b in bufs],
                [idx, x, dy, gain, early, b2, b3, w_p, w_p, rcv, *bufs], 4 * rows * d * PW,
                scratch=[pltpu.VMEM((rows, d), F32), pltpu.VMEM((2, rows, HEAD), F32), pltpu.SemaphoreType.DMA((2,))],
                aliases={10: 2, 11: 3})


def solution(mesh):
    sp = mesh.shape['sp']
    cross = [(a, a ^ 2) for a in range(sp)]
    pair = [(a, a ^ 1) for a in range(sp)]

    def over(val):
        return lax.ppermute(val, 'sp', cross)

    def near(val):
        return lax.ppermute(val, 'sp', pair)

    def after(val, *deps):
        return lax.optimization_barrier((val,) + deps)[0]

    def vec(*vals, dep=()):
        out = jnp.stack([jnp.asarray(v, jnp.int32) for v in vals])
        return after(out, *dep) if dep else out

    def step(x, dy, positions, gain, w_q, w_k, w_v, w_o):
        j = lax.axis_index('sp').astype(jnp.int32)
        rows, d = x.shape
        seq = rows * sp
        half = rows // 2
        j1, j2, j3 = [j ^ n for n in (1, 2, 3)]
        dev = (j, j1, j2, j3)
        bpr = rows // BLK
        ws = (w_q, w_k, w_v)

        def rows_of(val, blk):
            return lax.dynamic_slice_in_dim(val, blk * rows, rows, 0)

        gain_f = gain.astype(F32).reshape(1, d)

        xa, xb = after((x[:half], x[half:]), positions)
        pos2 = over(positions)
        pos1 = near(positions)
        x2a = over(after(xa, pos2))
        x2b = over(after(xb, pos2))
        x1 = near(x)
        pos3 = near(pos2)
        dy1 = near(after(dy, x1))

        pos = jnp.zeros((seq,), jnp.int32)
        for blk, val in zip(dev, (positions, pos1, pos2, pos3)):
            pos = lax.dynamic_update_slice(pos, val, (blk * rows,))
        inv_freq = ROPE_THETA ** (-jnp.arange(0, HEAD, 2).astype(F32) / HEAD)
        angles = pos.astype(F32)[:, None] * inv_freq[None, :]
        cos_h, sin_h = jnp.cos(angles), jnp.sin(angles)
        tabs = (jnp.concatenate([cos_h, cos_h], axis=1), jnp.concatenate([-sin_h, sin_h], axis=1))

        bufs = project(vec(j * bpr, j1 * bpr, j), x, x1, gain_f, ws, tabs, None, seq)
        dbufs = dout(vec(j * bpr, j1 * bpr, j, dep=(bufs[1],)), dy, dy1, w_o, None, seq)
        w_p = pack_weights(vec(j, dep=(dbufs[1],)), ws)

        x2a = after(x2a, w_p)
        dy2a = over(after(dy, x2a)[:half])
        x3a = near(x2a)
        bufs = project(vec(j2 * bpr, j3 * bpr, j), x2a, x3a, gain_f, ws, tabs, bufs, seq)
        x2b = after(x2b, bufs[1])
        dy2b = over(after(dy, x2b)[half:])
        x3b = near(x2b)
        bufs = project(vec(j2 * bpr + 1, j3 * bpr + 1, j), x2b, x3b, gain_f, ws, tabs, bufs, seq)
        h_all, q, k, v = bufs
        o, lse, o_hi, o_pair = attn_fwd(vec(j1), q, k, v, seq, rows)
        orv = over(o_hi)
        o1 = near(o_pair)
        qc, kc, vc = project_first(vec(j2, dep=(o,)), h_all, ws, tabs, seq // 2)
        oc = attn_fwd(vec(j), qc, kc, vc, seq, 0)[0]

        dy2a = after(dy2a, oc)
        dy3a = near(dy2a)
        dbufs = dout(vec(j2 * bpr, j3 * bpr, j), dy2a, dy3a, w_o, dbufs, seq)
        dy2b = after(dy2b, dbufs[1])
        dy3b = near(dy2b)
        dbufs = dout(vec(j2 * bpr + 1, j3 * bpr + 1, j), dy2b, dy3b, w_o, dbufs, seq)
        dy_all, do = dbufs

        ga, ga_pair = attn_bwd(vec(j1, 0), q, do, o, k, v, lse, tabs, rows)
        ga2 = over(ga)
        ga1 = near(ga_pair)
        gb, gb_pair = attn_bwd(vec(j1, 1, dep=(ga,)), q, do, o, k, v, lse, tabs, rows)
        gb2 = over(gb)
        gb1 = near(gb_pair)

        ox = lax.dynamic_update_slice(oc, after(orv, gb), (seq // 2, 0))
        o3 = near(rows_of(ox, j1))
        wo_fin, wo_snd = dw_o(vec(j, j2, dep=(gb,)), o, ox, dy_all)
        wo_rcv = near(wo_snd)
        result = out_proj(vec(*dev, dep=(wo_snd,)), x, (o, o1, ox, o3), w_o)
        fq, fk, fv, snd, wo_fin = dw_own(vec(j, j1, j3, dep=(result,)), h_all, ga, gb, wo_rcv, wo_fin)
        rcv = near(snd)

        ga2 = after(ga2, snd)
        ga3 = near(rows_of(ga2, j1))
        fq, fk, snd_a = dw_group(False, vec(j2), h_all, ga2, ga2, (fq, fk))
        rcv_a = near(snd_a)
        early, fq, fk, fv = dx_early(vec(*dev, dep=(snd_a,)), (ga, gb, ga1, gb1, ga2, ga3), w_p, rows,
                                     rcv, (fq, fk, fv))

        gb2 = after(gb2, early)
        gb3 = near(rows_of(gb2, j1))
        fq, fk, fv, snd_b = dw_group(True, vec(j2), h_all, ga2, gb2, (fq, fk, fv))
        rcv_b = near(snd_b)
        grad_x, dg, fq, fk = dx_late(vec(*dev, dep=(snd_b,)), x, dy, gain_f, early, gb2, gb3, w_p, rcv_a, (fq, fk))
        dg = jnp.sum(dg, axis=0)
        dg = dg + near(dg)
        dg = dg + over(dg)
        fq, fk, fv = place(vec(j3), rcv_b, (fq, fk, fv))
        return result, grad_x, fq, fk, fv, wo_fin, dg

    seq_spec = P(('dp', 'sp'), None)
    whole = P(None, None)
    part_rows = P('dp', None)
    return jax.shard_map(step, mesh=mesh,
                         in_specs=(seq_spec, seq_spec, P(('dp', 'sp')), P(None), whole, whole, whole, whole),
                         out_specs=(seq_spec, seq_spec, part_rows, part_rows, part_rows, part_rows, P('dp')),
                         check_vma=False)
```

```python
import math

import jax
import jax.numpy as jnp
from jax import lax
from jax.experimental import pallas as pl
from jax.experimental.pallas import tpu as pltpu
from jax.sharding import PartitionSpec as P


HEAD = 128
GROUP = 3
GW = GROUP * HEAD
QK = GW + HEAD
PW = QK + HEAD
PAIR = 2 * HEAD
ROPE_THETA = 1000000.0
NORM_EPS = 1e-05
NEG_LARGE = -1e30
BF = jnp.bfloat16
F32 = jnp.float32
SCALE = HEAD ** -0.5
SCALE2 = SCALE * math.log2(math.e)
BLK = 512
HB = BLK // 2
VMEM_LIMIT = 62 * 1024 * 1024
ANY = pl.BlockSpec(memory_space=pl.ANY)


def first_row(i, s):
    return (0, 0)


def row_map(i, s):
    return (i, 0)


def col_map(i, s):
    return (0, i)


def own_map(i, s):
    return (s[0], 0)


def sds(rows, cols, dtype=BF):
    return jax.ShapeDtypeStruct((rows, cols), dtype)


def call(body, grid, in_specs, out_specs, out_shape, args, flops, scratch=(), aliases=None):
    return pl.pallas_call(
        body,
        grid_spec=pltpu.PrefetchScalarGridSpec(
            num_scalar_prefetch=1, grid=grid, in_specs=in_specs, out_specs=out_specs, scratch_shapes=list(scratch)),
        out_shape=out_shape, input_output_aliases=aliases or {},
        compiler_params=pltpu.CompilerParams(dimension_semantics=("arbitrary",) * len(grid),
                                             vmem_limit_bytes=VMEM_LIMIT),
        cost_estimate=pl.CostEstimate(flops=int(flops), bytes_accessed=int(flops) // BLK,
                                      transcendentals=0))(*args)


def mm(a, b):
    return jnp.dot(a, b, preferred_element_type=F32)


def mm_nt(a, b):
    return lax.dot_general(a, b, (((1,), (1,)), ((), ())), preferred_element_type=F32)


def rotate(val, cos_t, sin_t):
    return val * cos_t + pltpu.roll(val, HEAD // 2, 1) * sin_t


def ds(start, size):
    return pl.ds(pl.multiple_of(start, size), size)


def split3(val):
    hi = val.astype(BF).astype(F32)
    mid = (val - hi).astype(BF).astype(F32)
    return hi, mid, val - hi - mid


def qkv_of(h, wq_ref, wk_ref, wv_ref, cos_ref, sin_ref, q_ref, k_ref, v_ref):
    cos_t, sin_t = cos_ref[...], sin_ref[...]
    out = mm(h, wq_ref[...])
    for c in range(wq_ref.shape[1] // HEAD):
        sl = slice(c * HEAD, c * HEAD + HEAD)
        q_ref[:, sl] = rotate(out[:, sl], cos_t, sin_t).astype(BF)
    out = mm(h, jnp.concatenate([wk_ref[...], wv_ref[...]], axis=1))
    for sl in (slice(0, HEAD), slice(HEAD, PAIR)):
        k_ref[:, sl] = rotate(out[:, sl], cos_t, sin_t).astype(BF)
    v_ref[...] = out[:, PAIR:].astype(BF)


def proj_body(s_ref, xa_ref, xb_ref, gain_ref, wq_ref, wk_ref, wv_ref, cos_ref, sin_ref, *rest):
    h_ref, q_ref, k_ref, v_ref, inv_ref = rest[-5:]
    half = pl.num_programs(0) // 2

    def norm(src):
        step = HEAD // 2

        def stats(c, _):
            sl = ds(c * step, step)
            xf = src[sl, :].astype(F32)
            inv = lax.rsqrt(jnp.mean(xf * xf, axis=-1, keepdims=True) + NORM_EPS)
            inv_ref[sl, :] = jnp.broadcast_to(inv, (step, HEAD))
            return 0

        def scale(c, _):
            sl = ds(c * step, step)
            inv, gain = inv_ref[sl, :], gain_ref[...]
            for n in range(src.shape[1] // HEAD):
                cols = slice(n * HEAD, n * HEAD + HEAD)
                h_ref[sl, cols] = (src[sl, cols].astype(F32) * inv * gain[:, cols]).astype(BF)
            return 0

        lax.fori_loop(0, src.shape[0] // step, stats, 0)
        lax.fori_loop(0, src.shape[0] // step, scale, 0)

    @pl.when(pl.program_id(0) < half)
    def _():
        norm(xa_ref)

    @pl.when(pl.program_id(0) >= half)
    def _():
        norm(xb_ref)

    qkv_of(h_ref[...], wq_ref, wk_ref, wv_ref, cos_ref, sin_ref, q_ref, k_ref, v_ref)


def two_source(rows):
    bm = HB if rows % BLK else BLK
    nb = rows // bm

    def a_map(i, s):
        return (jnp.minimum(i, nb - 1), 0)

    def b_map(i, s):
        return (jnp.maximum(i - nb, 0), 0)

    def o_map(i, s):
        return (jnp.where(i < nb, s[0] + i, s[1] + i - nb), 0)

    return bm, nb, a_map, b_map, o_map


def project(idx, xa, xb, gain, ws, tabs, bufs, seq):
    rows, d = xa.shape
    bm, nb, a_map, b_map, o_map = two_source(rows)
    widths = [w.shape[1] // 4 for w in ws]
    in_specs = [pl.BlockSpec((bm, d), a_map), pl.BlockSpec((bm, d), b_map), pl.BlockSpec((1, d), first_row)]
    in_specs += [pl.BlockSpec((d, w), lambda i, s: (0, s[2])) for w in widths]
    in_specs += [pl.BlockSpec((bm, HEAD), o_map)] * 2
    args = [idx, xa, xb, gain, *ws, *tabs]
    aliases = {}
    if bufs is not None:
        in_specs += [ANY] * len(bufs)
        aliases = {len(args) + n: n for n in range(len(bufs))}
        args += list(bufs)
    return call(proj_body, (2 * nb,), in_specs, [pl.BlockSpec((bm, w), o_map) for w in (d, *widths, HEAD)],
                [sds(seq, w) for w in (d, *widths)] + [sds(seq, HEAD, F32)], args, 4 * rows * d * sum(widths),
                aliases=aliases)


def projc_body(s_ref, h_ref, *rest):
    qkv_of(h_ref[...], *rest)


def project_first(idx, h, ws, tabs, rows):
    d = h.shape[1]
    widths = [w.shape[1] // 4 for w in ws]
    return call(projc_body, (rows // BLK,),
                [pl.BlockSpec((BLK, d), row_map)] + [pl.BlockSpec((d, w), lambda i, s: (0, s[0])) for w in widths]
                + [pl.BlockSpec((BLK, HEAD), row_map)] * 2,
                [pl.BlockSpec((BLK, w), row_map) for w in widths], [sds(rows, w) for w in widths],
                [idx, h, *ws, *tabs], 2 * rows * d * sum(widths))


def dout_body(s_ref, da_ref, db_ref, wo_ref, *rest):
    dy_out, do_out = rest[-2:]
    half = pl.num_programs(0) // 2

    @pl.when(pl.program_id(0) < half)
    def _():
        dy_out[...] = da_ref[...]

    @pl.when(pl.program_id(0) >= half)
    def _():
        dy_out[...] = db_ref[...]

    do_out[...] = mm_nt(dy_out[...], wo_ref[...]).astype(BF)


def dout(idx, da, db, w_o, bufs, seq):
    rows, d = da.shape
    bm, nb, a_map, b_map, o_map = two_source(rows)
    oc = w_o.shape[0] // 4
    in_specs = [pl.BlockSpec((bm, d), a_map), pl.BlockSpec((bm, d), b_map),
                pl.BlockSpec((oc, d), lambda i, s: (s[2], 0))]
    args = [idx, da, db, w_o]
    aliases = {}
    if bufs is not None:
        in_specs += [ANY] * 2
        aliases = {len(args) + n: n for n in range(2)}
        args += list(bufs)
    return call(dout_body, (2 * nb,), in_specs, [pl.BlockSpec((bm, w), o_map) for w in (d, oc)],
                [sds(seq, w) for w in (d, oc)], args, 4 * rows * d * oc, aliases=aliases)


def fwd_body(s_ref, q_ref, k_ref, v_ref, o_ref, lse_ref, *rest):
    qt, kk, vt, s_scr, acc, stat = rest[-6:]
    seq = k_ref.shape[0]
    nq = seq // BLK

    def setup(c, _):
        sl = ds(c * BLK, BLK)
        vt[:, sl] = v_ref[sl, :].T
        kk[sl, :HEAD] = k_ref[sl, :]
        kk[sl, HEAD:] = k_ref[sl, :]
        for h in range(GROUP):
            qf = q_ref[sl, h * HEAD:(h + 1) * HEAD].astype(F32) * SCALE2
            hi = qf.astype(BF)
            qt[h, :HEAD, sl] = hi.T
            qt[h, HEAD:, sl] = (qf - hi.astype(F32)).astype(BF).T
        return 0

    lax.fori_loop(0, nq, setup, 0)
    acc[...] = jnp.zeros_like(acc)
    stat[...] = jnp.zeros_like(stat)
    cur, old, den_row = 0, 1, 2

    def stage_a(h, i, j, masked, first):
        row = slice(h, h + 1)
        s = mm(kk[ds(j * BLK, BLK), :], qt[h, :, ds(i * BLK, BLK)])
        if masked:
            keep = lax.broadcasted_iota(jnp.int32, s.shape, 0) <= lax.broadcasted_iota(jnp.int32, s.shape, 1)
            s = jnp.where(keep, s, NEG_LARGE)
        s_scr[h] = s
        m_new = jnp.max(s, axis=0, keepdims=True)
        if first:
            stat[old, row] = jnp.zeros((1, BLK), F32)
        else:
            m_old = stat[cur, row]
            m_new = jnp.maximum(m_old, m_new)
            stat[old, row] = jnp.exp2(m_old - m_new)
        stat[cur, row] = m_new

    def stage_p(h):
        row = slice(h, h + 1)
        p = jnp.exp2(s_scr[h] - stat[cur, row])
        alpha = stat[old, row]
        stat[den_row, row] = stat[den_row, row] * alpha + jnp.sum(p, axis=0, keepdims=True)
        return p.astype(BF), alpha

    def stage_v(h, j, held):
        acc[h] = acc[h] * held[1] + mm(vt[:, ds(j * BLK, BLK)], held[0])

    def finish(h, i, den, top):
        row = slice(h, h + 1)
        o_ref[ds(i * BLK, BLK), h * HEAD:(h + 1) * HEAD] = (acc[h] / den).T.astype(BF)
        lse_ref[0, row, ds(i * BLK, BLK)] = top + jnp.log2(den)

    for h in range(GROUP):
        stage_a(h, 0, 0, True, True)

    def row(i, _):
        def inner(j, _):
            for h in range(GROUP):
                held = stage_p(h)
                stage_a(h, i, j + 1, False, False)
                stage_v(h, j, held)
            return 0

        lax.fori_loop(0, i - 1, inner, 0)

        @pl.when(i > 0)
        def _():
            for h in range(GROUP):
                held = stage_p(h)
                stage_a(h, i, i, True, False)
                stage_v(h, i - 1, held)

        nxt = jnp.minimum(i + 1, nq - 1)
        for h in range(GROUP):
            held = stage_p(h)
            final = (stat[den_row, h:h + 1], stat[cur, h:h + 1])
            stage_a(h, nxt, 0, False, True)
            stage_v(h, i, held)
            finish(h, i, *final)
        return 0

    lax.fori_loop(0, nq, row, 0)
    lse_ref[0, GROUP:, :] = jnp.zeros((8 - GROUP, seq), F32)
    if len(rest) > 6:
        hi_ref, pair_ref = rest[:2]
        hi_ref[...] = o_ref[seq // 2:, :]
        pair_ref[...] = o_ref[ds(s_ref[0] * pair_ref.shape[0], pair_ref.shape[0]), :]


def attn_fwd(idx, q, k, v, out_rows, rows):
    seq = k.shape[0]
    nq = seq // BLK
    nkv = k.shape[1] // HEAD
    extra = (seq // 2, rows) if rows else ()
    tiles = nkv * GROUP * nq * (nq + 1)
    qspec, kspec = pl.BlockSpec((seq, GW), col_map), pl.BlockSpec((seq, HEAD), col_map)
    return call(fwd_body, (nkv,), [qspec, kspec, kspec],
                [qspec, pl.BlockSpec((1, 8, seq), lambda g, s: (g, 0, 0))] + [pl.BlockSpec((r, GW), col_map) for r in extra],
                [sds(out_rows, q.shape[1]), jax.ShapeDtypeStruct((nkv, 8, seq), F32)] + [sds(r, q.shape[1]) for r in extra],
                [idx, q, k, v], tiles * BLK * BLK * PAIR,
                scratch=[pltpu.VMEM((GROUP, PAIR, seq), BF), pltpu.VMEM((seq, PAIR), BF),
                         pltpu.VMEM((HEAD, seq), BF), pltpu.VMEM((GROUP, BLK, BLK), F32),
                         pltpu.VMEM((GROUP, HEAD, BLK), F32), pltpu.VMEM((GROUP, 8, BLK), F32)])


def bwd_body(s_ref, q_ref, do_ref, o_ref, k_ref, v_ref, lse_ref, cos_ref, sin_ref, out_ref, pair_ref,
             qa, da, ka, va, q3t, do3t, dq3, dkt, dvt):
    i = pl.program_id(0)
    last = pl.num_programs(0) - 1
    seq = k_ref.shape[0]
    m3 = GROUP * HB

    @pl.when(i == 0)
    def _():
        dkt[...] = jnp.zeros_like(dkt)
        dvt[...] = jnp.zeros_like(dvt)

        def setup(c, _):
            sl = ds(c * BLK, BLK)
            third = lax.broadcasted_iota(jnp.int32, (BLK, HEAD), 1) // 3
            for n, (src, dst) in enumerate(((k_ref, ka), (v_ref, va))):
                dst[sl, :HEAD] = src[sl, :]
                dst[sl, HEAD:] = jnp.where(third == n, -1.0, 0.0).astype(BF)
            return 0

        lax.fori_loop(0, seq // BLK, setup, 0)

    srow = lax.broadcasted_iota(jnp.int32, (16, HB), 0)
    blank = jnp.zeros((HEAD - 16, HB), BF)

    def augment(rows, *vals):
        parts = jnp.zeros((16, HB), F32)
        for n, part in enumerate(split3(vals[0]) + split3(vals[1])):
            parts = jnp.where(srow == n, part, parts)
        block = jnp.concatenate([parts.astype(BF), blank], axis=0).T
        qa[rows, HEAD:] = block
        da[rows, HEAD:] = block

    def spots():
        for b in range(2):
            for h in range(GROUP):
                start = (b * GROUP + h) * HB
                yield h, slice(b * HB, (b + 1) * HB), slice(h * HEAD, (h + 1) * HEAD), slice(start, start + HB)

    for h, src, cols, rows in spots():
        qh, doh = q_ref[src, cols], do_ref[src, cols]
        qa[rows, :HEAD] = qh
        da[rows, :HEAD] = doh
        q3t[:, rows] = qh.T
        dt = doh.T
        do3t[:, rows] = dt
        delta = jnp.sum(dt.astype(F32) * o_ref[src, cols].T.astype(F32), axis=0, keepdims=True)
        augment(rows, lse_ref[0, h:h + 1, src] * (1.0 / SCALE2), delta)
    dq3[...] = jnp.zeros_like(dq3)

    def step(rows, start, width, masked):
        sl = pl.ds(pl.multiple_of(start, BLK), width)
        s = mm_nt(qa[rows, :], ka[sl, :])
        dp = mm_nt(da[rows, :], va[sl, :])
        p = jnp.exp2(s * SCALE2)
        if masked:
            off = width - HB
            tail = p[:, off:]
            keep = lax.broadcasted_iota(jnp.int32, tail.shape, 0) % HB >= lax.broadcasted_iota(jnp.int32, tail.shape, 1)
            tail = jnp.where(keep, tail, 0.0)
            p = jnp.concatenate([p[:, :off], tail], axis=1) if off else tail
        dvt[:, sl] += mm(do3t[:, rows], p.astype(BF))
        dsv = (p * dp).astype(BF)
        dkt[:, sl] += mm(q3t[:, rows], dsv)
        dq3[rows, :] += mm(dsv, ka[sl, :HEAD])

    def body(t, _):
        step(slice(0, 2 * m3), t * 2 * BLK, 2 * BLK, False)
        return 0

    lax.fori_loop(0, i // 2, body, 0)

    def tail_steps(start, width):
        step(slice(0, m3), start, width - HB, True)
        step(slice(m3, 2 * m3), start, width, True)

    @pl.when(i % 2 == 1)
    def _():
        tail_steps((i - 1) * BLK, 2 * BLK)

    @pl.when(i % 2 == 0)
    def _():
        tail_steps(i * BLK, BLK)

    for h, src, cols, rows in spots():
        rsl = ds(i * BLK + src.start, HB)
        out_ref[rsl, cols] = rotate(dq3[rows, :] * SCALE, cos_ref[rsl, :], -sin_ref[rsl, :]).astype(BF)

    @pl.when(i == last)
    def _():
        def fin(c, _):
            sl = ds(c * BLK, BLK)
            out_ref[sl, GW:QK] = rotate(dkt[:, sl].T * SCALE, cos_ref[sl, :], -sin_ref[sl, :]).astype(BF)
            out_ref[sl, QK:] = dvt[:, sl].T.astype(BF)
            return 0

        lax.fori_loop(0, seq // BLK, fin, 0)
        pair_ref[...] = out_ref[ds(s_ref[0] * pair_ref.shape[0], pair_ref.shape[0]), :]


def attn_bwd(idx, q, do, o, k, v, lse, tabs, rows):
    seq = k.shape[0]
    nq = seq // BLK
    qspec = pl.BlockSpec((BLK, GW), lambda i, s: (i, s[1]))
    kspec = pl.BlockSpec((seq, HEAD), lambda i, s: (0, s[1]))
    m3 = GROUP * BLK
    return call(bwd_body, (nq,),
                [qspec] * 3 + [kspec] * 2 + [pl.BlockSpec((1, 8, BLK), lambda i, s: (s[1], 0, i))]
                + [pl.BlockSpec((seq, HEAD), first_row)] * 2,
                [pl.BlockSpec((r, PW), first_row) for r in (seq, rows)], [sds(r, PW) for r in (seq, rows)],
                [idx, q, do, o, k, v, lse, *tabs], GROUP * nq * (nq + 1) * BLK * BLK * PW,
                scratch=[pltpu.VMEM((m3, PAIR), BF)] * 2 + [pltpu.VMEM((seq, PAIR), BF)] * 2
                + [pltpu.VMEM((HEAD, m3), BF)] * 2 + [pltpu.VMEM((m3, HEAD), F32)] + [pltpu.VMEM((HEAD, seq), F32)] * 2)


def out_body(s_ref, x_ref, *rest):
    ops, weights, out_ref = rest[:4], rest[4:8], rest[8]
    lhs = jnp.concatenate([r[...] for r in ops], axis=1)
    rhs = jnp.concatenate([r[...] for r in weights], axis=0)
    out_ref[...] = (x_ref[...].astype(F32) + mm(lhs, rhs)).astype(BF)


def out_proj(idx, x, pieces, w_o):
    rows, d = x.shape
    hw = pieces[0].shape[1]
    return call(out_body, (d // BLK,),
                [pl.BlockSpec((rows, BLK), col_map)]
                + [pl.BlockSpec((rows, hw), m) for m in (own_map, first_row, own_map, first_row)]
                + [pl.BlockSpec((hw, BLK), lambda n, s, p=p: (s[p], n)) for p in range(4)],
                pl.BlockSpec((rows, BLK), col_map), sds(rows, d), [idx, x, *pieces] + [w_o] * 4,
                2 * rows * d * d)


def dwo_body(s_ref, oa_ref, ob_ref, dy_ref, fin, snd, ot):
    hw = oa_ref.shape[1]

    @pl.when(jnp.logical_and(pl.program_id(0) == 0, pl.program_id(1) == 0))
    def _():
        def tr(c, _):
            sl = ds(c * BLK, BLK)
            ot[:hw, sl] = oa_ref[sl, :].T
            ot[hw:, sl] = ob_ref[sl, :].T
            return 0

        lax.fori_loop(0, oa_ref.shape[0] // BLK, tr, 0)

    val = mm(ot[ds(pl.program_id(1) * hw, hw), :], dy_ref[...])
    fin[...] = val
    snd[...] = val


def dw_o(idx, oa, ob, dy):
    seq, d = dy.shape
    hw = oa.shape[1]
    once = pl.BlockSpec((seq, hw), lambda i, p, s: (0, 0), pipeline_mode=pl.Buffered(1))
    return call(dwo_body, (d // BLK, 2),
                [once, once, pl.BlockSpec((seq, BLK), lambda i, p, s: (0, i))],
                [pl.BlockSpec((hw, BLK), lambda i, p, s: (s[p], i)), pl.BlockSpec((hw, BLK), lambda i, p, s: (p, i))],
                [sds(4 * hw, d, F32), sds(2 * hw, d, F32)], [idx, oa, ob, dy], 4 * seq * d * hw,
                scratch=[pltpu.VMEM((2 * hw, seq), BF)])


def dwown_body(s_ref, h_ref, ga_ref, gb_ref, gc_ref, wo_ref, _, fq, fk, fv, snd, wo_fin, ht, sem, wsem):
    i, steps = pl.program_id(0), pl.num_programs(0)
    rows, per = wo_ref.shape[0], steps // 2
    start = jnp.where(i < per, s_ref[1] * per + i, s_ref[3] * per + i - per)
    wcopy = pltpu.make_async_copy(wo_ref, wo_fin.at[ds(start * rows, rows), :], wsem)
    wcopy.start()

    @pl.when(i > 0)
    def _():
        for copy in scatter(snd, (fq, fk, fv), s_ref[0], s_ref[2], sem):
            copy.wait()

    ht[...] = h_ref[...].T
    lhs = ht[...]
    for g, q_at, k_at in ((ga_ref, 0, 2 * GW), (gb_ref, GW, 2 * GW + HEAD), (gc_ref, 2 * PW, 2 * PW + GW)):
        val = mm(lhs, g[:, :QK])
        snd[:, q_at:q_at + GW] = val[:, :GW]
        snd[:, k_at:k_at + HEAD] = val[:, GW:]
    snd[:, 2 * QK:2 * PW] = mm(lhs, jnp.concatenate([ga_ref[:, QK:], gb_ref[:, QK:]], axis=1))
    copies = scatter(snd, (fq, fk, fv), s_ref[0], s_ref[2], sem)
    for copy in copies:
        copy.start()

    @pl.when(i == steps - 1)
    def _():
        for copy in copies:
            copy.wait()

    wcopy.wait()


def scatter(rcv, outs, whole_dev, part_dev, sem):
    rows, src, copies = ds(pl.program_id(0) * rcv.shape[0], rcv.shape[0]), 0, []
    fq, fk, fv = outs
    for n, (out, col, w) in enumerate(((fq, whole_dev, 2 * GW), (fk, whole_dev, PAIR), (fv, whole_dev, PAIR),
                                       (fq, 2 * part_dev, GW), (fk, 2 * part_dev, HEAD))):
        copies.append(pltpu.make_async_copy(rcv.at[:, src:src + w], out.at[rows, ds(col * w, w)], sem.at[n]))
        src += w
    return copies


def dw_own(idx, h, ga, gb, gc, wo_rcv, wo_fin):
    seq, d = h.shape
    steps = d // HB
    gspec = pl.BlockSpec((seq, PW), first_row, pipeline_mode=pl.Buffered(1))
    widths = (2 * GW, PAIR, PAIR)
    sw = 2 * PW + QK
    return call(dwown_body, (steps,),
                [pl.BlockSpec((seq, HB), col_map)] + [gspec] * 3
                + [pl.BlockSpec((wo_rcv.shape[0] // steps, d), row_map), ANY],
                [ANY] * 3 + [pl.BlockSpec((HB, sw), row_map), ANY],
                [sds(d, 4 * w, F32) for w in widths] + [sds(d, sw, F32), sds(*wo_fin.shape, F32)],
                [idx, h, ga, gb, gc, wo_rcv, wo_fin], 2 * seq * d * sw,
                scratch=[pltpu.VMEM((HB, seq), BF), pltpu.SemaphoreType.DMA((5,)), pltpu.SemaphoreType.DMA],
                aliases={6: 4})


def dwgrp_body(s_ref, h_ref, ga_ref, gb_ref, *rest):
    fq, fk, fv, snd, ht = rest[-5:]
    ht[...] = h_ref[...].T
    lhs = ht[...]
    val = mm(lhs, gb_ref[:, :QK])
    fq[...] = val[:, :GW]
    fk[...] = val[:, GW:]
    snd[:, :QK] = val
    val = mm(lhs, jnp.concatenate([ga_ref[:, QK:], gb_ref[:, QK:]], axis=1))
    fv[...] = val
    snd[:, QK:] = val


def group_specs():
    return [pl.BlockSpec((HB, w), lambda i, s: (i, 2 * s[0] + 1)) for w in (GW, HEAD)] + \
        [pl.BlockSpec((HB, PAIR), lambda i, s: (i, s[0]))]


def dw_group(idx, h, ga, gb, bufs):
    seq, d = h.shape
    gspec = pl.BlockSpec((seq, PW), first_row, pipeline_mode=pl.Buffered(1))
    sw = QK + PAIR
    return call(dwgrp_body, (d // HB,),
                [pl.BlockSpec((seq, HB), col_map), gspec, gspec] + [ANY] * 3,
                group_specs() + [pl.BlockSpec((HB, sw), row_map)], [sds(*b.shape, F32) for b in bufs] + [sds(d, sw, F32)],
                [idx, h, ga, gb, *bufs], 2 * seq * d * sw, scratch=[pltpu.VMEM((HB, seq), BF)],
                aliases={4 + n: n for n in range(3)})


def place_body(s_ref, rcv, *rest):
    q_out, k_out, v_out = rest[-3:]
    q_out[...] = rcv[:, :GW]
    k_out[...] = rcv[:, GW:QK]
    v_out[...] = rcv[:, QK:]


def place(idx, rcv, bufs):
    d, w = rcv.shape
    return call(place_body, (d // HB,), [pl.BlockSpec((HB, w), row_map)] + [ANY] * 3, group_specs(),
                [sds(*b.shape, F32) for b in bufs], [idx, rcv, *bufs], d * w, aliases={2 + n: n for n in range(3)})


def pack_body(s_ref, q_ref, k_ref, v_ref, out_ref):
    out_ref[:, :GW] = q_ref[...]
    out_ref[:, GW:QK] = k_ref[...]
    out_ref[:, QK:] = v_ref[...]


def pack_weights(idx, ws):
    d, groups = ws[1].shape[0], ws[1].shape[1] // HEAD
    return call(pack_body, (groups,), [pl.BlockSpec((d, w), col_map) for w in (GW, HEAD, HEAD)],
                pl.BlockSpec((d, PW), col_map), sds(d, groups * PW), [idx, *ws], d * groups * PW)


def dx_body(s_ref, x_ref, dy_ref, gain_ref, inv_ref, *rest):
    pieces, weights, rcv = rest[:8], rest[8:12], rest[12]
    dx_ref, dg_ref, fq, fk, fv, acc, xs, tot, sem = rest[-9:]
    n = pl.program_id(0)
    bn = x_ref.shape[1]
    rows, d = acc.shape
    copies = scatter(rcv, (fq, fk, fv), s_ref[1], s_ref[3], sem)
    for copy in copies:
        copy.start()

    @pl.when(n == 0)
    def _():
        tot[...] = jnp.zeros_like(tot)

    lhs = jnp.concatenate([r[...] for r in pieces], axis=1)
    rhs = jnp.concatenate([r[...] for r in weights], axis=1)
    dh = mm_nt(lhs, rhs)
    inv = inv_ref[...]
    for c in range(bn // HEAD):
        cols = slice(c * HEAD, c * HEAD + HEAD)
        xb = x_ref[:, cols]
        xs[:, ds(n * bn + cols.start, HEAD)] = xb
        part, xf = dh[:, cols], xb.astype(F32)
        scaled = part * gain_ref[:, cols]
        tot[...] += scaled * xf
        acc[:, ds(n * bn + cols.start, HEAD)] = dy_ref[:, cols].astype(F32) + inv * scaled
        dg_ref[:, cols] = jnp.sum((part * (xf * inv)).reshape(rows // 8, 8, HEAD), axis=0)

    @pl.when(n == pl.num_programs(0) - 1)
    def _():
        step = HEAD // 2

        def stats(r, _):
            sl = ds(r * step, step)
            inv = inv_ref[sl, :]
            tot[sl, :] = jnp.broadcast_to(jnp.sum(tot[sl, :], axis=-1, keepdims=True) / d, (step, HEAD)) * inv * inv * inv
            return 0

        lax.fori_loop(0, rows // step, stats, 0)

        def epi(r, _):
            sl = ds(r * step, step)
            coef = tot[sl, :]
            for c in range(d // HEAD):
                cols = slice(c * HEAD, c * HEAD + HEAD)
                dx_ref[sl, cols] = (acc[sl, cols] - xs[sl, cols].astype(F32) * coef).astype(BF)
            return 0

        lax.fori_loop(0, rows // step, epi, 0)

    for copy in copies:
        copy.wait()


def dx_call(idx, x, dy, gain, inv, pieces, w_p, rcv, bufs):
    rows, d = x.shape
    bn = HB
    once = pl.Buffered(1)
    maps = (own_map, own_map, first_row, first_row) * 2
    return call(dx_body, (d // bn,),
                [pl.BlockSpec((rows, bn), col_map)] * 2 + [pl.BlockSpec((1, bn), col_map), pl.BlockSpec((rows, HEAD), own_map)]
                + [pl.BlockSpec((rows, PW), m, pipeline_mode=once) for m in maps]
                + [pl.BlockSpec((bn, 2 * PW), lambda n, s, p=p: (n, s[p])) for p in range(4)]
                + [pl.BlockSpec((bn, rcv.shape[1]), row_map)] + [ANY] * 3,
                [pl.BlockSpec((rows, d), first_row, pipeline_mode=once), pl.BlockSpec((8, bn), col_map)] + [ANY] * 3,
                [sds(rows, d), sds(8, d, F32)] + [sds(*b.shape, F32) for b in bufs],
                [idx, x, dy, gain, inv, *pieces] + [w_p] * 4 + [rcv, *bufs], 16 * rows * d * PW,
                scratch=[pltpu.VMEM((rows, d), F32), pltpu.VMEM((rows, d), BF), pltpu.VMEM((rows, HEAD), F32),
                         pltpu.SemaphoreType.DMA((5,))],
                aliases={18 + n: 2 + n for n in range(3)})


def solution(mesh):
    sp = mesh.shape['sp']
    cross = [(a, a ^ 2) for a in range(sp)]
    pair = [(a, a ^ 1) for a in range(sp)]

    def over(val):
        return lax.ppermute(val, 'sp', cross)

    def near(val):
        return lax.ppermute(val, 'sp', pair)

    def after(val, *deps):
        return lax.optimization_barrier((val,) + deps)[0]

    def vec(*vals, dep=()):
        out = jnp.stack([jnp.asarray(v, jnp.int32) for v in vals])
        return after(out, *dep) if dep else out

    def step(x, dy, positions, gain, w_q, w_k, w_v, w_o):
        j = lax.axis_index('sp').astype(jnp.int32)
        rows, d = x.shape
        seq = rows * sp
        half = rows // 2
        j1, j2, j3 = [j ^ n for n in (1, 2, 3)]
        dev = (j, j1, j2, j3)
        bpr, hpr = rows // BLK, rows // HB
        ws = (w_q, w_k, w_v)

        def rows_of(val, blk):
            return lax.dynamic_slice_in_dim(val, blk * rows, rows, 0)

        gain_f = gain.astype(F32).reshape(1, d)

        cut = rows - HB
        xa = x[:cut]
        pos2 = over(positions)
        pos1 = near(positions)
        x2a = over(xa)
        x2b = over(after(x, xa)[cut:])
        x1 = near(x)
        pos3 = near(pos2)
        dy1 = near(after(dy, x1))

        pos = jnp.zeros((seq,), jnp.int32)
        for blk, val in zip(dev, (positions, pos1, pos2, pos3)):
            pos = lax.dynamic_update_slice(pos, val, (blk * rows,))
        inv_freq = ROPE_THETA ** (-jnp.arange(0, HEAD, 2).astype(F32) / HEAD)
        angles = pos.astype(F32)[:, None] * inv_freq[None, :]
        cos_h, sin_h = jnp.cos(angles), jnp.sin(angles)
        tabs = (jnp.concatenate([cos_h, cos_h], axis=1), jnp.concatenate([-sin_h, sin_h], axis=1))

        bufs = project(vec(j * bpr, j1 * bpr, j), x, x1, gain_f, ws, tabs, None, seq)
        dbufs = dout(vec(j * bpr, j1 * bpr, j, dep=(bufs[1],)), dy, dy1, w_o, None, seq)
        w_p = pack_weights(vec(j, dep=(dbufs[1],)), ws)

        x2a = after(x2a, w_p)
        dy2a = over(after(dy, x2a)[:half])
        x3a = near(x2a)
        bufs = project(vec(j2 * hpr, j3 * hpr, j), x2a, x3a, gain_f, ws, tabs, bufs, seq)
        x2b = after(x2b, bufs[1])
        dy2b = over(after(dy, x2b)[half:])
        x3b = near(x2b)
        bufs = project(vec((j2 + 1) * hpr - 1, (j3 + 1) * hpr - 1, j), x2b, x3b, gain_f, ws, tabs, bufs, seq)
        h_all, q, k, v, inv = bufs
        o, lse, o_hi, o_pair = attn_fwd(vec(j1), q, k, v, seq, rows)
        orv = over(o_hi)
        o1 = near(o_pair)
        qc, kc, vc = project_first(vec(j2, dep=(o,)), h_all, ws, tabs, seq // 2)
        oc = attn_fwd(vec(j), qc, kc, vc, seq, 0)[0]

        dy2a = after(dy2a, oc)
        dy3a = near(dy2a)
        dbufs = dout(vec(j2 * bpr, j3 * bpr, j), dy2a, dy3a, w_o, dbufs, seq)
        dy2b = after(dy2b, dbufs[1])
        dy3b = near(dy2b)
        dbufs = dout(vec(j2 * bpr + 1, j3 * bpr + 1, j), dy2b, dy3b, w_o, dbufs, seq)
        dy_all, do = dbufs

        ga, ga_pair = attn_bwd(vec(j1, 0), q, do, o, k, v, lse, tabs, rows)
        ga2 = over(ga)
        ga1 = near(ga_pair)
        gb, gb_pair = attn_bwd(vec(j1, 1, dep=(ga,)), q, do, o, k, v, lse, tabs, rows)
        gb2 = over(gb)
        gb1 = near(gb_pair)

        ox = lax.dynamic_update_slice(oc, after(orv, gb), (seq // 2, 0))
        o3 = near(rows_of(ox, j1))
        wo_fin, wo_snd = dw_o(vec(j, j2, dep=(gb,)), o, ox, dy_all)
        wo_rcv = near(wo_snd)
        result = out_proj(vec(*dev, dep=(wo_snd,)), x, (o, o1, ox, o3), w_o)
        ga2 = after(ga2, wo_snd)
        ga3 = near(rows_of(ga2, j1))
        fq, fk, fv, snd, wo_fin = dw_own(vec(*dev, dep=(result,)), h_all, ga, gb, ga2, wo_rcv, wo_fin)
        rcv = near(snd)

        gb2 = after(gb2, snd)
        gb3 = near(rows_of(gb2, j1))
        fq, fk, fv, snd_b = dw_group(vec(j2), h_all, ga2, gb2, (fq, fk, fv))
        rcv_b = near(snd_b)
        grad_x, dg, fq, fk, fv = dx_call(vec(*dev, dep=(snd_b,)), x, dy, gain_f, inv,
                                         (ga, gb, ga1, gb1, ga2, gb2, ga3, gb3), w_p, rcv, (fq, fk, fv))
        dg = jnp.sum(dg, axis=0)
        dg = dg + near(dg)
        dg = dg + over(dg)
        fq, fk, fv = place(vec(j3), rcv_b, (fq, fk, fv))
        return result, grad_x, fq, fk, fv, wo_fin, dg

    seq_spec = P(('dp', 'sp'), None)
    whole = P(None, None)
    part_rows = P('dp', None)
    return jax.shard_map(step, mesh=mesh,
                         in_specs=(seq_spec, seq_spec, P(('dp', 'sp')), P(None), whole, whole, whole, whole),
                         out_specs=(seq_spec, seq_spec, part_rows, part_rows, part_rows, part_rows, P('dp')),
                         check_vma=False)
```

```python
import math

import jax
import jax.numpy as jnp
from jax import lax
from jax.experimental import pallas as pl
from jax.experimental.pallas import tpu as pltpu
from jax.sharding import PartitionSpec as P


HEAD = 128
GROUP = 3
GW = GROUP * HEAD
QK = GW + HEAD
PW = QK + HEAD
PAIR = 2 * HEAD
ROPE_THETA = 1000000.0
NORM_EPS = 1e-05
NEG_LARGE = -1e30
BF = jnp.bfloat16
F32 = jnp.float32
SCALE = HEAD ** -0.5
SCALE2 = SCALE * math.log2(math.e)
BLK = 512
HB = BLK // 2
VMEM_LIMIT = 62 * 1024 * 1024
ANY = pl.BlockSpec(memory_space=pl.ANY)


def first_row(i, s):
    return (0, 0)


def row_map(i, s):
    return (i, 0)


def col_map(i, s):
    return (0, i)


def own_map(i, s):
    return (s[0], 0)


def sds(rows, cols, dtype=BF):
    return jax.ShapeDtypeStruct((rows, cols), dtype)


def call(body, grid, in_specs, out_specs, out_shape, args, flops, scratch=(), aliases=None):
    return pl.pallas_call(
        body,
        grid_spec=pltpu.PrefetchScalarGridSpec(
            num_scalar_prefetch=1, grid=grid, in_specs=in_specs, out_specs=out_specs, scratch_shapes=list(scratch)),
        out_shape=out_shape, input_output_aliases=aliases or {},
        compiler_params=pltpu.CompilerParams(dimension_semantics=("arbitrary",) * len(grid),
                                             vmem_limit_bytes=VMEM_LIMIT),
        cost_estimate=pl.CostEstimate(flops=int(flops), bytes_accessed=int(flops) // BLK,
                                      transcendentals=0))(*args)


def mm(a, b):
    return jnp.dot(a, b, preferred_element_type=F32)


def mm_nt(a, b):
    return lax.dot_general(a, b, (((1,), (1,)), ((), ())), preferred_element_type=F32)


def rotate(val, cos_t, sin_t):
    return val * cos_t + pltpu.roll(val, HEAD // 2, 1) * sin_t


def ds(start, size):
    return pl.ds(pl.multiple_of(start, size), size)


def split3(val):
    hi = val.astype(BF).astype(F32)
    mid = (val - hi).astype(BF).astype(F32)
    return hi, mid, val - hi - mid


def qkv_of(h, wq_ref, wk_ref, wv_ref, cos_ref, sin_ref, q_ref, k_ref, v_ref):
    cos_t, sin_t = cos_ref[...], sin_ref[...]
    out = mm(h, wq_ref[...])
    for c in range(wq_ref.shape[1] // HEAD):
        sl = slice(c * HEAD, c * HEAD + HEAD)
        q_ref[:, sl] = rotate(out[:, sl], cos_t, sin_t).astype(BF)
    out = mm(h, jnp.concatenate([wk_ref[...], wv_ref[...]], axis=1))
    for sl in (slice(0, HEAD), slice(HEAD, PAIR)):
        k_ref[:, sl] = rotate(out[:, sl], cos_t, sin_t).astype(BF)
    v_ref[...] = out[:, PAIR:].astype(BF)


def proj_body(s_ref, xa_ref, xb_ref, gain_ref, wq_ref, wk_ref, wv_ref, cos_ref, sin_ref, *rest):
    h_ref, q_ref, k_ref, v_ref, inv_ref = rest[-5:]
    half = pl.num_programs(0) // 2

    def norm(src):
        step = HEAD // 2

        def stats(c, _):
            sl = ds(c * step, step)
            xf = src[sl, :].astype(F32)
            inv = lax.rsqrt(jnp.mean(xf * xf, axis=-1, keepdims=True) + NORM_EPS)
            inv_ref[sl, :] = jnp.broadcast_to(inv, (step, HEAD))
            return 0

        def scale(c, _):
            sl = ds(c * step, step)
            inv, gain = inv_ref[sl, :], gain_ref[...]
            for n in range(src.shape[1] // HEAD):
                cols = slice(n * HEAD, n * HEAD + HEAD)
                h_ref[sl, cols] = (src[sl, cols].astype(F32) * inv * gain[:, cols]).astype(BF)
            return 0

        lax.fori_loop(0, src.shape[0] // step, stats, 0)
        lax.fori_loop(0, src.shape[0] // step, scale, 0)

    @pl.when(pl.program_id(0) < half)
    def _():
        norm(xa_ref)

    @pl.when(pl.program_id(0) >= half)
    def _():
        norm(xb_ref)

    qkv_of(h_ref[...], wq_ref, wk_ref, wv_ref, cos_ref, sin_ref, q_ref, k_ref, v_ref)


def two_source(rows):
    bm = HB if rows % BLK else BLK
    nb = rows // bm

    def a_map(i, s):
        return (jnp.minimum(i, nb - 1), 0)

    def b_map(i, s):
        return (jnp.maximum(i - nb, 0), 0)

    def o_map(i, s):
        return (jnp.where(i < nb, s[0] + i, s[1] + i - nb), 0)

    return bm, nb, a_map, b_map, o_map


def project(idx, xa, xb, gain, ws, tabs, bufs, seq):
    rows, d = xa.shape
    bm, nb, a_map, b_map, o_map = two_source(rows)
    widths = [w.shape[1] // 4 for w in ws]
    in_specs = [pl.BlockSpec((bm, d), a_map), pl.BlockSpec((bm, d), b_map), pl.BlockSpec((1, d), first_row)]
    in_specs += [pl.BlockSpec((d, w), lambda i, s: (0, s[2])) for w in widths]
    in_specs += [pl.BlockSpec((bm, HEAD), o_map)] * 2
    args = [idx, xa, xb, gain, *ws, *tabs]
    aliases = {}
    if bufs is not None:
        in_specs += [ANY] * len(bufs)
        aliases = {len(args) + n: n for n in range(len(bufs))}
        args += list(bufs)
    return call(proj_body, (2 * nb,), in_specs, [pl.BlockSpec((bm, w), o_map) for w in (d, *widths, HEAD)],
                [sds(seq, w) for w in (d, *widths)] + [sds(seq, HEAD, F32)], args, 4 * rows * d * sum(widths),
                aliases=aliases)


def projc_body(s_ref, h_ref, *rest):
    qkv_of(h_ref[...], *rest)


def project_first(idx, h, ws, tabs, rows):
    d = h.shape[1]
    widths = [w.shape[1] // 4 for w in ws]
    return call(projc_body, (rows // BLK,),
                [pl.BlockSpec((BLK, d), row_map)] + [pl.BlockSpec((d, w), lambda i, s: (0, s[0])) for w in widths]
                + [pl.BlockSpec((BLK, HEAD), row_map)] * 2,
                [pl.BlockSpec((BLK, w), row_map) for w in widths], [sds(rows, w) for w in widths],
                [idx, h, *ws, *tabs], 2 * rows * d * sum(widths))


def dout_body(s_ref, da_ref, db_ref, wo_ref, *rest):
    dy_out, do_out = rest[-2:]
    half = pl.num_programs(0) // 2

    @pl.when(pl.program_id(0) < half)
    def _():
        dy_out[...] = da_ref[...]

    @pl.when(pl.program_id(0) >= half)
    def _():
        dy_out[...] = db_ref[...]

    do_out[...] = mm_nt(dy_out[...], wo_ref[...]).astype(BF)


def dout(idx, da, db, w_o, bufs, seq):
    rows, d = da.shape
    bm, nb, a_map, b_map, o_map = two_source(rows)
    oc = w_o.shape[0] // 4
    in_specs = [pl.BlockSpec((bm, d), a_map), pl.BlockSpec((bm, d), b_map),
                pl.BlockSpec((oc, d), lambda i, s: (s[2], 0))]
    args = [idx, da, db, w_o]
    aliases = {}
    if bufs is not None:
        in_specs += [ANY] * 2
        aliases = {len(args) + n: n for n in range(2)}
        args += list(bufs)
    return call(dout_body, (2 * nb,), in_specs, [pl.BlockSpec((bm, w), o_map) for w in (d, oc)],
                [sds(seq, w) for w in (d, oc)], args, 4 * rows * d * oc, aliases=aliases)


TASK = 4
HEADER = 3


def row_tasks(first, last):
    return [(i, i + 1, 1, -1) for i in range(first, last)]


def fwd_body(kind, s_ref, q_ref, k_ref, v_ref, *rest):
    qt, kk, vt, s_scr, acc, stat = rest[-6:]
    if kind == "rest":
        o1_ref, lse1_ref, st_ref, o_ref, lse_ref, hi_ref, pair_ref = rest[:7]
    else:
        o_ref, lse_ref = rest[:2]
    seq = k_ref.shape[0]

    def setup(c, _):
        sl = ds(c * BLK, BLK)
        vt[:, sl] = v_ref[sl, :].T
        kk[sl, :HEAD] = k_ref[sl, :]
        kk[sl, HEAD:] = k_ref[sl, :]
        for h in range(GROUP):
            qf = q_ref[sl, h * HEAD:(h + 1) * HEAD].astype(F32) * SCALE2
            hi = qf.astype(BF)
            qt[h, :HEAD, sl] = hi.T
            qt[h, HEAD:, sl] = (qf - hi.astype(F32)).astype(BF).T
        return 0

    lax.fori_loop(0, seq // BLK, setup, 0)
    acc[...] = jnp.zeros_like(acc)
    stat[...] = jnp.zeros_like(stat)
    cur, old, den_row = 0, 1, 2
    if kind == "rest":
        @pl.when(s_ref[1] == 0)
        def _():
            o_ref[:seq // 2, :] = o1_ref[...]
            lse_ref[0, :, :seq // 2] = lse1_ref[0]

    def task(t):
        return [s_ref[HEADER + t * TASK + n] for n in range(TASK)]

    def stage_a(h, i, j, masked, init=None):
        row = slice(h, h + 1)
        s = mm(kk[ds(j * BLK, BLK), :], qt[h, :, ds(i * BLK, BLK)])
        if masked is not False:
            keep = lax.broadcasted_iota(jnp.int32, s.shape, 0) <= lax.broadcasted_iota(jnp.int32, s.shape, 1)
            s = jnp.where(keep if masked is True else jnp.logical_or(keep, jnp.logical_not(masked)), s, NEG_LARGE)
        s_scr[h] = s
        m_new = jnp.max(s, axis=0, keepdims=True)
        if init is None:
            m_old = stat[cur, row]
        elif kind == "rest":
            m_old = jnp.where(init >= 0, lse1_ref[0, row, ds(jnp.maximum(init, 0) * BLK, BLK)], NEG_LARGE)
        else:
            m_old = jnp.full(m_new.shape, NEG_LARGE, F32)
        m_new = jnp.maximum(m_old, m_new)
        stat[old, row] = jnp.exp2(m_old - m_new)
        stat[cur, row] = m_new

    def stage_p(h):
        row = slice(h, h + 1)
        p = jnp.exp2(s_scr[h] - stat[cur, row])
        alpha = stat[old, row]
        stat[den_row, row] = stat[den_row, row] * alpha + jnp.sum(p, axis=0, keepdims=True)
        return p.astype(BF), alpha

    def stage_v(h, j, held):
        acc[h] = acc[h] * held[1] + mm(vt[:, ds(j * BLK, BLK)], held[0])

    def finish(h, i, den, top):
        row = slice(h, h + 1)
        out = acc[h] / den
        o_ref[ds(i * BLK, BLK), h * HEAD:(h + 1) * HEAD] = out.T.astype(BF)
        lse_ref[0, row, ds(i * BLK, BLK)] = top + jnp.log2(den)
        if kind == "local":
            rest[2][0, h, :, ds(i * BLK, BLK)] = out

    def pipeline(i, j, masked):
        for h in range(GROUP):
            held = stage_p(h)
            stage_a(h, i, j + 1, masked)
            stage_v(h, j, held)

    count = s_ref[HEADER - 1]
    i, steps, diag, init = task(0)
    for h in range(GROUP):
        stage_a(h, i, 0, jnp.logical_and(steps == 1, diag == 1), init)

    def row(t, _):
        i, steps, diag, _ = task(t)

        def inner(j, _):
            pipeline(i, j, False)
            return 0

        lax.fori_loop(0, steps - 2, inner, 0)

        @pl.when(jnp.logical_and(steps > 1, diag == 1))
        def _():
            pipeline(i, steps - 2, True)

        if kind == "rest":
            @pl.when(diag == 0)
            def _():
                pipeline(i, steps - 2, False)
        i2, _, _, init2 = task(jnp.minimum(t + 1, count - 1))
        for h in range(GROUP):
            held = stage_p(h)
            final = (stat[den_row, h:h + 1], stat[cur, h:h + 1])
            stage_a(h, i2, 0, False, init2)
            stage_v(h, steps - 1, held)
            finish(h, i, *final)
        if kind == "rest":
            @pl.when(init2 >= 0)
            def _():
                stat[den_row] = jnp.ones(stat.shape[1:], F32)
                for h in range(GROUP):
                    acc[h] = st_ref[0, h, :, ds(init2 * BLK, BLK)]
        return 0

    lax.fori_loop(0, count, row, 0)
    lse_ref[0, GROUP:, :] = jnp.zeros((8 - GROUP, seq), F32)
    if kind == "rest":
        hi_ref[...] = o_ref[seq // 2:, :]
        pair_ref[...] = o_ref[ds(s_ref[0] * pair_ref.shape[0], pair_ref.shape[0]), :]


def attn_fwd(kind, idx, q, k, v, rows=0, local=()):
    whole = q.shape[0]
    seq = whole if kind == "rest" else whole // (2 if kind == "local" else 1)
    nkv = k.shape[1] // HEAD

    def half_map(g, s):
        return (s[1], g)

    def head_map(g, s):
        return (g, 0, 0)

    def state_map(g, s):
        return (g, 0, 0, 0)

    at = half_map if kind == "local" else col_map
    lse_spec = pl.BlockSpec((1, 8, seq), head_map)
    outs, specs = [sds(seq * 2 if kind == "first" else seq, q.shape[1]), jax.ShapeDtypeStruct((nkv, 8, seq), F32)], []
    out_specs = [pl.BlockSpec((seq, GW), col_map), lse_spec]
    state = pl.BlockSpec((1, GROUP, HEAD, whole // 2), state_map)
    if kind == "local":
        outs.append(jax.ShapeDtypeStruct((nkv, GROUP, HEAD, seq), F32))
        out_specs.append(state)
    if kind == "rest":
        specs = [pl.BlockSpec((seq // 2, GW), col_map), pl.BlockSpec((1, 8, seq // 2), head_map), state]
        outs += [sds(r, q.shape[1]) for r in (seq // 2, rows)]
        out_specs += [pl.BlockSpec((r, GW), col_map) for r in (seq // 2, rows)]
    kspec = pl.BlockSpec((seq, HEAD), at)
    return call(lambda *refs: fwd_body(kind, *refs), (nkv,), [pl.BlockSpec((seq, GW), at), kspec, kspec] + specs,
                out_specs, outs, [idx, q, k, v, *local], nkv * GROUP * seq * seq * PAIR,
                scratch=[pltpu.VMEM((GROUP, PAIR, seq), BF), pltpu.VMEM((seq, PAIR), BF),
                         pltpu.VMEM((HEAD, seq), BF), pltpu.VMEM((GROUP, BLK, BLK), F32),
                         pltpu.VMEM((GROUP, HEAD, BLK), F32), pltpu.VMEM((GROUP, 8, BLK), F32)])


def bwd_body(s_ref, q_ref, do_ref, o_ref, k_ref, v_ref, lse_ref, cos_ref, sin_ref, out_ref, pair_ref,
             qa, da, ka, va, q3t, do3t, dq3, dkt, dvt):
    i = pl.program_id(0)
    last = pl.num_programs(0) - 1
    seq = k_ref.shape[0]
    m3 = GROUP * HB

    @pl.when(i == 0)
    def _():
        dkt[...] = jnp.zeros_like(dkt)
        dvt[...] = jnp.zeros_like(dvt)

        def setup(c, _):
            sl = ds(c * BLK, BLK)
            third = lax.broadcasted_iota(jnp.int32, (BLK, HEAD), 1) // 3
            for n, (src, dst) in enumerate(((k_ref, ka), (v_ref, va))):
                dst[sl, :HEAD] = src[sl, :]
                dst[sl, HEAD:] = jnp.where(third == n, -1.0, 0.0).astype(BF)
            return 0

        lax.fori_loop(0, seq // BLK, setup, 0)

    srow = lax.broadcasted_iota(jnp.int32, (16, HB), 0)
    blank = jnp.zeros((HEAD - 16, HB), BF)

    def augment(rows, *vals):
        parts = jnp.zeros((16, HB), F32)
        for n, part in enumerate(split3(vals[0]) + split3(vals[1])):
            parts = jnp.where(srow == n, part, parts)
        block = jnp.concatenate([parts.astype(BF), blank], axis=0).T
        qa[rows, HEAD:] = block
        da[rows, HEAD:] = block

    def spots():
        for b in range(2):
            for h in range(GROUP):
                start = (b * GROUP + h) * HB
                yield h, slice(b * HB, (b + 1) * HB), slice(h * HEAD, (h + 1) * HEAD), slice(start, start + HB)

    for h, src, cols, rows in spots():
        qh, doh = q_ref[src, cols], do_ref[src, cols]
        qa[rows, :HEAD] = qh
        da[rows, :HEAD] = doh
        q3t[:, rows] = qh.T
        dt = doh.T
        do3t[:, rows] = dt
        delta = jnp.sum(dt.astype(F32) * o_ref[src, cols].T.astype(F32), axis=0, keepdims=True)
        augment(rows, lse_ref[0, h:h + 1, src] * (1.0 / SCALE2), delta)
    dq3[...] = jnp.zeros_like(dq3)

    def step(rows, start, width, masked):
        sl = pl.ds(pl.multiple_of(start, BLK), width)
        s = mm_nt(qa[rows, :], ka[sl, :])
        dp = mm_nt(da[rows, :], va[sl, :])
        p = jnp.exp2(s * SCALE2)
        if masked:
            off = width - HB
            tail = p[:, off:]
            keep = lax.broadcasted_iota(jnp.int32, tail.shape, 0) % HB >= lax.broadcasted_iota(jnp.int32, tail.shape, 1)
            tail = jnp.where(keep, tail, 0.0)
            p = jnp.concatenate([p[:, :off], tail], axis=1) if off else tail
        dvt[:, sl] += mm(do3t[:, rows], p.astype(BF))
        dsv = (p * dp).astype(BF)
        dkt[:, sl] += mm(q3t[:, rows], dsv)
        dq3[rows, :] += mm(dsv, ka[sl, :HEAD])

    def body(t, _):
        step(slice(0, 2 * m3), t * 2 * BLK, 2 * BLK, False)
        return 0

    lax.fori_loop(0, i // 2, body, 0)

    def tail_steps(start, width):
        step(slice(0, m3), start, width - HB, True)
        step(slice(m3, 2 * m3), start, width, True)

    @pl.when(i % 2 == 1)
    def _():
        tail_steps((i - 1) * BLK, 2 * BLK)

    @pl.when(i % 2 == 0)
    def _():
        tail_steps(i * BLK, BLK)

    for h, src, cols, rows in spots():
        rsl = ds(i * BLK + src.start, HB)
        out_ref[rsl, cols] = rotate(dq3[rows, :] * SCALE, cos_ref[rsl, :], -sin_ref[rsl, :]).astype(BF)

    @pl.when(i == last)
    def _():
        def fin(c, _):
            sl = ds(c * BLK, BLK)
            out_ref[sl, GW:QK] = rotate(dkt[:, sl].T * SCALE, cos_ref[sl, :], -sin_ref[sl, :]).astype(BF)
            out_ref[sl, QK:] = dvt[:, sl].T.astype(BF)
            return 0

        lax.fori_loop(0, seq // BLK, fin, 0)
        pair_ref[...] = out_ref[ds(s_ref[0] * pair_ref.shape[0], pair_ref.shape[0]), :]


def attn_bwd(idx, q, do, o, k, v, lse, tabs, rows):
    seq = k.shape[0]
    nq = seq // BLK
    qspec = pl.BlockSpec((BLK, GW), lambda i, s: (i, s[1]))
    kspec = pl.BlockSpec((seq, HEAD), lambda i, s: (0, s[1]))
    m3 = GROUP * BLK
    return call(bwd_body, (nq,),
                [qspec] * 3 + [kspec] * 2 + [pl.BlockSpec((1, 8, BLK), lambda i, s: (s[1], 0, i))]
                + [pl.BlockSpec((seq, HEAD), first_row)] * 2,
                [pl.BlockSpec((r, PW), first_row) for r in (seq, rows)], [sds(r, PW) for r in (seq, rows)],
                [idx, q, do, o, k, v, lse, *tabs], GROUP * nq * (nq + 1) * BLK * BLK * PW,
                scratch=[pltpu.VMEM((m3, PAIR), BF)] * 2 + [pltpu.VMEM((seq, PAIR), BF)] * 2
                + [pltpu.VMEM((HEAD, m3), BF)] * 2 + [pltpu.VMEM((m3, HEAD), F32)] + [pltpu.VMEM((HEAD, seq), F32)] * 2)


def out_body(s_ref, x_ref, *rest):
    ops, weights, out_ref = rest[:4], rest[4:8], rest[8]
    lhs = jnp.concatenate([r[...] for r in ops], axis=1)
    rhs = jnp.concatenate([r[...] for r in weights], axis=0)
    out_ref[...] = (x_ref[...].astype(F32) + mm(lhs, rhs)).astype(BF)


def out_proj(idx, x, pieces, w_o):
    rows, d = x.shape
    hw = pieces[0].shape[1]
    return call(out_body, (d // BLK,),
                [pl.BlockSpec((rows, BLK), col_map)]
                + [pl.BlockSpec((rows, hw), m) for m in (own_map, first_row, own_map, first_row)]
                + [pl.BlockSpec((hw, BLK), lambda n, s, p=p: (s[p], n)) for p in range(4)],
                pl.BlockSpec((rows, BLK), col_map), sds(rows, d), [idx, x, *pieces] + [w_o] * 4,
                2 * rows * d * d)


def dwo_body(s_ref, oa_ref, ob_ref, dy_ref, fin, snd, ot):
    hw = oa_ref.shape[1]

    @pl.when(jnp.logical_and(pl.program_id(0) == 0, pl.program_id(1) == 0))
    def _():
        def tr(c, _):
            sl = ds(c * BLK, BLK)
            ot[:hw, sl] = oa_ref[sl, :].T
            ot[hw:, sl] = ob_ref[sl, :].T
            return 0

        lax.fori_loop(0, oa_ref.shape[0] // BLK, tr, 0)

    val = mm(ot[ds(pl.program_id(1) * hw, hw), :], dy_ref[...])
    fin[...] = val
    snd[...] = val


def dw_o(idx, oa, ob, dy):
    seq, d = dy.shape
    hw = oa.shape[1]
    once = pl.BlockSpec((seq, hw), lambda i, p, s: (0, 0), pipeline_mode=pl.Buffered(1))
    return call(dwo_body, (d // BLK, 2),
                [once, once, pl.BlockSpec((seq, BLK), lambda i, p, s: (0, i))],
                [pl.BlockSpec((hw, BLK), lambda i, p, s: (s[p], i)), pl.BlockSpec((hw, BLK), lambda i, p, s: (p, i))],
                [sds(4 * hw, d, F32), sds(2 * hw, d, F32)], [idx, oa, ob, dy], 4 * seq * d * hw,
                scratch=[pltpu.VMEM((2 * hw, seq), BF)])


def dwown_body(s_ref, h_ref, ga_ref, gb_ref, gc_ref, wo_ref, _, fq, fk, fv, snd, wo_fin, ht, sem, wsem):
    i, steps = pl.program_id(0), pl.num_programs(0)
    rows, per = wo_ref.shape[0], steps // 2
    start = jnp.where(i < per, s_ref[1] * per + i, s_ref[3] * per + i - per)
    wcopy = pltpu.make_async_copy(wo_ref, wo_fin.at[ds(start * rows, rows), :], wsem)
    wcopy.start()

    @pl.when(i > 1)
    def _():
        for copy in scatter(snd, (fq, fk, fv), s_ref[0], s_ref[2], sem.at[i % 2]):
            copy.wait()

    ht[...] = h_ref[...].T
    lhs = ht[...]
    for g, q_at, k_at in ((ga_ref, 0, 2 * GW), (gb_ref, GW, 2 * GW + HEAD), (gc_ref, 2 * PW, 2 * PW + GW)):
        val = mm(lhs, g[:, :QK])
        snd[:, q_at:q_at + GW] = val[:, :GW]
        snd[:, k_at:k_at + HEAD] = val[:, GW:]
    snd[:, 2 * QK:2 * PW] = mm(lhs, jnp.concatenate([ga_ref[:, QK:], gb_ref[:, QK:]], axis=1))
    for copy in scatter(snd, (fq, fk, fv), s_ref[0], s_ref[2], sem.at[i % 2]):
        copy.start()

    @pl.when(i == steps - 1)
    def _():
        for slot in range(2):
            for copy in scatter(snd, (fq, fk, fv), s_ref[0], s_ref[2], sem.at[slot]):
                copy.wait()

    wcopy.wait()


def scatter(rcv, outs, whole_dev, part_dev, sem):
    rows, src, copies = ds(pl.program_id(0) * rcv.shape[0], rcv.shape[0]), 0, []
    fq, fk, fv = outs
    for n, (out, col, w) in enumerate(((fq, whole_dev, 2 * GW), (fk, whole_dev, PAIR), (fv, whole_dev, PAIR),
                                       (fq, 2 * part_dev, GW), (fk, 2 * part_dev, HEAD))):
        copies.append(pltpu.make_async_copy(rcv.at[:, src:src + w], out.at[rows, ds(col * w, w)], sem.at[n]))
        src += w
    return copies


def dw_own(idx, h, ga, gb, gc, wo_rcv, wo_fin):
    seq, d = h.shape
    steps = d // HB
    gspec = pl.BlockSpec((seq, PW), first_row, pipeline_mode=pl.Buffered(1))
    widths = (2 * GW, PAIR, PAIR)
    sw = 2 * PW + QK
    return call(dwown_body, (steps,),
                [pl.BlockSpec((seq, HB), col_map)] + [gspec] * 3
                + [pl.BlockSpec((wo_rcv.shape[0] // steps, d), row_map), ANY],
                [ANY] * 3 + [pl.BlockSpec((HB, sw), row_map), ANY],
                [sds(d, 4 * w, F32) for w in widths] + [sds(d, sw, F32), sds(*wo_fin.shape, F32)],
                [idx, h, ga, gb, gc, wo_rcv, wo_fin], 2 * seq * d * sw,
                scratch=[pltpu.VMEM((HB, seq), BF), pltpu.SemaphoreType.DMA((2, 5)), pltpu.SemaphoreType.DMA],
                aliases={6: 4})


def dwgrp_body(s_ref, h_ref, ga_ref, gb_ref, *rest):
    fq, fk, fv, snd, ht = rest[-5:]
    ht[...] = h_ref[...].T
    lhs = ht[...]
    val = mm(lhs, gb_ref[:, :QK])
    fq[...] = val[:, :GW]
    fk[...] = val[:, GW:]
    snd[:, :QK] = val
    val = mm(lhs, jnp.concatenate([ga_ref[:, QK:], gb_ref[:, QK:]], axis=1))
    fv[...] = val
    snd[:, QK:] = val


def group_specs():
    return [pl.BlockSpec((HB, w), lambda i, s: (i, 2 * s[0] + 1)) for w in (GW, HEAD)] + \
        [pl.BlockSpec((HB, PAIR), lambda i, s: (i, s[0]))]


def dw_group(idx, h, ga, gb, bufs):
    seq, d = h.shape
    gspec = pl.BlockSpec((seq, PW), first_row, pipeline_mode=pl.Buffered(1))
    sw = QK + PAIR
    return call(dwgrp_body, (d // HB,),
                [pl.BlockSpec((seq, HB), col_map), gspec, gspec] + [ANY] * 3,
                group_specs() + [pl.BlockSpec((HB, sw), row_map)], [sds(*b.shape, F32) for b in bufs] + [sds(d, sw, F32)],
                [idx, h, ga, gb, *bufs], 2 * seq * d * sw, scratch=[pltpu.VMEM((HB, seq), BF)],
                aliases={4 + n: n for n in range(3)})


def place_body(s_ref, rcv, *rest):
    q_out, k_out, v_out = rest[-3:]
    q_out[...] = rcv[:, :GW]
    k_out[...] = rcv[:, GW:QK]
    v_out[...] = rcv[:, QK:]


def place(idx, rcv, bufs):
    d, w = rcv.shape
    return call(place_body, (d // HB,), [pl.BlockSpec((HB, w), row_map)] + [ANY] * 3, group_specs(),
                [sds(*b.shape, F32) for b in bufs], [idx, rcv, *bufs], d * w, aliases={2 + n: n for n in range(3)})


def dx_body(s_ref, x_ref, dy_ref, gain_ref, inv_ref, *rest):
    pieces, weights, rcv = rest[:8], rest[8:20], rest[20]
    dx_ref, dg_ref, fq, fk, fv, acc, xs, tot, sem = rest[-9:]
    n = pl.program_id(0)
    bn = x_ref.shape[1]
    rows, d = acc.shape
    copies = scatter(rcv, (fq, fk, fv), s_ref[1], s_ref[3], sem)
    for copy in copies:
        copy.start()

    @pl.when(n == 0)
    def _():
        tot[...] = jnp.zeros_like(tot)

    cuts = (slice(0, GW), slice(GW, QK), slice(QK, PW))
    lhs = jnp.concatenate([pieces[2 * p + g][:, c] for p in range(4) for c in cuts for g in range(2)], axis=1)
    rhs = jnp.concatenate([r[...] for r in weights], axis=1)
    dh = mm_nt(lhs, rhs)
    inv = inv_ref[...]
    for c in range(bn // HEAD):
        cols = slice(c * HEAD, c * HEAD + HEAD)
        xb = x_ref[:, cols]
        xs[:, ds(n * bn + cols.start, HEAD)] = xb
        part, xf = dh[:, cols], xb.astype(F32)
        scaled = part * gain_ref[:, cols]
        tot[...] += scaled * xf
        acc[:, ds(n * bn + cols.start, HEAD)] = dy_ref[:, cols].astype(F32) + inv * scaled
        dg_ref[:, cols] = jnp.sum((part * (xf * inv)).reshape(rows // 8, 8, HEAD), axis=0)

    @pl.when(n == pl.num_programs(0) - 1)
    def _():
        step = HEAD // 2

        def stats(r, _):
            sl = ds(r * step, step)
            inv = inv_ref[sl, :]
            tot[sl, :] = jnp.broadcast_to(jnp.sum(tot[sl, :], axis=-1, keepdims=True) / d, (step, HEAD)) * inv * inv * inv
            return 0

        lax.fori_loop(0, rows // step, stats, 0)

        def epi(r, _):
            sl = ds(r * step, step)
            coef = tot[sl, :]
            for c in range(d // HEAD):
                cols = slice(c * HEAD, c * HEAD + HEAD)
                dx_ref[sl, cols] = (acc[sl, cols] - xs[sl, cols].astype(F32) * coef).astype(BF)
            return 0

        lax.fori_loop(0, rows // step, epi, 0)

    for copy in copies:
        copy.wait()


def dx_call(idx, x, dy, gain, inv, pieces, ws, rcv, bufs):
    rows, d = x.shape
    bn = HB
    once = pl.Buffered(1)
    maps = (own_map, own_map, first_row, first_row) * 2
    return call(dx_body, (d // bn,),
                [pl.BlockSpec((rows, bn), col_map)] * 2 + [pl.BlockSpec((1, bn), col_map), pl.BlockSpec((rows, HEAD), own_map)]
                + [pl.BlockSpec((rows, PW), m, pipeline_mode=once) for m in maps]
                + [pl.BlockSpec((bn, w.shape[1] // 4), lambda n, s, p=p: (n, s[p])) for p in range(4) for w in ws]
                + [pl.BlockSpec((bn, rcv.shape[1]), row_map)] + [ANY] * 3,
                [pl.BlockSpec((rows, d), first_row, pipeline_mode=once), pl.BlockSpec((8, bn), col_map)] + [ANY] * 3,
                [sds(rows, d), sds(8, d, F32)] + [sds(*b.shape, F32) for b in bufs],
                [idx, x, dy, gain, inv, *pieces] + list(ws) * 4 + [rcv, *bufs], 16 * rows * d * PW,
                scratch=[pltpu.VMEM((rows, d), F32), pltpu.VMEM((rows, d), BF), pltpu.VMEM((rows, HEAD), F32),
                         pltpu.SemaphoreType.DMA((5,))],
                aliases={26 + n: 2 + n for n in range(3)})


def solution(mesh):
    sp = mesh.shape['sp']
    cross = [(a, a ^ 2) for a in range(sp)]
    pair = [(a, a ^ 1) for a in range(sp)]

    def over(val):
        return lax.ppermute(val, 'sp', cross)

    def near(val):
        return lax.ppermute(val, 'sp', pair)

    def after(val, *deps):
        return lax.optimization_barrier((val,) + deps)[0]

    def vec(*vals, dep=()):
        out = jnp.stack([jnp.asarray(v, jnp.int32) for v in vals])
        return after(out, *dep) if dep else out

    def step(x, dy, positions, gain, w_q, w_k, w_v, w_o):
        j = lax.axis_index('sp').astype(jnp.int32)
        rows, d = x.shape
        seq = rows * sp
        half = rows // 2
        j1, j2, j3 = [j ^ n for n in (1, 2, 3)]
        dev = (j, j1, j2, j3)
        bpr, hpr = rows // BLK, rows // HB
        ws = (w_q, w_k, w_v)

        def rows_of(val, blk):
            return lax.dynamic_slice_in_dim(val, blk * rows, rows, 0)

        gain_f = gain.astype(F32).reshape(1, d)

        cut = rows - HB
        xa = x[:cut]
        pos2 = over(positions)
        pos1 = near(positions)
        x2a = over(xa)
        x2b = over(after(x, xa)[cut:])
        x1 = near(x)
        pos3 = near(pos2)
        dy1 = near(after(dy, x1))

        pos = jnp.zeros((seq,), jnp.int32)
        for blk, val in zip(dev, (positions, pos1, pos2, pos3)):
            pos = lax.dynamic_update_slice(pos, val, (blk * rows,))
        inv_freq = ROPE_THETA ** (-jnp.arange(0, HEAD, 2).astype(F32) / HEAD)
        angles = pos.astype(F32)[:, None] * inv_freq[None, :]
        cos_h, sin_h = jnp.cos(angles), jnp.sin(angles)
        tabs = (jnp.concatenate([cos_h, cos_h], axis=1), jnp.concatenate([-sin_h, sin_h], axis=1))

        dya, dyb = dy[:half], dy[half:]
        bufs = project(vec(j * bpr, j1 * bpr, j, dep=(dya, dyb)), x, x1, gain_f, ws, tabs, None, seq)
        dbufs = dout(vec(j * bpr, j1 * bpr, j, dep=(bufs[1],)), dy, dy1, w_o, None, seq)

        chip, nh = j // 2, seq // BLK // 2
        tri = row_tasks(0, nh)
        square = [(i + nh, nh, 0, i) for i in range(nh)]

        def table(head, tasks):
            return jnp.concatenate([vec(*head, len(tasks)), jnp.asarray(tasks, jnp.int32).reshape(-1)])

        local = attn_fwd("local", after(table((j1, chip), tri), dbufs[1]), *bufs[1:4])
        rest_tasks = jnp.where(chip == 0, table((j1, 0), row_tasks(nh, 2 * nh) * 2).at[HEADER - 1].set(nh),
                               table((j1, 1), tri + square))

        x2a = after(x2a, local[0])
        dy2a = over(after(dya, x2a))
        x3a = near(x2a)
        bufs = project(vec(j2 * hpr, j3 * hpr, j), x2a, x3a, gain_f, ws, tabs, bufs, seq)
        x2b = after(x2b, bufs[1])
        dy2b = over(after(dyb, x2b))
        x3b = near(x2b)
        bufs = project(vec((j2 + 1) * hpr - 1, (j3 + 1) * hpr - 1, j), x2b, x3b, gain_f, ws, tabs, bufs, seq)
        h_all, q, k, v, inv = bufs
        o, lse, o_hi, o_pair = attn_fwd("rest", rest_tasks, q, k, v, rows, local)
        orv = over(o_hi)
        o1 = near(o_pair)
        dy2a = after(dy2a, o)
        dy3a = near(dy2a)
        qc, kc, vc = project_first(vec(j2, dep=(o,)), h_all, ws, tabs, seq // 2)
        oc = attn_fwd("first", table((j1, 0), tri), qc, kc, vc)[0]

        dy2b = after(dy2b, oc)
        dy3b = near(dy2b)
        dbufs = dout(vec(j2 * bpr, j3 * bpr, j, dep=(oc,)), dy2a, dy3a, w_o, dbufs, seq)
        dbufs = dout(vec(j2 * bpr + 1, j3 * bpr + 1, j), dy2b, dy3b, w_o, dbufs, seq)
        dy_all, do = dbufs

        ga, ga_pair = attn_bwd(vec(j1, 0), q, do, o, k, v, lse, tabs, rows)
        ga2 = over(ga)
        ga1 = near(ga_pair)
        gb, gb_pair = attn_bwd(vec(j1, 1, dep=(ga,)), q, do, o, k, v, lse, tabs, rows)
        gb2 = over(gb)
        gb1 = near(gb_pair)

        ox = lax.dynamic_update_slice(oc, after(orv, gb), (seq // 2, 0))
        o3 = near(rows_of(ox, j1))
        wo_fin, wo_snd = dw_o(vec(j, j2, dep=(gb,)), o, ox, dy_all)
        wo_rcv = near(wo_snd)
        result = out_proj(vec(*dev, dep=(wo_snd,)), x, (o, o1, ox, o3), w_o)
        ga2 = after(ga2, wo_snd)
        ga3 = near(rows_of(ga2, j1))
        fq, fk, fv, snd, wo_fin = dw_own(vec(*dev, dep=(result,)), h_all, ga, gb, ga2, wo_rcv, wo_fin)
        rcv = near(snd)

        gb2 = after(gb2, snd)
        gb3 = near(rows_of(gb2, j1))
        fq, fk, fv, snd_b = dw_group(vec(j2), h_all, ga2, gb2, (fq, fk, fv))
        rcv_b = near(snd_b)
        grad_x, dg, fq, fk, fv = dx_call(vec(*dev, dep=(snd_b,)), x, dy, gain_f, inv,
                                         (ga, gb, ga1, gb1, ga2, gb2, ga3, gb3), ws, rcv, (fq, fk, fv))
        dg = jnp.sum(dg, axis=0)
        dg = dg + near(dg)
        dg = dg + over(dg)
        fq, fk, fv = place(vec(j3), rcv_b, (fq, fk, fv))
        return result, grad_x, fq, fk, fv, wo_fin, dg

    seq_spec = P(('dp', 'sp'), None)
    whole = P(None, None)
    part_rows = P('dp', None)
    return jax.shard_map(step, mesh=mesh,
                         in_specs=(seq_spec, seq_spec, P(('dp', 'sp')), P(None), whole, whole, whole, whole),
                         out_specs=(seq_spec, seq_spec, part_rows, part_rows, part_rows, part_rows, P('dp')),
                         check_vma=False)
```

```python
import math

import jax
import jax.numpy as jnp
from jax import lax
from jax.experimental import pallas as pl
from jax.experimental.pallas import tpu as pltpu
from jax.sharding import PartitionSpec as P


HEAD = 128
GROUP = 3
GW = GROUP * HEAD
QK = GW + HEAD
PW = QK + HEAD
PAIR = 2 * HEAD
ROPE_THETA = 1000000.0
NORM_EPS = 1e-05
NEG_LARGE = -1e30
BF = jnp.bfloat16
F32 = jnp.float32
SCALE = HEAD ** -0.5
SCALE2 = SCALE * math.log2(math.e)
BLK = 512
HB = BLK // 2
VMEM_LIMIT = 62 * 1024 * 1024
ANY = pl.BlockSpec(memory_space=pl.ANY)


def first_row(i, s):
    return (0, 0)


def row_map(i, s):
    return (i, 0)


def col_map(i, s):
    return (0, i)


def own_map(i, s):
    return (s[0], 0)


def sds(rows, cols, dtype=BF):
    return jax.ShapeDtypeStruct((rows, cols), dtype)


def call(body, grid, in_specs, out_specs, out_shape, args, flops, scratch=(), aliases=None):
    return pl.pallas_call(
        body,
        grid_spec=pltpu.PrefetchScalarGridSpec(
            num_scalar_prefetch=1, grid=grid, in_specs=in_specs, out_specs=out_specs, scratch_shapes=list(scratch)),
        out_shape=out_shape, input_output_aliases=aliases or {},
        compiler_params=pltpu.CompilerParams(dimension_semantics=("arbitrary",) * len(grid),
                                             vmem_limit_bytes=VMEM_LIMIT),
        cost_estimate=pl.CostEstimate(flops=int(flops), bytes_accessed=int(flops) // BLK,
                                      transcendentals=0))(*args)


def down(shape):
    return lax.broadcasted_iota(jnp.int32, shape, 0)


def across(shape):
    return lax.broadcasted_iota(jnp.int32, shape, 1)


def one(h):
    return slice(h, h + 1)


def head_cols(h):
    return slice(h * HEAD, h * HEAD + HEAD)


def mm(a, b):
    return jnp.dot(a, b, preferred_element_type=F32)


def mm_nt(a, b):
    return lax.dot_general(a, b, (((1,), (1,)), ((), ())), preferred_element_type=F32)


def rotate(val, cos_t, sin_t):
    return val * cos_t + pltpu.roll(val, HEAD // 2, 1) * sin_t


def ds(start, size):
    return pl.ds(pl.multiple_of(start, size), size)


def split3(val):
    hi = val.astype(BF).astype(F32)
    mid = (val - hi).astype(BF).astype(F32)
    return hi, mid, val - hi - mid


def qkv_of(h, wq_ref, wk_ref, wv_ref, cos_ref, sin_ref, q_ref, k_ref, v_ref):
    cos_t, sin_t = cos_ref[...], sin_ref[...]
    out = mm(h, wq_ref[...])
    for c in range(wq_ref.shape[1] // HEAD):
        sl = head_cols(c)
        q_ref[:, sl] = rotate(out[:, sl], cos_t, sin_t).astype(BF)
    out = mm(h, jnp.concatenate([wk_ref[...], wv_ref[...]], axis=1))
    for sl in (slice(0, HEAD), slice(HEAD, PAIR)):
        k_ref[:, sl] = rotate(out[:, sl], cos_t, sin_t).astype(BF)
    v_ref[...] = out[:, PAIR:].astype(BF)


def proj_body(s_ref, xa_ref, xb_ref, gain_ref, wq_ref, wk_ref, wv_ref, cos_ref, sin_ref, *rest):
    h_ref, q_ref, k_ref, v_ref, inv_ref = rest[-5:]
    half = pl.num_programs(0) // 2

    def norm(src):
        step = HEAD // 2

        def stats(c, _):
            sl = ds(c * step, step)
            xf = src[sl, :].astype(F32)
            inv = lax.rsqrt(jnp.mean(xf * xf, axis=-1, keepdims=True) + NORM_EPS)
            inv_ref[sl, :] = jnp.broadcast_to(inv, (step, HEAD))
            return 0

        def scale(c, _):
            sl = ds(c * step, step)
            inv, gain = inv_ref[sl, :], gain_ref[...]
            for n in range(src.shape[1] // HEAD):
                cols = head_cols(n)
                h_ref[sl, cols] = (src[sl, cols].astype(F32) * inv * gain[:, cols]).astype(BF)
            return 0

        lax.fori_loop(0, src.shape[0] // step, stats, 0)
        lax.fori_loop(0, src.shape[0] // step, scale, 0)

    @pl.when(pl.program_id(0) < half)
    def _():
        norm(xa_ref)

    @pl.when(pl.program_id(0) >= half)
    def _():
        norm(xb_ref)

    qkv_of(h_ref[...], wq_ref, wk_ref, wv_ref, cos_ref, sin_ref, q_ref, k_ref, v_ref)


def two_source(rows):
    bm = HB if rows % BLK else BLK
    nb = rows // bm

    def a_map(i, s):
        return (jnp.minimum(i, nb - 1), 0)

    def b_map(i, s):
        return (jnp.maximum(i - nb, 0), 0)

    def o_map(i, s):
        return (jnp.where(i < nb, s[0] + i, s[1] + i - nb), 0)

    return bm, nb, a_map, b_map, o_map


def project(idx, xa, xb, gain, ws, tabs, bufs, seq):
    rows, d = xa.shape
    bm, nb, a_map, b_map, o_map = two_source(rows)
    widths = [w.shape[1] // 4 for w in ws]
    in_specs = [pl.BlockSpec((bm, d), a_map), pl.BlockSpec((bm, d), b_map), pl.BlockSpec((1, d), first_row)]
    in_specs += [pl.BlockSpec((d, w), lambda i, s: (0, s[2])) for w in widths]
    in_specs += [pl.BlockSpec((bm, HEAD), o_map)] * 2
    args = [idx, xa, xb, gain, *ws, *tabs]
    aliases = {}
    if bufs is not None:
        in_specs += [ANY] * len(bufs)
        aliases = {len(args) + n: n for n in range(len(bufs))}
        args += list(bufs)
    return call(proj_body, (2 * nb,), in_specs, [pl.BlockSpec((bm, w), o_map) for w in (d, *widths, HEAD)],
                [sds(seq, w) for w in (d, *widths)] + [sds(seq, HEAD, F32)], args, 4 * rows * d * sum(widths),
                aliases=aliases)


def projc_body(s_ref, h_ref, *rest):
    qkv_of(h_ref[...], *rest)


def project_first(idx, h, ws, tabs, rows):
    d = h.shape[1]
    widths = [w.shape[1] // 4 for w in ws]
    return call(projc_body, (rows // BLK,),
                [pl.BlockSpec((BLK, d), row_map)] + [pl.BlockSpec((d, w), lambda i, s: (0, s[0])) for w in widths]
                + [pl.BlockSpec((BLK, HEAD), row_map)] * 2,
                [pl.BlockSpec((BLK, w), row_map) for w in widths], [sds(rows, w) for w in widths],
                [idx, h, *ws, *tabs], 2 * rows * d * sum(widths))


def dout_body(s_ref, da_ref, db_ref, wo_ref, *rest):
    dy_out, do_out = rest[-2:]
    half = pl.num_programs(0) // 2

    @pl.when(pl.program_id(0) < half)
    def _():
        dy_out[...] = da_ref[...]

    @pl.when(pl.program_id(0) >= half)
    def _():
        dy_out[...] = db_ref[...]

    do_out[...] = mm_nt(dy_out[...], wo_ref[...]).astype(BF)


def dout(idx, da, db, w_o, bufs, seq):
    rows, d = da.shape
    bm, nb, a_map, b_map, o_map = two_source(rows)
    oc = w_o.shape[0] // 4
    in_specs = [pl.BlockSpec((bm, d), a_map), pl.BlockSpec((bm, d), b_map),
                pl.BlockSpec((oc, d), lambda i, s: (s[2], 0))]
    args = [idx, da, db, w_o]
    aliases = {}
    if bufs is not None:
        in_specs += [ANY] * 2
        aliases = {len(args) + n: n for n in range(2)}
        args += list(bufs)
    return call(dout_body, (2 * nb,), in_specs, [pl.BlockSpec((bm, w), o_map) for w in (d, oc)],
                [sds(seq, w) for w in (d, oc)], args, 4 * rows * d * oc, aliases=aliases)


TASK = 4
HEADER = 3


def row_tasks(first, last):
    return [(i, i + 1, 1, -1) for i in range(first, last)]


def fwd_body(kind, s_ref, q_ref, k_ref, v_ref, *rest):
    qt, kk, vt, s_scr, acc, stat = rest[-6:]
    if kind == "rest":
        o1_ref, lse1_ref, st_ref, o_ref, lse_ref, hi_ref, pair_ref = rest[:7]
    else:
        o_ref, lse_ref = rest[:2]
    seq = k_ref.shape[0]

    def setup(c, _):
        sl = ds(c * BLK, BLK)
        vt[:, sl] = v_ref[sl, :].T
        kk[sl, :HEAD] = k_ref[sl, :]
        kk[sl, HEAD:] = k_ref[sl, :]
        for h in range(GROUP):
            qf = q_ref[sl, head_cols(h)].astype(F32) * SCALE2
            hi = qf.astype(BF)
            qt[h, :HEAD, sl] = hi.T
            qt[h, HEAD:, sl] = (qf - hi.astype(F32)).astype(BF).T
        return 0

    lax.fori_loop(0, seq // BLK, setup, 0)
    acc[...] = jnp.zeros_like(acc)
    stat[...] = jnp.zeros_like(stat)
    cur, old, den_row = 0, 1, 2
    if kind == "rest":
        @pl.when(s_ref[1] == 0)
        def _():
            o_ref[:seq // 2, :] = o1_ref[...]
            lse_ref[0, :, :seq // 2] = lse1_ref[0]

    def task(t):
        return [s_ref[HEADER + t * TASK + n] for n in range(TASK)]

    def stage_a(h, i, j, masked, init=None):
        row = one(h)
        s = mm(kk[ds(j * BLK, BLK), :], qt[h, :, ds(i * BLK, BLK)])
        if masked is not False:
            keep = down(s.shape) <= across(s.shape)
            s = jnp.where(keep if masked is True else jnp.logical_or(keep, jnp.logical_not(masked)), s, NEG_LARGE)
        s_scr[h] = s
        m_new = jnp.max(s, axis=0, keepdims=True)
        if init is None:
            m_old = stat[cur, row]
        elif kind == "rest":
            m_old = jnp.where(init >= 0, lse1_ref[0, row, ds(jnp.maximum(init, 0) * BLK, BLK)], NEG_LARGE)
        else:
            m_old = jnp.full(m_new.shape, NEG_LARGE, F32)
        m_new = jnp.maximum(m_old, m_new)
        stat[old, row] = jnp.exp2(m_old - m_new)
        stat[cur, row] = m_new

    def stage_p(h):
        row = one(h)
        p = jnp.exp2(s_scr[h] - stat[cur, row])
        alpha = stat[old, row]
        stat[den_row, row] = stat[den_row, row] * alpha + jnp.sum(p, axis=0, keepdims=True)
        return p.astype(BF), alpha

    def stage_v(h, j, held):
        p, alpha = held
        acc[h] = acc[h] * alpha + mm(vt[:, ds(j * BLK, BLK)], p)

    def finish(h, i, den, top):
        row = one(h)
        out = acc[h] / den
        o_ref[ds(i * BLK, BLK), head_cols(h)] = out.T.astype(BF)
        lse_ref[0, row, ds(i * BLK, BLK)] = top + jnp.log2(den)
        if kind == "local":
            rest[2][0, h, :, ds(i * BLK, BLK)] = out

    def pipeline(i, j, masked):
        for h in range(GROUP):
            held = stage_p(h)
            stage_a(h, i, j + 1, masked)
            stage_v(h, j, held)

    count = s_ref[HEADER - 1]
    i, steps, diag, init = task(0)
    for h in range(GROUP):
        stage_a(h, i, 0, jnp.logical_and(steps == 1, diag == 1), init)

    def row(t, _):
        i, steps, diag, _ = task(t)

        def inner(j, _):
            pipeline(i, j, False)
            return 0

        lax.fori_loop(0, steps - 2, inner, 0)

        @pl.when(jnp.logical_and(steps > 1, diag == 1))
        def _():
            pipeline(i, steps - 2, True)

        if kind == "rest":
            @pl.when(diag == 0)
            def _():
                pipeline(i, steps - 2, False)
        i2, _, _, init2 = task(jnp.minimum(t + 1, count - 1))
        for h in range(GROUP):
            held = stage_p(h)
            final = (stat[den_row, one(h)], stat[cur, one(h)])
            stage_a(h, i2, 0, False, init2)
            stage_v(h, steps - 1, held)
            finish(h, i, *final)
        if kind == "rest":
            @pl.when(init2 >= 0)
            def _():
                stat[den_row] = jnp.ones(stat.shape[1:], F32)
                for h in range(GROUP):
                    acc[h] = st_ref[0, h, :, ds(init2 * BLK, BLK)]
        return 0

    lax.fori_loop(0, count, row, 0)
    lse_ref[0, GROUP:, :] = jnp.zeros((8 - GROUP, seq), F32)
    if kind == "rest":
        hi_ref[...] = o_ref[seq // 2:, :]
        pair_ref[...] = o_ref[ds(s_ref[0] * pair_ref.shape[0], pair_ref.shape[0]), :]


def attn_fwd(kind, idx, q, k, v, rows=0, local=()):
    whole = q.shape[0]
    seq = whole if kind == "rest" else whole // (2 if kind == "local" else 1)
    nkv = k.shape[1] // HEAD

    def half_map(g, s):
        return (s[1], g)

    def head_map(g, s):
        return (g, 0, 0)

    def state_map(g, s):
        return (g, 0, 0, 0)

    at = half_map if kind == "local" else col_map
    lse_spec = pl.BlockSpec((1, 8, seq), head_map)
    outs, specs = [sds(seq, q.shape[1]), jax.ShapeDtypeStruct((nkv, 8, seq), F32)], []
    out_specs = [pl.BlockSpec((seq, GW), col_map), lse_spec]
    state = pl.BlockSpec((1, GROUP, HEAD, whole // 2), state_map)
    if kind == "local":
        outs.append(jax.ShapeDtypeStruct((nkv, GROUP, HEAD, seq), F32))
        out_specs.append(state)
    if kind == "rest":
        specs = [pl.BlockSpec((seq // 2, GW), col_map), pl.BlockSpec((1, 8, seq // 2), head_map), state]
        outs += [sds(r, q.shape[1]) for r in (seq // 2, rows)]
        out_specs += [pl.BlockSpec((r, GW), col_map) for r in (seq // 2, rows)]
    kspec = pl.BlockSpec((seq, HEAD), at)
    return call(lambda *refs: fwd_body(kind, *refs), (nkv,), [pl.BlockSpec((seq, GW), at), kspec, kspec] + specs,
                out_specs, outs, [idx, q, k, v, *local], nkv * GROUP * seq * seq * PAIR,
                scratch=[pltpu.VMEM((GROUP, PAIR, seq), BF), pltpu.VMEM((seq, PAIR), BF),
                         pltpu.VMEM((HEAD, seq), BF), pltpu.VMEM((GROUP, BLK, BLK), F32),
                         pltpu.VMEM((GROUP, HEAD, BLK), F32), pltpu.VMEM((GROUP, 8, BLK), F32)])


def bwd_body(s_ref, q_ref, do_ref, o_ref, lse_ref, qn_ref, don_ref, on_ref, lsen_ref, k_ref, v_ref, cos_ref, sin_ref,
             out_ref, pair_ref, ka, va, dkt, dvt, *sets):
    i = pl.program_id(0)
    last = pl.num_programs(0) - 1
    seq = k_ref.shape[0]
    m3 = GROUP * HB
    sets = (sets[:5], sets[5:])

    def spots():
        for b in range(2):
            for h in range(GROUP):
                start = (b * GROUP + h) * HB
                yield h, slice(b * HB, (b + 1) * HB), head_cols(h), slice(start, start + HB)

    def prepare(q_src, do_src, o_src, lse_src, dst):
        qa, da, q3t, do3t, dq3 = dst
        srow = down((16, HB))
        blank = jnp.zeros((HEAD - 16, HB), BF)
        for h, src, cols, rows in spots():
            qh, doh = q_src[src, cols], do_src[src, cols]
            qa[rows, :HEAD] = qh
            da[rows, :HEAD] = doh
            q3t[:, rows] = qh.T
            dt = doh.T
            do3t[:, rows] = dt
            delta = jnp.sum(dt.astype(F32) * o_src[src, cols].T.astype(F32), axis=0, keepdims=True)
            parts = jnp.zeros((16, HB), F32)
            for n, part in enumerate(split3(lse_src[0, one(h), src] * (1.0 / SCALE2)) + split3(delta)):
                parts = jnp.where(srow == n, part, parts)
            block = jnp.concatenate([parts.astype(BF), blank], axis=0).T
            qa[rows, HEAD:] = block
            da[rows, HEAD:] = block
        dq3[...] = jnp.zeros_like(dq3)

    @pl.when(i == 0)
    def _():
        dkt[...] = jnp.zeros_like(dkt)
        dvt[...] = jnp.zeros_like(dvt)

        def setup(c, _):
            sl = ds(c * BLK, BLK)
            third = across((BLK, HEAD)) // 3
            for n, (src, dst) in enumerate(((k_ref, ka), (v_ref, va))):
                dst[sl, :HEAD] = src[sl, :]
                dst[sl, HEAD:] = jnp.where(third == n, -1.0, 0.0).astype(BF)
            return 0

        lax.fori_loop(0, seq // BLK, setup, 0)
        prepare(q_ref, do_ref, o_ref, lse_ref, sets[0])

    def run(mine, other, tail_width):
        qa, da, q3t, do3t, dq3 = mine

        def step(rows, start, width, masked):
            sl = pl.ds(pl.multiple_of(start, BLK), width)
            s = mm_nt(qa[rows, :], ka[sl, :])
            dp = mm_nt(da[rows, :], va[sl, :])
            p = jnp.exp2(s * SCALE2)
            if masked:
                off = width - HB
                tail = p[:, off:]
                keep = down(tail.shape) % HB >= across(tail.shape)
                tail = jnp.where(keep, tail, 0.0)
                p = jnp.concatenate([p[:, :off], tail], axis=1) if off else tail
            dvt[:, sl] += mm(do3t[:, rows], p.astype(BF))
            dsv = (p * dp).astype(BF)
            dkt[:, sl] += mm(q3t[:, rows], dsv)
            dq3[rows, :] += mm(dsv, ka[sl, :HEAD])

        def body(t, _):
            step(slice(0, 2 * m3), t * 2 * BLK, 2 * BLK, False)
            return 0

        lax.fori_loop(0, i // 2, body, 0)
        start = (i // 2) * 2 * BLK
        step(slice(0, m3), start, tail_width - HB, True)
        prepare(qn_ref, don_ref, on_ref, lsen_ref, other)
        step(slice(m3, 2 * m3), start, tail_width, True)
        for h, src, cols, rows in spots():
            rsl = ds(i * BLK + src.start, HB)
            out_ref[rsl, cols] = rotate(dq3[rows, :] * SCALE, cos_ref[rsl, :], -sin_ref[rsl, :]).astype(BF)

    @pl.when(i % 2 == 0)
    def _():
        run(*sets, BLK)

    @pl.when(i % 2 == 1)
    def _():
        run(*sets[::-1], 2 * BLK)

    @pl.when(i == last)
    def _():
        def fin(c, _):
            sl = ds(c * BLK, BLK)
            out_ref[sl, GW:QK] = rotate(dkt[:, sl].T * SCALE, cos_ref[sl, :], -sin_ref[sl, :]).astype(BF)
            out_ref[sl, QK:] = dvt[:, sl].T.astype(BF)
            return 0

        lax.fori_loop(0, seq // BLK, fin, 0)
        pair_ref[...] = out_ref[ds(s_ref[0] * pair_ref.shape[0], pair_ref.shape[0]), :]


def attn_bwd(idx, q, do, o, k, v, lse, tabs, rows):
    seq = k.shape[0]
    nq = seq // BLK
    m3 = GROUP * BLK
    kspec = pl.BlockSpec((seq, HEAD), lambda i, s: (0, s[1]))
    row_specs = []
    for ahead in range(2):
        row_specs += [pl.BlockSpec((BLK, GW), lambda i, s, a=ahead: (jnp.minimum(i + a, nq - 1), s[1]))] * 3
        row_specs += [pl.BlockSpec((1, 8, BLK), lambda i, s, a=ahead: (s[1], 0, jnp.minimum(i + a, nq - 1)))]
    one_set = [pltpu.VMEM((m3, PAIR), BF)] * 2 + [pltpu.VMEM((HEAD, m3), BF)] * 2 + [pltpu.VMEM((m3, HEAD), F32)]
    return call(bwd_body, (nq,),
                row_specs + [kspec] * 2 + [pl.BlockSpec((seq, HEAD), first_row)] * 2,
                [pl.BlockSpec((r, PW), first_row) for r in (seq, rows)], [sds(r, PW) for r in (seq, rows)],
                [idx] + [q, do, o, lse] * 2 + [k, v, *tabs], GROUP * nq * (nq + 1) * BLK * BLK * PW,
                scratch=[pltpu.VMEM((seq, PAIR), BF)] * 2 + [pltpu.VMEM((HEAD, seq), F32)] * 2 + one_set * 2)


def out_body(s_ref, x_ref, *rest):
    ops, weights, out_ref = rest[:5], rest[5:9], rest[9]
    o0, o1, oc, orv, o3 = [r[...] for r in ops]
    lhs = jnp.concatenate([o0, o1, jnp.where(s_ref[4] == 0, oc, orv), o3], axis=1)
    rhs = jnp.concatenate([r[...] for r in weights], axis=0)
    out_ref[...] = (x_ref[...].astype(F32) + mm(lhs, rhs)).astype(BF)


def out_proj(idx, x, pieces, w_o):
    def first_map(n, s):
        return (s[0] % 2, 0)

    rows, d = x.shape
    hw = pieces[0].shape[1]
    return call(out_body, (d // BLK,),
                [pl.BlockSpec((rows, BLK), col_map)]
                + [pl.BlockSpec((rows, hw), m) for m in (own_map, first_row, first_map, first_map, first_row)]
                + [pl.BlockSpec((hw, BLK), lambda n, s, p=p: (s[p], n)) for p in range(4)],
                pl.BlockSpec((rows, BLK), col_map), sds(rows, d), [idx, x, *pieces] + [w_o] * 4,
                2 * rows * d * d)


def dwo_body(s_ref, oa_ref, ob_ref, oc_ref, dy_ref, fin, snd, ot):
    half, hw = ob_ref.shape

    @pl.when(jnp.logical_and(pl.program_id(0) == 0, pl.program_id(1) == 0))
    def _():
        def tr(c, _):
            sl, up = ds(c * BLK, BLK), ds(c * BLK + half, BLK)
            ot[:hw, sl] = oa_ref[sl, :].T
            ot[:hw, up] = oa_ref[up, :].T
            ot[hw:, sl] = ob_ref[sl, :].T
            ot[hw:, up] = oc_ref[sl, :].T
            return 0

        lax.fori_loop(0, half // BLK, tr, 0)

    val = mm(ot[ds(pl.program_id(1) * hw, hw), :], dy_ref[...])
    fin[...] = val
    snd[...] = val


def dw_o(idx, oa, ob, oc, dy):
    seq, d = dy.shape
    hw = oa.shape[1]
    o_specs = [pl.BlockSpec(o.shape, lambda i, p, s: (0, 0), pipeline_mode=pl.Buffered(1)) for o in (oa, ob, oc)]
    return call(dwo_body, (d // BLK, 2),
                o_specs + [pl.BlockSpec((seq, BLK), lambda i, p, s: (0, i))],
                [pl.BlockSpec((hw, BLK), lambda i, p, s: (s[p], i)), pl.BlockSpec((hw, BLK), lambda i, p, s: (p, i))],
                [sds(4 * hw, d, F32), sds(2 * hw, d, F32)], [idx, oa, ob, oc, dy], 4 * seq * d * hw,
                scratch=[pltpu.VMEM((2 * hw, seq), BF)])


def dwown_body(s_ref, h_ref, ga_ref, gb_ref, gc_ref, wo_ref, _, fq, fk, fv, snd, wo_fin, g3, ht, sem, wsem):
    i, steps = pl.program_id(0), pl.num_programs(0)
    rows, per = wo_ref.shape[0], steps // 2
    start = jnp.where(i < per, s_ref[1] * per + i, s_ref[3] * per + i - per)
    wcopy = pltpu.make_async_copy(wo_ref, wo_fin.at[ds(start * rows, rows), :], wsem)
    wcopy.start()

    @pl.when(i > 1)
    def _():
        for copy in scatter(snd, (fq, fk, fv), s_ref[0], s_ref[2], sem.at[i % 2]):
            copy.wait()

    ht[...] = h_ref[...].T
    lhs = ht[...]
    for g, q_at, k_at in ((ga_ref, 0, 2 * GW), (gb_ref, GW, 2 * GW + HEAD), (gc_ref, 2 * PW, 2 * PW + GW)):
        val = mm(lhs, g[:, :QK])
        snd[:, q_at:q_at + GW] = val[:, :GW]
        snd[:, k_at:k_at + HEAD] = val[:, GW:]
    snd[:, 2 * QK:2 * PW] = mm(lhs, jnp.concatenate([ga_ref[:, QK:], gb_ref[:, QK:]], axis=1))
    for copy in scatter(snd, (fq, fk, fv), s_ref[0], s_ref[2], sem.at[i % 2]):
        copy.start()

    @pl.when(i == steps - 1)
    def _():
        g3[...] = gc_ref[ds(s_ref[1] * g3.shape[0], g3.shape[0]), :]
        for slot in range(2):
            for copy in scatter(snd, (fq, fk, fv), s_ref[0], s_ref[2], sem.at[slot]):
                copy.wait()

    wcopy.wait()


def scatter(rcv, outs, whole_dev, part_dev, sem):
    rows, src, copies = ds(pl.program_id(0) * rcv.shape[0], rcv.shape[0]), 0, []
    fq, fk, fv = outs
    for n, (out, col, w) in enumerate(((fq, whole_dev, 2 * GW), (fk, whole_dev, PAIR), (fv, whole_dev, PAIR),
                                       (fq, 2 * part_dev, GW), (fk, 2 * part_dev, HEAD))):
        copies.append(pltpu.make_async_copy(rcv.at[:, src:src + w], out.at[rows, ds(col * w, w)], sem.at[n]))
        src += w
    return copies


def dw_own(idx, h, ga, gb, gc, wo_rcv, wo_fin):
    seq, d = h.shape
    steps = d // HB
    gspec = pl.BlockSpec((seq, PW), first_row, pipeline_mode=pl.Buffered(1))
    widths = (2 * GW, PAIR, PAIR)
    sw = 2 * PW + QK
    return call(dwown_body, (steps,),
                [pl.BlockSpec((seq, HB), col_map)] + [gspec] * 3
                + [pl.BlockSpec((wo_rcv.shape[0] // steps, d), row_map), ANY],
                [ANY] * 3 + [pl.BlockSpec((HB, sw), row_map), ANY, pl.BlockSpec((seq // 4, PW), first_row)],
                [sds(d, 4 * w, F32) for w in widths] + [sds(d, sw, F32), sds(*wo_fin.shape, F32), sds(seq // 4, PW)],
                [idx, h, ga, gb, gc, wo_rcv, wo_fin], 2 * seq * d * sw,
                scratch=[pltpu.VMEM((HB, seq), BF), pltpu.SemaphoreType.DMA((2, 5)), pltpu.SemaphoreType.DMA],
                aliases={6: 4})


def dwgrp_body(s_ref, h_ref, ga_ref, gb_ref, *rest):
    fq, fk, fv, snd, ht = rest[-5:]
    ht[...] = h_ref[...].T
    lhs = ht[...]
    val = mm(lhs, gb_ref[:, :QK])
    fq[...] = val[:, :GW]
    fk[...] = val[:, GW:]
    snd[:, :QK] = val
    val = mm(lhs, jnp.concatenate([ga_ref[...], gb_ref[:, QK:]], axis=1))
    fv[...] = val
    snd[:, QK:] = val


def group_specs(bm):
    return [pl.BlockSpec((bm, w), lambda i, s: (i, 2 * s[0] + 1)) for w in (GW, HEAD)] + \
        [pl.BlockSpec((bm, PAIR), lambda i, s: (i, s[0]))]


def dw_group(idx, h, ga, gb, bufs):
    seq, d = h.shape
    gspec = pl.BlockSpec((seq, PW), first_row, pipeline_mode=pl.Buffered(1))
    sw = QK + PAIR
    return call(dwgrp_body, (d // HB,),
                [pl.BlockSpec((seq, HB), col_map),
                 pl.BlockSpec((seq, HEAD), lambda i, s: (0, QK // HEAD), pipeline_mode=pl.Buffered(1)), gspec] + [ANY] * 3,
                group_specs(HB) + [pl.BlockSpec((HB, sw), row_map)], [sds(*b.shape, F32) for b in bufs] + [sds(d, sw, F32)],
                [idx, h, ga, gb, *bufs], 2 * seq * d * sw, scratch=[pltpu.VMEM((HB, seq), BF)],
                aliases={4 + n: n for n in range(3)})


def place_body(s_ref, rcv, *rest):
    q_out, k_out, v_out = rest[-3:]
    q_out[...] = rcv[:, :GW]
    k_out[...] = rcv[:, GW:QK]
    v_out[...] = rcv[:, QK:]


def place(idx, rcv, bufs):
    d, w = rcv.shape
    bm = 2 * BLK
    return call(place_body, (d // bm,), [pl.BlockSpec((bm, w), row_map)] + [ANY] * 3, group_specs(bm),
                [sds(*b.shape, F32) for b in bufs], [idx, rcv, *bufs], d * w, aliases={2 + n: n for n in range(3)})


def dx_body(s_ref, x_ref, dy_ref, gain_ref, inv_ref, *rest):
    pieces, weights, rcv = rest[:8], rest[8:20], rest[20]
    dx_ref, dg_ref, fq, fk, fv, acc, xs, tot, sem = rest[-9:]
    n = pl.program_id(0)
    bn = x_ref.shape[1]
    rows, d = acc.shape
    copies = scatter(rcv, (fq, fk, fv), s_ref[1], s_ref[3], sem)
    for copy in copies:
        copy.start()

    @pl.when(n == 0)
    def _():
        tot[...] = jnp.zeros_like(tot)

    cuts = (slice(0, GW), slice(GW, QK), slice(QK, PW))
    lhs = jnp.concatenate([pieces[2 * p + g][:, c] for p in range(4) for c in cuts for g in range(2)], axis=1)
    rhs = jnp.concatenate([r[...] for r in weights], axis=1)
    dh = mm_nt(lhs, rhs)
    inv = inv_ref[...]
    for c in range(bn // HEAD):
        cols = head_cols(c)
        xb = x_ref[:, cols]
        xs[:, ds(n * bn + cols.start, HEAD)] = xb
        part, xf = dh[:, cols], xb.astype(F32)
        scaled = part * gain_ref[:, cols]
        tot[...] += scaled * xf
        acc[:, ds(n * bn + cols.start, HEAD)] = dy_ref[:, cols].astype(F32) + inv * scaled
        dg_ref[:, cols] = jnp.sum((part * (xf * inv)).reshape(rows // 8, 8, HEAD), axis=0)

    @pl.when(n == pl.num_programs(0) - 1)
    def _():
        step = HEAD // 2

        def stats(r, _):
            sl = ds(r * step, step)
            inv = inv_ref[sl, :]
            tot[sl, :] = jnp.broadcast_to(jnp.sum(tot[sl, :], axis=-1, keepdims=True) / d, (step, HEAD)) * inv * inv * inv
            return 0

        lax.fori_loop(0, rows // step, stats, 0)

        def epi(r, _):
            sl = ds(r * step, step)
            coef = tot[sl, :]
            for c in range(d // HEAD):
                cols = head_cols(c)
                dx_ref[sl, cols] = (acc[sl, cols] - xs[sl, cols].astype(F32) * coef).astype(BF)
            return 0

        lax.fori_loop(0, rows // step, epi, 0)

    for copy in copies:
        copy.wait()


def dx_call(idx, x, dy, gain, inv, pieces, ws, rcv, bufs):
    rows, d = x.shape
    bn = HB
    once = pl.Buffered(1)
    maps = (own_map, own_map, first_row, first_row) * 2
    return call(dx_body, (d // bn,),
                [pl.BlockSpec((rows, bn), col_map)] * 2 + [pl.BlockSpec((1, bn), col_map), pl.BlockSpec((rows, HEAD), own_map)]
                + [pl.BlockSpec((rows, PW), m, pipeline_mode=once) for m in maps]
                + [pl.BlockSpec((bn, w.shape[1] // 4), lambda n, s, p=p: (n, s[p])) for p in range(4) for w in ws]
                + [pl.BlockSpec((bn, rcv.shape[1]), row_map)] + [ANY] * 3,
                [pl.BlockSpec((rows, d), first_row, pipeline_mode=once), pl.BlockSpec((8, bn), col_map)] + [ANY] * 3,
                [sds(rows, d), sds(8, d, F32)] + [sds(*b.shape, F32) for b in bufs],
                [idx, x, dy, gain, inv, *pieces] + list(ws) * 4 + [rcv, *bufs], 16 * rows * d * PW,
                scratch=[pltpu.VMEM((rows, d), F32), pltpu.VMEM((rows, d), BF), pltpu.VMEM((rows, HEAD), F32),
                         pltpu.SemaphoreType.DMA((5,))],
                aliases={26 + n: 2 + n for n in range(3)})


def solution(mesh):
    sp = mesh.shape['sp']
    cross = [(a, a ^ 2) for a in range(sp)]
    pair = [(a, a ^ 1) for a in range(sp)]

    def over(val):
        return lax.ppermute(val, 'sp', cross)

    def near(val):
        return lax.ppermute(val, 'sp', pair)

    def after(val, *deps):
        return lax.optimization_barrier((val,) + deps)[0]

    def vec(*vals, dep=()):
        out = jnp.stack([jnp.asarray(v, jnp.int32) for v in vals])
        return after(out, *dep) if dep else out

    def step(x, dy, positions, gain, w_q, w_k, w_v, w_o):
        j = lax.axis_index('sp').astype(jnp.int32)
        rows, d = x.shape
        seq = rows * sp
        j1, j2, j3 = [j ^ n for n in (1, 2, 3)]
        dev = (j, j1, j2, j3)
        bpr, hpr = rows // BLK, rows // HB
        ws = (w_q, w_k, w_v)

        def rows_of(val, blk):
            return lax.dynamic_slice_in_dim(val, blk * rows, rows, 0)

        gain_f = gain.astype(F32).reshape(1, d)

        cut = rows - HB
        xa = x[:cut]
        positions = after(positions, xa)
        pos2 = over(positions)
        pos1 = near(positions)
        x2a = over(xa)
        x2b = over(after(x, xa)[cut:])
        x1 = near(x)
        pos3 = near(pos2)
        dy1 = near(after(dy, x1))

        pos = jnp.zeros((seq,), jnp.int32)
        for blk, val in zip(dev, (positions, pos1, pos2, pos3)):
            pos = lax.dynamic_update_slice(pos, val, (blk * rows,))
        inv_freq = ROPE_THETA ** (-jnp.arange(0, HEAD, 2).astype(F32) / HEAD)
        angles = pos.astype(F32)[:, None] * inv_freq[None, :]
        cos_h, sin_h = jnp.cos(angles), jnp.sin(angles)
        tabs = (jnp.concatenate([cos_h, cos_h], axis=1), jnp.concatenate([-sin_h, sin_h], axis=1))

        dya, dyb = dy[:cut], dy[cut:]
        bufs = project(vec(j * bpr, j1 * bpr, j, dep=(dya, dyb)), x, x1, gain_f, ws, tabs, None, seq)
        dbufs = dout(vec(j * bpr, j1 * bpr, j, dep=(bufs[1],)), dy, dy1, w_o, None, seq)

        chip, nh = j // 2, seq // BLK // 2
        tri = row_tasks(0, nh)
        square = [(i + nh, nh, 0, i) for i in range(nh)]

        def table(head, tasks):
            return jnp.concatenate([vec(*head, len(tasks)), jnp.asarray(tasks, jnp.int32).reshape(-1)])

        local = attn_fwd("local", after(table((j1, chip), tri), dbufs[1]), *bufs[1:4])
        rest_tasks = jnp.where(chip == 0, table((j1, 0), row_tasks(nh, 2 * nh) * 2).at[HEADER - 1].set(nh),
                               table((j1, 1), tri + square))

        x2a = after(x2a, local[0])
        dy2a = over(after(dya, x2a))
        x3a = near(x2a)
        bufs = project(vec(j2 * hpr, j3 * hpr, j), x2a, x3a, gain_f, ws, tabs, bufs, seq)
        x2b = after(x2b, bufs[1])
        dy2b = over(after(dyb, x2b))
        x3b = near(x2b)
        bufs = project(vec((j2 + 1) * hpr - 1, (j3 + 1) * hpr - 1, j), x2b, x3b, gain_f, ws, tabs, bufs, seq)
        h_all, q, k, v, inv = bufs
        o, lse, o_hi, o_pair = attn_fwd("rest", rest_tasks, q, k, v, rows, local)
        orv = over(o_hi)
        o1 = near(o_pair)
        qc, kc, vc = project_first(vec(j2, dep=(o,)), h_all, ws, tabs, seq // 2)
        dy2a = after(dy2a, qc)
        dy3a = near(dy2a)
        oc = attn_fwd("first", table((j1, 0), tri), qc, kc, vc)[0]

        dy2b = after(dy2b, oc)
        dy3b = near(dy2b)
        dbufs = dout(vec(j2 * hpr, j3 * hpr, j, dep=(oc,)), dy2a, dy3a, w_o, dbufs, seq)
        dbufs = dout(vec((j2 + 1) * hpr - 1, (j3 + 1) * hpr - 1, j), dy2b, dy3b, w_o, dbufs, seq)
        dy_all, do = dbufs

        ga, ga_pair = attn_bwd(vec(j1, 0), q, do, o, k, v, lse, tabs, rows)
        ga2 = over(ga)
        ga1 = near(ga_pair)
        gb, gb_pair = attn_bwd(vec(j1, 1, dep=(ga,)), q, do, o, k, v, lse, tabs, rows)
        gb2 = over(gb)
        gb1 = near(gb_pair)

        orv = after(orv, gb)
        o3 = near(jnp.where(chip == 0, rows_of(oc, j1 % 2), rows_of(orv, j1 % 2)))
        wo_fin, wo_snd = dw_o(vec(j, j2, dep=(gb,)), o, oc, orv, dy_all)
        wo_rcv = near(wo_snd)
        result = out_proj(vec(*dev, chip, dep=(wo_snd,)), x, (o, o1, oc, orv, o3), w_o)
        ga2 = after(ga2, wo_snd)
        fq, fk, fv, snd, wo_fin, g3 = dw_own(vec(*dev, dep=(result,)), h_all, ga, gb, ga2, wo_rcv, wo_fin)
        rcv = near(snd)
        ga3 = near(g3)

        gb2 = after(gb2, snd)
        gb3 = near(rows_of(gb2, j1))
        fq, fk, fv, snd_b = dw_group(vec(j2), h_all, ga2, gb2, (fq, fk, fv))
        rcv_b = near(snd_b)
        grad_x, dg, fq, fk, fv = dx_call(vec(*dev, dep=(snd_b,)), x, dy, gain_f, inv,
                                         (ga, gb, ga1, gb1, ga2, gb2, ga3, gb3), ws, rcv, (fq, fk, fv))
        dg = jnp.sum(dg, axis=0)
        dg = dg + near(dg)
        dg = dg + over(dg)
        fq, fk, fv = place(vec(j3), rcv_b, (fq, fk, fv))
        return result, grad_x, fq, fk, fv, wo_fin, dg

    seq_spec = P(('dp', 'sp'), None)
    whole = P(None, None)
    part_rows = P('dp', None)
    return jax.shard_map(step, mesh=mesh,
                         in_specs=(seq_spec, seq_spec, P(('dp', 'sp')), P(None), whole, whole, whole, whole),
                         out_specs=(seq_spec, seq_spec, part_rows, part_rows, part_rows, part_rows, P('dp')),
                         check_vma=False)
```

```python
import math

import jax
import jax.numpy as jnp
from jax import lax
from jax.experimental import pallas as pl
from jax.experimental.pallas import tpu as pltpu
from jax.sharding import PartitionSpec as P


HEAD = 128
GROUP = 3
GW = GROUP * HEAD
QK = GW + HEAD
PW = QK + HEAD
PAIR = 2 * HEAD
ROPE_THETA = 1000000.0
NORM_EPS = 1e-05
NEG_LARGE = -1e30
BF = jnp.bfloat16
F32 = jnp.float32
SCALE = HEAD ** -0.5
SCALE2 = SCALE * math.log2(math.e)
BLK = 512
HB = BLK // 2
VMEM_LIMIT = 62 * 1024 * 1024
ANY = pl.BlockSpec(memory_space=pl.ANY)


def first_row(i, s):
    return (0, 0)


def row_map(i, s):
    return (i, 0)


def col_map(i, s):
    return (0, i)


def own_map(i, s):
    return (s[0], 0)


def sds(rows, cols, dtype=BF):
    return jax.ShapeDtypeStruct((rows, cols), dtype)


def call(body, grid, in_specs, out_specs, out_shape, args, flops, scratch=(), aliases=None):
    return pl.pallas_call(
        body,
        grid_spec=pltpu.PrefetchScalarGridSpec(
            num_scalar_prefetch=1, grid=grid, in_specs=in_specs, out_specs=out_specs, scratch_shapes=list(scratch)),
        out_shape=out_shape, input_output_aliases=aliases or {},
        compiler_params=pltpu.CompilerParams(dimension_semantics=("arbitrary",) * len(grid),
                                             vmem_limit_bytes=VMEM_LIMIT),
        cost_estimate=pl.CostEstimate(flops=int(flops), bytes_accessed=int(flops) // BLK,
                                      transcendentals=0))(*args)


def down(shape):
    return lax.broadcasted_iota(jnp.int32, shape, 0)


def across(shape):
    return lax.broadcasted_iota(jnp.int32, shape, 1)


def loop(count, body):
    def run(c, _):
        body(c)
        return 0

    lax.fori_loop(0, count, run, 0)


def one(h):
    return slice(h, h + 1)


def head_cols(h):
    return slice(h * HEAD, h * HEAD + HEAD)


def mm(a, b):
    return jnp.dot(a, b, preferred_element_type=F32)


def mm_nt(a, b):
    return lax.dot_general(a, b, (((1,), (1,)), ((), ())), preferred_element_type=F32)


def rotate(val, cos_t, sin_t):
    return val * cos_t + pltpu.roll(val, HEAD // 2, 1) * sin_t


def ds(start, size):
    return pl.ds(pl.multiple_of(start, size), size)


def split3(val):
    hi = val.astype(BF).astype(F32)
    mid = (val - hi).astype(BF).astype(F32)
    return hi, mid, val - hi - mid


def qkv_of(h, wq_ref, wk_ref, wv_ref, cos_ref, sin_ref, q_ref, k_ref, v_ref):
    cos_t, sin_t = cos_ref[...], sin_ref[...]
    out = mm(h, wq_ref[...])
    for c in range(wq_ref.shape[1] // HEAD):
        sl = head_cols(c)
        q_ref[:, sl] = rotate(out[:, sl], cos_t, sin_t).astype(BF)
    out = mm(h, jnp.concatenate([wk_ref[...], wv_ref[...]], axis=1))
    for sl in (slice(0, HEAD), slice(HEAD, PAIR)):
        k_ref[:, sl] = rotate(out[:, sl], cos_t, sin_t).astype(BF)
    v_ref[...] = out[:, PAIR:].astype(BF)


def proj_body(s_ref, xa_ref, xb_ref, gain_ref, wq_ref, wk_ref, wv_ref, cos_ref, sin_ref, *rest):
    h_ref, q_ref, k_ref, v_ref, inv_ref = rest[-5:]
    half = pl.num_programs(0) // 2

    def norm(src):
        step = HEAD // 2

        def stats(c):
            sl = ds(c * step, step)
            xf = src[sl, :].astype(F32)
            inv = lax.rsqrt(jnp.mean(xf * xf, axis=-1, keepdims=True) + NORM_EPS)
            inv_ref[sl, :] = jnp.broadcast_to(inv, (step, HEAD))

        def scale(c):
            sl = ds(c * step, step)
            inv, gain = inv_ref[sl, :], gain_ref[...]
            for n in range(src.shape[1] // HEAD):
                cols = head_cols(n)
                h_ref[sl, cols] = (src[sl, cols].astype(F32) * inv * gain[:, cols]).astype(BF)

        loop(src.shape[0] // step, stats)
        loop(src.shape[0] // step, scale)

    @pl.when(pl.program_id(0) < half)
    def _():
        norm(xa_ref)

    @pl.when(pl.program_id(0) >= half)
    def _():
        norm(xb_ref)

    qkv_of(h_ref[...], wq_ref, wk_ref, wv_ref, cos_ref, sin_ref, q_ref, k_ref, v_ref)


def two_source(rows):
    bm = HB if rows % BLK else BLK
    nb = rows // bm

    def a_map(i, s):
        return (jnp.minimum(i, nb - 1), 0)

    def b_map(i, s):
        return (jnp.maximum(i - nb, 0), 0)

    def o_map(i, s):
        return (jnp.where(i < nb, s[0] + i, s[1] + i - nb), 0)

    return bm, nb, a_map, b_map, o_map


def project(idx, xa, xb, gain, ws, tabs, bufs, seq):
    rows, d = xa.shape
    bm, nb, a_map, b_map, o_map = two_source(rows)
    widths = [w.shape[1] // 4 for w in ws]
    in_specs = [pl.BlockSpec((bm, d), a_map), pl.BlockSpec((bm, d), b_map), pl.BlockSpec((1, d), first_row)]
    in_specs += [pl.BlockSpec((d, w), lambda i, s: (0, s[2])) for w in widths]
    in_specs += [pl.BlockSpec((bm, HEAD), o_map)] * 2
    args = [idx, xa, xb, gain, *ws, *tabs]
    aliases = {}
    if bufs is not None:
        in_specs += [ANY] * len(bufs)
        aliases = {len(args) + n: n for n in range(len(bufs))}
        args += list(bufs)
    return call(proj_body, (2 * nb,), in_specs, [pl.BlockSpec((bm, w), o_map) for w in (d, *widths, HEAD)],
                [sds(seq, w) for w in (d, *widths)] + [sds(seq, HEAD, F32)], args, 4 * rows * d * sum(widths),
                aliases=aliases)


def projc_body(s_ref, h_ref, *rest):
    qkv_of(h_ref[...], *rest)


def project_first(idx, h, ws, tabs, rows):
    d = h.shape[1]
    widths = [w.shape[1] // 4 for w in ws]
    return call(projc_body, (rows // BLK,),
                [pl.BlockSpec((BLK, d), row_map)] + [pl.BlockSpec((d, w), lambda i, s: (0, s[0])) for w in widths]
                + [pl.BlockSpec((BLK, HEAD), row_map)] * 2,
                [pl.BlockSpec((BLK, w), row_map) for w in widths], [sds(rows, w) for w in widths],
                [idx, h, *ws, *tabs], 2 * rows * d * sum(widths))


def dout_body(s_ref, da_ref, db_ref, wo_ref, *rest):
    dy_out, do_out = rest[-2:]
    half = pl.num_programs(0) // 2

    @pl.when(pl.program_id(0) < half)
    def _():
        dy_out[...] = da_ref[...]

    @pl.when(pl.program_id(0) >= half)
    def _():
        dy_out[...] = db_ref[...]

    do_out[...] = mm_nt(dy_out[...], wo_ref[...]).astype(BF)


def dout(idx, da, db, w_o, bufs, seq):
    rows, d = da.shape
    bm, nb, a_map, b_map, o_map = two_source(rows)
    oc = w_o.shape[0] // 4
    in_specs = [pl.BlockSpec((bm, d), a_map), pl.BlockSpec((bm, d), b_map),
                pl.BlockSpec((oc, d), lambda i, s: (s[2], 0))]
    args = [idx, da, db, w_o]
    aliases = {}
    if bufs is not None:
        in_specs += [ANY] * 2
        aliases = {len(args) + n: n for n in range(2)}
        args += list(bufs)
    return call(dout_body, (2 * nb,), in_specs, [pl.BlockSpec((bm, w), o_map) for w in (d, oc)],
                [sds(seq, w) for w in (d, oc)], args, 4 * rows * d * oc, aliases=aliases)


TASK = 4
HEADER = 3


def row_tasks(first, last):
    return [(i, i + 1, 1, -1) for i in range(first, last)]


def fwd_body(kind, s_ref, q_ref, k_ref, v_ref, *rest):
    qt, kk, vt, s_scr, acc, stat = rest[-6:]
    if kind == "rest":
        o1_ref, lse1_ref, st_ref, o_ref, lse_ref, hi_ref, pair_ref = rest[:7]
    else:
        o_ref, lse_ref = rest[:2]
    seq = k_ref.shape[0]

    def setup(c):
        sl = ds(c * BLK, BLK)
        vt[:, sl] = v_ref[sl, :].T
        kk[sl, :HEAD] = k_ref[sl, :]
        kk[sl, HEAD:] = k_ref[sl, :]
        for h in range(GROUP):
            qf = q_ref[sl, head_cols(h)].astype(F32) * SCALE2
            hi = qf.astype(BF)
            qt[h, :HEAD, sl] = hi.T
            qt[h, HEAD:, sl] = (qf - hi.astype(F32)).astype(BF).T

    loop(seq // BLK, setup)
    acc[...] = jnp.zeros_like(acc)
    stat[...] = jnp.zeros_like(stat)
    cur, old, den_row = 0, 1, 2
    if kind == "rest":
        @pl.when(s_ref[1] == 0)
        def _():
            o_ref[:seq // 2, :] = o1_ref[...]
            lse_ref[0, :, :seq // 2] = lse1_ref[0]

    def task(t):
        return [s_ref[HEADER + t * TASK + n] for n in range(TASK)]

    def stage_a(h, i, j, masked, init=None):
        row = one(h)
        if masked is True:
            top = mm(kk[ds(j * BLK, HB), :], qt[h, :, ds(i * BLK, BLK)])
            low = mm(kk[ds(j * BLK + HB, HB), :], qt[h, :, ds(i * BLK + HB, HB)])
            top = jnp.where(down(top.shape) <= across(top.shape), top, NEG_LARGE)
            low = jnp.where(down(low.shape) <= across(low.shape), low, NEG_LARGE)
            s_scr[h, :HB, :] = top
            s_scr[h, HB:, HB:] = low
            m_new = jnp.max(top, axis=0, keepdims=True)
            right = jnp.maximum(m_new[:, HB:], jnp.max(low, axis=0, keepdims=True))
            m_new = jnp.concatenate([m_new[:, :HB], right], axis=1)
        else:
            s = mm(kk[ds(j * BLK, BLK), :], qt[h, :, ds(i * BLK, BLK)])
            if masked is not False:
                keep = down(s.shape) <= across(s.shape)
                s = jnp.where(jnp.logical_or(keep, jnp.logical_not(masked)), s, NEG_LARGE)
            s_scr[h] = s
            m_new = jnp.max(s, axis=0, keepdims=True)
        if init is None:
            m_old = stat[cur, row]
        elif kind == "rest":
            m_old = jnp.where(init >= 0, lse1_ref[0, row, ds(jnp.maximum(init, 0) * BLK, BLK)], NEG_LARGE)
        else:
            m_old = jnp.full(m_new.shape, NEG_LARGE, F32)
        m_new = jnp.maximum(m_old, m_new)
        stat[old, row] = jnp.exp2(m_old - m_new)
        stat[cur, row] = m_new

    def stage_p(h, diag=False):
        row = one(h)
        m, alpha = stat[cur, row], stat[old, row]
        if diag:
            top = jnp.exp2(s_scr[h, :HB, :] - m)
            low = jnp.exp2(s_scr[h, HB:, HB:] - m[:, HB:])
            total = jnp.sum(top, axis=0, keepdims=True)
            right = total[:, HB:] + jnp.sum(low, axis=0, keepdims=True)
            total = jnp.concatenate([total[:, :HB], right], axis=1)
            top = top.astype(BF)
            p = (top[:, :HB], jnp.concatenate([top[:, HB:], low.astype(BF)], axis=0))
        else:
            p = jnp.exp2(s_scr[h] - m)
            total = jnp.sum(p, axis=0, keepdims=True)
            p = p.astype(BF)
        stat[den_row, row] = stat[den_row, row] * alpha + total
        return p, alpha

    def stage_v(h, j, held, diag=False):
        p, alpha = held
        if diag:
            acc[h, :, :HB] = acc[h, :, :HB] * alpha[:, :HB] + mm(vt[:, ds(j * BLK, HB)], p[0])
            acc[h, :, HB:] = acc[h, :, HB:] * alpha[:, HB:] + mm(vt[:, ds(j * BLK, BLK)], p[1])
        else:
            acc[h] = acc[h] * alpha + mm(vt[:, ds(j * BLK, BLK)], p)

    def finish(h, i, den, top):
        row = one(h)
        out = acc[h] / den
        o_ref[ds(i * BLK, BLK), head_cols(h)] = out.T.astype(BF)
        lse_ref[0, row, ds(i * BLK, BLK)] = top + jnp.log2(den)
        if kind == "local":
            rest[2][0, h, :, ds(i * BLK, BLK)] = out

    def pipeline(i, j, masked):
        for h in range(GROUP):
            held = stage_p(h)
            stage_a(h, i, j + 1, masked)
            stage_v(h, j, held)

    count = s_ref[HEADER - 1]
    i, steps, diag, init = task(0)
    for h in range(GROUP):
        stage_a(h, i, 0, jnp.logical_and(steps == 1, diag == 1), init)

    def row(t):
        i, steps, diag, _ = task(t)

        loop(steps - 2, lambda j: pipeline(i, j, False))

        pl.when(jnp.logical_and(steps > 1, diag == 1))(lambda: pipeline(i, steps - 2, True))
        if kind == "rest":
            pl.when(diag == 0)(lambda: pipeline(i, steps - 2, False))
        i2, _, _, init2 = task(jnp.minimum(t + 1, count - 1))

        def last_step(on_diag):
            for h in range(GROUP):
                held = stage_p(h, on_diag)
                final = (stat[den_row, one(h)], stat[cur, one(h)])
                stage_a(h, i2, 0, False, init2)
                stage_v(h, steps - 1, held, on_diag)
                finish(h, i, *final)

        if kind != "rest":
            last_step(True)
        else:
            pl.when(diag == 1)(lambda: last_step(True))
            pl.when(diag == 0)(lambda: last_step(False))

            @pl.when(init2 >= 0)
            def _():
                stat[den_row] = jnp.ones(stat.shape[1:], F32)
                for h in range(GROUP):
                    acc[h] = st_ref[0, h, :, ds(init2 * BLK, BLK)]

    loop(count, row)
    lse_ref[0, GROUP:, :] = jnp.zeros((8 - GROUP, seq), F32)
    if kind == "rest":
        hi_ref[...] = o_ref[seq - hi_ref.shape[0]:, :]
        pair_ref[...] = o_ref[ds(s_ref[0] * pair_ref.shape[0], pair_ref.shape[0]), :]


def attn_fwd(kind, idx, q, k, v, extra=(), local=()):
    whole = q.shape[0]
    seq = whole if kind == "rest" else whole // (2 if kind == "local" else 1)
    nkv = k.shape[1] // HEAD

    def half_map(g, s):
        return (s[1], g)

    def head_map(g, s):
        return (g, 0, 0)

    def state_map(g, s):
        return (g, 0, 0, 0)

    at = half_map if kind == "local" else col_map
    lse_spec = pl.BlockSpec((1, 8, seq), head_map)
    outs, specs = [sds(seq, q.shape[1]), jax.ShapeDtypeStruct((nkv, 8, seq), F32)], []
    out_specs = [pl.BlockSpec((seq, GW), col_map), lse_spec]
    state = pl.BlockSpec((1, GROUP, HEAD, whole // 2), state_map)
    if kind == "local":
        outs.append(jax.ShapeDtypeStruct((nkv, GROUP, HEAD, seq), F32))
        out_specs.append(state)
    if kind == "rest":
        specs = [pl.BlockSpec((seq // 2, GW), col_map), pl.BlockSpec((1, 8, seq // 2), head_map), state]
        outs += [sds(r, q.shape[1]) for r in extra]
        out_specs += [pl.BlockSpec((r, GW), col_map) for r in extra]
    kspec = pl.BlockSpec((seq, HEAD), at)
    return call(lambda *refs: fwd_body(kind, *refs), (nkv,), [pl.BlockSpec((seq, GW), at), kspec, kspec] + specs,
                out_specs, outs, [idx, q, k, v, *local], nkv * GROUP * seq * seq * PAIR,
                scratch=[pltpu.VMEM((GROUP, PAIR, seq), BF), pltpu.VMEM((seq, PAIR), BF),
                         pltpu.VMEM((HEAD, seq), BF), pltpu.VMEM((GROUP, BLK, BLK), F32),
                         pltpu.VMEM((GROUP, HEAD, BLK), F32), pltpu.VMEM((GROUP, 8, BLK), F32)])


def bwd_body(s_ref, q_ref, do_ref, o_ref, lse_ref, qn_ref, don_ref, on_ref, lsen_ref, k_ref, v_ref, cos_ref, sin_ref,
             out_ref, pair_ref, ka, va, dkt, dvt, *sets):
    i = pl.program_id(0)
    last = pl.num_programs(0) - 1
    seq = k_ref.shape[0]
    m3 = GROUP * HB
    sets = (sets[:5], sets[5:])

    def spots():
        for b in range(2):
            for h in range(GROUP):
                start = (b * GROUP + h) * HB
                yield h, slice(b * HB, (b + 1) * HB), head_cols(h), slice(start, start + HB)

    def prepare(q_src, do_src, o_src, lse_src, dst):
        qa, da, q3t, do3t, dq3 = dst
        srow = down((16, HB))
        blank = jnp.zeros((HEAD - 16, HB), BF)
        for h, src, cols, rows in spots():
            qh, doh = q_src[src, cols], do_src[src, cols]
            qa[rows, :HEAD] = qh
            da[rows, :HEAD] = doh
            q3t[:, rows] = qh.T
            dt = doh.T
            do3t[:, rows] = dt
            delta = jnp.sum(dt.astype(F32) * o_src[src, cols].T.astype(F32), axis=0, keepdims=True)
            parts = jnp.zeros((16, HB), F32)
            for n, part in enumerate(split3(lse_src[0, one(h), src] * (1.0 / SCALE2)) + split3(delta)):
                parts = jnp.where(srow == n, part, parts)
            block = jnp.concatenate([parts.astype(BF), blank], axis=0).T
            qa[rows, HEAD:] = block
            da[rows, HEAD:] = block
        dq3[...] = jnp.zeros_like(dq3)

    @pl.when(i == 0)
    def _():
        dkt[...] = jnp.zeros_like(dkt)
        dvt[...] = jnp.zeros_like(dvt)

        def setup(c):
            sl = ds(c * BLK, BLK)
            third = across((BLK, HEAD)) // 3
            for n, (src, dst) in enumerate(((k_ref, ka), (v_ref, va))):
                dst[sl, :HEAD] = src[sl, :]
                dst[sl, HEAD:] = jnp.where(third == n, -1.0, 0.0).astype(BF)

        loop(seq // BLK, setup)
        prepare(q_ref, do_ref, o_ref, lse_ref, sets[0])

    def run(mine, other, tail_width):
        qa, da, q3t, do3t, dq3 = mine

        def step(rows, start, width, masked):
            sl = pl.ds(pl.multiple_of(start, BLK), width)
            s = mm_nt(qa[rows, :], ka[sl, :])
            dp = mm_nt(da[rows, :], va[sl, :])
            p = jnp.exp2(s * SCALE2)
            if masked:
                off = width - HB
                tail = p[:, off:]
                keep = down(tail.shape) % HB >= across(tail.shape)
                tail = jnp.where(keep, tail, 0.0)
                p = jnp.concatenate([p[:, :off], tail], axis=1) if off else tail
            dvt[:, sl] += mm(do3t[:, rows], p.astype(BF))
            dsv = (p * dp).astype(BF)
            dkt[:, sl] += mm(q3t[:, rows], dsv)
            dq3[rows, :] += mm(dsv, ka[sl, :HEAD])

        def body(t):
            step(slice(0, 2 * m3), t * 2 * BLK, 2 * BLK, False)

        loop(i // 2, body)
        start = (i // 2) * 2 * BLK
        step(slice(0, m3), start, tail_width - HB, True)
        prepare(qn_ref, don_ref, on_ref, lsen_ref, other)
        step(slice(m3, 2 * m3), start, tail_width, True)
        for h, src, cols, rows in spots():
            rsl = ds(i * BLK + src.start, HB)
            out_ref[rsl, cols] = rotate(dq3[rows, :] * SCALE, cos_ref[rsl, :], -sin_ref[rsl, :]).astype(BF)

    @pl.when(i % 2 == 0)
    def _():
        run(*sets, BLK)

    @pl.when(i % 2 == 1)
    def _():
        run(*sets[::-1], 2 * BLK)

    @pl.when(i == last)
    def _():
        def fin(c):
            sl = ds(c * BLK, BLK)
            out_ref[sl, GW:QK] = rotate(dkt[:, sl].T * SCALE, cos_ref[sl, :], -sin_ref[sl, :]).astype(BF)
            out_ref[sl, QK:] = dvt[:, sl].T.astype(BF)

        loop(seq // BLK, fin)
        pair_ref[...] = out_ref[ds(s_ref[0] * pair_ref.shape[0], pair_ref.shape[0]), :]


def attn_bwd(idx, q, do, o, k, v, lse, tabs, rows):
    seq = k.shape[0]
    nq = seq // BLK
    m3 = GROUP * BLK
    kspec = pl.BlockSpec((seq, HEAD), lambda i, s: (0, s[1]))
    row_specs = []
    for ahead in range(2):
        row_specs += [pl.BlockSpec((BLK, GW), lambda i, s, a=ahead: (jnp.minimum(i + a, nq - 1), s[1]))] * 3
        row_specs += [pl.BlockSpec((1, 8, BLK), lambda i, s, a=ahead: (s[1], 0, jnp.minimum(i + a, nq - 1)))]
    one_set = [pltpu.VMEM((m3, PAIR), BF)] * 2 + [pltpu.VMEM((HEAD, m3), BF)] * 2 + [pltpu.VMEM((m3, HEAD), F32)]
    return call(bwd_body, (nq,),
                row_specs + [kspec] * 2 + [pl.BlockSpec((seq, HEAD), first_row)] * 2,
                [pl.BlockSpec((r, PW), first_row) for r in (seq, rows)], [sds(r, PW) for r in (seq, rows)],
                [idx] + [q, do, o, lse] * 2 + [k, v, *tabs], GROUP * nq * (nq + 1) * BLK * BLK * PW,
                scratch=[pltpu.VMEM((seq, PAIR), BF)] * 2 + [pltpu.VMEM((HEAD, seq), F32)] * 2 + one_set * 2)


def out_body(s_ref, x_ref, *rest):
    ops, weights, out_ref = rest[:4], rest[4:8], rest[8]
    lhs = jnp.concatenate([r[...] for r in ops], axis=1)
    rhs = jnp.concatenate([r[...] for r in weights], axis=0)
    out_ref[...] = (x_ref[...].astype(F32) + mm(lhs, rhs)).astype(BF)


def out_proj(idx, x, pieces, w_o):
    def chip_map(n, s):
        return (s[0] % 2, 0)

    rows, d = x.shape
    hw = pieces[0].shape[1]
    return call(out_body, (d // BLK,),
                [pl.BlockSpec((rows, BLK), col_map)]
                + [pl.BlockSpec((rows, hw), m) for m in (own_map, first_row, chip_map, first_row)]
                + [pl.BlockSpec((hw, BLK), lambda n, s, p=p: (s[p], n)) for p in range(4)],
                pl.BlockSpec((rows, BLK), col_map), sds(rows, d), [idx, x, *pieces] + [w_o] * 4,
                2 * rows * d * d)


def dwo_body(s_ref, oa_ref, ob_ref, oc_ref, dy_ref, fin, snd, ot):
    first, hw = ob_ref.shape

    @pl.when(jnp.logical_and(pl.program_id(0) == 0, pl.program_id(1) == 0))
    def _():
        for src, rows, base in ((oa_ref, slice(0, hw), 0), (ob_ref, slice(hw, 2 * hw), 0), (oc_ref, slice(hw, 2 * hw), first)):
            def tr(c):
                ot[rows, ds(c * BLK + base, BLK)] = src[ds(c * BLK, BLK), :].T

            loop(src.shape[0] // BLK, tr)

    val = mm(ot[ds(pl.program_id(1) * hw, hw), :], dy_ref[...])
    fin[...] = val
    snd[...] = val


def dw_o(idx, oa, ob, oc, dy):
    seq, d = dy.shape
    hw = oa.shape[1]
    o_specs = [pl.BlockSpec(o.shape, lambda i, p, s: (0, 0), pipeline_mode=pl.Buffered(1)) for o in (oa, ob, oc)]
    return call(dwo_body, (d // BLK, 2),
                o_specs + [pl.BlockSpec((seq, BLK), lambda i, p, s: (0, i))],
                [pl.BlockSpec((hw, BLK), lambda i, p, s: (s[p], i)), pl.BlockSpec((hw, BLK), lambda i, p, s: (p, i))],
                [sds(4 * hw, d, F32), sds(2 * hw, d, F32)], [idx, oa, ob, oc, dy], 4 * seq * d * hw,
                scratch=[pltpu.VMEM((2 * hw, seq), BF)])


def dwown_body(s_ref, h_ref, ga_ref, gb_ref, gc_ref, wo_ref, _, fq, fk, fv, snd, wo_fin, g3, ht, sem, wsem):
    i, steps = pl.program_id(0), pl.num_programs(0)
    rows, per = wo_ref.shape[0], steps // 2
    start = jnp.where(i < per, s_ref[1] * per + i, s_ref[3] * per + i - per)
    wcopy = pltpu.make_async_copy(wo_ref, wo_fin.at[ds(start * rows, rows), :], wsem)
    wcopy.start()

    @pl.when(i > 1)
    def _():
        for copy in scatter(snd, (fq, fk, fv), s_ref[0], s_ref[2], sem.at[i % 2]):
            copy.wait()

    ht[...] = h_ref[...].T
    lhs = ht[...]
    for g, q_at, k_at in ((ga_ref, 0, 2 * GW), (gb_ref, GW, 2 * GW + HEAD), (gc_ref, 2 * PW, 2 * PW + GW)):
        val = mm(lhs, g[:, :QK])
        snd[:, q_at:q_at + GW] = val[:, :GW]
        snd[:, k_at:k_at + HEAD] = val[:, GW:]
    snd[:, 2 * QK:2 * PW] = mm(lhs, jnp.concatenate([ga_ref[:, QK:], gb_ref[:, QK:]], axis=1))
    for copy in scatter(snd, (fq, fk, fv), s_ref[0], s_ref[2], sem.at[i % 2]):
        copy.start()

    @pl.when(i == steps - 1)
    def _():
        g3[...] = gc_ref[ds(s_ref[1] * g3.shape[0], g3.shape[0]), :]
        for slot in range(2):
            for copy in scatter(snd, (fq, fk, fv), s_ref[0], s_ref[2], sem.at[slot]):
                copy.wait()

    wcopy.wait()


def scatter(rcv, outs, whole_dev, part_dev, sem):
    rows, src, copies = ds(pl.program_id(0) * rcv.shape[0], rcv.shape[0]), 0, []
    fq, fk, fv = outs
    for n, (out, col, w) in enumerate(((fq, whole_dev, 2 * GW), (fk, whole_dev, PAIR), (fv, whole_dev, PAIR),
                                       (fq, 2 * part_dev, GW), (fk, 2 * part_dev, HEAD))):
        copies.append(pltpu.make_async_copy(rcv.at[:, src:src + w], out.at[rows, ds(col * w, w)], sem.at[n]))
        src += w
    return copies


def dw_own(idx, h, ga, gb, gc, wo_rcv, wo_fin):
    seq, d = h.shape
    steps = d // HB
    gspec = pl.BlockSpec((seq, PW), first_row, pipeline_mode=pl.Buffered(1))
    widths = (2 * GW, PAIR, PAIR)
    sw = 2 * PW + QK
    return call(dwown_body, (steps,),
                [pl.BlockSpec((seq, HB), col_map)] + [gspec] * 3
                + [pl.BlockSpec((wo_rcv.shape[0] // steps, d), row_map), ANY],
                [ANY] * 3 + [pl.BlockSpec((HB, sw), row_map), ANY, pl.BlockSpec((seq // 4, PW), first_row)],
                [sds(d, 4 * w, F32) for w in widths] + [sds(d, sw, F32), sds(*wo_fin.shape, F32), sds(seq // 4, PW)],
                [idx, h, ga, gb, gc, wo_rcv, wo_fin], 2 * seq * d * sw,
                scratch=[pltpu.VMEM((HB, seq), BF), pltpu.SemaphoreType.DMA((2, 5)), pltpu.SemaphoreType.DMA],
                aliases={6: 4})


def dwgrp_body(s_ref, h_ref, ga_ref, gb_ref, *rest):
    fq, fk, fv, snd, ht = rest[-5:]
    ht[...] = h_ref[...].T
    lhs = ht[...]
    val = mm(lhs, gb_ref[:, :QK])
    fq[...] = val[:, :GW]
    fk[...] = val[:, GW:]
    snd[:, :QK] = val
    val = mm(lhs, jnp.concatenate([ga_ref[...], gb_ref[:, QK:]], axis=1))
    fv[...] = val
    snd[:, QK:] = val


def group_specs(bm):
    return [pl.BlockSpec((bm, w), lambda i, s: (i, 2 * s[0] + 1)) for w in (GW, HEAD)] + \
        [pl.BlockSpec((bm, PAIR), lambda i, s: (i, s[0]))]


def dw_group(idx, h, ga, gb, bufs):
    seq, d = h.shape
    gspec = pl.BlockSpec((seq, PW), first_row, pipeline_mode=pl.Buffered(1))
    sw = QK + PAIR
    return call(dwgrp_body, (d // HB,),
                [pl.BlockSpec((seq, HB), col_map),
                 pl.BlockSpec((seq, HEAD), lambda i, s: (0, QK // HEAD), pipeline_mode=pl.Buffered(1)), gspec] + [ANY] * 3,
                group_specs(HB) + [pl.BlockSpec((HB, sw), row_map)], [sds(*b.shape, F32) for b in bufs] + [sds(d, sw, F32)],
                [idx, h, ga, gb, *bufs], 2 * seq * d * sw, scratch=[pltpu.VMEM((HB, seq), BF)],
                aliases={4 + n: n for n in range(3)})


def place_body(s_ref, rcv, *rest):
    q_out, k_out, v_out = rest[-3:]
    q_out[...] = rcv[:, :GW]
    k_out[...] = rcv[:, GW:QK]
    v_out[...] = rcv[:, QK:]


def place(idx, rcv, bufs):
    d, w = rcv.shape
    bm = 2 * BLK
    return call(place_body, (d // bm,), [pl.BlockSpec((bm, w), row_map)] + [ANY] * 3, group_specs(bm),
                [sds(*b.shape, F32) for b in bufs], [idx, rcv, *bufs], d * w, aliases={2 + n: n for n in range(3)})


def dx_body(s_ref, x_ref, dy_ref, gain_ref, inv_ref, *rest):
    pieces, weights, rcv = rest[:8], rest[8:20], rest[20]
    dx_ref, dg_ref, fq, fk, fv, acc, xs, tot, sem = rest[-9:]
    n = pl.program_id(0)
    bn = x_ref.shape[1]
    rows, d = acc.shape
    copies = scatter(rcv, (fq, fk, fv), s_ref[1], s_ref[3], sem)
    for copy in copies:
        copy.start()

    @pl.when(n == 0)
    def _():
        tot[...] = jnp.zeros_like(tot)

    cuts = (slice(0, GW), slice(GW, QK), slice(QK, PW))
    lhs = jnp.concatenate([pieces[2 * p + g][:, c] for p in range(4) for c in cuts for g in range(2)], axis=1)
    rhs = jnp.concatenate([r[...] for r in weights], axis=1)
    dh = mm_nt(lhs, rhs)
    inv = inv_ref[...]
    for c in range(bn // HEAD):
        cols = head_cols(c)
        xb = x_ref[:, cols]
        xs[:, ds(n * bn + cols.start, HEAD)] = xb
        part, xf = dh[:, cols], xb.astype(F32)
        scaled = part * gain_ref[:, cols]
        tot[...] += scaled * xf
        acc[:, ds(n * bn + cols.start, HEAD)] = dy_ref[:, cols].astype(F32) + inv * scaled
        dg_ref[:, cols] = jnp.sum((part * (xf * inv)).reshape(rows // 8, 8, HEAD), axis=0)

    @pl.when(n == pl.num_programs(0) - 1)
    def _():
        step = HEAD // 2

        def stats(r):
            sl = ds(r * step, step)
            inv = inv_ref[sl, :]
            tot[sl, :] = jnp.broadcast_to(jnp.sum(tot[sl, :], axis=-1, keepdims=True) / d, (step, HEAD)) * inv * inv * inv

        loop(rows // step, stats)

        def epi(r):
            sl = ds(r * step, step)
            coef = tot[sl, :]
            for c in range(d // HEAD):
                cols = head_cols(c)
                dx_ref[sl, cols] = (acc[sl, cols] - xs[sl, cols].astype(F32) * coef).astype(BF)

        loop(rows // step, epi)

    for copy in copies:
        copy.wait()


def dx_call(idx, x, dy, gain, inv, pieces, ws, rcv, bufs):
    rows, d = x.shape
    bn = HB
    once = pl.Buffered(1)
    maps = (own_map, own_map, first_row, first_row) * 2
    return call(dx_body, (d // bn,),
                [pl.BlockSpec((rows, bn), col_map)] * 2 + [pl.BlockSpec((1, bn), col_map), pl.BlockSpec((rows, HEAD), own_map)]
                + [pl.BlockSpec((rows, PW), m, pipeline_mode=once) for m in maps]
                + [pl.BlockSpec((bn, w.shape[1] // 4), lambda n, s, p=p: (n, s[p])) for p in range(4) for w in ws]
                + [pl.BlockSpec((bn, rcv.shape[1]), row_map)] + [ANY] * 3,
                [pl.BlockSpec((rows, d), first_row, pipeline_mode=once), pl.BlockSpec((8, bn), col_map)] + [ANY] * 3,
                [sds(rows, d), sds(8, d, F32)] + [sds(*b.shape, F32) for b in bufs],
                [idx, x, dy, gain, inv, *pieces] + list(ws) * 4 + [rcv, *bufs], 16 * rows * d * PW,
                scratch=[pltpu.VMEM((rows, d), F32), pltpu.VMEM((rows, d), BF), pltpu.VMEM((rows, HEAD), F32),
                         pltpu.SemaphoreType.DMA((5,))],
                aliases={26 + n: 2 + n for n in range(3)})


def solution(mesh):
    sp = mesh.shape['sp']
    cross = [(a, a ^ 2) for a in range(sp)]
    pair = [(a, a ^ 1) for a in range(sp)]

    def over(val):
        return lax.ppermute(val, 'sp', cross)

    def near(val):
        return lax.ppermute(val, 'sp', pair)

    def after(val, *deps):
        return lax.optimization_barrier((val,) + deps)[0]

    def vec(*vals, dep=()):
        out = jnp.stack([jnp.asarray(v, jnp.int32) for v in vals])
        return after(out, *dep) if dep else out

    def step(x, dy, positions, gain, w_q, w_k, w_v, w_o):
        j = lax.axis_index('sp').astype(jnp.int32)
        rows, d = x.shape
        seq = rows * sp
        j1, j2, j3 = [j ^ n for n in (1, 2, 3)]
        dev = (j, j1, j2, j3)
        bpr, hpr = rows // BLK, rows // HB
        ws = (w_q, w_k, w_v)

        def rows_of(val, blk):
            return lax.dynamic_slice_in_dim(val, blk * rows, rows, 0)

        gain_f = gain.astype(F32).reshape(1, d)

        cut = rows - HB
        xa = x[:cut]
        positions = after(positions, xa)
        pos2 = over(positions)
        pos1 = near(positions)
        x2a = over(xa)
        x2b = over(after(x, xa)[cut:])
        x1 = near(x)
        pos3 = near(pos2)
        dy1 = near(after(dy, x1))

        pos = jnp.zeros((seq,), jnp.int32)
        for blk, val in zip(dev, (positions, pos1, pos2, pos3)):
            pos = lax.dynamic_update_slice(pos, val, (blk * rows,))
        inv_freq = ROPE_THETA ** (-jnp.arange(0, HEAD, 2).astype(F32) / HEAD)
        angles = pos.astype(F32)[:, None] * inv_freq[None, :]
        cos_h, sin_h = jnp.cos(angles), jnp.sin(angles)
        tabs = (jnp.concatenate([cos_h, cos_h], axis=1), jnp.concatenate([-sin_h, sin_h], axis=1))

        dya, dyb = dy[:cut], dy[cut:]
        bufs = project(vec(j * bpr, j1 * bpr, j, dep=(dya, dyb)), x, x1, gain_f, ws, tabs, None, seq)
        dbufs = dout(vec(j * bpr, j1 * bpr, j, dep=(bufs[1],)), dy, dy1, w_o, None, seq)

        chip, nh = j // 2, seq // BLK // 2
        tri = row_tasks(0, nh)
        first = seq // 2 - BLK
        square = [(i + nh, nh, 0, i) for i in range(nh)]

        def table(head, tasks):
            return jnp.concatenate([vec(*head, len(tasks)), jnp.asarray(tasks, jnp.int32).reshape(-1)])

        local = attn_fwd("local", after(table((j1, chip), tri), dbufs[1]), *bufs[1:4])
        rest_tasks = jnp.where(chip == 0, table((j1, 0), row_tasks(nh, 2 * nh) * 2).at[HEADER - 1].set(nh),
                               table((j1, 1), tri + square))

        x2a = after(x2a, local[0])
        dy2a = over(after(dya, x2a))
        x3a = near(x2a)
        bufs = project(vec(j2 * hpr, j3 * hpr, j), x2a, x3a, gain_f, ws, tabs, bufs, seq)
        x2b = after(x2b, bufs[1])
        dy2b = over(after(dyb, x2b))
        x3b = near(x2b)
        bufs = project(vec((j2 + 1) * hpr - 1, (j3 + 1) * hpr - 1, j), x2b, x3b, gain_f, ws, tabs, bufs, seq)
        h_all, q, k, v, inv = bufs
        o, lse, o_hi, o_pair = attn_fwd("rest", rest_tasks, q, k, v, (seq - first, rows), local)
        orv = over(o_hi)
        o1 = near(o_pair)
        qc, kc, vc = project_first(vec(j2, dep=(o,)), h_all, ws, tabs, first)
        dy2a = after(dy2a, qc)
        dy3a = near(dy2a)
        oc = attn_fwd("first", table((j1, 0), tri[:-1]), qc, kc, vc)[0]

        dy2b = after(dy2b, oc)
        dy3b = near(dy2b)
        dbufs = dout(vec(j2 * hpr, j3 * hpr, j, dep=(oc,)), dy2a, dy3a, w_o, dbufs, seq)
        dbufs = dout(vec((j2 + 1) * hpr - 1, (j3 + 1) * hpr - 1, j), dy2b, dy3b, w_o, dbufs, seq)
        dy_all, do = dbufs

        ga, ga_pair = attn_bwd(vec(j1, 0), q, do, o, k, v, lse, tabs, rows)
        ga2 = over(ga)
        ga1 = near(ga_pair)
        gb, gb_pair = attn_bwd(vec(j1, 1, dep=(ga,)), q, do, o, k, v, lse, tabs, rows)
        gb2 = over(gb)
        gb1 = near(gb_pair)

        orv = after(orv, gb)
        ox = jnp.where(chip == 0, jnp.concatenate([oc, orv[:BLK]]), orv[BLK:])
        o3 = near(rows_of(ox, j1 % 2))
        wo_fin, wo_snd = dw_o(vec(j, j2, dep=(gb,)), o, oc, orv, dy_all)
        wo_rcv = near(wo_snd)
        result = out_proj(vec(*dev, dep=(wo_snd,)), x, (o, o1, ox, o3), w_o)
        ga2 = after(ga2, wo_snd)
        fq, fk, fv, snd, wo_fin, g3 = dw_own(vec(*dev, dep=(result,)), h_all, ga, gb, ga2, wo_rcv, wo_fin)
        rcv = near(snd)
        ga3 = near(g3)

        gb2 = after(gb2, snd)
        gb3 = near(rows_of(gb2, j1))
        fq, fk, fv, snd_b = dw_group(vec(j2), h_all, ga2, gb2, (fq, fk, fv))
        rcv_b = near(snd_b)
        grad_x, dg, fq, fk, fv = dx_call(vec(*dev, dep=(snd_b,)), x, dy, gain_f, inv,
                                         (ga, gb, ga1, gb1, ga2, gb2, ga3, gb3), ws, rcv, (fq, fk, fv))
        dg = jnp.sum(dg, axis=0)
        dg = dg + near(dg)
        dg = dg + over(dg)
        fq, fk, fv = place(vec(j3), rcv_b, (fq, fk, fv))
        return result, grad_x, fq, fk, fv, wo_fin, dg

    seq_spec = P(('dp', 'sp'), None)
    whole = P(None, None)
    part_rows = P('dp', None)
    return jax.shard_map(step, mesh=mesh,
                         in_specs=(seq_spec, seq_spec, P(('dp', 'sp')), P(None), whole, whole, whole, whole),
                         out_specs=(seq_spec, seq_spec, part_rows, part_rows, part_rows, part_rows, P('dp')),
                         check_vma=False)
```

```python
import math

import jax
import jax.numpy as jnp
from jax import lax
from jax.experimental import pallas as pl
from jax.experimental.pallas import tpu as pltpu
from jax.sharding import PartitionSpec as P


HEAD = 128
GROUP = 3
GW = GROUP * HEAD
QK = GW + HEAD
PW = QK + HEAD
PAIR = 2 * HEAD
ROPE_THETA = 1000000.0
NORM_EPS = 1e-05
NEG_LARGE = -1e30
BF = jnp.bfloat16
F32 = jnp.float32
SCALE = HEAD ** -0.5
SCALE2 = SCALE * math.log2(math.e)
BLK = 512
HB = BLK // 2
VMEM_LIMIT = 62 * 1024 * 1024
ANY = pl.BlockSpec(memory_space=pl.ANY)


def first_row(i, s):
    return (0, 0)


def row_map(i, s):
    return (i, 0)


def col_map(i, s):
    return (0, i)


def own_map(i, s):
    return (s[0], 0)


def sds(rows, cols, dtype=BF):
    return jax.ShapeDtypeStruct((rows, cols), dtype)


def call(body, grid, in_specs, out_specs, out_shape, args, flops, scratch=(), aliases=None):
    return pl.pallas_call(
        body,
        grid_spec=pltpu.PrefetchScalarGridSpec(
            num_scalar_prefetch=1, grid=grid, in_specs=in_specs, out_specs=out_specs, scratch_shapes=list(scratch)),
        out_shape=out_shape, input_output_aliases=aliases or {},
        compiler_params=pltpu.CompilerParams(dimension_semantics=("arbitrary",) * len(grid),
                                             vmem_limit_bytes=VMEM_LIMIT),
        cost_estimate=pl.CostEstimate(flops=int(flops), bytes_accessed=int(flops) // BLK,
                                      transcendentals=0))(*args)


def down(shape):
    return lax.broadcasted_iota(jnp.int32, shape, 0)


def across(shape):
    return lax.broadcasted_iota(jnp.int32, shape, 1)


def loop(count, body):
    def run(c, _):
        body(c)
        return 0

    lax.fori_loop(0, count, run, 0)


def one(h):
    return slice(h, h + 1)


def head_cols(h):
    return slice(h * HEAD, h * HEAD + HEAD)


def mm(a, b):
    return jnp.dot(a, b, preferred_element_type=F32)


def mm_nt(a, b):
    return lax.dot_general(a, b, (((1,), (1,)), ((), ())), preferred_element_type=F32)


def rotate(val, cos_t, sin_t):
    return val * cos_t + pltpu.roll(val, HEAD // 2, 1) * sin_t


def ds(start, size):
    return pl.ds(pl.multiple_of(start, size), size)


def split3(val):
    hi = val.astype(BF).astype(F32)
    mid = (val - hi).astype(BF).astype(F32)
    return hi, mid, val - hi - mid


def qkv_of(h, wq_ref, wk_ref, wv_ref, cos_ref, sin_ref, q_ref, k_ref, v_ref):
    cos_t, sin_t = cos_ref[...], sin_ref[...]
    out = mm(h, wq_ref[...])
    for c in range(wq_ref.shape[1] // HEAD):
        sl = head_cols(c)
        q_ref[:, sl] = rotate(out[:, sl], cos_t, sin_t).astype(BF)
    out = mm(h, jnp.concatenate([wk_ref[...], wv_ref[...]], axis=1))
    for sl in (slice(0, HEAD), slice(HEAD, PAIR)):
        k_ref[:, sl] = rotate(out[:, sl], cos_t, sin_t).astype(BF)
    v_ref[...] = out[:, PAIR:].astype(BF)


def proj_body(s_ref, xa_ref, xb_ref, gain_ref, wq_ref, wk_ref, wv_ref, cos_ref, sin_ref, *rest):
    h_ref, q_ref, k_ref, v_ref, inv_ref = rest[-5:]
    half = pl.num_programs(0) // 2

    def norm(src):
        step = HEAD

        def stats(c):
            sl = ds(c * step, step)
            xf = src[sl, :].astype(F32)
            inv = lax.rsqrt(jnp.mean(xf * xf, axis=-1, keepdims=True) + NORM_EPS)
            inv_ref[sl, :] = jnp.broadcast_to(inv, (step, HEAD))

        def scale(c):
            sl = ds(c * step, step)
            inv, gain = inv_ref[sl, :], gain_ref[...]
            for n in range(src.shape[1] // HEAD):
                cols = head_cols(n)
                h_ref[sl, cols] = (src[sl, cols].astype(F32) * inv * gain[:, cols]).astype(BF)

        loop(src.shape[0] // step, stats)
        loop(src.shape[0] // step, scale)

    @pl.when(pl.program_id(0) < half)
    def _():
        norm(xa_ref)

    @pl.when(pl.program_id(0) >= half)
    def _():
        norm(xb_ref)

    qkv_of(h_ref[...], wq_ref, wk_ref, wv_ref, cos_ref, sin_ref, q_ref, k_ref, v_ref)


def two_source(rows):
    bm = HB if rows % BLK else BLK
    nb = rows // bm

    def a_map(i, s):
        return (jnp.minimum(i, nb - 1), 0)

    def b_map(i, s):
        return (jnp.maximum(i - nb, 0), 0)

    def o_map(i, s):
        return (jnp.where(i < nb, s[0] + i, s[1] + i - nb), 0)

    return bm, nb, a_map, b_map, o_map


def project(idx, xa, xb, gain, ws, tabs, bufs, seq):
    rows, d = xa.shape
    bm, nb, a_map, b_map, o_map = two_source(rows)
    widths = [w.shape[1] // 4 for w in ws]
    in_specs = [pl.BlockSpec((bm, d), a_map), pl.BlockSpec((bm, d), b_map), pl.BlockSpec((1, d), first_row)]
    in_specs += [pl.BlockSpec((d, w), lambda i, s: (0, s[2])) for w in widths]
    in_specs += [pl.BlockSpec((bm, HEAD), o_map)] * 2
    args = [idx, xa, xb, gain, *ws, *tabs]
    aliases = {}
    if bufs is not None:
        in_specs += [ANY] * len(bufs)
        aliases = {len(args) + n: n for n in range(len(bufs))}
        args += list(bufs)
    return call(proj_body, (2 * nb,), in_specs, [pl.BlockSpec((bm, w), o_map) for w in (d, *widths, HEAD)],
                [sds(seq, w) for w in (d, *widths)] + [sds(seq, HEAD, F32)], args, 4 * rows * d * sum(widths),
                aliases=aliases)


def projc_body(s_ref, h_ref, *rest):
    qkv_of(h_ref[...], *rest)


def project_first(idx, h, ws, tabs, rows):
    d = h.shape[1]
    widths = [w.shape[1] // 4 for w in ws]
    return call(projc_body, (rows // BLK,),
                [pl.BlockSpec((BLK, d), row_map)] + [pl.BlockSpec((d, w), lambda i, s: (0, s[0])) for w in widths]
                + [pl.BlockSpec((BLK, HEAD), row_map)] * 2,
                [pl.BlockSpec((BLK, w), row_map) for w in widths], [sds(rows, w) for w in widths],
                [idx, h, *ws, *tabs], 2 * rows * d * sum(widths))


def dout_body(s_ref, da_ref, db_ref, wo_ref, *rest):
    dy_out, do_out = rest[-2:]
    half = pl.num_programs(0) // 2

    @pl.when(pl.program_id(0) < half)
    def _():
        dy_out[...] = da_ref[...]

    @pl.when(pl.program_id(0) >= half)
    def _():
        dy_out[...] = db_ref[...]

    do_out[...] = mm_nt(dy_out[...], wo_ref[...]).astype(BF)


def dout(idx, da, db, w_o, bufs, seq):
    rows, d = da.shape
    bm, nb, a_map, b_map, o_map = two_source(rows)
    oc = w_o.shape[0] // 4
    in_specs = [pl.BlockSpec((bm, d), a_map), pl.BlockSpec((bm, d), b_map),
                pl.BlockSpec((oc, d), lambda i, s: (s[2], 0))]
    args = [idx, da, db, w_o]
    aliases = {}
    if bufs is not None:
        in_specs += [ANY] * 2
        aliases = {len(args) + n: n for n in range(2)}
        args += list(bufs)
    return call(dout_body, (2 * nb,), in_specs, [pl.BlockSpec((bm, w), o_map) for w in (d, oc)],
                [sds(seq, w) for w in (d, oc)], args, 4 * rows * d * oc, aliases=aliases)


TASK = 4
HEADER = 3


def row_tasks(first, last):
    return [(i, i + 1, 1, -1) for i in range(first, last)]


def fwd_body(kind, s_ref, q_ref, k_ref, v_ref, *rest):
    qt, kk, vt, s_scr, acc, stat = rest[-6:]
    if kind == "rest":
        o1_ref, lse1_ref, st_ref, o_ref, lse_ref, hi_ref, pair_ref = rest[:7]
    else:
        o_ref, lse_ref = rest[:2]
    seq = k_ref.shape[0]

    def setup(c):
        sl = ds(c * BLK, BLK)
        vt[:, sl] = v_ref[sl, :].T
        kk[sl, :HEAD] = k_ref[sl, :]
        kk[sl, HEAD:] = k_ref[sl, :]
        for h in range(GROUP):
            qf = q_ref[sl, head_cols(h)].astype(F32) * SCALE2
            hi = qf.astype(BF)
            qt[h, :HEAD, sl] = hi.T
            qt[h, HEAD:, sl] = (qf - hi.astype(F32)).astype(BF).T

    loop(seq // BLK, setup)
    acc[...] = jnp.zeros_like(acc)
    stat[...] = jnp.zeros_like(stat)
    cur, old, den_row = 0, 1, 2
    if kind == "rest":
        @pl.when(s_ref[1] == 0)
        def _():
            o_ref[:seq // 2, :] = o1_ref[...]
            lse_ref[0, :, :seq // 2] = lse1_ref[0]

    def task(t):
        return [s_ref[HEADER + t * TASK + n] for n in range(TASK)]

    def stage_a(h, i, j, masked, init=None):
        row = one(h)
        if masked is True:
            top = mm(kk[ds(j * BLK, HB), :], qt[h, :, ds(i * BLK, BLK)])
            low = mm(kk[ds(j * BLK + HB, HB), :], qt[h, :, ds(i * BLK + HB, HB)])
            top = jnp.where(down(top.shape) <= across(top.shape), top, NEG_LARGE)
            low = jnp.where(down(low.shape) <= across(low.shape), low, NEG_LARGE)
            s_scr[h, :HB, :] = top
            s_scr[h, HB:, HB:] = low
            m_new = jnp.max(top, axis=0, keepdims=True)
            right = jnp.maximum(m_new[:, HB:], jnp.max(low, axis=0, keepdims=True))
            m_new = jnp.concatenate([m_new[:, :HB], right], axis=1)
        else:
            s = mm(kk[ds(j * BLK, BLK), :], qt[h, :, ds(i * BLK, BLK)])
            if masked is not False:
                keep = down(s.shape) <= across(s.shape)
                s = jnp.where(jnp.logical_or(keep, jnp.logical_not(masked)), s, NEG_LARGE)
            s_scr[h] = s
            m_new = jnp.max(s, axis=0, keepdims=True)
        if init is None:
            m_old = stat[cur, row]
        elif kind == "rest":
            m_old = jnp.where(init >= 0, lse1_ref[0, row, ds(jnp.maximum(init, 0) * BLK, BLK)], NEG_LARGE)
        else:
            m_old = jnp.full(m_new.shape, NEG_LARGE, F32)
        m_new = jnp.maximum(m_old, m_new)
        stat[old, row] = jnp.exp2(m_old - m_new)
        stat[cur, row] = m_new

    def stage_p(h, diag=False):
        row = one(h)
        m, alpha = stat[cur, row], stat[old, row]
        if diag:
            top = jnp.exp2(s_scr[h, :HB, :] - m)
            low = jnp.exp2(s_scr[h, HB:, HB:] - m[:, HB:])
            total = jnp.sum(top, axis=0, keepdims=True)
            right = total[:, HB:] + jnp.sum(low, axis=0, keepdims=True)
            total = jnp.concatenate([total[:, :HB], right], axis=1)
            top = top.astype(BF)
            p = (top[:, :HB], jnp.concatenate([top[:, HB:], low.astype(BF)], axis=0))
        else:
            p = jnp.exp2(s_scr[h] - m)
            total = jnp.sum(p, axis=0, keepdims=True)
            p = p.astype(BF)
        stat[den_row, row] = stat[den_row, row] * alpha + total
        return p, alpha

    def stage_v(h, j, held, diag=False):
        p, alpha = held
        if diag:
            acc[h, :, :HB] = acc[h, :, :HB] * alpha[:, :HB] + mm(vt[:, ds(j * BLK, HB)], p[0])
            acc[h, :, HB:] = acc[h, :, HB:] * alpha[:, HB:] + mm(vt[:, ds(j * BLK, BLK)], p[1])
        else:
            acc[h] = acc[h] * alpha + mm(vt[:, ds(j * BLK, BLK)], p)

    def finish(h, i, den, top):
        row = one(h)
        out = acc[h] / den
        o_ref[ds(i * BLK, BLK), head_cols(h)] = out.T.astype(BF)
        lse_ref[0, row, ds(i * BLK, BLK)] = top + jnp.log2(den)
        if kind == "local":
            rest[2][0, h, :, ds(i * BLK, BLK)] = out

    def pipeline(i, j, masked):
        for h in range(GROUP):
            held = stage_p(h)
            stage_a(h, i, j + 1, masked)
            stage_v(h, j, held)

    count = s_ref[HEADER - 1]
    i, steps, diag, init = task(0)
    for h in range(GROUP):
        stage_a(h, i, 0, jnp.logical_and(steps == 1, diag == 1), init)

    def row(t):
        i, steps, diag, _ = task(t)

        loop(steps - 2, lambda j: pipeline(i, j, False))

        pl.when(jnp.logical_and(steps > 1, diag == 1))(lambda: pipeline(i, steps - 2, True))
        if kind == "rest":
            pl.when(diag == 0)(lambda: pipeline(i, steps - 2, False))
        i2, _, _, init2 = task(jnp.minimum(t + 1, count - 1))

        def last_step(on_diag):
            for h in range(GROUP):
                held = stage_p(h, on_diag)
                final = (stat[den_row, one(h)], stat[cur, one(h)])
                stage_a(h, i2, 0, False, init2)
                stage_v(h, steps - 1, held, on_diag)
                finish(h, i, *final)

        if kind != "rest":
            last_step(True)
        else:
            pl.when(diag == 1)(lambda: last_step(True))
            pl.when(diag == 0)(lambda: last_step(False))

            @pl.when(init2 >= 0)
            def _():
                stat[den_row] = jnp.ones(stat.shape[1:], F32)
                for h in range(GROUP):
                    acc[h] = st_ref[0, h, :, ds(init2 * BLK, BLK)]

    loop(count, row)
    lse_ref[0, GROUP:, :] = jnp.zeros((8 - GROUP, seq), F32)
    if kind == "rest":
        hi_ref[...] = o_ref[seq - hi_ref.shape[0]:, :]
        pair_ref[...] = o_ref[ds(s_ref[0] * pair_ref.shape[0], pair_ref.shape[0]), :]


def attn_fwd(kind, idx, q, k, v, extra=(), local=()):
    whole = q.shape[0]
    seq = whole if kind == "rest" else whole // (2 if kind == "local" else 1)
    nkv = k.shape[1] // HEAD

    def half_map(g, s):
        return (s[1], g)

    def head_map(g, s):
        return (g, 0, 0)

    def state_map(g, s):
        return (g, 0, 0, 0)

    at = half_map if kind == "local" else col_map
    lse_spec = pl.BlockSpec((1, 8, seq), head_map)
    outs, specs = [sds(seq, q.shape[1]), jax.ShapeDtypeStruct((nkv, 8, seq), F32)], []
    out_specs = [pl.BlockSpec((seq, GW), col_map), lse_spec]
    state = pl.BlockSpec((1, GROUP, HEAD, whole // 2), state_map)
    if kind == "local":
        outs.append(jax.ShapeDtypeStruct((nkv, GROUP, HEAD, seq), F32))
        out_specs.append(state)
    if kind == "rest":
        specs = [pl.BlockSpec((seq // 2, GW), col_map), pl.BlockSpec((1, 8, seq // 2), head_map), state]
        outs += [sds(r, q.shape[1]) for r in extra]
        out_specs += [pl.BlockSpec((r, GW), col_map) for r in extra]
    kspec = pl.BlockSpec((seq, HEAD), at)
    return call(lambda *refs: fwd_body(kind, *refs), (nkv,), [pl.BlockSpec((seq, GW), at), kspec, kspec] + specs,
                out_specs, outs, [idx, q, k, v, *local], nkv * GROUP * seq * seq * PAIR,
                scratch=[pltpu.VMEM((GROUP, PAIR, seq), BF), pltpu.VMEM((seq, PAIR), BF),
                         pltpu.VMEM((HEAD, seq), BF), pltpu.VMEM((GROUP, BLK, BLK), F32),
                         pltpu.VMEM((GROUP, HEAD, BLK), F32), pltpu.VMEM((GROUP, 8, BLK), F32)])


def bwd_body(s_ref, q_ref, do_ref, o_ref, lse_ref, qn_ref, don_ref, on_ref, lsen_ref, k_ref, v_ref, cos_hbm, sin_hbm,
             out_ref, pair_ref, ka, va, dkt, dvt, tab, tab_sem, *sets):
    i = pl.program_id(0)
    last = pl.num_programs(0) - 1
    seq = k_ref.shape[0]
    m3 = GROUP * HB
    sets = (sets[:5], sets[5:])
    cos_ref, sin_ref = tab.at[0], tab.at[1]

    def spots():
        for b in range(2):
            for h in range(GROUP):
                start = (b * GROUP + h) * HB
                yield h, slice(b * HB, (b + 1) * HB), head_cols(h), slice(start, start + HB)

    def prepare(q_src, do_src, o_src, lse_src, dst):
        qa, da, q3t, do3t, dq3 = dst
        srow = down((16, HB))
        blank = jnp.zeros((HEAD - 16, HB), BF)
        for h, src, cols, rows in spots():
            qh, doh = q_src[src, cols], do_src[src, cols]
            qa[rows, :HEAD] = qh
            da[rows, :HEAD] = doh
            q3t[:, rows] = qh.T
            dt = doh.T
            do3t[:, rows] = dt
            delta = jnp.sum(dt.astype(F32) * o_src[src, cols].T.astype(F32), axis=0, keepdims=True)
            parts = jnp.zeros((16, HB), F32)
            for n, part in enumerate(split3(lse_src[0, one(h), src] * (1.0 / SCALE2)) + split3(delta)):
                parts = jnp.where(srow == n, part, parts)
            block = jnp.concatenate([parts.astype(BF), blank], axis=0).T
            qa[rows, HEAD:] = block
            da[rows, HEAD:] = block
        dq3[...] = jnp.zeros_like(dq3)

    @pl.when(i == 0)
    def _():
        copies = [pltpu.make_async_copy(src, tab.at[n], tab_sem.at[n]) for n, src in enumerate((cos_hbm, sin_hbm))]
        for copy in copies:
            copy.start()
        dkt[...] = jnp.zeros_like(dkt)
        dvt[...] = jnp.zeros_like(dvt)

        def setup(c):
            sl = ds(c * BLK, BLK)
            third = across((BLK, HEAD)) // 3
            for n, (src, dst) in enumerate(((k_ref, ka), (v_ref, va))):
                dst[sl, :HEAD] = src[sl, :]
                dst[sl, HEAD:] = jnp.where(third == n, -1.0, 0.0).astype(BF)

        loop(seq // BLK, setup)
        prepare(q_ref, do_ref, o_ref, lse_ref, sets[0])
        for copy in copies:
            copy.wait()

    def run(mine, other, tail_width):
        qa, da, q3t, do3t, dq3 = mine

        def step(rows, start, width, masked):
            sl = pl.ds(pl.multiple_of(start, BLK), width)
            s = mm_nt(qa[rows, :], ka[sl, :])
            dp = mm_nt(da[rows, :], va[sl, :])
            p = jnp.exp2(s * SCALE2)
            if masked:
                off = width - HB
                tail = p[:, off:]
                keep = down(tail.shape) % HB >= across(tail.shape)
                tail = jnp.where(keep, tail, 0.0)
                p = jnp.concatenate([p[:, :off], tail], axis=1) if off else tail
            dvt[:, sl] += mm(do3t[:, rows], p.astype(BF))
            dsv = (p * dp).astype(BF)
            dkt[:, sl] += mm(q3t[:, rows], dsv)
            dq3[rows, :] += mm(dsv, ka[sl, :HEAD])

        def body(t):
            step(slice(0, 2 * m3), t * 2 * BLK, 2 * BLK, False)

        loop(i // 2, body)
        start = (i // 2) * 2 * BLK
        step(slice(0, m3), start, tail_width - HB, True)
        prepare(qn_ref, don_ref, on_ref, lsen_ref, other)
        step(slice(m3, 2 * m3), start, tail_width, True)
        for h, src, cols, rows in spots():
            rsl = ds(i * BLK + src.start, HB)
            out_ref[rsl, cols] = rotate(dq3[rows, :] * SCALE, cos_ref[rsl, :], -sin_ref[rsl, :]).astype(BF)

    @pl.when(i % 2 == 0)
    def _():
        run(*sets, BLK)

    @pl.when(i % 2 == 1)
    def _():
        run(*sets[::-1], 2 * BLK)

    @pl.when(i == last)
    def _():
        def fin(c):
            sl = ds(c * 2 * BLK, 2 * BLK)
            out_ref[sl, GW:QK] = rotate(dkt[:, sl].T * SCALE, cos_ref[sl, :], -sin_ref[sl, :]).astype(BF)
            out_ref[sl, QK:] = dvt[:, sl].T.astype(BF)

        loop(seq // BLK // 2, fin)
        pair_ref[...] = out_ref[ds(s_ref[0] * pair_ref.shape[0], pair_ref.shape[0]), :]


def attn_bwd(idx, q, do, o, k, v, lse, tabs, rows):
    seq = k.shape[0]
    nq = seq // BLK
    m3 = GROUP * BLK
    kspec = pl.BlockSpec((seq, HEAD), lambda i, s: (0, s[1]))
    row_specs = []
    for ahead in range(2):
        row_specs += [pl.BlockSpec((BLK, GW), lambda i, s, a=ahead: (jnp.minimum(i + a, nq - 1), s[1]))] * 3
        row_specs += [pl.BlockSpec((1, 8, BLK), lambda i, s, a=ahead: (s[1], 0, jnp.minimum(i + a, nq - 1)))]
    one_set = [pltpu.VMEM((m3, PAIR), BF)] * 2 + [pltpu.VMEM((HEAD, m3), BF)] * 2 + [pltpu.VMEM((m3, HEAD), F32)]
    return call(bwd_body, (nq,),
                row_specs + [kspec] * 2 + [ANY] * 2,
                [pl.BlockSpec((r, PW), first_row) for r in (seq, rows)], [sds(r, PW) for r in (seq, rows)],
                [idx] + [q, do, o, lse] * 2 + [k, v, *tabs], GROUP * nq * (nq + 1) * BLK * BLK * PW,
                scratch=[pltpu.VMEM((seq, PAIR), BF)] * 2 + [pltpu.VMEM((HEAD, seq), F32)] * 2
                + [pltpu.VMEM((2, seq, HEAD), F32), pltpu.SemaphoreType.DMA((2,))] + one_set * 2)


def out_body(s_ref, x_ref, *rest):
    ops, weights, out_ref = rest[:4], rest[4:8], rest[8]
    lhs = jnp.concatenate([r[...] for r in ops], axis=1)
    rhs = jnp.concatenate([r[...] for r in weights], axis=0)
    out_ref[...] = (x_ref[...].astype(F32) + mm(lhs, rhs)).astype(BF)


def out_proj(idx, x, pieces, w_o):
    def chip_map(n, s):
        return (s[0] % 2, 0)

    rows, d = x.shape
    hw = pieces[0].shape[1]
    return call(out_body, (d // BLK,),
                [pl.BlockSpec((rows, BLK), col_map)]
                + [pl.BlockSpec((rows, hw), m) for m in (own_map, first_row, chip_map, first_row)]
                + [pl.BlockSpec((hw, BLK), lambda n, s, p=p: (s[p], n)) for p in range(4)],
                pl.BlockSpec((rows, BLK), col_map), sds(rows, d), [idx, x, *pieces] + [w_o] * 4,
                2 * rows * d * d)


def dwo_body(s_ref, oa_ref, ob_ref, oc_ref, dy_ref, fin, snd, ot):
    first, hw = ob_ref.shape

    @pl.when(jnp.logical_and(pl.program_id(0) == 0, pl.program_id(1) == 0))
    def _():
        for src, rows, base in ((oa_ref, slice(0, hw), 0), (ob_ref, slice(hw, 2 * hw), 0), (oc_ref, slice(hw, 2 * hw), first)):
            def tr(c):
                ot[rows, ds(c * BLK + base, BLK)] = src[ds(c * BLK, BLK), :].T

            loop(src.shape[0] // BLK, tr)

    val = mm(ot[ds(pl.program_id(1) * hw, hw), :], dy_ref[...])
    fin[...] = val
    snd[...] = val


def dw_o(idx, oa, ob, oc, dy):
    seq, d = dy.shape
    hw = oa.shape[1]
    o_specs = [pl.BlockSpec(o.shape, lambda i, p, s: (0, 0), pipeline_mode=pl.Buffered(1)) for o in (oa, ob, oc)]
    return call(dwo_body, (d // BLK, 2),
                o_specs + [pl.BlockSpec((seq, BLK), lambda i, p, s: (0, i))],
                [pl.BlockSpec((hw, BLK), lambda i, p, s: (s[p], i)), pl.BlockSpec((hw, BLK), lambda i, p, s: (p, i))],
                [sds(4 * hw, d, F32), sds(2 * hw, d, F32)], [idx, oa, ob, oc, dy], 4 * seq * d * hw,
                scratch=[pltpu.VMEM((2 * hw, seq), BF)])


def dwown_body(s_ref, h_ref, ga_ref, gb_ref, gc_ref, wo_ref, _, fq, fk, fv, snd, wo_fin, g3, ht, sem, wsem):
    i, steps = pl.program_id(0), pl.num_programs(0)
    rows, per = wo_ref.shape[0], steps // 2
    start = jnp.where(i < per, s_ref[1] * per + i, s_ref[3] * per + i - per)
    wcopy = pltpu.make_async_copy(wo_ref, wo_fin.at[ds(start * rows, rows), :], wsem)
    wcopy.start()

    @pl.when(i > 1)
    def _():
        for copy in scatter(snd, (fq, fk, fv), s_ref[0], s_ref[2], sem.at[i % 2]):
            copy.wait()

    ht[...] = h_ref[...].T
    lhs = ht[...]
    for g, q_at, k_at in ((ga_ref, 0, 2 * GW), (gb_ref, GW, 2 * GW + HEAD), (gc_ref, 2 * PW, 2 * PW + GW)):
        val = mm(lhs, g[:, :QK])
        snd[:, q_at:q_at + GW] = val[:, :GW]
        snd[:, k_at:k_at + HEAD] = val[:, GW:]
    snd[:, 2 * QK:2 * PW] = mm(lhs, jnp.concatenate([ga_ref[:, QK:], gb_ref[:, QK:]], axis=1))
    for copy in scatter(snd, (fq, fk, fv), s_ref[0], s_ref[2], sem.at[i % 2]):
        copy.start()

    @pl.when(i == steps - 1)
    def _():
        g3[...] = gc_ref[ds(s_ref[1] * g3.shape[0], g3.shape[0]), :]
        for slot in range(2):
            for copy in scatter(snd, (fq, fk, fv), s_ref[0], s_ref[2], sem.at[slot]):
                copy.wait()

    wcopy.wait()


def scatter(rcv, outs, whole_dev, part_dev, sem):
    rows, src, copies = ds(pl.program_id(0) * rcv.shape[0], rcv.shape[0]), 0, []
    fq, fk, fv = outs
    for n, (out, col, w) in enumerate(((fq, whole_dev, 2 * GW), (fk, whole_dev, PAIR), (fv, whole_dev, PAIR),
                                       (fq, 2 * part_dev, GW), (fk, 2 * part_dev, HEAD))):
        copies.append(pltpu.make_async_copy(rcv.at[:, src:src + w], out.at[rows, ds(col * w, w)], sem.at[n]))
        src += w
    return copies


def dw_own(idx, h, ga, gb, gc, wo_rcv, wo_fin):
    seq, d = h.shape
    steps = d // HB
    gspec = pl.BlockSpec((seq, PW), first_row, pipeline_mode=pl.Buffered(1))
    widths = (2 * GW, PAIR, PAIR)
    sw = 2 * PW + QK
    return call(dwown_body, (steps,),
                [pl.BlockSpec((seq, HB), col_map)] + [gspec] * 3
                + [pl.BlockSpec((wo_rcv.shape[0] // steps, d), row_map), ANY],
                [ANY] * 3 + [pl.BlockSpec((HB, sw), row_map), ANY, pl.BlockSpec((seq // 4, PW), first_row)],
                [sds(d, 4 * w, F32) for w in widths] + [sds(d, sw, F32), sds(*wo_fin.shape, F32), sds(seq // 4, PW)],
                [idx, h, ga, gb, gc, wo_rcv, wo_fin], 2 * seq * d * sw,
                scratch=[pltpu.VMEM((HB, seq), BF), pltpu.SemaphoreType.DMA((2, 5)), pltpu.SemaphoreType.DMA],
                aliases={6: 4})


def dwgrp_body(s_ref, h_ref, ga_ref, gb_ref, *rest):
    fq, fk, fv, snd, ht = rest[-5:]
    ht[...] = h_ref[...].T
    lhs = ht[...]
    val = mm(lhs, gb_ref[:, :QK])
    fq[...] = val[:, :GW]
    fk[...] = val[:, GW:]
    snd[:, :QK] = val
    val = mm(lhs, jnp.concatenate([ga_ref[...], gb_ref[:, QK:]], axis=1))
    fv[...] = val
    snd[:, QK:] = val


def group_specs(bm):
    return [pl.BlockSpec((bm, w), lambda i, s: (i, 2 * s[0] + 1)) for w in (GW, HEAD)] + \
        [pl.BlockSpec((bm, PAIR), lambda i, s: (i, s[0]))]


def dw_group(idx, h, ga, gb, bufs):
    seq, d = h.shape
    gspec = pl.BlockSpec((seq, PW), first_row, pipeline_mode=pl.Buffered(1))
    sw = QK + PAIR
    return call(dwgrp_body, (d // HB,),
                [pl.BlockSpec((seq, HB), col_map),
                 pl.BlockSpec((seq, HEAD), lambda i, s: (0, QK // HEAD), pipeline_mode=pl.Buffered(1)), gspec] + [ANY] * 3,
                group_specs(HB) + [pl.BlockSpec((HB, sw), row_map)], [sds(*b.shape, F32) for b in bufs] + [sds(d, sw, F32)],
                [idx, h, ga, gb, *bufs], 2 * seq * d * sw, scratch=[pltpu.VMEM((HB, seq), BF)],
                aliases={4 + n: n for n in range(3)})


def place_body(s_ref, rcv, *rest):
    q_out, k_out, v_out = rest[-3:]
    q_out[...] = rcv[:, :GW]
    k_out[...] = rcv[:, GW:QK]
    v_out[...] = rcv[:, QK:]


def place(idx, rcv, bufs):
    d, w = rcv.shape
    bm = 2 * BLK
    return call(place_body, (d // bm,), [pl.BlockSpec((bm, w), row_map)] + [ANY] * 3, group_specs(bm),
                [sds(*b.shape, F32) for b in bufs], [idx, rcv, *bufs], d * w, aliases={2 + n: n for n in range(3)})


def dx_body(s_ref, x_ref, dy_ref, gain_ref, inv_ref, *rest):
    pieces, weights, rcv = rest[:8], rest[8:20], rest[20]
    dx_ref, dg_ref, fq, fk, fv, acc, xs, tot, sem = rest[-9:]
    n = pl.program_id(0)
    bn = x_ref.shape[1]
    rows, d = acc.shape
    copies = scatter(rcv, (fq, fk, fv), s_ref[1], s_ref[3], sem)
    for copy in copies:
        copy.start()

    @pl.when(n == 0)
    def _():
        tot[...] = jnp.zeros_like(tot)

    cuts = (slice(0, GW), slice(GW, QK), slice(QK, PW))
    lhs = jnp.concatenate([pieces[2 * p + g][:, c] for p in range(4) for c in cuts for g in range(2)], axis=1)
    rhs = jnp.concatenate([r[...] for r in weights], axis=1)
    dh = mm_nt(lhs, rhs)
    inv = inv_ref[...]
    for c in range(bn // HEAD):
        cols = head_cols(c)
        xb = x_ref[:, cols]
        xs[:, ds(n * bn + cols.start, HEAD)] = xb
        part, xf = dh[:, cols], xb.astype(F32)
        scaled = part * gain_ref[:, cols]
        tot[...] += scaled * xf
        acc[:, ds(n * bn + cols.start, HEAD)] = dy_ref[:, cols].astype(F32) + inv * scaled
        dg_ref[:, cols] = jnp.sum((part * (xf * inv)).reshape(rows // 8, 8, HEAD), axis=0)

    @pl.when(n == pl.num_programs(0) - 1)
    def _():
        step = HEAD // 2

        def stats(r):
            sl = ds(r * step, step)
            inv = inv_ref[sl, :]
            tot[sl, :] = jnp.broadcast_to(jnp.sum(tot[sl, :], axis=-1, keepdims=True) / d, (step, HEAD)) * inv * inv * inv

        loop(rows // step, stats)

        def epi(r):
            sl = ds(r * step, step)
            coef = tot[sl, :]
            for c in range(d // HEAD):
                cols = head_cols(c)
                dx_ref[sl, cols] = (acc[sl, cols] - xs[sl, cols].astype(F32) * coef).astype(BF)

        loop(rows // step, epi)

    for copy in copies:
        copy.wait()


def dx_call(idx, x, dy, gain, inv, pieces, ws, rcv, bufs):
    rows, d = x.shape
    bn = HB
    once = pl.Buffered(1)
    maps = (own_map, own_map, first_row, first_row) * 2
    return call(dx_body, (d // bn,),
                [pl.BlockSpec((rows, bn), col_map)] * 2 + [pl.BlockSpec((1, bn), col_map), pl.BlockSpec((rows, HEAD), own_map)]
                + [pl.BlockSpec((rows, PW), m, pipeline_mode=once) for m in maps]
                + [pl.BlockSpec((bn, w.shape[1] // 4), lambda n, s, p=p: (n, s[p])) for p in range(4) for w in ws]
                + [pl.BlockSpec((bn, rcv.shape[1]), row_map)] + [ANY] * 3,
                [pl.BlockSpec((rows, d), first_row, pipeline_mode=once), pl.BlockSpec((8, bn), col_map)] + [ANY] * 3,
                [sds(rows, d), sds(8, d, F32)] + [sds(*b.shape, F32) for b in bufs],
                [idx, x, dy, gain, inv, *pieces] + list(ws) * 4 + [rcv, *bufs], 16 * rows * d * PW,
                scratch=[pltpu.VMEM((rows, d), F32), pltpu.VMEM((rows, d), BF), pltpu.VMEM((rows, HEAD), F32),
                         pltpu.SemaphoreType.DMA((5,))],
                aliases={26 + n: 2 + n for n in range(3)})


def solution(mesh):
    sp = mesh.shape['sp']
    cross = [(a, a ^ 2) for a in range(sp)]
    pair = [(a, a ^ 1) for a in range(sp)]

    def over(val):
        return lax.ppermute(val, 'sp', cross)

    def near(val):
        return lax.ppermute(val, 'sp', pair)

    def after(val, *deps):
        return lax.optimization_barrier((val,) + deps)[0]

    def vec(*vals, dep=()):
        out = jnp.stack([jnp.asarray(v, jnp.int32) for v in vals])
        return after(out, *dep) if dep else out

    def step(x, dy, positions, gain, w_q, w_k, w_v, w_o):
        j = lax.axis_index('sp').astype(jnp.int32)
        rows, d = x.shape
        seq = rows * sp
        j1, j2, j3 = [j ^ n for n in (1, 2, 3)]
        dev = (j, j1, j2, j3)
        bpr, hpr = rows // BLK, rows // HB
        ws = (w_q, w_k, w_v)

        def rows_of(val, blk):
            return lax.dynamic_slice_in_dim(val, blk * rows, rows, 0)

        gain_f = gain.astype(F32).reshape(1, d)

        cut = rows - HB
        xa = x[:cut]
        positions = after(positions, xa)
        pos2 = over(positions)
        pos1 = near(positions)
        x2a = over(xa)
        x2b = over(after(x, xa)[cut:])
        x1 = near(x)
        pos3 = near(pos2)
        dy1 = near(after(dy, x1))

        pos = jnp.zeros((seq,), jnp.int32)
        for blk, val in zip(dev, (positions, pos1, pos2, pos3)):
            pos = lax.dynamic_update_slice(pos, val, (blk * rows,))
        inv_freq = ROPE_THETA ** (-jnp.arange(0, HEAD, 2).astype(F32) / HEAD)
        angles = pos.astype(F32)[:, None] * inv_freq[None, :]
        cos_h, sin_h = jnp.cos(angles), jnp.sin(angles)
        tabs = (jnp.concatenate([cos_h, cos_h], axis=1), jnp.concatenate([-sin_h, sin_h], axis=1))

        dya, dyb = dy[:cut], dy[cut:]
        bufs = project(vec(j * bpr, j1 * bpr, j, dep=(dya, dyb)), x, x1, gain_f, ws, tabs, None, seq)
        dbufs = dout(vec(j * bpr, j1 * bpr, j, dep=(bufs[1],)), dy, dy1, w_o, None, seq)

        chip, nh = j // 2, seq // BLK // 2
        tri = row_tasks(0, nh)
        first = seq // 2 - BLK
        square = [(i + nh, nh, 0, i) for i in range(nh)]

        def table(head, tasks):
            return jnp.concatenate([vec(*head, len(tasks)), jnp.asarray(tasks, jnp.int32).reshape(-1)])

        local = attn_fwd("local", after(table((j1, chip), tri), dbufs[1]), *bufs[1:4])
        rest_tasks = jnp.where(chip == 0, table((j1, 0), row_tasks(nh, 2 * nh) * 2).at[HEADER - 1].set(nh),
                               table((j1, 1), tri + square))

        x2a = after(x2a, local[0])
        dy2a = over(after(dya, x2a))
        x3a = near(x2a)
        bufs = project(vec(j2 * hpr, j3 * hpr, j), x2a, x3a, gain_f, ws, tabs, bufs, seq)
        x2b = after(x2b, bufs[1])
        dy2b = over(after(dyb, x2b))
        x3b = near(x2b)
        bufs = project(vec((j2 + 1) * hpr - 1, (j3 + 1) * hpr - 1, j), x2b, x3b, gain_f, ws, tabs, bufs, seq)
        h_all, q, k, v, inv = bufs
        o, lse, o_hi, o_pair = attn_fwd("rest", rest_tasks, q, k, v, (seq - first, rows), local)
        orv = over(o_hi)
        o1 = near(o_pair)
        qc, kc, vc = project_first(vec(j2, dep=(o,)), h_all, ws, tabs, first)
        dy2a = after(dy2a, qc)
        dy3a = near(dy2a)
        oc = attn_fwd("first", table((j1, 0), tri[:-1]), qc, kc, vc)[0]

        dbufs = dout(vec(j2 * hpr, j3 * hpr, j, dep=(oc,)), dy2a, dy3a, w_o, dbufs, seq)
        dy2b = after(dy2b, dbufs[1])
        dy3b = near(dy2b)
        dbufs = dout(vec((j2 + 1) * hpr - 1, (j3 + 1) * hpr - 1, j), dy2b, dy3b, w_o, dbufs, seq)
        dy_all, do = dbufs

        ga, ga_pair = attn_bwd(vec(j1, 0), q, do, o, k, v, lse, tabs, rows)
        ga2 = over(ga)
        ga1 = near(ga_pair)
        gb, gb_pair = attn_bwd(vec(j1, 1, dep=(ga,)), q, do, o, k, v, lse, tabs, rows)
        gb2 = over(gb)
        gb1 = near(gb_pair)

        orv = after(orv, gb)
        ox = jnp.where(chip == 0, jnp.concatenate([oc, orv[:BLK]]), orv[BLK:])
        o3 = near(rows_of(ox, j1 % 2))
        wo_fin, wo_snd = dw_o(vec(j, j2, dep=(gb,)), o, oc, orv, dy_all)
        wo_rcv = near(wo_snd)
        result = out_proj(vec(*dev, dep=(wo_snd,)), x, (o, o1, ox, o3), w_o)
        ga2 = after(ga2, wo_snd)
        fq, fk, fv, snd, wo_fin, g3 = dw_own(vec(*dev, dep=(result,)), h_all, ga, gb, ga2, wo_rcv, wo_fin)
        rcv = near(snd)
        ga3 = near(g3)

        gb2 = after(gb2, snd)
        gb3 = near(rows_of(gb2, j1))
        fq, fk, fv, snd_b = dw_group(vec(j2), h_all, ga2, gb2, (fq, fk, fv))
        rcv_b = near(snd_b)
        grad_x, dg, fq, fk, fv = dx_call(vec(*dev, dep=(snd_b,)), x, dy, gain_f, inv,
                                         (ga, gb, ga1, gb1, ga2, gb2, ga3, gb3), ws, rcv, (fq, fk, fv))
        dg = jnp.sum(dg, axis=0)
        dg = dg + near(dg)
        dg = dg + over(dg)
        fq, fk, fv = place(vec(j3), rcv_b, (fq, fk, fv))
        return result, grad_x, fq, fk, fv, wo_fin, dg

    seq_spec = P(('dp', 'sp'), None)
    whole = P(None, None)
    part_rows = P('dp', None)
    return jax.shard_map(step, mesh=mesh,
                         in_specs=(seq_spec, seq_spec, P(('dp', 'sp')), P(None), whole, whole, whole, whole),
                         out_specs=(seq_spec, seq_spec, part_rows, part_rows, part_rows, part_rows, P('dp')),
                         check_vma=False)
```

```python
import math

import jax
import jax.numpy as jnp
from jax import lax
from jax.experimental import pallas as pl
from jax.experimental.pallas import tpu as pltpu
from jax.sharding import PartitionSpec as P


HEAD = 128
GROUP = 3
GW = GROUP * HEAD
QK = GW + HEAD
PW = QK + HEAD
PAIR = 2 * HEAD
ROPE_THETA = 1000000.0
NORM_EPS = 1e-05
NEG_LARGE = -1e30
BF = jnp.bfloat16
F32 = jnp.float32
SCALE = HEAD ** -0.5
SCALE2 = SCALE * math.log2(math.e)
BLK = 512
HB = BLK // 2
VMEM_LIMIT = 62 * 1024 * 1024
ANY = pl.BlockSpec(memory_space=pl.ANY)


def first_row(i, s):
    return (0, 0)


def row_map(i, s):
    return (i, 0)


def col_map(i, s):
    return (0, i)


def own_map(i, s):
    return (s[0], 0)


def sds(rows, cols, dtype=BF):
    return jax.ShapeDtypeStruct((rows, cols), dtype)


def call(body, grid, in_specs, out_specs, out_shape, args, flops, scratch=(), aliases=None):
    return pl.pallas_call(
        body,
        grid_spec=pltpu.PrefetchScalarGridSpec(
            num_scalar_prefetch=1, grid=grid, in_specs=in_specs, out_specs=out_specs, scratch_shapes=list(scratch)),
        out_shape=out_shape, input_output_aliases=aliases or {},
        compiler_params=pltpu.CompilerParams(dimension_semantics=("arbitrary",) * len(grid),
                                             vmem_limit_bytes=VMEM_LIMIT),
        cost_estimate=pl.CostEstimate(flops=int(flops), bytes_accessed=int(flops) // BLK,
                                      transcendentals=0))(*args)


def down(shape):
    return lax.broadcasted_iota(jnp.int32, shape, 0)


def across(shape):
    return lax.broadcasted_iota(jnp.int32, shape, 1)


def loop(count, body):
    def run(c, _):
        body(c)
        return 0

    lax.fori_loop(0, count, run, 0)


def one(h):
    return slice(h, h + 1)


def head_cols(h):
    return slice(h * HEAD, h * HEAD + HEAD)


def mm(a, b):
    return jnp.dot(a, b, preferred_element_type=F32)


def mm_nt(a, b):
    return lax.dot_general(a, b, (((1,), (1,)), ((), ())), preferred_element_type=F32)


def rotate(val, cos_t, sin_t):
    return val * cos_t + pltpu.roll(val, HEAD // 2, 1) * sin_t


def ds(start, size):
    return pl.ds(pl.multiple_of(start, size), size)


def split3(val):
    hi = val.astype(BF).astype(F32)
    mid = (val - hi).astype(BF).astype(F32)
    return hi, mid, val - hi - mid


def qkv_of(h, wq_ref, wk_ref, wv_ref, cos_ref, sin_ref, q_ref, k_ref, v_ref):
    cos_t, sin_t = cos_ref[...], sin_ref[...]
    out = mm(h, wq_ref[...])
    for c in range(wq_ref.shape[1] // HEAD):
        sl = head_cols(c)
        q_ref[:, sl] = rotate(out[:, sl], cos_t, sin_t).astype(BF)
    out = mm(h, jnp.concatenate([wk_ref[...], wv_ref[...]], axis=1))
    for sl in (slice(0, HEAD), slice(HEAD, PAIR)):
        k_ref[:, sl] = rotate(out[:, sl], cos_t, sin_t).astype(BF)
    v_ref[...] = out[:, PAIR:].astype(BF)


def proj_body(s_ref, xa_ref, xb_ref, gain_ref, wq_ref, wk_ref, wv_ref, cos_ref, sin_ref, *rest):
    h_ref, q_ref, k_ref, v_ref, inv_ref = rest[-5:]
    half = pl.num_programs(0) // 2

    def norm(src):
        step = HEAD

        def stats(c):
            sl = ds(c * step, step)
            xf = src[sl, :].astype(F32)
            inv = lax.rsqrt(jnp.mean(xf * xf, axis=-1, keepdims=True) + NORM_EPS)
            inv_ref[sl, :] = jnp.broadcast_to(inv, (step, HEAD))

        def scale(c):
            sl = ds(c * step, step)
            inv, gain = inv_ref[sl, :], gain_ref[...]
            for n in range(src.shape[1] // HEAD):
                cols = head_cols(n)
                h_ref[sl, cols] = (src[sl, cols].astype(F32) * inv * gain[:, cols]).astype(BF)

        loop(src.shape[0] // step, stats)
        loop(src.shape[0] // step, scale)

    @pl.when(pl.program_id(0) < half)
    def _():
        norm(xa_ref)

    @pl.when(pl.program_id(0) >= half)
    def _():
        norm(xb_ref)

    qkv_of(h_ref[...], wq_ref, wk_ref, wv_ref, cos_ref, sin_ref, q_ref, k_ref, v_ref)


def two_source(rows):
    bm = HB if rows % BLK else BLK
    nb = rows // bm

    def a_map(i, s):
        return (jnp.minimum(i, nb - 1), 0)

    def b_map(i, s):
        return (jnp.maximum(i - nb, 0), 0)

    def o_map(i, s):
        return (jnp.where(i < nb, s[0] + i, s[1] + i - nb), 0)

    return bm, nb, a_map, b_map, o_map


def project(idx, xa, xb, gain, ws, tabs, bufs, seq):
    rows, d = xa.shape
    bm, nb, a_map, b_map, o_map = two_source(rows)
    widths = [w.shape[1] // 4 for w in ws]
    in_specs = [pl.BlockSpec((bm, d), a_map), pl.BlockSpec((bm, d), b_map), pl.BlockSpec((1, d), first_row)]
    in_specs += [pl.BlockSpec((d, w), lambda i, s: (0, s[2])) for w in widths]
    in_specs += [pl.BlockSpec((bm, HEAD), o_map)] * 2
    args = [idx, xa, xb, gain, *ws, *tabs]
    aliases = {}
    if bufs is not None:
        in_specs += [ANY] * len(bufs)
        aliases = {len(args) + n: n for n in range(len(bufs))}
        args += list(bufs)
    return call(proj_body, (2 * nb,), in_specs, [pl.BlockSpec((bm, w), o_map) for w in (d, *widths, HEAD)],
                [sds(seq, w) for w in (d, *widths)] + [sds(seq, HEAD, F32)], args, 4 * rows * d * sum(widths),
                aliases=aliases)


def projc_body(s_ref, h_ref, *rest):
    qkv_of(h_ref[...], *rest)


def project_first(idx, h, ws, tabs, rows):
    seq, d = h.shape
    widths = [w.shape[1] // 4 for w in ws]
    return call(projc_body, (rows // BLK,),
                [pl.BlockSpec((BLK, d), row_map)] + [pl.BlockSpec((d, w), lambda i, s: (0, s[0])) for w in widths]
                + [pl.BlockSpec((BLK, HEAD), row_map)] * 2,
                [pl.BlockSpec((BLK, w), row_map) for w in widths], [sds(seq, w) for w in widths],
                [idx, h, *ws, *tabs], 2 * rows * d * sum(widths))


def dout_body(s_ref, da_ref, db_ref, wo_ref, *rest):
    dy_out, do_out = rest[-2:]
    half = pl.num_programs(0) // 2

    @pl.when(pl.program_id(0) < half)
    def _():
        dy_out[...] = da_ref[...]

    @pl.when(pl.program_id(0) >= half)
    def _():
        dy_out[...] = db_ref[...]

    do_out[...] = mm_nt(dy_out[...], wo_ref[...]).astype(BF)


def dout(idx, da, db, w_o, bufs, seq):
    rows, d = da.shape
    bm, nb, a_map, b_map, o_map = two_source(rows)
    oc = w_o.shape[0] // 4
    in_specs = [pl.BlockSpec((bm, d), a_map), pl.BlockSpec((bm, d), b_map),
                pl.BlockSpec((oc, d), lambda i, s: (s[2], 0))]
    args = [idx, da, db, w_o]
    aliases = {}
    if bufs is not None:
        in_specs += [ANY] * 2
        aliases = {len(args) + n: n for n in range(2)}
        args += list(bufs)
    return call(dout_body, (2 * nb,), in_specs, [pl.BlockSpec((bm, w), o_map) for w in (d, oc)],
                [sds(seq, w) for w in (d, oc)], args, 4 * rows * d * oc, aliases=aliases)


TASK = 4
HEADER = 3


def row_tasks(first, last):
    return [(i, i + 1, 1, -1) for i in range(first, last)]


def fwd_body(kind, s_ref, q_ref, k_ref, v_ref, *rest):
    qt, kk, vt, s_scr, acc, stat = rest[-6:]
    if kind == "rest":
        o1_ref, lse1_ref, st_ref, o_ref, lse_ref, hi_ref, pair_ref = rest[:7]
    else:
        o_ref, lse_ref = rest[:2]
    seq = k_ref.shape[0]

    def setup(c):
        sl = ds(c * BLK, BLK)
        vt[:, sl] = v_ref[sl, :].T
        kk[sl, :HEAD] = k_ref[sl, :]
        kk[sl, HEAD:] = k_ref[sl, :]
        for h in range(GROUP):
            qf = q_ref[sl, head_cols(h)].astype(F32) * SCALE2
            hi = qf.astype(BF)
            qt[h, :HEAD, sl] = hi.T
            qt[h, HEAD:, sl] = (qf - hi.astype(F32)).astype(BF).T

    loop(seq // BLK, setup)
    acc[...] = jnp.zeros_like(acc)
    stat[...] = jnp.zeros_like(stat)
    cur, old, den_row = 0, 1, 2
    if kind == "rest":
        @pl.when(s_ref[1] == 0)
        def _():
            o_ref[:seq // 2, :] = o1_ref[...]
            lse_ref[0, :, :seq // 2] = lse1_ref[0]

    def task(t):
        return [s_ref[HEADER + t * TASK + n] for n in range(TASK)]

    def stage_a(h, i, j, masked, init=None):
        row = one(h)
        if masked is True:
            top = mm(kk[ds(j * BLK, HB), :], qt[h, :, ds(i * BLK, BLK)])
            low = mm(kk[ds(j * BLK + HB, HB), :], qt[h, :, ds(i * BLK + HB, HB)])
            top = jnp.where(down(top.shape) <= across(top.shape), top, NEG_LARGE)
            low = jnp.where(down(low.shape) <= across(low.shape), low, NEG_LARGE)
            s_scr[h, :HB, :] = top
            s_scr[h, HB:, HB:] = low
            m_new = jnp.max(top, axis=0, keepdims=True)
            right = jnp.maximum(m_new[:, HB:], jnp.max(low, axis=0, keepdims=True))
            m_new = jnp.concatenate([m_new[:, :HB], right], axis=1)
        else:
            s = mm(kk[ds(j * BLK, BLK), :], qt[h, :, ds(i * BLK, BLK)])
            if masked is not False:
                keep = down(s.shape) <= across(s.shape)
                s = jnp.where(jnp.logical_or(keep, jnp.logical_not(masked)), s, NEG_LARGE)
            s_scr[h] = s
            m_new = jnp.max(s, axis=0, keepdims=True)
        if init is None:
            m_old = stat[cur, row]
        elif kind == "rest":
            m_old = jnp.where(init >= 0, lse1_ref[0, row, ds(jnp.maximum(init, 0) * BLK, BLK)], NEG_LARGE)
        else:
            m_old = jnp.full(m_new.shape, NEG_LARGE, F32)
        m_new = jnp.maximum(m_old, m_new)
        stat[old, row] = jnp.exp2(m_old - m_new)
        stat[cur, row] = m_new

    def stage_p(h, diag=False):
        row = one(h)
        m, alpha = stat[cur, row], stat[old, row]
        if diag:
            top = jnp.exp2(s_scr[h, :HB, :] - m)
            low = jnp.exp2(s_scr[h, HB:, HB:] - m[:, HB:])
            total = jnp.sum(top, axis=0, keepdims=True)
            right = total[:, HB:] + jnp.sum(low, axis=0, keepdims=True)
            total = jnp.concatenate([total[:, :HB], right], axis=1)
            top = top.astype(BF)
            p = (top[:, :HB], jnp.concatenate([top[:, HB:], low.astype(BF)], axis=0))
        else:
            p = jnp.exp2(s_scr[h] - m)
            total = jnp.sum(p, axis=0, keepdims=True)
            p = p.astype(BF)
        stat[den_row, row] = stat[den_row, row] * alpha + total
        return p, alpha

    def stage_v(h, j, held, diag=False):
        p, alpha = held
        if diag:
            acc[h, :, :HB] = acc[h, :, :HB] * alpha[:, :HB] + mm(vt[:, ds(j * BLK, HB)], p[0])
            acc[h, :, HB:] = acc[h, :, HB:] * alpha[:, HB:] + mm(vt[:, ds(j * BLK, BLK)], p[1])
        else:
            acc[h] = acc[h] * alpha + mm(vt[:, ds(j * BLK, BLK)], p)

    def finish(h, i, den, top):
        row = one(h)
        out = acc[h] / den
        o_ref[ds(i * BLK, BLK), head_cols(h)] = out.T.astype(BF)
        lse_ref[0, row, ds(i * BLK, BLK)] = top + jnp.log2(den)
        if kind == "local":
            rest[2][0, h, :, ds(i * BLK, BLK)] = out

    def pipeline(i, j, masked):
        for h in range(GROUP):
            held = stage_p(h)
            stage_a(h, i, j + 1, masked)
            stage_v(h, j, held)

    count = s_ref[HEADER - 1]
    i, steps, diag, init = task(0)
    for h in range(GROUP):
        stage_a(h, i, 0, jnp.logical_and(steps == 1, diag == 1), init)

    def row(t):
        i, steps, diag, _ = task(t)

        loop(steps - 2, lambda j: pipeline(i, j, False))

        pl.when(jnp.logical_and(steps > 1, diag == 1))(lambda: pipeline(i, steps - 2, True))
        if kind == "rest":
            pl.when(diag == 0)(lambda: pipeline(i, steps - 2, False))
        i2, _, _, init2 = task(jnp.minimum(t + 1, count - 1))

        def last_step(on_diag):
            for h in range(GROUP):
                held = stage_p(h, on_diag)
                final = (stat[den_row, one(h)], stat[cur, one(h)])
                stage_a(h, i2, 0, False, init2)
                stage_v(h, steps - 1, held, on_diag)
                finish(h, i, *final)

        if kind != "rest":
            last_step(True)
        else:
            pl.when(diag == 1)(lambda: last_step(True))
            pl.when(diag == 0)(lambda: last_step(False))

            @pl.when(init2 >= 0)
            def _():
                stat[den_row] = jnp.ones(stat.shape[1:], F32)
                for h in range(GROUP):
                    acc[h] = st_ref[0, h, :, ds(init2 * BLK, BLK)]

    loop(count, row)
    lse_ref[0, GROUP:, :] = jnp.zeros((8 - GROUP, seq), F32)
    if kind == "rest":
        hi_ref[...] = o_ref[seq - hi_ref.shape[0]:, :]
        pair_ref[...] = o_ref[ds(s_ref[0] * pair_ref.shape[0], pair_ref.shape[0]), :]


def attn_fwd(kind, idx, q, k, v, extra=(), local=()):
    whole = q.shape[0]
    seq = whole if kind == "rest" else whole // 2
    nkv = k.shape[1] // HEAD

    def half_map(g, s):
        return (s[1], g)

    def head_map(g, s):
        return (g, 0, 0)

    def state_map(g, s):
        return (g, 0, 0, 0)

    at = half_map if kind == "local" else col_map
    lse_spec = pl.BlockSpec((1, 8, seq), head_map)
    outs, specs = [sds(seq, q.shape[1]), jax.ShapeDtypeStruct((nkv, 8, seq), F32)], []
    out_specs = [pl.BlockSpec((seq, GW), col_map), lse_spec]
    state = pl.BlockSpec((1, GROUP, HEAD, whole // 2), state_map)
    if kind == "local":
        outs.append(jax.ShapeDtypeStruct((nkv, GROUP, HEAD, seq), F32))
        out_specs.append(state)
    if kind == "rest":
        specs = [pl.BlockSpec((seq // 2, GW), col_map), pl.BlockSpec((1, 8, seq // 2), head_map), state]
        outs += [sds(r, q.shape[1]) for r in extra]
        out_specs += [pl.BlockSpec((r, GW), col_map) for r in extra]
    kspec = pl.BlockSpec((seq, HEAD), at)
    return call(lambda *refs: fwd_body(kind, *refs), (nkv,), [pl.BlockSpec((seq, GW), at), kspec, kspec] + specs,
                out_specs, outs, [idx, q, k, v, *local], nkv * GROUP * seq * seq * PAIR,
                scratch=[pltpu.VMEM((GROUP, PAIR, seq), BF), pltpu.VMEM((seq, PAIR), BF),
                         pltpu.VMEM((HEAD, seq), BF), pltpu.VMEM((GROUP, BLK, BLK), F32),
                         pltpu.VMEM((GROUP, HEAD, BLK), F32), pltpu.VMEM((GROUP, 8, BLK), F32)])


def bwd_body(s_ref, q_ref, do_ref, o_ref, lse_ref, qn_ref, don_ref, on_ref, lsen_ref, k_ref, v_ref, cos_hbm, sin_hbm,
             out_ref, pair_ref, ka, va, dkt, dvt, tab, tab_sem, *sets):
    i = pl.program_id(0)
    last = pl.num_programs(0) - 1
    seq = k_ref.shape[0]
    m3 = GROUP * HB
    cos_ref, sin_ref = tab.at[0], tab.at[1]

    def spots():
        for b in range(2):
            for h in range(GROUP):
                start = (b * GROUP + h) * HB
                yield h, slice(b * HB, (b + 1) * HB), head_cols(h), slice(start, start + HB)

    def pick(n):
        return [ref.at[n] for ref in sets]

    def prepare(q_src, do_src, o_src, lse_src, dst):
        qa, da, q3t, do3t, dq3 = dst
        srow = down((16, HB))
        blank = jnp.zeros((HEAD - 16, HB), BF)
        for h, src, cols, rows in spots():
            qh, doh = q_src[src, cols], do_src[src, cols]
            qa[rows, :HEAD] = qh
            da[rows, :HEAD] = doh
            q3t[:, rows] = qh.T
            dt = doh.T
            do3t[:, rows] = dt
            delta = jnp.sum(dt.astype(F32) * o_src[src, cols].T.astype(F32), axis=0, keepdims=True)
            parts = jnp.zeros((16, HB), F32)
            for n, part in enumerate(split3(lse_src[0, one(h), src] * (1.0 / SCALE2)) + split3(delta)):
                parts = jnp.where(srow == n, part, parts)
            block = jnp.concatenate([parts.astype(BF), blank], axis=0).T
            qa[rows, HEAD:] = block
            da[rows, HEAD:] = block
        dq3[...] = jnp.zeros_like(dq3)

    @pl.when(i == 0)
    def _():
        copies = [pltpu.make_async_copy(src, tab.at[n], tab_sem.at[n]) for n, src in enumerate((cos_hbm, sin_hbm))]
        for copy in copies:
            copy.start()
        dkt[...] = jnp.zeros_like(dkt)
        dvt[...] = jnp.zeros_like(dvt)

        def setup(c):
            sl = ds(c * BLK, BLK)
            third = across((BLK, HEAD)) // 3
            for n, (src, dst) in enumerate(((k_ref, ka), (v_ref, va))):
                dst[sl, :HEAD] = src[sl, :]
                dst[sl, HEAD:] = jnp.where(third == n, -1.0, 0.0).astype(BF)

        loop(seq // BLK, setup)
        prepare(q_ref, do_ref, o_ref, lse_ref, pick(0))
        for copy in copies:
            copy.wait()

    def step(mine, rows, start, width, masked):
        qa, da, q3t, do3t, dq3 = mine
        sl = pl.ds(pl.multiple_of(start, BLK), width)
        s = mm_nt(qa[rows, :], ka[sl, :])
        dp = mm_nt(da[rows, :], va[sl, :])
        p = jnp.exp2(s * SCALE2)
        if masked:
            off = width - HB
            tail = p[:, off:]
            keep = down(tail.shape) % HB >= across(tail.shape)
            tail = jnp.where(keep, tail, 0.0)
            p = jnp.concatenate([p[:, :off], tail], axis=1) if off else tail
        dvt[:, sl] += mm(do3t[:, rows], p.astype(BF))
        dsv = (p * dp).astype(BF)
        dkt[:, sl] += mm(q3t[:, rows], dsv)
        dq3[rows, :] += mm(dsv, ka[sl, :HEAD])

    par, start = i % 2, (i // 2) * 2 * BLK
    loop(i // 2, lambda t: step(pick(par), slice(0, 2 * m3), t * 2 * BLK, 2 * BLK, False))

    def tail_steps(n):
        mine, width = pick(n), (n + 1) * BLK
        step(mine, slice(0, m3), start, width - HB, True)
        prepare(qn_ref, don_ref, on_ref, lsen_ref, pick(1 - n))
        step(mine, slice(m3, 2 * m3), start, width, True)
        for h, src, cols, rows in spots():
            rsl = ds(i * BLK + src.start, HB)
            out_ref[rsl, cols] = rotate(mine[-1][rows, :] * SCALE, cos_ref[rsl, :], -sin_ref[rsl, :]).astype(BF)

    pl.when(par == 0)(lambda: tail_steps(0))
    pl.when(par == 1)(lambda: tail_steps(1))

    @pl.when(i == last)
    def _():
        def fin(c):
            sl = ds(c * 2 * BLK, 2 * BLK)
            out_ref[sl, GW:QK] = rotate(dkt[:, sl].T * SCALE, cos_ref[sl, :], -sin_ref[sl, :]).astype(BF)
            out_ref[sl, QK:] = dvt[:, sl].T.astype(BF)

        loop(seq // BLK // 2, fin)
        pair_ref[...] = out_ref[ds(s_ref[0] * pair_ref.shape[0], pair_ref.shape[0]), :]


def attn_bwd(idx, q, do, o, k, v, lse, tabs, rows):
    seq = k.shape[0]
    nq = seq // BLK
    m3 = GROUP * BLK
    kspec = pl.BlockSpec((seq, HEAD), lambda i, s: (0, s[1]))
    row_specs = []
    for ahead in range(2):
        row_specs += [pl.BlockSpec((BLK, GW), lambda i, s, a=ahead: (jnp.minimum(i + a, nq - 1), s[1]))] * 3
        row_specs += [pl.BlockSpec((1, 8, BLK), lambda i, s, a=ahead: (s[1], 0, jnp.minimum(i + a, nq - 1)))]
    two_sets = [pltpu.VMEM((2, m3, PAIR), BF)] * 2 + [pltpu.VMEM((2, HEAD, m3), BF)] * 2 + [pltpu.VMEM((2, m3, HEAD), F32)]
    return call(bwd_body, (nq,),
                row_specs + [kspec] * 2 + [ANY] * 2,
                [pl.BlockSpec((r, PW), first_row) for r in (seq, rows)], [sds(r, PW) for r in (seq, rows)],
                [idx] + [q, do, o, lse] * 2 + [k, v, *tabs], GROUP * nq * (nq + 1) * BLK * BLK * PW,
                scratch=[pltpu.VMEM((seq, PAIR), BF)] * 2 + [pltpu.VMEM((HEAD, seq), F32)] * 2
                + [pltpu.VMEM((2, seq, HEAD), F32), pltpu.SemaphoreType.DMA((2,))] + two_sets)


def out_body(s_ref, x_ref, *rest):
    ops, weights, out_ref = rest[:4], rest[4:8], rest[8]
    lhs = jnp.concatenate([r[...] for r in ops], axis=1)
    rhs = jnp.concatenate([r[...] for r in weights], axis=0)
    out_ref[...] = (x_ref[...].astype(F32) + mm(lhs, rhs)).astype(BF)


def out_proj(idx, x, pieces, w_o):
    def chip_map(n, s):
        return (s[0] % 2, 0)

    rows, d = x.shape
    hw = pieces[0].shape[1]
    return call(out_body, (d // BLK,),
                [pl.BlockSpec((rows, BLK), col_map)]
                + [pl.BlockSpec((rows, hw), m) for m in (own_map, first_row, chip_map, first_row)]
                + [pl.BlockSpec((hw, BLK), lambda n, s, p=p: (s[p], n)) for p in range(4)],
                pl.BlockSpec((rows, BLK), col_map), sds(rows, d), [idx, x, *pieces] + [w_o] * 4,
                2 * rows * d * d)


def dwo_body(s_ref, oa_ref, ob_ref, oc_ref, dy_ref, fin, snd, ot):
    first, hw = ob_ref.shape

    @pl.when(jnp.logical_and(pl.program_id(0) == 0, pl.program_id(1) == 0))
    def _():
        for src, rows, base in ((oa_ref, slice(0, hw), 0), (ob_ref, slice(hw, 2 * hw), 0), (oc_ref, slice(hw, 2 * hw), first)):
            def tr(c):
                ot[rows, ds(c * BLK + base, BLK)] = src[ds(c * BLK, BLK), :].T

            loop(src.shape[0] // BLK, tr)

    val = mm(ot[ds(pl.program_id(1) * hw, hw), :], dy_ref[...])
    fin[...] = val
    snd[...] = val


def dw_o(idx, oa, ob, oc, dy):
    seq, d = dy.shape
    hw = oa.shape[1]
    o_specs = [pl.BlockSpec((r, hw), lambda i, p, s: (0, 0), pipeline_mode=pl.Buffered(1))
               for r in (seq, seq - oc.shape[0], oc.shape[0])]
    return call(dwo_body, (d // BLK, 2),
                o_specs + [pl.BlockSpec((seq, BLK), lambda i, p, s: (0, i))],
                [pl.BlockSpec((hw, BLK), lambda i, p, s: (s[p], i)), pl.BlockSpec((hw, BLK), lambda i, p, s: (p, i))],
                [sds(4 * hw, d, F32), sds(2 * hw, d, F32)], [idx, oa, ob, oc, dy], 4 * seq * d * hw,
                scratch=[pltpu.VMEM((2 * hw, seq), BF)])


def dwown_body(s_ref, h_ref, ga_ref, gb_ref, gc_ref, wo_ref, _, fq, fk, fv, snd, wo_fin, g3, ht, sem, wsem):
    i, steps = pl.program_id(0), pl.num_programs(0)
    rows, per = wo_ref.shape[0], steps // 2
    start = jnp.where(i < per, s_ref[1] * per + i, s_ref[3] * per + i - per)
    wcopy = pltpu.make_async_copy(wo_ref, wo_fin.at[ds(start * rows, rows), :], wsem)
    wcopy.start()

    @pl.when(i > 1)
    def _():
        for copy in scatter(snd, (fq, fk, fv), s_ref[0], s_ref[2], sem.at[i % 2]):
            copy.wait()

    ht[...] = h_ref[...].T
    lhs = ht[...]
    for g, q_at, k_at in ((ga_ref, 0, 2 * GW), (gb_ref, GW, 2 * GW + HEAD), (gc_ref, 2 * PW, 2 * PW + GW)):
        val = mm(lhs, g[:, :QK])
        snd[:, q_at:q_at + GW] = val[:, :GW]
        snd[:, k_at:k_at + HEAD] = val[:, GW:]
    snd[:, 2 * QK:2 * PW] = mm(lhs, jnp.concatenate([ga_ref[:, QK:], gb_ref[:, QK:]], axis=1))
    for copy in scatter(snd, (fq, fk, fv), s_ref[0], s_ref[2], sem.at[i % 2]):
        copy.start()

    @pl.when(i == steps - 1)
    def _():
        g3[...] = gc_ref[ds(s_ref[1] * g3.shape[0], g3.shape[0]), :]
        for slot in range(2):
            for copy in scatter(snd, (fq, fk, fv), s_ref[0], s_ref[2], sem.at[slot]):
                copy.wait()

    wcopy.wait()


def scatter(rcv, outs, whole_dev, part_dev, sem):
    rows, src, copies = ds(pl.program_id(0) * rcv.shape[0], rcv.shape[0]), 0, []
    fq, fk, fv = outs
    for n, (out, col, w) in enumerate(((fq, whole_dev, 2 * GW), (fk, whole_dev, PAIR), (fv, whole_dev, PAIR),
                                       (fq, 2 * part_dev, GW), (fk, 2 * part_dev, HEAD))):
        copies.append(pltpu.make_async_copy(rcv.at[:, src:src + w], out.at[rows, ds(col * w, w)], sem.at[n]))
        src += w
    return copies


def dw_own(idx, h, ga, gb, gc, wo_rcv, wo_fin):
    seq, d = h.shape
    steps = d // HB
    gspec = pl.BlockSpec((seq, PW), first_row, pipeline_mode=pl.Buffered(1))
    widths = (2 * GW, PAIR, PAIR)
    sw = 2 * PW + QK
    return call(dwown_body, (steps,),
                [pl.BlockSpec((seq, HB), col_map)] + [gspec] * 3
                + [pl.BlockSpec((wo_rcv.shape[0] // steps, d), row_map), ANY],
                [ANY] * 3 + [pl.BlockSpec((HB, sw), row_map), ANY, pl.BlockSpec((seq // 4, PW), first_row)],
                [sds(d, 4 * w, F32) for w in widths] + [sds(d, sw, F32), sds(*wo_fin.shape, F32), sds(seq // 4, PW)],
                [idx, h, ga, gb, gc, wo_rcv, wo_fin], 2 * seq * d * sw,
                scratch=[pltpu.VMEM((HB, seq), BF), pltpu.SemaphoreType.DMA((2, 5)), pltpu.SemaphoreType.DMA],
                aliases={6: 4})


def dwgrp_body(s_ref, h_ref, ga_ref, gb_ref, *rest):
    fq, fk, fv, snd, ht = rest[-5:]
    ht[...] = h_ref[...].T
    lhs = ht[...]
    val = mm(lhs, gb_ref[:, :QK])
    fq[...] = val[:, :GW]
    fk[...] = val[:, GW:]
    snd[:, :QK] = val
    val = mm(lhs, jnp.concatenate([ga_ref[...], gb_ref[:, QK:]], axis=1))
    fv[...] = val
    snd[:, QK:] = val


def group_specs(bm):
    return [pl.BlockSpec((bm, w), lambda i, s: (i, 2 * s[0] + 1)) for w in (GW, HEAD)] + \
        [pl.BlockSpec((bm, PAIR), lambda i, s: (i, s[0]))]


def dw_group(idx, h, ga, gb, bufs):
    seq, d = h.shape
    gspec = pl.BlockSpec((seq, PW), first_row, pipeline_mode=pl.Buffered(1))
    sw = QK + PAIR
    return call(dwgrp_body, (d // HB,),
                [pl.BlockSpec((seq, HB), col_map),
                 pl.BlockSpec((seq, HEAD), lambda i, s: (0, QK // HEAD), pipeline_mode=pl.Buffered(1)), gspec] + [ANY] * 3,
                group_specs(HB) + [pl.BlockSpec((HB, sw), row_map)], [sds(*b.shape, F32) for b in bufs] + [sds(d, sw, F32)],
                [idx, h, ga, gb, *bufs], 2 * seq * d * sw, scratch=[pltpu.VMEM((HB, seq), BF)],
                aliases={4 + n: n for n in range(3)})


def place_body(s_ref, rcv, *rest):
    q_out, k_out, v_out = rest[-3:]
    q_out[...] = rcv[:, :GW]
    k_out[...] = rcv[:, GW:QK]
    v_out[...] = rcv[:, QK:]


def place(idx, rcv, bufs):
    d, w = rcv.shape
    bm = 2 * BLK
    return call(place_body, (d // bm,), [pl.BlockSpec((bm, w), row_map)] + [ANY] * 3, group_specs(bm),
                [sds(*b.shape, F32) for b in bufs], [idx, rcv, *bufs], d * w, aliases={2 + n: n for n in range(3)})


def dx_body(s_ref, x_ref, dy_ref, gain_ref, inv_ref, *rest):
    pieces, weights, rcv = rest[:8], rest[8:20], rest[20]
    dx_ref, dg_ref, fq, fk, fv, acc, xs, tot, sem = rest[-9:]
    n = pl.program_id(0)
    bn = x_ref.shape[1]
    rows, d = acc.shape
    copies = scatter(rcv, (fq, fk, fv), s_ref[1], s_ref[3], sem)
    for copy in copies:
        copy.start()

    @pl.when(n == 0)
    def _():
        tot[...] = jnp.zeros_like(tot)

    cuts = (slice(0, GW), slice(GW, QK), slice(QK, PW))
    lhs = jnp.concatenate([pieces[2 * p + g][:, c] for p in range(4) for c in cuts for g in range(2)], axis=1)
    rhs = jnp.concatenate([r[...] for r in weights], axis=1)
    dh = mm_nt(lhs, rhs)
    inv = inv_ref[...]
    for c in range(bn // HEAD):
        cols = head_cols(c)
        xb = x_ref[:, cols]
        xs[:, ds(n * bn + cols.start, HEAD)] = xb
        part, xf = dh[:, cols], xb.astype(F32)
        scaled = part * gain_ref[:, cols]
        tot[...] += scaled * xf
        acc[:, ds(n * bn + cols.start, HEAD)] = dy_ref[:, cols].astype(F32) + inv * scaled
        dg_ref[:, cols] = jnp.sum((part * (xf * inv)).reshape(rows // 8, 8, HEAD), axis=0)

    @pl.when(n == pl.num_programs(0) - 1)
    def _():
        step = HEAD // 2

        def stats(r):
            sl = ds(r * step, step)
            inv = inv_ref[sl, :]
            tot[sl, :] = jnp.broadcast_to(jnp.sum(tot[sl, :], axis=-1, keepdims=True) / d, (step, HEAD)) * inv * inv * inv

        loop(rows // step, stats)

        def epi(r):
            sl = ds(r * step, step)
            coef = tot[sl, :]
            for c in range(d // HEAD):
                cols = head_cols(c)
                dx_ref[sl, cols] = (acc[sl, cols] - xs[sl, cols].astype(F32) * coef).astype(BF)

        loop(rows // step, epi)

    for copy in copies:
        copy.wait()


def dx_call(idx, x, dy, gain, inv, pieces, ws, rcv, bufs):
    rows, d = x.shape
    bn = HB
    once = pl.Buffered(1)
    maps = (own_map, own_map, first_row, first_row) * 2
    return call(dx_body, (d // bn,),
                [pl.BlockSpec((rows, bn), col_map)] * 2 + [pl.BlockSpec((1, bn), col_map), pl.BlockSpec((rows, HEAD), own_map)]
                + [pl.BlockSpec((rows, PW), m, pipeline_mode=once) for m in maps]
                + [pl.BlockSpec((bn, w.shape[1] // 4), lambda n, s, p=p: (n, s[p])) for p in range(4) for w in ws]
                + [pl.BlockSpec((bn, rcv.shape[1]), row_map)] + [ANY] * 3,
                [pl.BlockSpec((rows, d), first_row, pipeline_mode=once), pl.BlockSpec((8, bn), col_map)] + [ANY] * 3,
                [sds(rows, d), sds(8, d, F32)] + [sds(*b.shape, F32) for b in bufs],
                [idx, x, dy, gain, inv, *pieces] + list(ws) * 4 + [rcv, *bufs], 16 * rows * d * PW,
                scratch=[pltpu.VMEM((rows, d), F32), pltpu.VMEM((rows, d), BF), pltpu.VMEM((rows, HEAD), F32),
                         pltpu.SemaphoreType.DMA((5,))],
                aliases={26 + n: 2 + n for n in range(3)})


def solution(mesh):
    sp = mesh.shape['sp']
    cross = [(a, a ^ 2) for a in range(sp)]
    pair = [(a, a ^ 1) for a in range(sp)]

    def over(val):
        return lax.ppermute(val, 'sp', cross)

    def near(val):
        return lax.ppermute(val, 'sp', pair)

    def after(val, *deps):
        return lax.optimization_barrier((val,) + deps)[0]

    def vec(*vals, dep=()):
        out = jnp.stack([jnp.asarray(v, jnp.int32) for v in vals])
        return after(out, *dep) if dep else out

    def step(x, dy, positions, gain, w_q, w_k, w_v, w_o):
        j = lax.axis_index('sp').astype(jnp.int32)
        rows, d = x.shape
        seq = rows * sp
        j1, j2, j3 = [j ^ n for n in (1, 2, 3)]
        dev = (j, j1, j2, j3)
        bpr, hpr = rows // BLK, rows // HB
        ws = (w_q, w_k, w_v)

        def rows_of(val, blk):
            return lax.dynamic_slice_in_dim(val, blk * rows, rows, 0)

        gain_f = gain.astype(F32).reshape(1, d)

        cut = rows - HB
        xa = x[:cut]
        positions = after(positions, xa)
        pos2 = over(positions)
        pos1 = near(positions)
        x2a = over(xa)
        x2b = over(after(x, xa)[cut:])
        x1 = near(x)
        pos3 = near(pos2)
        dy1 = near(after(dy, x1))

        pos = jnp.zeros((seq,), jnp.int32)
        for blk, val in zip(dev, (positions, pos1, pos2, pos3)):
            pos = lax.dynamic_update_slice(pos, val, (blk * rows,))
        inv_freq = ROPE_THETA ** (-jnp.arange(0, HEAD, 2).astype(F32) / HEAD)
        angles = pos.astype(F32)[:, None] * inv_freq[None, :]
        cos_h, sin_h = jnp.cos(angles), jnp.sin(angles)
        tabs = (jnp.concatenate([cos_h, cos_h], axis=1), jnp.concatenate([-sin_h, sin_h], axis=1))

        dya, dyb = dy[:cut], dy[cut:]
        bufs = project(vec(j * bpr, j1 * bpr, j, dep=(dya, dyb)), x, x1, gain_f, ws, tabs, None, seq)
        dbufs = dout(vec(j * bpr, j1 * bpr, j, dep=(bufs[1],)), dy, dy1, w_o, None, seq)

        chip, nh = j // 2, seq // BLK // 2
        tri = row_tasks(0, nh)
        first = seq // 2 - BLK
        square = [(i + nh, nh, 0, i) for i in range(nh)]

        def table(head, tasks):
            return jnp.concatenate([vec(*head, len(tasks)), jnp.asarray(tasks, jnp.int32).reshape(-1)])

        c_tasks = table((j1, 0), tri).at[HEADER - 1].set(nh - 1)
        local = attn_fwd("local", after(table((j1, chip), tri), dbufs[1]), *bufs[1:4])
        rest_tasks = jnp.where(chip == 0, table((j1, 0), row_tasks(nh, 2 * nh) * 2).at[HEADER - 1].set(nh),
                               table((j1, 1), tri + square))

        x2a = after(x2a, local[0])
        dy2a = over(after(dya, x2a))
        x3a = near(x2a)
        bufs = project(vec(j2 * hpr, j3 * hpr, j), x2a, x3a, gain_f, ws, tabs, bufs, seq)
        x2b = after(x2b, bufs[1])
        dy2b = over(after(dyb, x2b))
        x3b = near(x2b)
        bufs = project(vec((j2 + 1) * hpr - 1, (j3 + 1) * hpr - 1, j), x2b, x3b, gain_f, ws, tabs, bufs, seq)
        h_all, q, k, v, inv = bufs
        o, lse, o_hi, o_pair = attn_fwd("rest", rest_tasks, q, k, v, (seq - first, rows), local)
        orv = over(o_hi)
        o1 = near(o_pair)
        qc, kc, vc = project_first(vec(j2, dep=(o,)), h_all, ws, tabs, first)
        dy2a = after(dy2a, qc)
        dy3a = near(dy2a)
        oc = attn_fwd("local", c_tasks, qc, kc, vc)[0]

        dbufs = dout(vec(j2 * hpr, j3 * hpr, j, dep=(oc,)), dy2a, dy3a, w_o, dbufs, seq)
        dy2b = after(dy2b, dbufs[1])
        dy3b = near(dy2b)
        dbufs = dout(vec((j2 + 1) * hpr - 1, (j3 + 1) * hpr - 1, j), dy2b, dy3b, w_o, dbufs, seq)
        dy_all, do = dbufs

        ga, ga_pair = attn_bwd(vec(j1, 0), q, do, o, k, v, lse, tabs, rows)
        ga2 = over(ga)
        ga1 = near(ga_pair)
        gb, gb_pair = attn_bwd(vec(j1, 1, dep=(ga,)), q, do, o, k, v, lse, tabs, rows)
        gb2 = over(gb)
        gb1 = near(gb_pair)

        orv = after(orv, gb)
        ox = jnp.where(chip == 0, jnp.concatenate([oc[:first], orv[:BLK]]), orv[BLK:])
        o3 = near(rows_of(ox, j1 % 2))
        wo_fin, wo_snd = dw_o(vec(j, j2, dep=(gb,)), o, oc, orv, dy_all)
        wo_rcv = near(wo_snd)
        result = out_proj(vec(*dev, dep=(wo_snd,)), x, (o, o1, ox, o3), w_o)
        ga2 = after(ga2, wo_snd)
        fq, fk, fv, snd, wo_fin, g3 = dw_own(vec(*dev, dep=(result,)), h_all, ga, gb, ga2, wo_rcv, wo_fin)
        rcv = near(snd)
        ga3 = near(g3)

        gb2 = after(gb2, snd)
        gb3 = near(rows_of(gb2, j1))
        fq, fk, fv, snd_b = dw_group(vec(j2), h_all, ga2, gb2, (fq, fk, fv))
        rcv_b = near(snd_b)
        grad_x, dg, fq, fk, fv = dx_call(vec(*dev, dep=(snd_b,)), x, dy, gain_f, inv,
                                         (ga, gb, ga1, gb1, ga2, gb2, ga3, gb3), ws, rcv, (fq, fk, fv))
        dg = jnp.sum(dg, axis=0)
        dg = dg + near(dg)
        dg = dg + over(dg)
        fq, fk, fv = place(vec(j3), rcv_b, (fq, fk, fv))
        return result, grad_x, fq, fk, fv, wo_fin, dg

    seq_spec = P(('dp', 'sp'), None)
    whole = P(None, None)
    part_rows = P('dp', None)
    return jax.shard_map(step, mesh=mesh,
                         in_specs=(seq_spec, seq_spec, P(('dp', 'sp')), P(None), whole, whole, whole, whole),
                         out_specs=(seq_spec, seq_spec, part_rows, part_rows, part_rows, part_rows, P('dp')),
                         check_vma=False)
```

```python
import math

import jax
import jax.numpy as jnp
from jax import lax
from jax.experimental import pallas as pl
from jax.experimental.pallas import tpu as pltpu
from jax.sharding import PartitionSpec as P


HEAD = 128
GROUP = 3
GW = GROUP * HEAD
QK = GW + HEAD
PW = QK + HEAD
PAIR = 2 * HEAD
ROPE_THETA = 1000000.0
NORM_EPS = 1e-05
NEG_LARGE = -1e30
BF = jnp.bfloat16
F32 = jnp.float32
SCALE = HEAD ** -0.5
SCALE2 = SCALE * math.log2(math.e)
BLK = 512
HB = BLK // 2
VMEM_LIMIT = 65011712
ANY = pl.BlockSpec(memory_space=pl.ANY)


def first_row(i, s):
    return (0, 0)


def row_map(i, s):
    return (i, 0)


def col_map(i, s):
    return (0, i)


def own_map(i, s):
    return (s[0], 0)


def sds(rows, cols, dtype=BF):
    return jax.ShapeDtypeStruct((rows, cols), dtype)


def call(body, grid, in_specs, out_specs, out_shape, args, flops, scratch=(), aliases=None):
    return pl.pallas_call(
        body,
        grid_spec=pltpu.PrefetchScalarGridSpec(
            num_scalar_prefetch=1, grid=grid, in_specs=in_specs, out_specs=out_specs, scratch_shapes=list(scratch)),
        out_shape=out_shape, input_output_aliases=aliases or {},
        compiler_params=pltpu.CompilerParams(dimension_semantics=("arbitrary",) * len(grid),
                                             vmem_limit_bytes=VMEM_LIMIT),
        cost_estimate=pl.CostEstimate(flops=int(flops), bytes_accessed=int(flops) // BLK,
                                      transcendentals=0))(*args)


def down(shape):
    return lax.broadcasted_iota(jnp.int32, shape, 0)


def across(shape):
    return lax.broadcasted_iota(jnp.int32, shape, 1)


def loop(count, body):
    def run(c, _):
        body(c)
        return 0

    lax.fori_loop(0, count, run, 0)


def one(h):
    return slice(h, h + 1)


def head_cols(h):
    return slice(h * HEAD, h * HEAD + HEAD)


def mm(a, b):
    return jnp.dot(a, b, preferred_element_type=F32)


def mm_nt(a, b):
    return lax.dot_general(a, b, (((1,), (1,)), ((), ())), preferred_element_type=F32)


def rotate(val, cos_t, sin_t):
    return val * cos_t + pltpu.roll(val, HEAD // 2, 1) * sin_t


def ds(start, size):
    return pl.ds(pl.multiple_of(start, size), size)


def split3(val):
    hi = val.astype(BF).astype(F32)
    mid = (val - hi).astype(BF).astype(F32)
    return hi, mid, val - hi - mid


def qkv_of(h, wq_ref, wk_ref, wv_ref, cos_ref, sin_ref, q_ref, k_ref, v_ref):
    cos_t, sin_t = cos_ref[...], sin_ref[...]
    out = mm(h, wq_ref[...])
    for c in range(wq_ref.shape[1] // HEAD):
        sl = head_cols(c)
        q_ref[:, sl] = rotate(out[:, sl], cos_t, sin_t).astype(BF)
    out = mm(h, jnp.concatenate([wk_ref[...], wv_ref[...]], axis=1))
    for sl in (slice(0, HEAD), slice(HEAD, PAIR)):
        k_ref[:, sl] = rotate(out[:, sl], cos_t, sin_t).astype(BF)
    v_ref[...] = out[:, PAIR:].astype(BF)


def proj_body(s_ref, xa_ref, xb_ref, gain_ref, wq_ref, wk_ref, wv_ref, cos_ref, sin_ref, *rest):
    h_ref, q_ref, k_ref, v_ref, inv_ref = rest[-5:]
    half = pl.num_programs(0) // 2

    def norm(src):
        step = HEAD

        def stats(c):
            sl = ds(c * step, step)
            xf = src[sl, :].astype(F32)
            inv = lax.rsqrt(jnp.mean(xf * xf, axis=-1, keepdims=True) + NORM_EPS)
            inv_ref[sl, :] = jnp.broadcast_to(inv, (step, HEAD))

        def scale(c):
            sl = ds(c * step, step)
            inv, gain = inv_ref[sl, :], gain_ref[...]
            for n in range(src.shape[1] // HEAD):
                cols = head_cols(n)
                h_ref[sl, cols] = (src[sl, cols].astype(F32) * inv * gain[:, cols]).astype(BF)

        loop(src.shape[0] // step, stats)
        loop(src.shape[0] // step, scale)

    @pl.when(pl.program_id(0) < half)
    def _():
        norm(xa_ref)

    @pl.when(pl.program_id(0) >= half)
    def _():
        norm(xb_ref)

    qkv_of(h_ref[...], wq_ref, wk_ref, wv_ref, cos_ref, sin_ref, q_ref, k_ref, v_ref)


def two_source(rows):
    bm = HB if rows % BLK else BLK
    nb = rows // bm

    def a_map(i, s):
        return (jnp.minimum(i, nb - 1), 0)

    def b_map(i, s):
        return (jnp.maximum(i - nb, 0), 0)

    def o_map(i, s):
        return (jnp.where(i < nb, s[0] + i, s[1] + i - nb), 0)

    return bm, nb, a_map, b_map, o_map


def project(idx, xa, xb, gain, ws, tabs, bufs, seq):
    rows, d = xa.shape
    bm, nb, a_map, b_map, o_map = two_source(rows)
    widths = [w.shape[1] // 4 for w in ws]
    in_specs = [pl.BlockSpec((bm, d), a_map), pl.BlockSpec((bm, d), b_map), pl.BlockSpec((1, d), first_row)]
    in_specs += [pl.BlockSpec((d, w), lambda i, s: (0, s[2])) for w in widths]
    in_specs += [pl.BlockSpec((bm, HEAD), o_map)] * 2
    args = [idx, xa, xb, gain, *ws, *tabs]
    aliases = {}
    if bufs is not None:
        in_specs += [ANY] * len(bufs)
        aliases = {len(args) + n: n for n in range(len(bufs))}
        args += list(bufs)
    return call(proj_body, (2 * nb,), in_specs, [pl.BlockSpec((bm, w), o_map) for w in (d, *widths, HEAD)],
                [sds(seq, w) for w in (d, *widths)] + [sds(seq, HEAD, F32)], args, 4 * rows * d * sum(widths),
                aliases=aliases)


def projc_body(s_ref, h_ref, *rest):
    qkv_of(h_ref[...], *rest)


def project_first(idx, h, ws, tabs, rows):
    seq, d = h.shape
    widths = [w.shape[1] // 4 for w in ws]
    return call(projc_body, (rows // BLK,),
                [pl.BlockSpec((BLK, d), row_map)] + [pl.BlockSpec((d, w), lambda i, s: (0, s[0])) for w in widths]
                + [pl.BlockSpec((BLK, HEAD), row_map)] * 2,
                [pl.BlockSpec((BLK, w), row_map) for w in widths], [sds(seq, w) for w in widths],
                [idx, h, *ws, *tabs], 2 * rows * d * sum(widths))


def dout_body(s_ref, da_ref, db_ref, wo_ref, *rest):
    dy_out, do_out = rest[-2:]
    half = pl.num_programs(0) // 2

    @pl.when(pl.program_id(0) < half)
    def _():
        dy_out[...] = da_ref[...]

    @pl.when(pl.program_id(0) >= half)
    def _():
        dy_out[...] = db_ref[...]

    do_out[...] = mm_nt(dy_out[...], wo_ref[...]).astype(BF)


def dout(idx, da, db, w_o, bufs, seq):
    rows, d = da.shape
    bm, nb, a_map, b_map, o_map = two_source(rows)
    oc = w_o.shape[0] // 4
    in_specs = [pl.BlockSpec((bm, d), a_map), pl.BlockSpec((bm, d), b_map),
                pl.BlockSpec((oc, d), lambda i, s: (s[2], 0))]
    args = [idx, da, db, w_o]
    aliases = {}
    if bufs is not None:
        in_specs += [ANY] * 2
        aliases = {len(args) + n: n for n in range(2)}
        args += list(bufs)
    return call(dout_body, (2 * nb,), in_specs, [pl.BlockSpec((bm, w), o_map) for w in (d, oc)],
                [sds(seq, w) for w in (d, oc)], args, 4 * rows * d * oc, aliases=aliases)


TASK = 4
HEADER = 3


def row_tasks(first, last):
    return [(i, i + 1, 1, -1) for i in range(first, last)]


def fwd_body(kind, s_ref, q_ref, k_ref, v_ref, *rest):
    qt, kk, vt, s_scr, acc, stat = rest[-6:]
    if kind == "rest":
        o1_ref, lse1_ref, st_ref, o_ref, lse_ref, hi_ref, pair_ref = rest[:7]
    else:
        o_ref, lse_ref = rest[:2]
    seq = k_ref.shape[0]

    def setup(c):
        sl = ds(c * BLK, BLK)
        vt[:, sl] = v_ref[sl, :].T
        kk[sl, :HEAD] = k_ref[sl, :]
        kk[sl, HEAD:] = k_ref[sl, :]
        for h in range(GROUP):
            qf = q_ref[sl, head_cols(h)].astype(F32) * SCALE2
            hi = qf.astype(BF)
            qt[h, :HEAD, sl] = hi.T
            qt[h, HEAD:, sl] = (qf - hi.astype(F32)).astype(BF).T

    loop(seq // BLK, setup)
    acc[...] = jnp.zeros_like(acc)
    stat[...] = jnp.zeros_like(stat)
    cur, old, den_row = 0, 1, 2
    lse_ref[...] = jnp.zeros_like(lse_ref)
    if kind == "rest":
        @pl.when(s_ref[1] == 0)
        def _():
            o_ref[:seq // 2, :] = o1_ref[...]
            lse_ref[0, :, :seq // 2] = lse1_ref[0]

    def task(t):
        return [s_ref[HEADER + t * TASK + n] for n in range(TASK)]

    def stage_a(h, i, j, masked, init=None):
        row = one(h)
        if masked is True:
            top = mm(kk[ds(j * BLK, HB), :], qt[h, :, ds(i * BLK, BLK)])
            low = mm(kk[ds(j * BLK + HB, HB), :], qt[h, :, ds(i * BLK + HB, HB)])
            top = jnp.where(down(top.shape) <= across(top.shape), top, NEG_LARGE)
            low = jnp.where(down(low.shape) <= across(low.shape), low, NEG_LARGE)
            s_scr[h, :HB, :] = top
            s_scr[h, HB:, HB:] = low
            m_new = jnp.max(top, axis=0, keepdims=True)
            right = jnp.maximum(m_new[:, HB:], jnp.max(low, axis=0, keepdims=True))
            m_new = jnp.concatenate([m_new[:, :HB], right], axis=1)
        else:
            s = mm(kk[ds(j * BLK, BLK), :], qt[h, :, ds(i * BLK, BLK)])
            if masked is not False:
                keep = down(s.shape) <= across(s.shape)
                s = jnp.where(jnp.logical_or(keep, jnp.logical_not(masked)), s, NEG_LARGE)
            s_scr[h] = s
            m_new = jnp.max(s, axis=0, keepdims=True)
        if init is None:
            m_old = stat[cur, row]
        elif kind == "rest":
            m_old = jnp.where(init >= 0, lse1_ref[0, row, ds(jnp.maximum(init, 0) * BLK, BLK)], NEG_LARGE)
        else:
            m_old = jnp.full(m_new.shape, NEG_LARGE, F32)
        m_new = jnp.maximum(m_old, m_new)
        stat[old, row] = jnp.exp2(m_old - m_new)
        stat[cur, row] = m_new

    def stage_p(h, diag=False):
        row = one(h)
        m, alpha = stat[cur, row], stat[old, row]
        if diag:
            top = jnp.exp2(s_scr[h, :HB, :] - m)
            low = jnp.exp2(s_scr[h, HB:, HB:] - m[:, HB:])
            total = jnp.sum(top, axis=0, keepdims=True)
            right = total[:, HB:] + jnp.sum(low, axis=0, keepdims=True)
            total = jnp.concatenate([total[:, :HB], right], axis=1)
            top = top.astype(BF)
            p = (top[:, :HB], jnp.concatenate([top[:, HB:], low.astype(BF)], axis=0))
        else:
            p = jnp.exp2(s_scr[h] - m)
            total = jnp.sum(p, axis=0, keepdims=True)
            p = p.astype(BF)
        stat[den_row, row] = stat[den_row, row] * alpha + total
        return p, alpha

    def stage_v(h, j, held, diag=False):
        p, alpha = held
        if diag:
            acc[h, :, :HB] = acc[h, :, :HB] * alpha[:, :HB] + mm(vt[:, ds(j * BLK, HB)], p[0])
            acc[h, :, HB:] = acc[h, :, HB:] * alpha[:, HB:] + mm(vt[:, ds(j * BLK, BLK)], p[1])
        else:
            acc[h] = acc[h] * alpha + mm(vt[:, ds(j * BLK, BLK)], p)

    def finish(h, i, den, top):
        row = one(h)
        out = acc[h] / den
        o_ref[ds(i * BLK, BLK), head_cols(h)] = out.T.astype(BF)
        lse_ref[0, row, ds(i * BLK, BLK)] = top + jnp.log2(den)
        if kind == "local":
            rest[2][0, h, :, ds(i * BLK, BLK)] = out

    def pipeline(i, j, masked):
        for h in range(GROUP):
            held = stage_p(h)
            stage_a(h, i, j + 1, masked)
            stage_v(h, j, held)

    count = s_ref[HEADER - 1]
    i, steps, diag, init = task(0)
    for h in range(GROUP):
        stage_a(h, i, 0, jnp.logical_and(steps == 1, diag == 1), init)

    def row(t):
        i, steps, diag, _ = task(t)

        loop(steps - 2, lambda j: pipeline(i, j, False))

        pl.when(jnp.logical_and(steps > 1, diag == 1))(lambda: pipeline(i, steps - 2, True))
        if kind == "rest":
            pl.when(diag == 0)(lambda: pipeline(i, steps - 2, False))
        i2, _, _, init2 = task(jnp.minimum(t + 1, count - 1))

        def last_step(on_diag):
            for h in range(GROUP):
                held = stage_p(h, on_diag)
                final = (stat[den_row, one(h)], stat[cur, one(h)])
                stage_a(h, i2, 0, False, init2)
                stage_v(h, steps - 1, held, on_diag)
                finish(h, i, *final)

        if kind != "rest":
            last_step(True)
        else:
            pl.when(diag == 1)(lambda: last_step(True))
            pl.when(diag == 0)(lambda: last_step(False))

            @pl.when(init2 >= 0)
            def _():
                stat[den_row] = jnp.ones(stat.shape[1:], F32)
                for h in range(GROUP):
                    acc[h] = st_ref[0, h, :, ds(init2 * BLK, BLK)]

    loop(count, row)
    if kind == "rest":
        hi_ref[...] = o_ref[seq - hi_ref.shape[0]:, :]
        pair_ref[...] = o_ref[ds(s_ref[0] * pair_ref.shape[0], pair_ref.shape[0]), :]


def attn_fwd(kind, idx, q, k, v, extra=(), local=()):
    whole = q.shape[0]
    seq = whole if kind == "rest" else whole // 2
    nkv = k.shape[1] // HEAD

    def half_map(g, s):
        return (s[1], g)

    def head_map(g, s):
        return (g, 0, 0)

    def state_map(g, s):
        return (g, 0, 0, 0)

    at = half_map if kind == "local" else col_map
    lse_spec = pl.BlockSpec((1, 8, seq), head_map)
    outs, specs = [sds(seq, q.shape[1]), jax.ShapeDtypeStruct((nkv, 8, seq), F32)], []
    out_specs = [pl.BlockSpec((seq, GW), col_map), lse_spec]
    state = pl.BlockSpec((1, GROUP, HEAD, whole // 2), state_map)
    if kind == "local":
        outs.append(jax.ShapeDtypeStruct((nkv, GROUP, HEAD, seq), F32))
        out_specs.append(state)
    if kind == "rest":
        specs = [pl.BlockSpec((seq // 2, GW), col_map), pl.BlockSpec((1, 8, seq // 2), head_map), state]
        outs += [sds(r, q.shape[1]) for r in extra]
        out_specs += [pl.BlockSpec((r, GW), col_map) for r in extra]
    kspec = pl.BlockSpec((seq, HEAD), at)
    return call(lambda *refs: fwd_body(kind, *refs), (nkv,), [pl.BlockSpec((seq, GW), at), kspec, kspec] + specs,
                out_specs, outs, [idx, q, k, v, *local], nkv * GROUP * seq * seq * PAIR,
                scratch=[pltpu.VMEM((GROUP, PAIR, seq), BF), pltpu.VMEM((seq, PAIR), BF),
                         pltpu.VMEM((HEAD, seq), BF), pltpu.VMEM((GROUP, BLK, BLK), F32),
                         pltpu.VMEM((GROUP, HEAD, BLK), F32), pltpu.VMEM((GROUP, 8, BLK), F32)])


def bwd_body(s_ref, q_ref, do_ref, o_ref, lse_ref, qn_ref, don_ref, on_ref, lsen_ref, k_ref, v_ref, cos_hbm, sin_hbm,
             out_ref, pair_ref, ka, va, dkt, dvt, tab, tab_sem, *sets):
    i = pl.program_id(0)
    last = pl.num_programs(0) - 1
    seq = k_ref.shape[0]
    m3 = GROUP * HB
    cos_ref, sin_ref = tab.at[0], tab.at[1]

    def spots():
        for b in range(2):
            for h in range(GROUP):
                start = (b * GROUP + h) * HB
                yield h, slice(b * HB, (b + 1) * HB), head_cols(h), slice(start, start + HB)

    def pick(n):
        return [ref.at[n] for ref in sets]

    def prepare(q_src, do_src, o_src, lse_src, dst):
        qa, da, q3t, do3t, dq3 = dst
        srow = down((16, HB))
        blank = jnp.zeros((HEAD - 16, HB), BF)
        for h, src, cols, rows in spots():
            qh, doh = q_src[src, cols], do_src[src, cols]
            qa[rows, :HEAD] = qh
            da[rows, :HEAD] = doh
            q3t[:, rows] = qh.T
            dt = doh.T
            do3t[:, rows] = dt
            delta = jnp.sum(dt.astype(F32) * o_src[src, cols].T.astype(F32), axis=0, keepdims=True)
            parts = jnp.zeros((16, HB), F32)
            for n, part in enumerate(split3(lse_src[0, one(h), src] * (1.0 / SCALE2)) + split3(delta)):
                parts = jnp.where(srow == n, part, parts)
            block = jnp.concatenate([parts.astype(BF), blank], axis=0).T
            qa[rows, HEAD:] = block
            da[rows, HEAD:] = block
        dq3[...] = jnp.zeros_like(dq3)

    @pl.when(i == 0)
    def _():
        copies = [pltpu.make_async_copy(src, tab.at[n], tab_sem.at[n]) for n, src in enumerate((cos_hbm, sin_hbm))]
        for copy in copies:
            copy.start()
        dkt[...] = jnp.zeros_like(dkt)
        dvt[...] = jnp.zeros_like(dvt)

        def setup(c):
            sl = ds(c * BLK, BLK)
            third = across((BLK, HEAD)) // 3
            for n, (src, dst) in enumerate(((k_ref, ka), (v_ref, va))):
                dst[sl, :HEAD] = src[sl, :]
                dst[sl, HEAD:] = jnp.where(third == n, -1.0, 0.0).astype(BF)

        loop(seq // BLK, setup)
        prepare(q_ref, do_ref, o_ref, lse_ref, pick(0))
        for copy in copies:
            copy.wait()

    def step(mine, rows, start, width, masked):
        qa, da, q3t, do3t, dq3 = mine
        sl = pl.ds(pl.multiple_of(start, BLK), width)
        s = mm_nt(qa[rows, :], ka[sl, :])
        dp = mm_nt(da[rows, :], va[sl, :])
        p = jnp.exp2(s * SCALE2)
        if masked:
            off = width - HB
            tail = p[:, off:]
            keep = down(tail.shape) % HB >= across(tail.shape)
            tail = jnp.where(keep, tail, 0.0)
            p = jnp.concatenate([p[:, :off], tail], axis=1) if off else tail
        dvt[:, sl] += mm(do3t[:, rows], p.astype(BF))
        dsv = (p * dp).astype(BF)
        dkt[:, sl] += mm(q3t[:, rows], dsv)
        dq3[rows, :] += mm(dsv, ka[sl, :HEAD])

    par, start = i % 2, (i // 2) * 2 * BLK
    loop(i // 2, lambda t: step(pick(par), slice(0, 2 * m3), t * 2 * BLK, 2 * BLK, False))

    def tail_steps(n):
        mine, width = pick(n), (n + 1) * BLK
        step(mine, slice(0, m3), start, width - HB, True)
        prepare(qn_ref, don_ref, on_ref, lsen_ref, pick(1 - n))
        step(mine, slice(m3, 2 * m3), start, width, True)
        for h, src, cols, rows in spots():
            rsl = ds(i * BLK + src.start, HB)
            out_ref[rsl, cols] = rotate(mine[-1][rows, :] * SCALE, cos_ref[rsl, :], -sin_ref[rsl, :]).astype(BF)

    pl.when(par == 0)(lambda: tail_steps(0))
    pl.when(par == 1)(lambda: tail_steps(1))

    @pl.when(i == last)
    def _():
        def fin(c):
            sl = ds(c * 2 * BLK, 2 * BLK)
            out_ref[sl, GW:QK] = rotate(dkt[:, sl].T * SCALE, cos_ref[sl, :], -sin_ref[sl, :]).astype(BF)
            out_ref[sl, QK:] = dvt[:, sl].T.astype(BF)

        loop(seq // BLK // 2, fin)
        pair_ref[...] = out_ref[ds(s_ref[0] * pair_ref.shape[0], pair_ref.shape[0]), :]


def attn_bwd(idx, q, do, o, k, v, lse, tabs, rows):
    seq = k.shape[0]
    nq = seq // BLK
    m3 = GROUP * BLK
    kspec = pl.BlockSpec((seq, HEAD), lambda i, s: (0, s[1]))
    row_specs = []
    for ahead in range(2):
        row_specs += [pl.BlockSpec((BLK, GW), lambda i, s, a=ahead: (jnp.minimum(i + a, nq - 1), s[1]))] * 3
        row_specs += [pl.BlockSpec((1, 8, BLK), lambda i, s, a=ahead: (s[1], 0, jnp.minimum(i + a, nq - 1)))]
    two_sets = [pltpu.VMEM((2, m3, PAIR), BF)] * 2 + [pltpu.VMEM((2, HEAD, m3), BF)] * 2 + [pltpu.VMEM((2, m3, HEAD), F32)]
    return call(bwd_body, (nq,),
                row_specs + [kspec] * 2 + [ANY] * 2,
                [pl.BlockSpec((r, PW), first_row) for r in (seq, rows)], [sds(r, PW) for r in (seq, rows)],
                [idx] + [q, do, o, lse] * 2 + [k, v, *tabs], GROUP * nq * (nq + 1) * BLK * BLK * PW,
                scratch=[pltpu.VMEM((seq, PAIR), BF)] * 2 + [pltpu.VMEM((HEAD, seq), F32)] * 2
                + [pltpu.VMEM((2, seq, HEAD), F32), pltpu.SemaphoreType.DMA((2,))] + two_sets)


def out_body(s_ref, x_ref, *rest):
    ops, out_ref = rest[:-1], rest[-1]
    lhs = jnp.concatenate([r[...] for r in ops[:4]], axis=1)
    rhs = jnp.concatenate([r[...] for r in ops[4:]], axis=0)
    out_ref[...] = (x_ref[...].astype(F32) + mm(lhs, rhs)).astype(BF)


def out_proj(idx, x, pieces, w_o):
    def chip_map(n, s):
        return (s[0] % 2, 0)

    rows, d = x.shape
    hw = pieces[0].shape[1]
    return call(out_body, (d // BLK,),
                [pl.BlockSpec((rows, BLK), col_map)]
                + [pl.BlockSpec((rows, hw), m) for m in (own_map, first_row, chip_map, first_row)]
                + [pl.BlockSpec((hw, BLK), lambda n, s, p=p: (s[p], n)) for p in range(4)],
                pl.BlockSpec((rows, BLK), col_map), sds(rows, d), [idx, x, *pieces] + [w_o] * 4,
                2 * rows * d * d)


def dwo_body(s_ref, oa_ref, ob_ref, oc_ref, dy_ref, fin, snd, ot):
    first, hw = ob_ref.shape

    @pl.when(jnp.logical_and(pl.program_id(0) == 0, pl.program_id(1) == 0))
    def _():
        for src, rows, base in ((oa_ref, slice(0, hw), 0), (ob_ref, slice(hw, 2 * hw), 0), (oc_ref, slice(hw, 2 * hw), first)):
            def tr(c):
                ot[rows, ds(c * BLK + base, BLK)] = src[ds(c * BLK, BLK), :].T

            loop(src.shape[0] // BLK, tr)

    val = mm(ot[ds(pl.program_id(1) * hw, hw), :], dy_ref[...])
    fin[...] = val
    snd[...] = val


def dw_o(idx, oa, ob, oc, dy):
    seq, d = dy.shape
    hw = oa.shape[1]
    o_specs = [pl.BlockSpec((r, hw), lambda i, p, s: (0, 0), pipeline_mode=pl.Buffered(1))
               for r in (seq, seq - oc.shape[0], oc.shape[0])]
    return call(dwo_body, (d // BLK, 2),
                o_specs + [pl.BlockSpec((seq, BLK), lambda i, p, s: (0, i))],
                [pl.BlockSpec((hw, BLK), lambda i, p, s: (s[p], i)), pl.BlockSpec((hw, BLK), lambda i, p, s: (p, i))],
                [sds(4 * hw, d, F32), sds(2 * hw, d, F32)], [idx, oa, ob, oc, dy], 4 * seq * d * hw,
                scratch=[pltpu.VMEM((2 * hw, seq), BF)])


def dwown_body(s_ref, h_ref, ga_ref, gb_ref, gc_ref, wo_ref, _, fq, fk, fv, snd, wo_fin, g3, ht, sem, wsem):
    i, steps = pl.program_id(0), pl.num_programs(0)
    rows, per = wo_ref.shape[0], steps // 2
    start = jnp.where(i < per, s_ref[1] * per + i, s_ref[3] * per + i - per)
    wcopy = pltpu.make_async_copy(wo_ref, wo_fin.at[ds(start * rows, rows), :], wsem)
    wcopy.start()

    @pl.when(i > 1)
    def _():
        for copy in scatter(snd, (fq, fk, fv), s_ref[0], s_ref[2], sem.at[i % 2]):
            copy.wait()

    ht[...] = h_ref[...].T
    lhs = ht[...]
    for g, q_at, k_at in ((ga_ref, 0, 2 * GW), (gb_ref, GW, 2 * GW + HEAD), (gc_ref, 2 * PW, 2 * PW + GW)):
        val = mm(lhs, g[:, :QK])
        snd[:, q_at:q_at + GW] = val[:, :GW]
        snd[:, k_at:k_at + HEAD] = val[:, GW:]
    snd[:, 2 * QK:2 * PW] = mm(lhs, jnp.concatenate([ga_ref[:, QK:], gb_ref[:, QK:]], axis=1))
    for copy in scatter(snd, (fq, fk, fv), s_ref[0], s_ref[2], sem.at[i % 2]):
        copy.start()

    @pl.when(i == steps - 1)
    def _():
        g3[...] = gc_ref[ds(s_ref[1] * g3.shape[0], g3.shape[0]), :]
        for slot in range(2):
            for copy in scatter(snd, (fq, fk, fv), s_ref[0], s_ref[2], sem.at[slot]):
                copy.wait()

    wcopy.wait()


def scatter(rcv, outs, whole_dev, part_dev, sem):
    rows, src, copies = ds(pl.program_id(0) * rcv.shape[0], rcv.shape[0]), 0, []
    fq, fk, fv = outs
    for n, (out, col, w) in enumerate(((fq, whole_dev, 2 * GW), (fk, whole_dev, PAIR), (fv, whole_dev, PAIR),
                                       (fq, 2 * part_dev, GW), (fk, 2 * part_dev, HEAD))):
        copies.append(pltpu.make_async_copy(rcv.at[:, src:src + w], out.at[rows, ds(col * w, w)], sem.at[n]))
        src += w
    return copies


def dw_own(idx, h, ga, gb, gc, wo_rcv, wo_fin):
    seq, d = h.shape
    steps = d // HB
    gspec = pl.BlockSpec((seq, PW), first_row, pipeline_mode=pl.Buffered(1))
    widths = (2 * GW, PAIR, PAIR)
    sw = 2 * PW + QK
    return call(dwown_body, (steps,),
                [pl.BlockSpec((seq, HB), col_map)] + [gspec] * 3
                + [pl.BlockSpec((wo_rcv.shape[0] // steps, d), row_map), ANY],
                [ANY] * 3 + [pl.BlockSpec((HB, sw), row_map), ANY, pl.BlockSpec((seq // 4, PW), first_row)],
                [sds(d, 4 * w, F32) for w in widths] + [sds(d, sw, F32), sds(*wo_fin.shape, F32), sds(seq // 4, PW)],
                [idx, h, ga, gb, gc, wo_rcv, wo_fin], 2 * seq * d * sw,
                scratch=[pltpu.VMEM((HB, seq), BF), pltpu.SemaphoreType.DMA((2, 5)), pltpu.SemaphoreType.DMA],
                aliases={6: 4})


def dwgrp_body(s_ref, h_ref, ga_ref, gb_ref, *rest):
    fq, fk, fv, snd, g3, ht = rest[-6:]

    @pl.when(pl.program_id(0) == 0)
    def _():
        g3[...] = gb_ref[ds(s_ref[1] * g3.shape[0], g3.shape[0]), :]

    ht[...] = h_ref[...].T
    lhs = ht[...]
    val = mm(lhs, gb_ref[:, :QK])
    fq[...] = val[:, :GW]
    fk[...] = val[:, GW:]
    snd[:, :QK] = val
    val = mm(lhs, jnp.concatenate([ga_ref[...], gb_ref[:, QK:]], axis=1))
    fv[...] = val
    snd[:, QK:] = val


def group_specs(bm):
    return [pl.BlockSpec((bm, w), lambda i, s: (i, 2 * s[0] + 1)) for w in (GW, HEAD)] + \
        [pl.BlockSpec((bm, PAIR), lambda i, s: (i, s[0]))]


def dw_group(idx, h, ga, gb, bufs):
    seq, d = h.shape
    gspec = pl.BlockSpec((seq, PW), first_row, pipeline_mode=pl.Buffered(1))
    sw = QK + PAIR
    return call(dwgrp_body, (d // HB,),
                [pl.BlockSpec((seq, HB), col_map),
                 pl.BlockSpec((seq, HEAD), lambda i, s: (0, QK // HEAD), pipeline_mode=pl.Buffered(1)), gspec] + [ANY] * 3,
                group_specs(HB) + [pl.BlockSpec((HB, sw), row_map), pl.BlockSpec((seq // 4, PW), first_row)],
                [sds(*b.shape, F32) for b in bufs] + [sds(d, sw, F32), sds(seq // 4, PW)],
                [idx, h, ga, gb, *bufs], 2 * seq * d * sw, scratch=[pltpu.VMEM((HB, seq), BF)],
                aliases={4 + n: n for n in range(3)})


def place_body(s_ref, rcv, *rest):
    q_out, k_out, v_out = rest[-3:]
    q_out[...] = rcv[:, :GW]
    k_out[...] = rcv[:, GW:QK]
    v_out[...] = rcv[:, QK:]


def place(idx, rcv, bufs):
    d, w = rcv.shape
    bm = BLK
    return call(place_body, (d // bm,), [pl.BlockSpec((bm, w), row_map)] + [ANY] * 3, group_specs(bm),
                [sds(*b.shape, F32) for b in bufs], [idx, rcv, *bufs], d * w, aliases={2 + n: n for n in range(3)})


def dx_body(s_ref, x_ref, dy_ref, gain_ref, inv_ref, *rest):
    pieces, weights, rcv = rest[:8], rest[8:20], rest[20]
    dx_ref, dg_ref, fq, fk, fv, acc, xs, tot, sem = rest[-9:]
    n = pl.program_id(0)
    bn = x_ref.shape[1]
    rows, d = acc.shape
    copies = scatter(rcv, (fq, fk, fv), s_ref[1], s_ref[3], sem)
    for copy in copies:
        copy.start()

    @pl.when(n == 0)
    def _():
        tot[...] = jnp.zeros_like(tot)

    cuts = (slice(0, GW), slice(GW, QK), slice(QK, PW))
    lhs = jnp.concatenate([pieces[2 * p + g][:, c] for p in range(4) for c in cuts for g in range(2)], axis=1)
    rhs = jnp.concatenate([r[...] for r in weights], axis=1)
    dh = mm_nt(lhs, rhs)
    inv = inv_ref[...]
    for c in range(bn // HEAD):
        cols = head_cols(c)
        xb = x_ref[:, cols]
        xs[:, ds(n * bn + cols.start, HEAD)] = xb
        part, xf = dh[:, cols], xb.astype(F32)
        scaled = part * gain_ref[:, cols]
        tot[...] += scaled * xf
        acc[:, ds(n * bn + cols.start, HEAD)] = dy_ref[:, cols].astype(F32) + inv * scaled
        dg_ref[:, cols] = jnp.sum((part * (xf * inv)).reshape(rows // 8, 8, HEAD), axis=0)

    @pl.when(n == pl.num_programs(0) - 1)
    def _():
        step = HEAD // 2

        def stats(r):
            sl = ds(r * step, step)
            inv = inv_ref[sl, :]
            tot[sl, :] = jnp.broadcast_to(jnp.sum(tot[sl, :], axis=-1, keepdims=True) / d, (step, HEAD)) * inv * inv * inv

        loop(rows // step, stats)

        def epi(r):
            sl = ds(r * step, step)
            coef = tot[sl, :]
            for c in range(d // HEAD):
                cols = head_cols(c)
                dx_ref[sl, cols] = (acc[sl, cols] - xs[sl, cols].astype(F32) * coef).astype(BF)

        loop(rows // step, epi)

    for copy in copies:
        copy.wait()


def dx_call(idx, x, dy, gain, inv, pieces, ws, rcv, bufs):
    rows, d = x.shape
    bn = HB
    once = pl.Buffered(1)
    maps = (own_map, own_map, first_row, first_row) * 2
    return call(dx_body, (d // bn,),
                [pl.BlockSpec((rows, bn), col_map)] * 2 + [pl.BlockSpec((1, bn), col_map), pl.BlockSpec((rows, HEAD), own_map)]
                + [pl.BlockSpec((rows, PW), m, pipeline_mode=once) for m in maps]
                + [pl.BlockSpec((bn, w.shape[1] // 4), lambda n, s, p=p: (n, s[p])) for p in range(4) for w in ws]
                + [pl.BlockSpec((bn, rcv.shape[1]), row_map)] + [ANY] * 3,
                [pl.BlockSpec((rows, d), first_row, pipeline_mode=once), pl.BlockSpec((8, bn), col_map)] + [ANY] * 3,
                [sds(rows, d), sds(8, d, F32)] + [sds(*b.shape, F32) for b in bufs],
                [idx, x, dy, gain, inv, *pieces] + list(ws) * 4 + [rcv, *bufs], 16 * rows * d * PW,
                scratch=[pltpu.VMEM((rows, d), F32), pltpu.VMEM((rows, d), BF), pltpu.VMEM((rows, HEAD), F32),
                         pltpu.SemaphoreType.DMA((5,))],
                aliases={26 + n: 2 + n for n in range(3)})


def solution(mesh):
    sp = mesh.shape['sp']
    cross = [(a, a ^ 2) for a in range(sp)]
    pair = [(a, a ^ 1) for a in range(sp)]

    def over(val):
        return lax.ppermute(val, 'sp', cross)

    def near(val):
        return lax.ppermute(val, 'sp', pair)

    def both(val):
        return lax.ppermute(val, 'sp', [(a, a ^ 3) for a in range(sp)])

    def after(val, *deps):
        return lax.optimization_barrier((val,) + deps)[0]

    def vec(*vals, dep=()):
        out = jnp.stack([jnp.asarray(v, jnp.int32) for v in vals])
        return after(out, *dep) if dep else out

    def step(x, dy, positions, gain, w_q, w_k, w_v, w_o):
        j = lax.axis_index('sp').astype(jnp.int32)
        rows, d = x.shape
        seq = rows * sp
        j1, j2, j3 = [j ^ n for n in (1, 2, 3)]
        dev = (j, j1, j2, j3)
        bpr, hpr = rows // BLK, rows // HB
        ws = (w_q, w_k, w_v)

        def rows_of(val, blk):
            return lax.dynamic_slice_in_dim(val, blk * rows, rows, 0)

        gain_f = gain.astype(F32).reshape(1, d)

        cut = rows - HB
        xa = x[:cut]
        positions = after(positions, xa)
        pos2 = over(positions)
        pos1 = near(positions)
        x2a = over(xa)
        x2b = over(after(x, xa)[cut:])
        x1 = near(x)
        pos3 = near(pos2)
        dy1 = near(after(dy, x1))

        pos = jnp.zeros((seq,), jnp.int32)
        for blk, val in zip(dev, (positions, pos1, pos2, pos3)):
            pos = lax.dynamic_update_slice(pos, val, (blk * rows,))
        inv_freq = ROPE_THETA ** (-jnp.arange(0, HEAD, 2).astype(F32) / HEAD)
        angles = pos.astype(F32)[:, None] * inv_freq[None, :]
        cos_h, sin_h = jnp.cos(angles), jnp.sin(angles)
        tabs = (jnp.concatenate([cos_h, cos_h], axis=1), jnp.concatenate([-sin_h, sin_h], axis=1))

        dya, dyb = dy[:cut], dy[cut:]
        bufs = project(vec(j * bpr, j1 * bpr, j, dep=(dya, dyb)), x, x1, gain_f, ws, tabs, None, seq)
        dbufs = dout(vec(j * bpr, j1 * bpr, j, dep=bufs), dy, dy1, w_o, None, seq)

        chip, nh = j // 2, seq // BLK // 2
        tri = row_tasks(0, nh)
        first = seq // 2 - BLK
        square = [(i + nh, nh, 0, i) for i in range(nh)]

        def table(head, tasks):
            return jnp.concatenate([vec(*head, len(tasks)), jnp.asarray(tasks, jnp.int32).reshape(-1)])

        c_tasks = table((j1, 0), tri).at[HEADER - 1].set(nh - 1)
        local = attn_fwd("local", after(table((j1, chip), tri), *dbufs), *bufs[1:4])
        rest_tasks = jnp.where(chip == 0, table((j1, 0), row_tasks(nh, 2 * nh) * 2).at[HEADER - 1].set(nh),
                               table((j1, 1), tri + square))

        x2a = after(x2a, *local)
        dy2a = over(after(dya, x2a))
        x3a = near(x2a)
        bufs = project(vec(j2 * hpr, j3 * hpr, j), x2a, x3a, gain_f, ws, tabs, bufs, seq)
        x2b = after(x2b, *bufs)
        dy2b = over(after(dyb, x2b))
        x3b = near(x2b)
        bufs = project(vec((j2 + 1) * hpr - 1, (j3 + 1) * hpr - 1, j), x2b, x3b, gain_f, ws, tabs, bufs, seq)
        h_all, q, k, v, inv = bufs
        o, lse, o_hi, o_pair = attn_fwd("rest", rest_tasks, q, k, v, (seq - first, rows), local)
        orv = over(o_hi)
        o1 = near(o_pair)
        qc, kc, vc = project_first(vec(j2, dep=(o,)), h_all, ws, tabs, first)
        dy2a = after(dy2a, qc)
        dy3a = near(dy2a)
        oc = attn_fwd("local", c_tasks, qc, kc, vc)[0]

        dbufs = dout(vec(j2 * hpr, j3 * hpr, j, dep=(oc,)), dy2a, dy3a, w_o, dbufs, seq)
        dy2b = after(dy2b, *dbufs)
        dy3b = near(dy2b)
        dbufs = dout(vec((j2 + 1) * hpr - 1, (j3 + 1) * hpr - 1, j), dy2b, dy3b, w_o, dbufs, seq)
        dy_all, do = dbufs

        ga, ga_pair = attn_bwd(vec(j1, 0), q, do, o, k, v, lse, tabs, rows)
        ga2 = over(ga)
        ga1 = near(ga_pair)
        gb, gb_pair = attn_bwd(vec(j1, 1, dep=(ga,)), q, do, o, k, v, lse, tabs, rows)
        gb2 = over(gb)
        gb1 = near(gb_pair)

        orv = after(orv, gb)
        shifted = jnp.concatenate([orv[:first], orv[:BLK]])
        upper = down(oc.shape) >= first
        ox = jnp.where(chip == 0, jnp.where(upper, shifted, oc), orv[BLK:])
        o3 = near(rows_of(ox, j1 % 2))
        wo_fin, wo_snd = dw_o(vec(j, j2, dep=(gb,)), o, oc, orv, dy_all)
        wo_rcv = near(wo_snd)
        result = out_proj(vec(*dev, dep=(wo_snd,)), x, (o, o1, ox, o3), w_o)
        ga2 = after(ga2, wo_snd)
        fq, fk, fv, snd, wo_fin, g3 = dw_own(vec(*dev, dep=(result,)), h_all, ga, gb, ga2, wo_rcv, wo_fin)
        rcv = near(snd)
        ga3 = near(g3)

        gb2 = after(gb2, snd)
        fq, fk, fv, snd_b, g3b = dw_group(vec(j2, j1), h_all, ga2, gb2, (fq, fk, fv))
        gb3 = near(g3b)
        rcv_b = near(snd_b)
        grad_x, dg, fq, fk, fv = dx_call(vec(*dev, dep=(snd_b,)), x, dy, gain_f, inv,
                                         (ga, gb, ga1, gb1, ga2, gb2, ga3, gb3), ws, rcv, (fq, fk, fv))
        dg = jnp.sum(dg, axis=0)
        dg = (dg + near(dg)) + (over(dg) + both(dg))
        fq, fk, fv = place(vec(j3), rcv_b, (fq, fk, fv))
        return result, grad_x, fq, fk, fv, wo_fin, dg

    seq_spec = P(('dp', 'sp'), None)
    whole = P(None, None)
    part_rows = P('dp', None)
    return jax.shard_map(step, mesh=mesh,
                         in_specs=(seq_spec, seq_spec, P(('dp', 'sp')), P(None), whole, whole, whole, whole),
                         out_specs=(seq_spec, seq_spec, part_rows, part_rows, part_rows, part_rows, P('dp')),
                         check_vma=False)
```

```python
import math

import jax
import jax.numpy as jnp
from jax import lax
from jax.experimental import pallas as pl
from jax.experimental.pallas import tpu as pltpu
from jax.sharding import PartitionSpec as P


HEAD = 128
GROUP = 3
GW = GROUP * HEAD
QK = GW + HEAD
PW = QK + HEAD
PAIR = 2 * HEAD
ROPE_THETA = 1000000.0
NORM_EPS = 1e-05
NEG_LARGE = -1e30
BF = jnp.bfloat16
F32 = jnp.float32
SCALE = HEAD ** -0.5
SCALE2 = SCALE * math.log2(math.e)
BLK = 512
HB = BLK // 2
VMEM_LIMIT = 65011712
ANY = pl.BlockSpec(memory_space=pl.ANY)


def first_row(i, s):
    return (0, 0)


def at_row(r):
    return (r, 0)


def at_col(c):
    return (0, c)


def row_map(i, s):
    return at_row(i)


def col_map(i, s):
    return at_col(i)


def own_map(i, s):
    return at_row(s[0])


def sds(rows, cols, dtype=BF):
    return jax.ShapeDtypeStruct((rows, cols), dtype)


def call(body, grid, in_specs, out_specs, out_shape, args, flops, scratch=(), aliases=None):
    return pl.pallas_call(
        body,
        grid_spec=pltpu.PrefetchScalarGridSpec(
            num_scalar_prefetch=1, grid=grid, in_specs=in_specs, out_specs=out_specs, scratch_shapes=list(scratch)),
        out_shape=out_shape, input_output_aliases=aliases or {},
        compiler_params=pltpu.CompilerParams(dimension_semantics=("arbitrary",) * len(grid),
                                             vmem_limit_bytes=VMEM_LIMIT),
        cost_estimate=pl.CostEstimate(flops=int(flops), bytes_accessed=int(flops) // BLK,
                                      transcendentals=0))(*args)


def down(shape):
    return lax.broadcasted_iota(jnp.int32, shape, 0)


def across(shape):
    return lax.broadcasted_iota(jnp.int32, shape, 1)


def loop(count, body):
    def run(c, _):
        body(c)
        return 0

    lax.fori_loop(0, count, run, 0)


def one(h):
    return slice(h, h + 1)


def head_cols(h):
    return slice(h * HEAD, h * HEAD + HEAD)


def mm(a, b):
    return jnp.dot(a, b, preferred_element_type=F32)


def mm_nt(a, b):
    return lax.dot_general(a, b, (((1,), (1,)), ((), ())), preferred_element_type=F32)


def rotate(val, cos_t, sin_t):
    return val * cos_t + pltpu.roll(val, HEAD // 2, 1) * sin_t


def ds(start, size):
    return pl.ds(pl.multiple_of(start, size), size)


def split3(val):
    hi = val.astype(BF).astype(F32)
    mid = (val - hi).astype(BF).astype(F32)
    return hi, mid, val - hi - mid


def qkv_of(h, wq_ref, wk_ref, wv_ref, cos_ref, sin_ref, q_ref, k_ref, v_ref):
    cos_t, sin_t = cos_ref[...], sin_ref[...]
    out = mm(h, wq_ref[...])
    for c in range(wq_ref.shape[1] // HEAD):
        sl = head_cols(c)
        q_ref[:, sl] = rotate(out[:, sl], cos_t, sin_t).astype(BF)
    out = mm(h, jnp.concatenate([wk_ref[...], wv_ref[...]], axis=1))
    for sl in (slice(0, HEAD), slice(HEAD, PAIR)):
        k_ref[:, sl] = rotate(out[:, sl], cos_t, sin_t).astype(BF)
    v_ref[...] = out[:, PAIR:].astype(BF)


def proj_body(s_ref, xa_ref, xb_ref, gain_ref, wq_ref, wk_ref, wv_ref, cos_ref, sin_ref, *rest):
    h_ref, q_ref, k_ref, v_ref, inv_ref = rest[-5:]
    half = pl.num_programs(0) // 2

    def norm(src):
        step = HEAD

        def stats(c):
            sl = ds(c * step, step)
            xf = src[sl, :].astype(F32)
            inv = lax.rsqrt(jnp.mean(xf * xf, axis=-1, keepdims=True) + NORM_EPS)
            inv_ref[sl, :] = jnp.broadcast_to(inv, (step, HEAD))

        def scale(c):
            sl = ds(c * step, step)
            inv, gain = inv_ref[sl, :], gain_ref[...]
            for n in range(src.shape[1] // HEAD):
                cols = head_cols(n)
                h_ref[sl, cols] = (src[sl, cols].astype(F32) * inv * gain[:, cols]).astype(BF)

        loop(src.shape[0] // step, stats)
        loop(src.shape[0] // step, scale)

    @pl.when(pl.program_id(0) < half)
    def _():
        norm(xa_ref)

    @pl.when(pl.program_id(0) >= half)
    def _():
        norm(xb_ref)

    qkv_of(h_ref[...], wq_ref, wk_ref, wv_ref, cos_ref, sin_ref, q_ref, k_ref, v_ref)


def two_source(rows):
    bm = HB if rows % BLK else BLK
    nb = rows // bm

    def a_map(i, s):
        return at_row(jnp.minimum(i, nb - 1))

    def b_map(i, s):
        return at_row(jnp.maximum(i - nb, 0))

    def o_map(i, s):
        return at_row(jnp.where(i < nb, s[0] + i, s[1] + i - nb))

    return bm, nb, a_map, b_map, o_map


def project(idx, xa, xb, gain, ws, tabs, bufs, seq):
    rows, d = xa.shape
    bm, nb, a_map, b_map, o_map = two_source(rows)
    widths = [w.shape[1] // 4 for w in ws]
    in_specs = [pl.BlockSpec((bm, d), a_map), pl.BlockSpec((bm, d), b_map), pl.BlockSpec((1, d), first_row)]
    in_specs += [pl.BlockSpec((d, w), lambda i, s: at_col(s[2])) for w in widths]
    in_specs += [pl.BlockSpec((bm, HEAD), o_map)] * 2
    args = [idx, xa, xb, gain, *ws, *tabs]
    aliases = {}
    if bufs is not None:
        in_specs += [ANY] * len(bufs)
        aliases = {len(args) + n: n for n in range(len(bufs))}
        args += list(bufs)
    return call(proj_body, (2 * nb,), in_specs, [pl.BlockSpec((bm, w), o_map) for w in (d, *widths, HEAD)],
                [sds(seq, w) for w in (d, *widths)] + [sds(seq, HEAD, F32)], args, 4 * rows * d * sum(widths),
                aliases=aliases)


def projc_body(s_ref, h_ref, *rest):
    qkv_of(h_ref[...], *rest)


def project_first(idx, h, ws, tabs, rows):
    seq, d = h.shape
    widths = [w.shape[1] // 4 for w in ws]
    return call(projc_body, (rows // BLK,),
                [pl.BlockSpec((BLK, d), row_map)] + [pl.BlockSpec((d, w), lambda i, s: at_col(s[0])) for w in widths]
                + [pl.BlockSpec((BLK, HEAD), row_map)] * 2,
                [pl.BlockSpec((BLK, w), row_map) for w in widths], [sds(seq, w) for w in widths],
                [idx, h, *ws, *tabs], 2 * rows * d * sum(widths))


def dout_body(s_ref, da_ref, db_ref, wo_ref, *rest):
    dy_out, do_out = rest[-2:]
    half = pl.num_programs(0) // 2

    @pl.when(pl.program_id(0) < half)
    def _():
        dy_out[...] = da_ref[...]

    @pl.when(pl.program_id(0) >= half)
    def _():
        dy_out[...] = db_ref[...]

    do_out[...] = mm_nt(dy_out[...], wo_ref[...]).astype(BF)


def dout(idx, da, db, w_o, bufs, seq):
    rows, d = da.shape
    bm, nb, a_map, b_map, o_map = two_source(rows)
    oc = w_o.shape[0] // 4
    in_specs = [pl.BlockSpec((bm, d), a_map), pl.BlockSpec((bm, d), b_map),
                pl.BlockSpec((oc, d), lambda i, s: at_row(s[2]))]
    args = [idx, da, db, w_o]
    aliases = {}
    if bufs is not None:
        in_specs += [ANY] * 2
        aliases = {len(args) + n: n for n in range(2)}
        args += list(bufs)
    return call(dout_body, (2 * nb,), in_specs, [pl.BlockSpec((bm, w), o_map) for w in (d, oc)],
                [sds(seq, w) for w in (d, oc)], args, 4 * rows * d * oc, aliases=aliases)


TASK = 4
HEADER = 3


def row_tasks(first, last):
    return [(i, i + 1, 1, -1) for i in range(first, last)]


def fwd_body(kind, s_ref, q_ref, k_ref, v_ref, *rest):
    qt, kk, vt, s_scr, acc, stat = rest[-6:]
    if kind == "rest":
        o1_ref, lse1_ref, st_ref, o_ref, lse_ref, hi_ref, pair_ref = rest[:7]
    else:
        o_ref, lse_ref = rest[:2]
    seq = k_ref.shape[0]

    def setup(c):
        sl = ds(c * BLK, BLK)
        vt[:, sl] = v_ref[sl, :].T
        kk[sl, :HEAD] = k_ref[sl, :]
        kk[sl, HEAD:] = k_ref[sl, :]
        for h in range(GROUP):
            qf = q_ref[sl, head_cols(h)].astype(F32) * SCALE2
            hi = qf.astype(BF)
            qt[h, :HEAD, sl] = hi.T
            qt[h, HEAD:, sl] = (qf - hi.astype(F32)).astype(BF).T

    loop(seq // BLK, setup)
    acc[...] = jnp.zeros_like(acc)
    stat[...] = jnp.zeros_like(stat)
    cur, old, den_row = 0, 1, 2
    lse_ref[...] = jnp.zeros_like(lse_ref)
    if kind == "rest":
        @pl.when(s_ref[1] == 0)
        def _():
            o_ref[:seq // 2, :] = o1_ref[...]
            lse_ref[0, :, :seq // 2] = lse1_ref[0]

    def task(t):
        return [s_ref[HEADER + t * TASK + n] for n in range(TASK)]

    def stage_a(h, i, j, masked, init=None):
        row = one(h)
        if masked is True:
            top = mm(kk[ds(j * BLK, HB), :], qt[h, :, ds(i * BLK, BLK)])
            low = mm(kk[ds(j * BLK + HB, HB), :], qt[h, :, ds(i * BLK + HB, HB)])
            top = jnp.where(down(top.shape) <= across(top.shape), top, NEG_LARGE)
            low = jnp.where(down(low.shape) <= across(low.shape), low, NEG_LARGE)
            s_scr[h, :HB, :] = top
            s_scr[h, HB:, HB:] = low
            m_new = jnp.max(top, axis=0, keepdims=True)
            right = jnp.maximum(m_new[:, HB:], jnp.max(low, axis=0, keepdims=True))
            m_new = jnp.concatenate([m_new[:, :HB], right], axis=1)
        else:
            s = mm(kk[ds(j * BLK, BLK), :], qt[h, :, ds(i * BLK, BLK)])
            if masked is not False:
                keep = down(s.shape) <= across(s.shape)
                s = jnp.where(jnp.logical_or(keep, jnp.logical_not(masked)), s, NEG_LARGE)
            s_scr[h] = s
            m_new = jnp.max(s, axis=0, keepdims=True)
        if init is None:
            m_old = stat[cur, row]
        elif kind == "rest":
            m_old = jnp.where(init >= 0, lse1_ref[0, row, ds(jnp.maximum(init, 0) * BLK, BLK)], NEG_LARGE)
        else:
            m_old = jnp.full(m_new.shape, NEG_LARGE, F32)
        m_new = jnp.maximum(m_old, m_new)
        stat[old, row] = jnp.exp2(m_old - m_new)
        stat[cur, row] = m_new

    def stage_p(h, diag=False):
        row = one(h)
        m, alpha = stat[cur, row], stat[old, row]
        if diag:
            top = jnp.exp2(s_scr[h, :HB, :] - m)
            low = jnp.exp2(s_scr[h, HB:, HB:] - m[:, HB:])
            total = jnp.sum(top, axis=0, keepdims=True)
            right = total[:, HB:] + jnp.sum(low, axis=0, keepdims=True)
            total = jnp.concatenate([total[:, :HB], right], axis=1)
            top = top.astype(BF)
            p = (top[:, :HB], jnp.concatenate([top[:, HB:], low.astype(BF)], axis=0))
        else:
            p = jnp.exp2(s_scr[h] - m)
            total = jnp.sum(p, axis=0, keepdims=True)
            p = p.astype(BF)
        stat[den_row, row] = stat[den_row, row] * alpha + total
        return p, alpha

    def stage_v(h, j, held, diag=False):
        p, alpha = held
        if diag:
            acc[h, :, :HB] = acc[h, :, :HB] * alpha[:, :HB] + mm(vt[:, ds(j * BLK, HB)], p[0])
            acc[h, :, HB:] = acc[h, :, HB:] * alpha[:, HB:] + mm(vt[:, ds(j * BLK, BLK)], p[1])
        else:
            acc[h] = acc[h] * alpha + mm(vt[:, ds(j * BLK, BLK)], p)

    def finish(h, i, den, top):
        row = one(h)
        out = acc[h] / den
        o_ref[ds(i * BLK, BLK), head_cols(h)] = out.T.astype(BF)
        lse_ref[0, row, ds(i * BLK, BLK)] = top + jnp.log2(den)
        if kind == "local":
            rest[2][0, h, :, ds(i * BLK, BLK)] = out

    def pipeline(i, j, masked):
        for h in range(GROUP):
            held = stage_p(h)
            stage_a(h, i, j + 1, masked)
            stage_v(h, j, held)

    count = s_ref[HEADER - 1]
    i, steps, diag, init = task(0)
    for h in range(GROUP):
        stage_a(h, i, 0, jnp.logical_and(steps == 1, diag == 1), init)

    def row(t):
        i, steps, diag, _ = task(t)

        loop(steps - 2, lambda j: pipeline(i, j, False))

        pl.when(jnp.logical_and(steps > 1, diag == 1))(lambda: pipeline(i, steps - 2, True))
        if kind == "rest":
            pl.when(diag == 0)(lambda: pipeline(i, steps - 2, False))
        i2, _, _, init2 = task(jnp.minimum(t + 1, count - 1))

        def last_step(on_diag):
            for h in range(GROUP):
                held = stage_p(h, on_diag)
                final = (stat[den_row, one(h)], stat[cur, one(h)])
                stage_a(h, i2, 0, False, init2)
                stage_v(h, steps - 1, held, on_diag)
                finish(h, i, *final)

        if kind != "rest":
            last_step(True)
        else:
            pl.when(diag == 1)(lambda: last_step(True))
            pl.when(diag == 0)(lambda: last_step(False))

            @pl.when(init2 >= 0)
            def _():
                stat[den_row] = jnp.ones(stat.shape[1:], F32)
                for h in range(GROUP):
                    acc[h] = st_ref[0, h, :, ds(init2 * BLK, BLK)]

    loop(count, row)
    if kind == "rest":
        hi_ref[...] = o_ref[seq - hi_ref.shape[0]:, :]
        pair_ref[...] = o_ref[ds(s_ref[0] * pair_ref.shape[0], pair_ref.shape[0]), :]


def attn_fwd(kind, idx, q, k, v, extra=(), local=()):
    whole = q.shape[0]
    seq = whole if kind == "rest" else whole // 2
    nkv = k.shape[1] // HEAD

    def half_map(g, s):
        return (s[1], g)

    def head_map(g, s):
        return (g, 0, 0)

    def state_map(g, s):
        return (g, 0, 0, 0)

    at = half_map if kind == "local" else col_map
    lse_spec = pl.BlockSpec((1, 8, seq), head_map)
    outs, specs = [sds(seq, q.shape[1]), jax.ShapeDtypeStruct((nkv, 8, seq), F32)], []
    out_specs = [pl.BlockSpec((seq, GW), col_map), lse_spec]
    state = pl.BlockSpec((1, GROUP, HEAD, whole // 2), state_map)
    if kind == "local":
        outs.append(jax.ShapeDtypeStruct((nkv, GROUP, HEAD, seq), F32))
        out_specs.append(state)
    if kind == "rest":
        specs = [pl.BlockSpec((seq // 2, GW), col_map), pl.BlockSpec((1, 8, seq // 2), head_map), state]
        outs += [sds(r, q.shape[1]) for r in extra]
        out_specs += [pl.BlockSpec((r, GW), col_map) for r in extra]
    kspec = pl.BlockSpec((seq, HEAD), at)
    return call(lambda *refs: fwd_body(kind, *refs), (nkv,), [pl.BlockSpec((seq, GW), at), kspec, kspec] + specs,
                out_specs, outs, [idx, q, k, v, *local], nkv * GROUP * seq * seq * PAIR,
                scratch=[pltpu.VMEM((GROUP, PAIR, seq), BF), pltpu.VMEM((seq, PAIR), BF),
                         pltpu.VMEM((HEAD, seq), BF), pltpu.VMEM((GROUP, BLK, BLK), F32),
                         pltpu.VMEM((GROUP, HEAD, BLK), F32), pltpu.VMEM((GROUP, 8, BLK), F32)])


def bwd_body(s_ref, q_ref, do_ref, o_ref, lse_ref, qn_ref, don_ref, on_ref, lsen_ref, k_ref, v_ref, cos_hbm, sin_hbm,
             out_ref, pair_ref, ka, va, dkt, dvt, tab, tab_sem, *sets):
    i = pl.program_id(0)
    last = pl.num_programs(0) - 1
    seq = k_ref.shape[0]
    m3 = GROUP * HB
    cos_ref, sin_ref = tab.at[0], tab.at[1]

    def spots():
        for b in range(2):
            for h in range(GROUP):
                start = (b * GROUP + h) * HB
                yield h, slice(b * HB, (b + 1) * HB), head_cols(h), slice(start, start + HB)

    def pick(n):
        return [ref.at[n] for ref in sets]

    def prepare(q_src, do_src, o_src, lse_src, dst):
        qa, da, q3t, do3t, dq3 = dst
        srow = down((16, HB))
        blank = jnp.zeros((HEAD - 16, HB), BF)
        for h, src, cols, rows in spots():
            qh, doh = q_src[src, cols], do_src[src, cols]
            qa[rows, :HEAD] = qh
            da[rows, :HEAD] = doh
            q3t[:, rows] = qh.T
            dt = doh.T
            do3t[:, rows] = dt
            delta = jnp.sum(dt.astype(F32) * o_src[src, cols].T.astype(F32), axis=0, keepdims=True)
            parts = jnp.zeros((16, HB), F32)
            for n, part in enumerate(split3(lse_src[0, one(h), src] * (1.0 / SCALE2)) + split3(delta)):
                parts = jnp.where(srow == n, part, parts)
            block = jnp.concatenate([parts.astype(BF), blank], axis=0).T
            qa[rows, HEAD:] = block
            da[rows, HEAD:] = block
        dq3[...] = jnp.zeros_like(dq3)

    @pl.when(i == 0)
    def _():
        copies = [pltpu.make_async_copy(src, tab.at[n], tab_sem.at[n]) for n, src in enumerate((cos_hbm, sin_hbm))]
        for copy in copies:
            copy.start()
        dkt[...] = jnp.zeros_like(dkt)
        dvt[...] = jnp.zeros_like(dvt)

        def setup(c):
            sl = ds(c * BLK, BLK)
            third = across((BLK, HEAD)) // 3
            for n, (src, dst) in enumerate(((k_ref, ka), (v_ref, va))):
                dst[sl, :HEAD] = src[sl, :]
                dst[sl, HEAD:] = jnp.where(third == n, -1.0, 0.0).astype(BF)

        loop(seq // BLK, setup)
        prepare(q_ref, do_ref, o_ref, lse_ref, pick(0))
        for copy in copies:
            copy.wait()

    def step(mine, rows, start, width, masked):
        qa, da, q3t, do3t, dq3 = mine
        sl = pl.ds(pl.multiple_of(start, BLK), width)
        s = mm_nt(qa[rows, :], ka[sl, :])
        dp = mm_nt(da[rows, :], va[sl, :])
        p = jnp.exp2(s * SCALE2)
        if masked:
            off = width - HB
            tail = p[:, off:]
            keep = down(tail.shape) % HB >= across(tail.shape)
            tail = jnp.where(keep, tail, 0.0)
            p = jnp.concatenate([p[:, :off], tail], axis=1) if off else tail
        dvt[:, sl] += mm(do3t[:, rows], p.astype(BF))
        dsv = (p * dp).astype(BF)
        dkt[:, sl] += mm(q3t[:, rows], dsv)
        dq3[rows, :] += mm(dsv, ka[sl, :HEAD])

    par, start = i % 2, (i // 2) * 2 * BLK
    loop(i // 2, lambda t: step(pick(par), slice(0, 2 * m3), t * 2 * BLK, 2 * BLK, False))

    def tail_steps(n):
        mine, width = pick(n), (n + 1) * BLK
        step(mine, slice(0, m3), start, width - HB, True)
        prepare(qn_ref, don_ref, on_ref, lsen_ref, pick(1 - n))
        step(mine, slice(m3, 2 * m3), start, width, True)
        for h, src, cols, rows in spots():
            rsl = ds(i * BLK + src.start, HB)
            out_ref[rsl, cols] = rotate(mine[-1][rows, :] * SCALE, cos_ref[rsl, :], -sin_ref[rsl, :]).astype(BF)

    pl.when(par == 0)(lambda: tail_steps(0))
    pl.when(par == 1)(lambda: tail_steps(1))

    @pl.when(i == last)
    def _():
        def fin(c):
            sl = ds(c * 2 * BLK, 2 * BLK)
            out_ref[sl, GW:QK] = rotate(dkt[:, sl].T * SCALE, cos_ref[sl, :], -sin_ref[sl, :]).astype(BF)
            out_ref[sl, QK:] = dvt[:, sl].T.astype(BF)

        loop(seq // BLK // 2, fin)
        pair_ref[...] = out_ref[ds(s_ref[0] * pair_ref.shape[0], pair_ref.shape[0]), :]


def attn_bwd(idx, q, do, o, k, v, lse, tabs, rows):
    seq = k.shape[0]
    nq = seq // BLK
    m3 = GROUP * BLK
    kspec = pl.BlockSpec((seq, HEAD), lambda i, s: at_col(s[1]))
    row_specs = []
    for ahead in range(2):
        row_specs += [pl.BlockSpec((BLK, GW), lambda i, s, a=ahead: (jnp.minimum(i + a, nq - 1), s[1]))] * 3
        row_specs += [pl.BlockSpec((1, 8, BLK), lambda i, s, a=ahead: (s[1], 0, jnp.minimum(i + a, nq - 1)))]
    two_sets = [pltpu.VMEM((2, m3, PAIR), BF)] * 2 + [pltpu.VMEM((2, HEAD, m3), BF)] * 2 + [pltpu.VMEM((2, m3, HEAD), F32)]
    return call(bwd_body, (nq,),
                row_specs + [kspec] * 2 + [ANY] * 2,
                [pl.BlockSpec((r, PW), first_row) for r in (seq, rows)], [sds(r, PW) for r in (seq, rows)],
                [idx] + [q, do, o, lse] * 2 + [k, v, *tabs], GROUP * nq * (nq + 1) * BLK * BLK * PW,
                scratch=[pltpu.VMEM((seq, PAIR), BF)] * 2 + [pltpu.VMEM((HEAD, seq), F32)] * 2
                + [pltpu.VMEM((2, seq, HEAD), F32), pltpu.SemaphoreType.DMA((2,))] + two_sets)


def half(i, s, n):
    return s[n] * 2 + i


def pick_body(s_ref, oa, ra, ob, rb, own, pair):
    for n, (low, high, out) in enumerate(((oa, ra, own), (ob, rb, pair))):
        out[...] = jnp.where(half(pl.program_id(0), s_ref, n) < s_ref[2], low[...], high[...])


def pick_rows(idx, low, high, rows):
    w = low.shape[1]
    specs = []
    for n in range(2):
        specs.append(pl.BlockSpec((BLK, w), lambda i, s, n=n: at_row(jnp.minimum(half(i, s, n), s[2] - 1))))
        specs.append(pl.BlockSpec((BLK, w), lambda i, s, n=n: at_row(jnp.maximum(half(i, s, n) - s[2], 0))))
    return call(pick_body, (rows // BLK,), specs, [pl.BlockSpec((BLK, w), row_map)] * 2, [sds(rows, w)] * 2,
                [idx, low, high, low, high], rows * w)


def out_body(s_ref, x_ref, *rest):
    ops, out_ref = rest[:-1], rest[-1]
    lhs = jnp.concatenate([r[...] for r in ops[:4]], axis=1)
    rhs = jnp.concatenate([r[...] for r in ops[4:]], axis=0)
    out_ref[...] = (x_ref[...].astype(F32) + mm(lhs, rhs)).astype(BF)


def out_proj(idx, x, pieces, w_o):
    rows, d = x.shape
    hw = pieces[0].shape[1]
    return call(out_body, (d // BLK,),
                [pl.BlockSpec((rows, BLK), col_map)]
                + [pl.BlockSpec((rows, hw), m) for m in (own_map, first_row, first_row, first_row)]
                + [pl.BlockSpec((hw, BLK), lambda n, s, p=p: (s[p], n)) for p in range(4)],
                pl.BlockSpec((rows, BLK), col_map), sds(rows, d), [idx, x, *pieces] + [w_o] * 4,
                2 * rows * d * d)


def dwo_body(s_ref, oa_ref, ob_ref, oc_ref, dy_ref, fin, snd, ot):
    first, hw = ob_ref.shape

    @pl.when(jnp.logical_and(pl.program_id(0) == 0, pl.program_id(1) == 0))
    def _():
        for src, rows, base in ((oa_ref, slice(0, hw), 0), (ob_ref, slice(hw, 2 * hw), 0), (oc_ref, slice(hw, 2 * hw), first)):
            def tr(c):
                ot[rows, ds(c * BLK + base, BLK)] = src[ds(c * BLK, BLK), :].T

            loop(src.shape[0] // BLK, tr)

    val = mm(ot[ds(pl.program_id(1) * hw, hw), :], dy_ref[...])
    fin[...] = val
    snd[...] = val


def dw_o(idx, oa, ob, oc, dy):
    seq, d = dy.shape
    hw = oa.shape[1]
    o_specs = [pl.BlockSpec((r, hw), lambda i, p, s: first_row(i, s), pipeline_mode=pl.Buffered(1))
               for r in (seq, seq - oc.shape[0], oc.shape[0])]
    return call(dwo_body, (d // BLK, 2),
                o_specs + [pl.BlockSpec((seq, BLK), lambda i, p, s: at_col(i))],
                [pl.BlockSpec((hw, BLK), lambda i, p, s: (s[p], i)), pl.BlockSpec((hw, BLK), lambda i, p, s: (p, i))],
                [sds(4 * hw, d, F32), sds(2 * hw, d, F32)], [idx, oa, ob, oc, dy], 4 * seq * d * hw,
                scratch=[pltpu.VMEM((2 * hw, seq), BF)])


def dwown_body(s_ref, h_ref, ga_ref, gb_ref, gc_ref, wo_ref, _, fq, fk, fv, snd, wo_fin, g3, ht, sem, wsem):
    i, steps = pl.program_id(0), pl.num_programs(0)
    rows, per = wo_ref.shape[0], steps // 2
    start = jnp.where(i < per, s_ref[1] * per + i, s_ref[3] * per + i - per)
    wcopy = pltpu.make_async_copy(wo_ref, wo_fin.at[ds(start * rows, rows), :], wsem)
    wcopy.start()

    @pl.when(i > 1)
    def _():
        for copy in scatter(snd, (fq, fk, fv), s_ref[0], s_ref[2], sem.at[i % 2]):
            copy.wait()

    ht[...] = h_ref[...].T
    lhs = ht[...]
    for g, q_at, k_at in ((ga_ref, 0, 2 * GW), (gb_ref, GW, 2 * GW + HEAD), (gc_ref, 2 * PW, 2 * PW + GW)):
        val = mm(lhs, g[:, :QK])
        snd[:, q_at:q_at + GW] = val[:, :GW]
        snd[:, k_at:k_at + HEAD] = val[:, GW:]
    snd[:, 2 * QK:2 * PW] = mm(lhs, jnp.concatenate([ga_ref[:, QK:], gb_ref[:, QK:]], axis=1))
    for copy in scatter(snd, (fq, fk, fv), s_ref[0], s_ref[2], sem.at[i % 2]):
        copy.start()

    @pl.when(i == steps - 1)
    def _():
        g3[...] = gc_ref[ds(s_ref[1] * g3.shape[0], g3.shape[0]), :]
        for slot in range(2):
            for copy in scatter(snd, (fq, fk, fv), s_ref[0], s_ref[2], sem.at[slot]):
                copy.wait()

    wcopy.wait()


def scatter(rcv, outs, whole_dev, part_dev, sem):
    rows, src, copies = ds(pl.program_id(0) * rcv.shape[0], rcv.shape[0]), 0, []
    fq, fk, fv = outs
    for n, (out, col, w) in enumerate(((fq, whole_dev, 2 * GW), (fk, whole_dev, PAIR), (fv, whole_dev, PAIR),
                                       (fq, 2 * part_dev, GW), (fk, 2 * part_dev, HEAD))):
        copies.append(pltpu.make_async_copy(rcv.at[:, src:src + w], out.at[rows, ds(col * w, w)], sem.at[n]))
        src += w
    return copies


def dw_own(idx, h, ga, gb, gc, wo_rcv, wo_fin):
    seq, d = h.shape
    steps = d // HB
    gspec = pl.BlockSpec((seq, PW), first_row, pipeline_mode=pl.Buffered(1))
    widths = (2 * GW, PAIR, PAIR)
    sw = 2 * PW + QK
    return call(dwown_body, (steps,),
                [pl.BlockSpec((seq, HB), col_map)] + [gspec] * 3
                + [pl.BlockSpec((wo_rcv.shape[0] // steps, d), row_map), ANY],
                [ANY] * 3 + [pl.BlockSpec((HB, sw), row_map), ANY, pl.BlockSpec((seq // 4, PW), first_row)],
                [sds(d, 4 * w, F32) for w in widths] + [sds(d, sw, F32), sds(*wo_fin.shape, F32), sds(seq // 4, PW)],
                [idx, h, ga, gb, gc, wo_rcv, wo_fin], 2 * seq * d * sw,
                scratch=[pltpu.VMEM((HB, seq), BF), pltpu.SemaphoreType.DMA((2, 5)), pltpu.SemaphoreType.DMA],
                aliases={6: 4})


def dwgrp_body(s_ref, h_ref, ga_ref, gb_ref, *rest):
    fq, fk, fv, snd, g3, ht = rest[-6:]

    @pl.when(pl.program_id(0) == 0)
    def _():
        g3[...] = gb_ref[ds(s_ref[1] * g3.shape[0], g3.shape[0]), :]

    ht[...] = h_ref[...].T
    lhs = ht[...]
    val = mm(lhs, gb_ref[:, :QK])
    fq[...] = val[:, :GW]
    fk[...] = val[:, GW:]
    snd[:, :QK] = val
    val = mm(lhs, jnp.concatenate([ga_ref[...], gb_ref[:, QK:]], axis=1))
    fv[...] = val
    snd[:, QK:] = val


def group_specs(bm):
    return [pl.BlockSpec((bm, w), lambda i, s: (i, 2 * s[0] + 1)) for w in (GW, HEAD)] + \
        [pl.BlockSpec((bm, PAIR), lambda i, s: (i, s[0]))]


def dw_group(idx, h, ga, gb, bufs):
    seq, d = h.shape
    gspec = pl.BlockSpec((seq, PW), first_row, pipeline_mode=pl.Buffered(1))
    sw = QK + PAIR
    return call(dwgrp_body, (d // HB,),
                [pl.BlockSpec((seq, HB), col_map),
                 pl.BlockSpec((seq, HEAD), lambda i, s: at_col(QK // HEAD), pipeline_mode=pl.Buffered(1)), gspec] + [ANY] * 3,
                group_specs(HB) + [pl.BlockSpec((HB, sw), row_map), pl.BlockSpec((seq // 4, PW), first_row)],
                [sds(*b.shape, F32) for b in bufs] + [sds(d, sw, F32), sds(seq // 4, PW)],
                [idx, h, ga, gb, *bufs], 2 * seq * d * sw, scratch=[pltpu.VMEM((HB, seq), BF)],
                aliases={4 + n: n for n in range(3)})


def place_body(s_ref, rcv, *rest):
    q_out, k_out, v_out = rest[-3:]
    q_out[...] = rcv[:, :GW]
    k_out[...] = rcv[:, GW:QK]
    v_out[...] = rcv[:, QK:]


def place(idx, rcv, bufs):
    d, w = rcv.shape
    bm = BLK
    return call(place_body, (d // bm,), [pl.BlockSpec((bm, w), row_map)] + [ANY] * 3, group_specs(bm),
                [sds(*b.shape, F32) for b in bufs], [idx, rcv, *bufs], d * w, aliases={2 + n: n for n in range(3)})


def dx_body(s_ref, x_ref, dy_ref, gain_ref, inv_ref, *rest):
    pieces, weights, rcv = rest[:8], rest[8:20], rest[20]
    dx_ref, dg_ref, fq, fk, fv, acc, xs, tot, sem = rest[-9:]
    n = pl.program_id(0)
    bn = x_ref.shape[1]
    rows, d = acc.shape
    copies = scatter(rcv, (fq, fk, fv), s_ref[1], s_ref[3], sem)
    for copy in copies:
        copy.start()

    @pl.when(n == 0)
    def _():
        tot[...] = jnp.zeros_like(tot)

    cuts = (slice(0, GW), slice(GW, QK), slice(QK, PW))
    lhs = jnp.concatenate([pieces[2 * p + g][:, c] for p in range(4) for c in cuts for g in range(2)], axis=1)
    rhs = jnp.concatenate([r[...] for r in weights], axis=1)
    dh = mm_nt(lhs, rhs)
    inv = inv_ref[...]
    for c in range(bn // HEAD):
        cols = head_cols(c)
        xb = x_ref[:, cols]
        xs[:, ds(n * bn + cols.start, HEAD)] = xb
        part, xf = dh[:, cols], xb.astype(F32)
        scaled = part * gain_ref[:, cols]
        tot[...] += scaled * xf
        acc[:, ds(n * bn + cols.start, HEAD)] = dy_ref[:, cols].astype(F32) + inv * scaled
        dg_ref[:, cols] = jnp.sum((part * (xf * inv)).reshape(rows // 8, 8, HEAD), axis=0)

    @pl.when(n == pl.num_programs(0) - 1)
    def _():
        step = HEAD // 2

        def stats(r):
            sl = ds(r * step, step)
            inv = inv_ref[sl, :]
            tot[sl, :] = jnp.broadcast_to(jnp.sum(tot[sl, :], axis=-1, keepdims=True) / d, (step, HEAD)) * inv * inv * inv

        loop(rows // step, stats)

        def epi(r):
            sl = ds(r * step, step)
            coef = tot[sl, :]
            for c in range(d // HEAD):
                cols = head_cols(c)
                dx_ref[sl, cols] = (acc[sl, cols] - xs[sl, cols].astype(F32) * coef).astype(BF)

        loop(rows // step, epi)

    for copy in copies:
        copy.wait()


def dx_call(idx, x, dy, gain, inv, pieces, ws, rcv, bufs):
    rows, d = x.shape
    bn = HB
    once = pl.Buffered(1)
    maps = (own_map, own_map, first_row, first_row) * 2
    return call(dx_body, (d // bn,),
                [pl.BlockSpec((rows, bn), col_map)] * 2 + [pl.BlockSpec((1, bn), col_map), pl.BlockSpec((rows, HEAD), own_map)]
                + [pl.BlockSpec((rows, PW), m, pipeline_mode=once) for m in maps]
                + [pl.BlockSpec((bn, w.shape[1] // 4), lambda n, s, p=p: (n, s[p])) for p in range(4) for w in ws]
                + [pl.BlockSpec((bn, rcv.shape[1]), row_map)] + [ANY] * 3,
                [pl.BlockSpec((rows, d), first_row, pipeline_mode=once), pl.BlockSpec((8, bn), col_map)] + [ANY] * 3,
                [sds(rows, d), sds(8, d, F32)] + [sds(*b.shape, F32) for b in bufs],
                [idx, x, dy, gain, inv, *pieces] + list(ws) * 4 + [rcv, *bufs], 16 * rows * d * PW,
                scratch=[pltpu.VMEM((rows, d), F32), pltpu.VMEM((rows, d), BF), pltpu.VMEM((rows, HEAD), F32),
                         pltpu.SemaphoreType.DMA((5,))],
                aliases={26 + n: 2 + n for n in range(3)})


def solution(mesh):
    sp = mesh.shape['sp']
    cross = [(a, a ^ 2) for a in range(sp)]
    pair = [(a, a ^ 1) for a in range(sp)]

    def over(val):
        return lax.ppermute(val, 'sp', cross)

    def near(val):
        return lax.ppermute(val, 'sp', pair)

    def both(val):
        return lax.ppermute(val, 'sp', [(a, a ^ 3) for a in range(sp)])

    def after(val, *deps):
        return lax.optimization_barrier((val,) + deps)[0]

    def vec(*vals, dep=()):
        out = jnp.stack([jnp.asarray(v, jnp.int32) for v in vals])
        return after(out, *dep) if dep else out

    def step(x, dy, positions, gain, w_q, w_k, w_v, w_o):
        j = lax.axis_index('sp').astype(jnp.int32)
        rows, d = x.shape
        seq = rows * sp
        j1, j2, j3 = [j ^ n for n in (1, 2, 3)]
        dev = (j, j1, j2, j3)
        bpr, hpr = rows // BLK, rows // HB
        ws = (w_q, w_k, w_v)

        gain_f = gain.astype(F32).reshape(1, d)

        cut = rows - HB
        xa = x[:cut]
        positions = after(positions, xa)
        pos2 = over(positions)
        pos1 = near(positions)
        x2a = over(xa)
        x2b = over(after(x, xa)[cut:])
        x1 = near(x)
        pos3 = near(pos2)
        dy1 = near(after(dy, x1))

        pos = jnp.zeros((seq,), jnp.int32)
        for blk, val in zip(dev, (positions, pos1, pos2, pos3)):
            pos = lax.dynamic_update_slice(pos, val, (blk * rows,))
        inv_freq = ROPE_THETA ** (-jnp.arange(0, HEAD, 2).astype(F32) / HEAD)
        angles = pos.astype(F32)[:, None] * inv_freq[None, :]
        cos_h, sin_h = jnp.cos(angles), jnp.sin(angles)
        tabs = (jnp.concatenate([cos_h, cos_h], axis=1), jnp.concatenate([-sin_h, sin_h], axis=1))

        dya, dyb = dy[:cut], dy[cut:]
        bufs = project(vec(j * bpr, j1 * bpr, j, dep=(dya, dyb)), x, x1, gain_f, ws, tabs, None, seq)
        dbufs = dout(vec(j * bpr, j1 * bpr, j, dep=bufs), dy, dy1, w_o, None, seq)

        chip, nh = j // 2, seq // BLK // 2
        tri = row_tasks(0, nh)
        first = seq // 2 - BLK
        square = [(i + nh, nh, 0, i) for i in range(nh)]

        def table(head, tasks):
            return jnp.concatenate([vec(*head, len(tasks)), jnp.asarray(tasks, jnp.int32).reshape(-1)])

        c_tasks = table((j1, 0), tri).at[HEADER - 1].set(nh - 1)
        local = attn_fwd("local", after(table((j1, chip), tri), *dbufs), *bufs[1:4])
        rest_tasks = jnp.where(chip == 0, table((j1, 0), row_tasks(nh, 2 * nh) * 2).at[HEADER - 1].set(nh),
                               table((j1, 1), tri + square))

        x2a = after(x2a, *local)
        dy2a = over(after(dya, x2a))
        x3a = near(x2a)
        bufs = project(vec(j2 * hpr, j3 * hpr, j), x2a, x3a, gain_f, ws, tabs, bufs, seq)
        x2b = after(x2b, *bufs)
        dy2b = over(after(dyb, x2b))
        x3b = near(x2b)
        bufs = project(vec((j2 + 1) * hpr - 1, (j3 + 1) * hpr - 1, j), x2b, x3b, gain_f, ws, tabs, bufs, seq)
        h_all, q, k, v, inv = bufs
        o, lse, o_hi, o_pair = attn_fwd("rest", rest_tasks, q, k, v, (seq - first, rows), local)
        orv = over(o_hi)
        o1 = near(o_pair)
        qc, kc, vc = project_first(vec(j2, dep=(o,)), h_all, ws, tabs, first)
        dy2a = after(dy2a, qc)
        dy3a = near(dy2a)
        oc = attn_fwd("local", c_tasks, qc, kc, vc)[0]

        dbufs = dout(vec(j2 * hpr, j3 * hpr, j, dep=(oc,)), dy2a, dy3a, w_o, dbufs, seq)
        dy2b = after(dy2b, *dbufs)
        dy3b = near(dy2b)
        dbufs = dout(vec((j2 + 1) * hpr - 1, (j3 + 1) * hpr - 1, j), dy2b, dy3b, w_o, dbufs, seq)
        dy_all, do = dbufs

        ga, ga_pair = attn_bwd(vec(j1, 0), q, do, o, k, v, lse, tabs, rows)
        ga2 = over(ga)
        ga1 = near(ga_pair)
        gb, gb_pair = attn_bwd(vec(j1, 1, dep=(ga,)), q, do, o, k, v, lse, tabs, rows)
        gb2 = over(gb)
        gb1 = near(gb_pair)

        orv = after(orv, gb)
        ox, ox_pair = pick_rows(vec(j, j1, nh - 1, dep=(gb,)), oc, orv, rows)
        o3 = near(ox_pair)
        wo_fin, wo_snd = dw_o(vec(j, j2, dep=(gb,)), o, oc, orv, dy_all)
        wo_rcv = near(wo_snd)
        result = out_proj(vec(*dev, dep=(wo_snd,)), x, (o, o1, ox, o3), w_o)
        ga2 = after(ga2, wo_snd)
        fq, fk, fv, snd, wo_fin, g3 = dw_own(vec(*dev, dep=(result,)), h_all, ga, gb, ga2, wo_rcv, wo_fin)
        rcv = near(snd)
        ga3 = near(g3)

        gb2 = after(gb2, snd)
        fq, fk, fv, snd_b, g3b = dw_group(vec(j2, j1), h_all, ga2, gb2, (fq, fk, fv))
        gb3 = near(g3b)
        rcv_b = near(snd_b)
        grad_x, dg, fq, fk, fv = dx_call(vec(*dev, dep=(snd_b,)), x, dy, gain_f, inv,
                                         (ga, gb, ga1, gb1, ga2, gb2, ga3, gb3), ws, rcv, (fq, fk, fv))
        dg = jnp.sum(dg, axis=0)
        dg = (dg + near(dg)) + (over(dg) + both(dg))
        fq, fk, fv = place(vec(j3), rcv_b, (fq, fk, fv))
        return result, grad_x, fq, fk, fv, wo_fin, dg

    seq_spec = P(('dp', 'sp'), None)
    whole = P(None, None)
    part_rows = P('dp', None)
    return jax.shard_map(step, mesh=mesh,
                         in_specs=(seq_spec, seq_spec, P(('dp', 'sp')), P(None), whole, whole, whole, whole),
                         out_specs=(seq_spec, seq_spec, part_rows, part_rows, part_rows, part_rows, P('dp')),
                         check_vma=False)
```

```python
import math

import jax
import jax.numpy as jnp
from jax import lax
from jax.experimental import pallas as pl
from jax.experimental.pallas import tpu as pltpu
from jax.sharding import PartitionSpec as P


HEAD = 128
GROUP = 3
GW = GROUP * HEAD
QK = GW + HEAD
PW = QK + HEAD
PAIR = 2 * HEAD
ROPE_THETA = 1000000.0
NORM_EPS = 1e-05
NEG_LARGE = -1e30
BF = jnp.bfloat16
F32 = jnp.float32
SCALE = HEAD ** -0.5
SCALE2 = SCALE * math.log2(math.e)
BLK = 512
HB = BLK // 2
VMEM_LIMIT = 65011712
ANY = pl.BlockSpec(memory_space=pl.ANY)


def first_row(i, s):
    return (0, 0)


def at_row(r):
    return (r, 0)


def at_col(c):
    return (0, c)


def row_map(i, s):
    return at_row(i)


def col_map(i, s):
    return at_col(i)


def own_map(i, s):
    return at_row(s[0])


def sds(rows, cols, dtype=BF):
    return jax.ShapeDtypeStruct((rows, cols), dtype)


def call(body, grid, in_specs, out_specs, out_shape, args, flops, scratch=(), aliases=None):
    return pl.pallas_call(
        body,
        grid_spec=pltpu.PrefetchScalarGridSpec(
            num_scalar_prefetch=1, grid=grid, in_specs=in_specs, out_specs=out_specs, scratch_shapes=list(scratch)),
        out_shape=out_shape, input_output_aliases=aliases or {},
        compiler_params=pltpu.CompilerParams(dimension_semantics=("arbitrary",) * len(grid),
                                             vmem_limit_bytes=VMEM_LIMIT),
        cost_estimate=pl.CostEstimate(flops=int(flops), bytes_accessed=int(flops) // BLK,
                                      transcendentals=0))(*args)


def down(shape):
    return lax.broadcasted_iota(jnp.int32, shape, 0)


def across(shape):
    return lax.broadcasted_iota(jnp.int32, shape, 1)


def loop(count, body):
    def run(c, _):
        body(c)
        return 0

    lax.fori_loop(0, count, run, 0)


def one(h):
    return slice(h, h + 1)


def head_cols(h):
    return slice(h * HEAD, h * HEAD + HEAD)


def mm(a, b):
    return jnp.dot(a, b, preferred_element_type=F32)


def mm_nt(a, b):
    return lax.dot_general(a, b, (((1,), (1,)), ((), ())), preferred_element_type=F32)


def rotate(val, cos_t, sin_t):
    return val * cos_t + pltpu.roll(val, HEAD // 2, 1) * sin_t


def ds(start, size):
    return pl.ds(pl.multiple_of(start, size), size)


def split3(val):
    hi = val.astype(BF).astype(F32)
    mid = (val - hi).astype(BF).astype(F32)
    return hi, mid, val - hi - mid


def qkv_of(h, wq_ref, wk_ref, wv_ref, cos_ref, sin_ref, q_ref, k_ref, v_ref):
    cos_t, sin_t = cos_ref[...], sin_ref[...]
    out = mm(h, wq_ref[...])
    for c in range(wq_ref.shape[1] // HEAD):
        sl = head_cols(c)
        q_ref[:, sl] = rotate(out[:, sl], cos_t, sin_t).astype(BF)
    out = mm(h, jnp.concatenate([wk_ref[...], wv_ref[...]], axis=1))
    for sl in (slice(0, HEAD), slice(HEAD, PAIR)):
        k_ref[:, sl] = rotate(out[:, sl], cos_t, sin_t).astype(BF)
    v_ref[...] = out[:, PAIR:].astype(BF)


def proj_body(s_ref, xa_ref, xb_ref, gain_ref, wq_ref, wk_ref, wv_ref, cos_ref, sin_ref, *rest):
    h_ref, q_ref, k_ref, v_ref, inv_ref = rest[-5:]
    half = pl.num_programs(0) // 2

    def norm(src):
        step = HEAD

        def stats(c):
            sl = ds(c * step, step)
            xf = src[sl, :].astype(F32)
            inv = lax.rsqrt(jnp.mean(xf * xf, axis=-1, keepdims=True) + NORM_EPS)
            inv_ref[sl, :] = jnp.broadcast_to(inv, (step, HEAD))

        def scale(c):
            sl = ds(c * step, step)
            inv, gain = inv_ref[sl, :], gain_ref[...]
            for n in range(src.shape[1] // HEAD):
                cols = head_cols(n)
                h_ref[sl, cols] = (src[sl, cols].astype(F32) * inv * gain[:, cols]).astype(BF)

        loop(src.shape[0] // step, stats)
        loop(src.shape[0] // step, scale)

    @pl.when(pl.program_id(0) < half)
    def _():
        norm(xa_ref)

    @pl.when(pl.program_id(0) >= half)
    def _():
        norm(xb_ref)

    qkv_of(h_ref[...], wq_ref, wk_ref, wv_ref, cos_ref, sin_ref, q_ref, k_ref, v_ref)


def two_source(rows):
    bm = HB if rows % BLK else BLK
    nb = rows // bm

    def a_map(i, s):
        return at_row(jnp.minimum(i, nb - 1))

    def b_map(i, s):
        return at_row(jnp.maximum(i - nb, 0))

    def o_map(i, s):
        return at_row(jnp.where(i < nb, s[0] + i, s[1] + i - nb))

    return bm, nb, a_map, b_map, o_map


def project(idx, xa, xb, gain, ws, tabs, bufs, seq):
    rows, d = xa.shape
    bm, nb, a_map, b_map, o_map = two_source(rows)
    widths = [w.shape[1] // 4 for w in ws]
    in_specs = [pl.BlockSpec((bm, d), a_map), pl.BlockSpec((bm, d), b_map), pl.BlockSpec((1, d), first_row)]
    in_specs += [pl.BlockSpec((d, w), lambda i, s: at_col(s[2])) for w in widths]
    in_specs += [pl.BlockSpec((bm, HEAD), o_map)] * 2
    args = [idx, xa, xb, gain, *ws, *tabs]
    aliases = {}
    if bufs is not None:
        in_specs += [ANY] * len(bufs)
        aliases = {len(args) + n: n for n in range(len(bufs))}
        args += list(bufs)
    return call(proj_body, (2 * nb,), in_specs, [pl.BlockSpec((bm, w), o_map) for w in (d, *widths, HEAD)],
                [sds(seq, w) for w in (d, *widths)] + [sds(seq, HEAD, F32)], args, 4 * rows * d * sum(widths),
                aliases=aliases)


def projc_body(s_ref, h_ref, *rest):
    qkv_of(h_ref[...], *rest)


def project_first(idx, h, ws, tabs, rows):
    seq, d = h.shape
    widths = [w.shape[1] // 4 for w in ws]
    return call(projc_body, (rows // BLK,),
                [pl.BlockSpec((BLK, d), row_map)] + [pl.BlockSpec((d, w), lambda i, s: at_col(s[0])) for w in widths]
                + [pl.BlockSpec((BLK, HEAD), row_map)] * 2,
                [pl.BlockSpec((BLK, w), row_map) for w in widths], [sds(seq, w) for w in widths],
                [idx, h, *ws, *tabs], 2 * rows * d * sum(widths))


def dout_body(s_ref, da_ref, db_ref, wo_ref, *rest):
    dy_out, do_out = rest[-2:]
    half = pl.num_programs(0) // 2

    @pl.when(pl.program_id(0) < half)
    def _():
        dy_out[...] = da_ref[...]

    @pl.when(pl.program_id(0) >= half)
    def _():
        dy_out[...] = db_ref[...]

    do_out[...] = mm_nt(dy_out[...], wo_ref[...]).astype(BF)


def dout(idx, da, db, w_o, bufs, seq):
    rows, d = da.shape
    bm, nb, a_map, b_map, o_map = two_source(rows)
    oc = w_o.shape[0] // 4
    in_specs = [pl.BlockSpec((bm, d), a_map), pl.BlockSpec((bm, d), b_map),
                pl.BlockSpec((oc, d), lambda i, s: at_row(s[2]))]
    args = [idx, da, db, w_o]
    aliases = {}
    if bufs is not None:
        in_specs += [ANY] * 2
        aliases = {len(args) + n: n for n in range(2)}
        args += list(bufs)
    return call(dout_body, (2 * nb,), in_specs, [pl.BlockSpec((bm, w), o_map) for w in (d, oc)],
                [sds(seq, w) for w in (d, oc)], args, 4 * rows * d * oc, aliases=aliases)


TASK = 4
HEADER = 3


def row_tasks(first, last):
    return [(i, i + 1, 1, -1) for i in range(first, last)]


def fwd_body(kind, s_ref, q_ref, k_ref, v_ref, *rest):
    qt, kk, vt, s_scr, acc, stat = rest[-6:]
    if kind == "rest":
        o1_ref, lse1_ref, st_ref, o_ref, lse_ref, hi_ref, pair_ref = rest[:7]
    else:
        o_ref, lse_ref = rest[:2]
    seq = k_ref.shape[0]

    def setup(c):
        sl = ds(c * BLK, BLK)
        vt[:, sl] = v_ref[sl, :].T
        kk[sl, :HEAD] = k_ref[sl, :]
        kk[sl, HEAD:] = k_ref[sl, :]
        for h in range(GROUP):
            qf = q_ref[sl, head_cols(h)].astype(F32) * SCALE2
            hi = qf.astype(BF)
            qt[h, :HEAD, sl] = hi.T
            qt[h, HEAD:, sl] = (qf - hi.astype(F32)).astype(BF).T

    loop(seq // BLK, setup)
    acc[...] = jnp.zeros_like(acc)
    stat[...] = jnp.zeros_like(stat)
    cur, old, den_row = 0, 1, 2
    lse_ref[...] = jnp.zeros_like(lse_ref)
    if kind == "rest":
        @pl.when(s_ref[1] == 0)
        def _():
            o_ref[:seq // 2, :] = o1_ref[...]
            lse_ref[0, :, :seq // 2] = lse1_ref[0]

    def task(t):
        return [s_ref[HEADER + t * TASK + n] for n in range(TASK)]

    def stage_a(h, i, j, masked, init=None):
        row = one(h)
        if masked is True:
            top = mm(kk[ds(j * BLK, HB), :], qt[h, :, ds(i * BLK, BLK)])
            low = mm(kk[ds(j * BLK + HB, HB), :], qt[h, :, ds(i * BLK + HB, HB)])
            top = jnp.where(down(top.shape) <= across(top.shape), top, NEG_LARGE)
            low = jnp.where(down(low.shape) <= across(low.shape), low, NEG_LARGE)
            s_scr[h, :HB, :] = top
            s_scr[h, HB:, HB:] = low
            m_new = jnp.max(top, axis=0, keepdims=True)
            right = jnp.maximum(m_new[:, HB:], jnp.max(low, axis=0, keepdims=True))
            m_new = jnp.concatenate([m_new[:, :HB], right], axis=1)
        else:
            s = mm(kk[ds(j * BLK, BLK), :], qt[h, :, ds(i * BLK, BLK)])
            if masked is not False:
                keep = down(s.shape) <= across(s.shape)
                s = jnp.where(jnp.logical_or(keep, jnp.logical_not(masked)), s, NEG_LARGE)
            s_scr[h] = s
            m_new = jnp.max(s, axis=0, keepdims=True)
        if init is None:
            m_old = stat[cur, row]
        elif kind == "rest":
            m_old = jnp.where(init >= 0, lse1_ref[0, row, ds(jnp.maximum(init, 0) * BLK, BLK)], NEG_LARGE)
        else:
            m_old = jnp.full(m_new.shape, NEG_LARGE, F32)
        m_new = jnp.maximum(m_old, m_new)
        stat[old, row] = jnp.exp2(m_old - m_new)
        stat[cur, row] = m_new

    def stage_p(h, diag=False):
        row = one(h)
        m, alpha = stat[cur, row], stat[old, row]
        if diag:
            top = jnp.exp2(s_scr[h, :HB, :] - m)
            low = jnp.exp2(s_scr[h, HB:, HB:] - m[:, HB:])
            total = jnp.sum(top, axis=0, keepdims=True)
            right = total[:, HB:] + jnp.sum(low, axis=0, keepdims=True)
            total = jnp.concatenate([total[:, :HB], right], axis=1)
            top = top.astype(BF)
            p = (top[:, :HB], jnp.concatenate([top[:, HB:], low.astype(BF)], axis=0))
        else:
            p = jnp.exp2(s_scr[h] - m)
            total = jnp.sum(p, axis=0, keepdims=True)
            p = p.astype(BF)
        stat[den_row, row] = stat[den_row, row] * alpha + total
        return p, alpha

    def stage_v(h, j, held, diag=False):
        p, alpha = held
        if diag:
            acc[h, :, :HB] = acc[h, :, :HB] * alpha[:, :HB] + mm(vt[:, ds(j * BLK, HB)], p[0])
            acc[h, :, HB:] = acc[h, :, HB:] * alpha[:, HB:] + mm(vt[:, ds(j * BLK, BLK)], p[1])
        else:
            acc[h] = acc[h] * alpha + mm(vt[:, ds(j * BLK, BLK)], p)

    def finish(h, i, den, top):
        row = one(h)
        out = acc[h] / den
        o_ref[ds(i * BLK, BLK), head_cols(h)] = out.T.astype(BF)
        lse_ref[0, row, ds(i * BLK, BLK)] = top + jnp.log2(den)
        if kind == "local":
            rest[2][0, h, :, ds(i * BLK, BLK)] = out

    def pipeline(i, j, masked):
        for h in range(GROUP):
            held = stage_p(h)
            stage_a(h, i, j + 1, masked)
            stage_v(h, j, held)

    count = s_ref[HEADER - 1]
    i, steps, diag, init = task(0)
    for h in range(GROUP):
        stage_a(h, i, 0, jnp.logical_and(steps == 1, diag == 1), init)

    def row(t):
        i, steps, diag, _ = task(t)

        loop(steps - 2, lambda j: pipeline(i, j, False))

        pl.when(jnp.logical_and(steps > 1, diag == 1))(lambda: pipeline(i, steps - 2, True))
        if kind == "rest":
            pl.when(diag == 0)(lambda: pipeline(i, steps - 2, False))
        i2, _, _, init2 = task(jnp.minimum(t + 1, count - 1))

        def last_step(on_diag):
            for h in range(GROUP):
                held = stage_p(h, on_diag)
                final = (stat[den_row, one(h)], stat[cur, one(h)])
                stage_a(h, i2, 0, False, init2)
                stage_v(h, steps - 1, held, on_diag)
                finish(h, i, *final)

        if kind != "rest":
            last_step(True)
        else:
            pl.when(diag == 1)(lambda: last_step(True))
            pl.when(diag == 0)(lambda: last_step(False))

            @pl.when(init2 >= 0)
            def _():
                stat[den_row] = jnp.ones(stat.shape[1:], F32)
                for h in range(GROUP):
                    acc[h] = st_ref[0, h, :, ds(init2 * BLK, BLK)]

    loop(count, row)
    if kind == "rest":
        hi_ref[...] = o_ref[seq - hi_ref.shape[0]:, :]
        pair_ref[...] = o_ref[ds(s_ref[0] * pair_ref.shape[0], pair_ref.shape[0]), :]


def attn_fwd(kind, idx, q, k, v, extra=(), local=()):
    whole = q.shape[0]
    seq = whole if kind == "rest" else whole // 2
    nkv = k.shape[1] // HEAD

    def half_map(g, s):
        return (s[1], g)

    def head_map(g, s):
        return (g, 0, 0)

    def state_map(g, s):
        return (g, 0, 0, 0)

    at = half_map if kind == "local" else col_map
    lse_spec = pl.BlockSpec((1, 8, seq), head_map)
    outs, specs = [sds(seq, q.shape[1]), jax.ShapeDtypeStruct((nkv, 8, seq), F32)], []
    out_specs = [pl.BlockSpec((seq, GW), col_map), lse_spec]
    state = pl.BlockSpec((1, GROUP, HEAD, whole // 2), state_map)
    if kind == "local":
        outs.append(jax.ShapeDtypeStruct((nkv, GROUP, HEAD, seq), F32))
        out_specs.append(state)
    if kind == "rest":
        specs = [pl.BlockSpec((seq // 2, GW), col_map), pl.BlockSpec((1, 8, seq // 2), head_map), state]
        outs += [sds(r, q.shape[1]) for r in extra]
        out_specs += [pl.BlockSpec((r, GW), col_map) for r in extra]
    kspec = pl.BlockSpec((seq, HEAD), at)
    return call(lambda *refs: fwd_body(kind, *refs), (nkv,), [pl.BlockSpec((seq, GW), at), kspec, kspec] + specs,
                out_specs, outs, [idx, q, k, v, *local], nkv * GROUP * seq * seq * PAIR,
                scratch=[pltpu.VMEM((GROUP, PAIR, seq), BF), pltpu.VMEM((seq, PAIR), BF),
                         pltpu.VMEM((HEAD, seq), BF), pltpu.VMEM((GROUP, BLK, BLK), F32),
                         pltpu.VMEM((GROUP, HEAD, BLK), F32), pltpu.VMEM((GROUP, 8, BLK), F32)])


def bwd_body(s_ref, q_ref, do_ref, o_ref, lse_ref, qn_ref, don_ref, on_ref, lsen_ref, k_ref, v_ref, cos_hbm, sin_hbm,
             out_ref, pair_ref, ka, va, dkt, dvt, tab, tab_sem, *sets):
    i = pl.program_id(0)
    last = pl.num_programs(0) - 1
    seq = k_ref.shape[0]
    m3 = GROUP * HB
    cos_ref, sin_ref = tab.at[0], tab.at[1]

    def spots():
        for b in range(2):
            for h in range(GROUP):
                start = (b * GROUP + h) * HB
                yield h, slice(b * HB, (b + 1) * HB), head_cols(h), slice(start, start + HB)

    def pick(n):
        return [ref.at[n] for ref in sets]

    def prepare(q_src, do_src, o_src, lse_src, dst):
        qa, da, q3t, do3t, dq3 = dst
        srow = down((16, HB))
        blank = jnp.zeros((HEAD - 16, HB), BF)
        for h, src, cols, rows in spots():
            qh, doh = q_src[src, cols], do_src[src, cols]
            qa[rows, :HEAD] = qh
            da[rows, :HEAD] = doh
            q3t[:, rows] = qh.T
            dt = doh.T
            do3t[:, rows] = dt
            delta = jnp.sum(dt.astype(F32) * o_src[src, cols].T.astype(F32), axis=0, keepdims=True)
            parts = jnp.zeros((16, HB), F32)
            for n, part in enumerate(split3(lse_src[0, one(h), src] * (1.0 / SCALE2)) + split3(delta)):
                parts = jnp.where(srow == n, part, parts)
            block = jnp.concatenate([parts.astype(BF), blank], axis=0).T
            qa[rows, HEAD:] = block
            da[rows, HEAD:] = block
        dq3[...] = jnp.zeros_like(dq3)

    @pl.when(i == 0)
    def _():
        copies = [pltpu.make_async_copy(src, tab.at[n], tab_sem.at[n]) for n, src in enumerate((cos_hbm, sin_hbm))]
        for copy in copies:
            copy.start()
        dkt[...] = jnp.zeros_like(dkt)
        dvt[...] = jnp.zeros_like(dvt)

        def setup(c):
            sl = ds(c * BLK, BLK)
            third = across((BLK, HEAD)) // 3
            for n, (src, dst) in enumerate(((k_ref, ka), (v_ref, va))):
                dst[sl, :HEAD] = src[sl, :]
                dst[sl, HEAD:] = jnp.where(third == n, -1.0, 0.0).astype(BF)

        loop(seq // BLK, setup)
        prepare(q_ref, do_ref, o_ref, lse_ref, pick(0))
        for copy in copies:
            copy.wait()

    def step(mine, rows, start, width, masked):
        qa, da, q3t, do3t, dq3 = mine
        sl = pl.ds(pl.multiple_of(start, BLK), width)
        s = mm_nt(qa[rows, :], ka[sl, :])
        dp = mm_nt(da[rows, :], va[sl, :])
        p = jnp.exp2(s * SCALE2)
        if masked:
            off = width - HB
            tail = p[:, off:]
            keep = down(tail.shape) % HB >= across(tail.shape)
            tail = jnp.where(keep, tail, 0.0)
            p = jnp.concatenate([p[:, :off], tail], axis=1) if off else tail
        dvt[:, sl] += mm(do3t[:, rows], p.astype(BF))
        dsv = (p * dp).astype(BF)
        dkt[:, sl] += mm(q3t[:, rows], dsv)
        dq3[rows, :] += mm(dsv, ka[sl, :HEAD])

    par, start = i % 2, (i // 2) * 2 * BLK
    loop(i // 2, lambda t: step(pick(par), slice(0, 2 * m3), t * 2 * BLK, 2 * BLK, False))

    def tail_steps(n):
        mine, width = pick(n), (n + 1) * BLK
        step(mine, slice(0, m3), start, width - HB, True)
        prepare(qn_ref, don_ref, on_ref, lsen_ref, pick(1 - n))
        step(mine, slice(m3, 2 * m3), start, width, True)
        for h, src, cols, rows in spots():
            rsl = ds(i * BLK + src.start, HB)
            out_ref[rsl, cols] = rotate(mine[-1][rows, :] * SCALE, cos_ref[rsl, :], -sin_ref[rsl, :]).astype(BF)

    pl.when(par == 0)(lambda: tail_steps(0))
    pl.when(par == 1)(lambda: tail_steps(1))

    @pl.when(i == last)
    def _():
        def fin(c):
            sl = ds(c * 2 * BLK, 2 * BLK)
            out_ref[sl, GW:QK] = rotate(dkt[:, sl].T * SCALE, cos_ref[sl, :], -sin_ref[sl, :]).astype(BF)
            out_ref[sl, QK:] = dvt[:, sl].T.astype(BF)

        loop(seq // BLK // 2, fin)
        pair_ref[...] = out_ref[ds(s_ref[0] * pair_ref.shape[0], pair_ref.shape[0]), :]


def attn_bwd(idx, q, do, o, k, v, lse, tabs, rows):
    seq = k.shape[0]
    nq = seq // BLK
    m3 = GROUP * BLK
    kspec = pl.BlockSpec((seq, HEAD), lambda i, s: at_col(s[1]))
    row_specs = []
    for ahead in range(2):
        row_specs += [pl.BlockSpec((BLK, GW), lambda i, s, a=ahead: (jnp.minimum(i + a, nq - 1), s[1]))] * 3
        row_specs += [pl.BlockSpec((1, 8, BLK), lambda i, s, a=ahead: (s[1], 0, jnp.minimum(i + a, nq - 1)))]
    two_sets = [pltpu.VMEM((2, m3, PAIR), BF)] * 2 + [pltpu.VMEM((2, HEAD, m3), BF)] * 2 + [pltpu.VMEM((2, m3, HEAD), F32)]
    return call(bwd_body, (nq,),
                row_specs + [kspec] * 2 + [ANY] * 2,
                [pl.BlockSpec((r, PW), first_row) for r in (seq, rows)], [sds(r, PW) for r in (seq, rows)],
                [idx] + [q, do, o, lse] * 2 + [k, v, *tabs], GROUP * nq * (nq + 1) * BLK * BLK * PW,
                scratch=[pltpu.VMEM((seq, PAIR), BF)] * 2 + [pltpu.VMEM((HEAD, seq), F32)] * 2
                + [pltpu.VMEM((2, seq, HEAD), F32), pltpu.SemaphoreType.DMA((2,))] + two_sets)


def half(i, s, n):
    return s[n] * 2 + i


def pick_body(s_ref, oa, ra, ob, rb, own, pair):
    for n, (low, high, out) in enumerate(((oa, ra, own), (ob, rb, pair))):
        out[...] = jnp.where(half(pl.program_id(0), s_ref, n) < s_ref[2], low[...], high[...])


def pick_rows(idx, low, high, rows):
    w = low.shape[1]
    specs = []
    for n in range(2):
        specs.append(pl.BlockSpec((BLK, w), lambda i, s, n=n: at_row(jnp.minimum(half(i, s, n), s[2] - 1))))
        specs.append(pl.BlockSpec((BLK, w), lambda i, s, n=n: at_row(jnp.maximum(half(i, s, n) - s[2], 0))))
    return call(pick_body, (rows // BLK,), specs, [pl.BlockSpec((BLK, w), row_map)] * 2, [sds(rows, w)] * 2,
                [idx, low, high, low, high], rows * w)


def out_body(s_ref, x_ref, *rest):
    ops, out_ref = rest[:-1], rest[-1]
    lhs = jnp.concatenate([r[...] for r in ops[:4]], axis=1)
    rhs = jnp.concatenate([r[...] for r in ops[4:]], axis=0)
    out_ref[...] = (x_ref[...].astype(F32) + mm(lhs, rhs)).astype(BF)


def out_proj(idx, x, pieces, w_o):
    rows, d = x.shape
    hw = pieces[0].shape[1]
    return call(out_body, (d // BLK,),
                [pl.BlockSpec((rows, BLK), col_map)]
                + [pl.BlockSpec((rows, hw), m) for m in (own_map, first_row, first_row, first_row)]
                + [pl.BlockSpec((hw, BLK), lambda n, s, p=p: (s[p], n)) for p in range(4)],
                pl.BlockSpec((rows, BLK), col_map), sds(rows, d), [idx, x, *pieces] + [w_o] * 4,
                2 * rows * d * d)


def dwo_body(s_ref, oa_ref, ob_ref, oc_ref, dy_ref, fin, snd, ot):
    first, hw = ob_ref.shape

    @pl.when(jnp.logical_and(pl.program_id(0) == 0, pl.program_id(1) == 0))
    def _():
        for src, rows, base in ((oa_ref, slice(0, hw), 0), (ob_ref, slice(hw, 2 * hw), 0), (oc_ref, slice(hw, 2 * hw), first)):
            def tr(c):
                ot[rows, ds(c * BLK + base, BLK)] = src[ds(c * BLK, BLK), :].T

            loop(src.shape[0] // BLK, tr)

    val = mm(ot[ds(pl.program_id(1) * hw, hw), :], dy_ref[...])
    fin[...] = val
    snd[...] = val


def dw_o(idx, oa, ob, oc, dy):
    seq, d = dy.shape
    hw = oa.shape[1]
    o_specs = [pl.BlockSpec((r, hw), lambda i, p, s: first_row(i, s), pipeline_mode=pl.Buffered(1))
               for r in (seq, seq - oc.shape[0], oc.shape[0])]
    return call(dwo_body, (d // BLK, 2),
                o_specs + [pl.BlockSpec((seq, BLK), lambda i, p, s: at_col(i))],
                [pl.BlockSpec((hw, BLK), lambda i, p, s: (s[p], i)), pl.BlockSpec((hw, BLK), lambda i, p, s: (p, i))],
                [sds(4 * hw, d, F32), sds(2 * hw, d, F32)], [idx, oa, ob, oc, dy], 4 * seq * d * hw,
                scratch=[pltpu.VMEM((2 * hw, seq), BF)])


def dwown_body(s_ref, h_ref, ga_ref, gb_ref, gc_ref, wo_ref, _, fq, fk, fv, snd, wo_fin, g3, ht, sem, wsem):
    i, steps = pl.program_id(0), pl.num_programs(0)
    rows, per = wo_ref.shape[0], steps // 2
    start = jnp.where(i < per, s_ref[1] * per + i, s_ref[3] * per + i - per)
    wcopy = pltpu.make_async_copy(wo_ref, wo_fin.at[ds(start * rows, rows), :], wsem)
    wcopy.start()

    @pl.when(i > 1)
    def _():
        for copy in scatter(snd, (fq, fk, fv), s_ref[0], s_ref[2], sem.at[i % 2]):
            copy.wait()

    ht[...] = h_ref[...].T
    lhs = ht[...]
    for g, q_at, k_at in ((ga_ref, 0, 2 * GW), (gb_ref, GW, 2 * GW + HEAD), (gc_ref, 2 * PW, 2 * PW + GW)):
        val = mm(lhs, g[:, :QK])
        snd[:, q_at:q_at + GW] = val[:, :GW]
        snd[:, k_at:k_at + HEAD] = val[:, GW:]
    snd[:, 2 * QK:2 * PW] = mm(lhs, jnp.concatenate([ga_ref[:, QK:], gb_ref[:, QK:]], axis=1))
    for copy in scatter(snd, (fq, fk, fv), s_ref[0], s_ref[2], sem.at[i % 2]):
        copy.start()

    @pl.when(i == steps - 1)
    def _():
        g3[...] = gc_ref[ds(s_ref[1] * g3.shape[0], g3.shape[0]), :]
        for slot in range(2):
            for copy in scatter(snd, (fq, fk, fv), s_ref[0], s_ref[2], sem.at[slot]):
                copy.wait()

    wcopy.wait()


def scatter(rcv, outs, whole_dev, part_dev, sem):
    rows, src, copies = ds(pl.program_id(0) * rcv.shape[0], rcv.shape[0]), 0, []
    fq, fk, fv = outs
    for n, (out, col, w) in enumerate(((fq, whole_dev, 2 * GW), (fk, whole_dev, PAIR), (fv, whole_dev, PAIR),
                                       (fq, 2 * part_dev, GW), (fk, 2 * part_dev, HEAD))):
        copies.append(pltpu.make_async_copy(rcv.at[:, src:src + w], out.at[rows, ds(col * w, w)], sem.at[n]))
        src += w
    return copies


def dw_own(idx, h, ga, gb, gc, wo_rcv, wo_fin):
    seq, d = h.shape
    steps = d // HB
    gspec = pl.BlockSpec((seq, PW), first_row, pipeline_mode=pl.Buffered(1))
    widths = (2 * GW, PAIR, PAIR)
    sw = 2 * PW + QK
    return call(dwown_body, (steps,),
                [pl.BlockSpec((seq, HB), col_map)] + [gspec] * 3
                + [pl.BlockSpec((wo_rcv.shape[0] // steps, d), row_map), ANY],
                [ANY] * 3 + [pl.BlockSpec((HB, sw), row_map), ANY, pl.BlockSpec((seq // 4, PW), first_row)],
                [sds(d, 4 * w, F32) for w in widths] + [sds(d, sw, F32), sds(*wo_fin.shape, F32), sds(seq // 4, PW)],
                [idx, h, ga, gb, gc, wo_rcv, wo_fin], 2 * seq * d * sw,
                scratch=[pltpu.VMEM((HB, seq), BF), pltpu.SemaphoreType.DMA((2, 5)), pltpu.SemaphoreType.DMA],
                aliases={6: 4})


def dwgrp_body(s_ref, h_ref, ga_ref, gb_ref, *rest):
    fq, fk, fv, snd, g3, ht = rest[-6:]

    @pl.when(pl.program_id(0) == 0)
    def _():
        g3[...] = gb_ref[ds(s_ref[1] * g3.shape[0], g3.shape[0]), :]

    ht[...] = h_ref[...].T
    lhs = ht[...]
    val = mm(lhs, gb_ref[:, :QK])
    fq[...] = val[:, :GW]
    fk[...] = val[:, GW:]
    snd[:, :QK] = val
    val = mm(lhs, jnp.concatenate([ga_ref[...], gb_ref[:, QK:]], axis=1))
    fv[...] = val
    snd[:, QK:] = val


def group_specs(bm):
    return [pl.BlockSpec((bm, w), lambda i, s: (i, 2 * s[0] + 1)) for w in (GW, HEAD)] + \
        [pl.BlockSpec((bm, PAIR), lambda i, s: (i, s[0]))]


def dw_group(idx, h, ga, gb, bufs):
    seq, d = h.shape
    gspec = pl.BlockSpec((seq, PW), first_row, pipeline_mode=pl.Buffered(1))
    sw = QK + PAIR
    return call(dwgrp_body, (d // HB,),
                [pl.BlockSpec((seq, HB), col_map),
                 pl.BlockSpec((seq, HEAD), lambda i, s: at_col(QK // HEAD), pipeline_mode=pl.Buffered(1)), gspec] + [ANY] * 3,
                group_specs(HB) + [pl.BlockSpec((HB, sw), row_map), pl.BlockSpec((seq // 4, PW), first_row)],
                [sds(*b.shape, F32) for b in bufs] + [sds(d, sw, F32), sds(seq // 4, PW)],
                [idx, h, ga, gb, *bufs], 2 * seq * d * sw, scratch=[pltpu.VMEM((HB, seq), BF)],
                aliases={4 + n: n for n in range(3)})


def place_body(s_ref, rcv, *rest):
    q_out, k_out, v_out = rest[-3:]
    q_out[...] = rcv[:, :GW]
    k_out[...] = rcv[:, GW:QK]
    v_out[...] = rcv[:, QK:]


def place(idx, rcv, bufs):
    d, w = rcv.shape
    bm = BLK
    return call(place_body, (d // bm,), [pl.BlockSpec((bm, w), row_map)] + [ANY] * 3, group_specs(bm),
                [sds(*b.shape, F32) for b in bufs], [idx, rcv, *bufs], d * w, aliases={2 + n: n for n in range(3)})


def dx_body(s_ref, x_ref, dy_ref, gain_ref, inv_ref, *rest):
    pieces, weights, rcv = rest[:8], rest[8:20], rest[20]
    dx_ref, dg_ref, fq, fk, fv, acc, xs, tot, sem = rest[-9:]
    n = pl.program_id(0)
    bn = x_ref.shape[1]
    rows, d = acc.shape
    copies = scatter(rcv, (fq, fk, fv), s_ref[1], s_ref[3], sem)
    for copy in copies:
        copy.start()

    @pl.when(n == 0)
    def _():
        tot[...] = jnp.zeros_like(tot)

    cuts = (slice(0, GW), slice(GW, QK), slice(QK, PW))
    lhs = jnp.concatenate([pieces[2 * p + g][:, c] for p in range(4) for c in cuts for g in range(2)], axis=1)
    rhs = jnp.concatenate([r[...] for r in weights], axis=1)
    dh = mm_nt(lhs, rhs)
    inv = inv_ref[...]
    for c in range(bn // HEAD):
        cols = head_cols(c)
        xb = x_ref[:, cols]
        xs[:, ds(n * bn + cols.start, HEAD)] = xb
        part, xf = dh[:, cols], xb.astype(F32)
        scaled = part * gain_ref[:, cols]
        tot[...] += scaled * xf
        acc[:, ds(n * bn + cols.start, HEAD)] = dy_ref[:, cols].astype(F32) + inv * scaled
        dg_ref[:, cols] = jnp.sum((part * (xf * inv)).reshape(rows // 8, 8, HEAD), axis=0)

    @pl.when(n == pl.num_programs(0) - 1)
    def _():
        step = HEAD // 2

        def stats(r):
            sl = ds(r * step, step)
            inv = inv_ref[sl, :]
            tot[sl, :] = jnp.broadcast_to(jnp.sum(tot[sl, :], axis=-1, keepdims=True) / d, (step, HEAD)) * inv * inv * inv

        loop(rows // step, stats)

        def epi(r):
            sl = ds(r * step, step)
            coef = tot[sl, :]
            for c in range(d // HEAD):
                cols = head_cols(c)
                dx_ref[sl, cols] = (acc[sl, cols] - xs[sl, cols].astype(F32) * coef).astype(BF)

        loop(rows // step, epi)

    for copy in copies:
        copy.wait()


def dx_call(idx, x, dy, gain, inv, pieces, ws, rcv, bufs):
    rows, d = x.shape
    bn = HB
    once = pl.Buffered(1)
    maps = (own_map, own_map, first_row, first_row) * 2
    return call(dx_body, (d // bn,),
                [pl.BlockSpec((rows, bn), col_map)] * 2 + [pl.BlockSpec((1, bn), col_map), pl.BlockSpec((rows, HEAD), own_map)]
                + [pl.BlockSpec((rows, PW), m, pipeline_mode=once) for m in maps]
                + [pl.BlockSpec((bn, w.shape[1] // 4), lambda n, s, p=p: (n, s[p])) for p in range(4) for w in ws]
                + [pl.BlockSpec((bn, rcv.shape[1]), row_map)] + [ANY] * 3,
                [pl.BlockSpec((rows, d), first_row, pipeline_mode=once), pl.BlockSpec((8, bn), col_map)] + [ANY] * 3,
                [sds(rows, d), sds(8, d, F32)] + [sds(*b.shape, F32) for b in bufs],
                [idx, x, dy, gain, inv, *pieces] + list(ws) * 4 + [rcv, *bufs], 16 * rows * d * PW,
                scratch=[pltpu.VMEM((rows, d), F32), pltpu.VMEM((rows, d), BF), pltpu.VMEM((rows, HEAD), F32),
                         pltpu.SemaphoreType.DMA((5,))],
                aliases={26 + n: 2 + n for n in range(3)})


def solution(mesh):
    sp = mesh.shape['sp']
    cross = [(a, a ^ 2) for a in range(sp)]
    pair = [(a, a ^ 1) for a in range(sp)]

    def over(val):
        return lax.ppermute(val, 'sp', cross)

    def near(val):
        return lax.ppermute(val, 'sp', pair)

    def both(val):
        return lax.ppermute(val, 'sp', [(a, a ^ 3) for a in range(sp)])

    def after(val, *deps):
        return lax.optimization_barrier((val,) + deps)[0]

    def vec(*vals, dep=()):
        out = jnp.stack([jnp.asarray(v, jnp.int32) for v in vals])
        return after(out, *dep) if dep else out

    def step(x, dy, positions, gain, w_q, w_k, w_v, w_o):
        j = lax.axis_index('sp').astype(jnp.int32)
        rows, d = x.shape
        seq = rows * sp
        j1, j2, j3 = [j ^ n for n in (1, 2, 3)]
        dev = (j, j1, j2, j3)
        bpr, hpr = rows // BLK, rows // HB
        ws = (w_q, w_k, w_v)

        gain_f = gain.astype(F32).reshape(1, d)

        pieces = ((BLK, HB), (0, BLK), (BLK + HB, HB))
        first_piece = x[BLK:BLK + HB]
        positions = after(positions, first_piece)
        pos2 = over(positions)
        pos1 = near(positions)
        x2 = []
        for n, (start, size) in enumerate(pieces):
            x2.append(over(after(x, first_piece)[start:start + size] if n else first_piece))
        x1 = near(x)
        pos3 = near(pos2)
        dy1 = near(after(dy, x1))

        pos = jnp.zeros((seq,), jnp.int32)
        for blk, val in zip(dev, (positions, pos1, pos2, pos3)):
            pos = lax.dynamic_update_slice(pos, val, (blk * rows,))
        inv_freq = ROPE_THETA ** (-jnp.arange(0, HEAD, 2).astype(F32) / HEAD)
        angles = pos.astype(F32)[:, None] * inv_freq[None, :]
        cos_h, sin_h = jnp.cos(angles), jnp.sin(angles)
        tabs = (jnp.concatenate([cos_h, cos_h], axis=1), jnp.concatenate([-sin_h, sin_h], axis=1))

        cut = rows - HB
        dya, dyb = dy[:cut], dy[cut:]
        bufs = project(vec(j * bpr, j1 * bpr, j, dep=(dya, dyb)), x, x1, gain_f, ws, tabs, None, seq)
        dbufs = dout(vec(j * bpr, j1 * bpr, j, dep=bufs), dy, dy1, w_o, None, seq)

        chip, nh = j // 2, seq // BLK // 2
        tri = row_tasks(0, nh)
        first = seq // 2 - BLK
        square = [(i + nh, nh, 0, i) for i in range(nh)]

        def table(head, tasks):
            return jnp.concatenate([vec(*head, len(tasks)), jnp.asarray(tasks, jnp.int32).reshape(-1)])

        c_tasks = table((j1, 0), tri).at[HEADER - 1].set(nh - 1)
        local = attn_fwd("local", after(table((j1, chip), tri), *dbufs), *bufs[1:4])
        rest_tasks = jnp.where(chip == 0, table((j1, 0), row_tasks(nh, 2 * nh) * 2).at[HEADER - 1].set(nh),
                               table((j1, 1), tri + square))

        dy2a = over(after(dya, *bufs))
        dy2b = over(after(dyb, *bufs))
        deps, done = [tuple(bufs), tuple(local)], tuple(local)
        for n, (start, size) in enumerate(pieces):
            got = after(x2[n], *(deps[n] if n < len(deps) else done))
            x3 = near(got)
            idx = vec(*((dev * rows + start) // size for dev in (j2, j3)), j, dep=done)
            bufs = project(idx, got, x3, gain_f, ws, tabs, bufs, seq)
            done = tuple(bufs)
        h_all, q, k, v, inv = bufs
        o, lse, o_hi, o_pair = attn_fwd("rest", rest_tasks, q, k, v, (seq - first, rows), local)
        orv = over(o_hi)
        o1 = near(o_pair)
        qc, kc, vc = project_first(vec(j2, dep=(o,)), h_all, ws, tabs, first)
        dy2a = after(dy2a, qc)
        dy3a = near(dy2a)
        oc = attn_fwd("local", c_tasks, qc, kc, vc)[0]

        dbufs = dout(vec(j2 * hpr, j3 * hpr, j, dep=(oc,)), dy2a, dy3a, w_o, dbufs, seq)
        dy2b = after(dy2b, *dbufs)
        dy3b = near(dy2b)
        dbufs = dout(vec((j2 + 1) * hpr - 1, (j3 + 1) * hpr - 1, j), dy2b, dy3b, w_o, dbufs, seq)
        dy_all, do = dbufs

        ga, ga_pair = attn_bwd(vec(j1, 0), q, do, o, k, v, lse, tabs, rows)
        ga2 = over(ga)
        ga1 = near(ga_pair)
        gb, gb_pair = attn_bwd(vec(j1, 1, dep=(ga,)), q, do, o, k, v, lse, tabs, rows)
        gb2 = over(gb)
        gb1 = near(gb_pair)

        orv = after(orv, gb)
        ox, ox_pair = pick_rows(vec(j, j1, nh - 1, dep=(gb,)), oc, orv, rows)
        o3 = near(ox_pair)
        wo_fin, wo_snd = dw_o(vec(j, j2, dep=(gb,)), o, oc, orv, dy_all)
        wo_rcv = near(wo_snd)
        result = out_proj(vec(*dev, dep=(wo_snd,)), x, (o, o1, ox, o3), w_o)
        ga2 = after(ga2, wo_snd)
        fq, fk, fv, snd, wo_fin, g3 = dw_own(vec(*dev, dep=(result,)), h_all, ga, gb, ga2, wo_rcv, wo_fin)
        rcv = near(snd)
        ga3 = near(g3)

        gb2 = after(gb2, snd)
        fq, fk, fv, snd_b, g3b = dw_group(vec(j2, j1), h_all, ga2, gb2, (fq, fk, fv))
        gb3 = near(g3b)
        rcv_b = near(snd_b)
        grad_x, dg, fq, fk, fv = dx_call(vec(*dev, dep=(snd_b,)), x, dy, gain_f, inv,
                                         (ga, gb, ga1, gb1, ga2, gb2, ga3, gb3), ws, rcv, (fq, fk, fv))
        dg = jnp.sum(dg, axis=0)
        dg = (dg + near(dg)) + (over(dg) + both(dg))
        fq, fk, fv = place(vec(j3), rcv_b, (fq, fk, fv))
        return result, grad_x, fq, fk, fv, wo_fin, dg

    seq_spec = P(('dp', 'sp'), None)
    whole = P(None, None)
    part_rows = P('dp', None)
    return jax.shard_map(step, mesh=mesh,
                         in_specs=(seq_spec, seq_spec, P(('dp', 'sp')), P(None), whole, whole, whole, whole),
                         out_specs=(seq_spec, seq_spec, part_rows, part_rows, part_rows, part_rows, P('dp')),
                         check_vma=False)
```

```python
import math

import jax
import jax.numpy as jnp
from jax import lax
from jax.experimental import pallas as pl
from jax.experimental.pallas import tpu as pltpu
from jax.sharding import PartitionSpec as P


HEAD = 128
GROUP = 3
GW = GROUP * HEAD
QK = GW + HEAD
PW = QK + HEAD
PAIR = 2 * HEAD
ROPE_THETA = 1000000.0
NORM_EPS = 1e-05
NEG_LARGE = -1e30
BF = jnp.bfloat16
F32 = jnp.float32
SCALE = HEAD ** -0.5
SCALE2 = SCALE * math.log2(math.e)
BLK = 512
HB = BLK // 2
VMEM_LIMIT = 65011712
ANY = pl.BlockSpec(memory_space=pl.ANY)


def first_row(i, s):
    return (0, 0)


def at_row(r):
    return (r, 0)


def at_col(c):
    return (0, c)


def row_map(i, s):
    return at_row(i)


def col_map(i, s):
    return at_col(i)


def own_map(i, s):
    return at_row(s[0])


def sds(rows, cols, dtype=BF):
    return jax.ShapeDtypeStruct((rows, cols), dtype)


def call(body, grid, in_specs, out_specs, out_shape, args, flops, scratch=(), aliases=None):
    return pl.pallas_call(
        body,
        grid_spec=pltpu.PrefetchScalarGridSpec(
            num_scalar_prefetch=1, grid=grid, in_specs=in_specs, out_specs=out_specs, scratch_shapes=list(scratch)),
        out_shape=out_shape, input_output_aliases=aliases or {},
        compiler_params=pltpu.CompilerParams(dimension_semantics=("arbitrary",) * len(grid),
                                             vmem_limit_bytes=VMEM_LIMIT),
        cost_estimate=pl.CostEstimate(flops=int(flops), bytes_accessed=int(flops) // BLK,
                                      transcendentals=0))(*args)


def down(shape):
    return lax.broadcasted_iota(jnp.int32, shape, 0)


def across(shape):
    return lax.broadcasted_iota(jnp.int32, shape, 1)


def loop(count, body):
    def run(c, _):
        body(c)
        return 0

    lax.fori_loop(0, count, run, 0)


def one(h):
    return slice(h, h + 1)


def head_cols(h):
    return slice(h * HEAD, h * HEAD + HEAD)


def mm(a, b):
    return jnp.dot(a, b, preferred_element_type=F32)


def mm_nt(a, b):
    return lax.dot_general(a, b, (((1,), (1,)), ((), ())), preferred_element_type=F32)


def rotate(val, cos_t, sin_t):
    return val * cos_t + pltpu.roll(val, HEAD // 2, 1) * sin_t


def ds(start, size):
    return pl.ds(pl.multiple_of(start, size), size)


def split3(val):
    hi = val.astype(BF).astype(F32)
    mid = (val - hi).astype(BF).astype(F32)
    return hi, mid, val - hi - mid


def qkv_of(h, wq_ref, wk_ref, wv_ref, cos_ref, sin_ref, q_ref, k_ref, v_ref):
    cos_t, sin_t = cos_ref[...], sin_ref[...]
    out = mm(h, wq_ref[...])
    for c in range(wq_ref.shape[1] // HEAD):
        sl = head_cols(c)
        q_ref[:, sl] = rotate(out[:, sl], cos_t, sin_t).astype(BF)
    out = mm(h, jnp.concatenate([wk_ref[...], wv_ref[...]], axis=1))
    for sl in (slice(0, HEAD), slice(HEAD, PAIR)):
        k_ref[:, sl] = rotate(out[:, sl], cos_t, sin_t).astype(BF)
    v_ref[...] = out[:, PAIR:].astype(BF)


def proj_body(s_ref, xa_ref, xb_ref, gain_ref, wq_ref, wk_ref, wv_ref, cos_ref, sin_ref, *rest):
    h_ref, q_ref, k_ref, v_ref, inv_ref = rest[-5:]
    half = pl.num_programs(0) // 2

    def norm(src):
        step = HEAD

        def stats(c):
            sl = ds(c * step, step)
            xf = src[sl, :].astype(F32)
            inv = lax.rsqrt(jnp.mean(xf * xf, axis=-1, keepdims=True) + NORM_EPS)
            inv_ref[sl, :] = jnp.broadcast_to(inv, (step, HEAD))

        def scale(c):
            sl = ds(c * step, step)
            inv, gain = inv_ref[sl, :], gain_ref[...]
            for n in range(src.shape[1] // HEAD):
                cols = head_cols(n)
                h_ref[sl, cols] = (src[sl, cols].astype(F32) * inv * gain[:, cols]).astype(BF)

        loop(src.shape[0] // step, stats)
        loop(src.shape[0] // step, scale)

    @pl.when(pl.program_id(0) < half)
    def _():
        norm(xa_ref)

    @pl.when(pl.program_id(0) >= half)
    def _():
        norm(xb_ref)

    qkv_of(h_ref[...], wq_ref, wk_ref, wv_ref, cos_ref, sin_ref, q_ref, k_ref, v_ref)


def two_source(rows):
    bm = HB
    nb = rows // bm

    def a_map(i, s):
        return at_row(jnp.minimum(i, nb - 1))

    def b_map(i, s):
        return at_row(jnp.maximum(i - nb, 0))

    def o_map(i, s):
        return at_row(jnp.where(i < nb, s[0] + i, s[1] + i - nb))

    return bm, nb, a_map, b_map, o_map


def project(idx, xa, xb, gain, ws, tabs, bufs, seq):
    rows, d = xa.shape
    bm, nb, a_map, b_map, o_map = two_source(rows)
    widths = [w.shape[1] // 4 for w in ws]
    in_specs = [pl.BlockSpec((bm, d), a_map), pl.BlockSpec((bm, d), b_map), pl.BlockSpec((1, d), first_row)]
    in_specs += [pl.BlockSpec((d, w), lambda i, s: at_col(s[2])) for w in widths]
    in_specs += [pl.BlockSpec((bm, HEAD), o_map)] * 2
    args = [idx, xa, xb, gain, *ws, *tabs]
    aliases = {}
    if bufs is not None:
        in_specs += [ANY] * len(bufs)
        aliases = {len(args) + n: n for n in range(len(bufs))}
        args += list(bufs)
    return call(proj_body, (2 * nb,), in_specs, [pl.BlockSpec((bm, w), o_map) for w in (d, *widths, HEAD)],
                [sds(seq, w) for w in (d, *widths)] + [sds(seq, HEAD, F32)], args, 4 * rows * d * sum(widths),
                aliases=aliases)


def projc_body(s_ref, h_ref, *rest):
    qkv_of(h_ref[...], *rest)


def project_first(idx, h, ws, tabs, rows):
    seq, d = h.shape
    widths = [w.shape[1] // 4 for w in ws]
    return call(projc_body, (rows // BLK,),
                [pl.BlockSpec((BLK, d), row_map)] + [pl.BlockSpec((d, w), lambda i, s: at_col(s[0])) for w in widths]
                + [pl.BlockSpec((BLK, HEAD), row_map)] * 2,
                [pl.BlockSpec((BLK, w), row_map) for w in widths], [sds(seq, w) for w in widths],
                [idx, h, *ws, *tabs], 2 * rows * d * sum(widths))


def dout_body(s_ref, da_ref, db_ref, wo_ref, *rest):
    dy_out, do_out = rest[-2:]
    half = pl.num_programs(0) // 2

    @pl.when(pl.program_id(0) < half)
    def _():
        dy_out[...] = da_ref[...]

    @pl.when(pl.program_id(0) >= half)
    def _():
        dy_out[...] = db_ref[...]

    do_out[...] = mm_nt(dy_out[...], wo_ref[...]).astype(BF)


def dout(idx, da, db, w_o, bufs, seq):
    rows, d = da.shape
    bm, nb, a_map, b_map, o_map = two_source(rows)
    oc = w_o.shape[0] // 4
    in_specs = [pl.BlockSpec((bm, d), a_map), pl.BlockSpec((bm, d), b_map),
                pl.BlockSpec((oc, d), lambda i, s: at_row(s[2]))]
    args = [idx, da, db, w_o]
    aliases = {}
    if bufs is not None:
        in_specs += [ANY] * 2
        aliases = {len(args) + n: n for n in range(2)}
        args += list(bufs)
    return call(dout_body, (2 * nb,), in_specs, [pl.BlockSpec((bm, w), o_map) for w in (d, oc)],
                [sds(seq, w) for w in (d, oc)], args, 4 * rows * d * oc, aliases=aliases)


TASK = 4
HEADER = 3


def row_tasks(first, last):
    return [(i, i + 1, 1, -1) for i in range(first, last)]


def fwd_body(kind, s_ref, q_ref, k_ref, v_ref, *rest):
    qt, kk, vt, s_scr, acc, stat = rest[-6:]
    if kind == "rest":
        o1_ref, lse1_ref, st_ref, o_ref, lse_ref, hi_ref, pair_ref = rest[:7]
    else:
        o_ref, lse_ref = rest[:2]
    seq = k_ref.shape[0]

    def setup(c):
        sl = ds(c * BLK, BLK)
        vt[:, sl] = v_ref[sl, :].T
        kk[sl, :HEAD] = k_ref[sl, :]
        kk[sl, HEAD:] = k_ref[sl, :]
        for h in range(GROUP):
            qf = q_ref[sl, head_cols(h)].astype(F32) * SCALE2
            hi = qf.astype(BF)
            qt[h, :HEAD, sl] = hi.T
            qt[h, HEAD:, sl] = (qf - hi.astype(F32)).astype(BF).T

    loop(seq // BLK, setup)
    acc[...] = jnp.zeros_like(acc)
    stat[...] = jnp.zeros_like(stat)
    cur, old, den_row = 0, 1, 2
    lse_ref[...] = jnp.zeros_like(lse_ref)
    if kind == "rest":
        @pl.when(s_ref[1] == 0)
        def _():
            o_ref[:seq // 2, :] = o1_ref[...]
            lse_ref[0, :, :seq // 2] = lse1_ref[0]

    def task(t):
        return [s_ref[HEADER + t * TASK + n] for n in range(TASK)]

    def stage_a(h, i, j, masked, init=None):
        row = one(h)
        if masked is True:
            top = mm(kk[ds(j * BLK, HB), :], qt[h, :, ds(i * BLK, BLK)])
            low = mm(kk[ds(j * BLK + HB, HB), :], qt[h, :, ds(i * BLK + HB, HB)])
            top = jnp.where(down(top.shape) <= across(top.shape), top, NEG_LARGE)
            low = jnp.where(down(low.shape) <= across(low.shape), low, NEG_LARGE)
            s_scr[h, :HB, :] = top
            s_scr[h, HB:, HB:] = low
            m_new = jnp.max(top, axis=0, keepdims=True)
            right = jnp.maximum(m_new[:, HB:], jnp.max(low, axis=0, keepdims=True))
            m_new = jnp.concatenate([m_new[:, :HB], right], axis=1)
        else:
            s = mm(kk[ds(j * BLK, BLK), :], qt[h, :, ds(i * BLK, BLK)])
            if masked is not False:
                keep = down(s.shape) <= across(s.shape)
                s = jnp.where(jnp.logical_or(keep, jnp.logical_not(masked)), s, NEG_LARGE)
            s_scr[h] = s
            m_new = jnp.max(s, axis=0, keepdims=True)
        if init is None:
            m_old = stat[cur, row]
        elif kind == "rest":
            m_old = jnp.where(init >= 0, lse1_ref[0, row, ds(jnp.maximum(init, 0) * BLK, BLK)], NEG_LARGE)
        else:
            m_old = jnp.full(m_new.shape, NEG_LARGE, F32)
        m_new = jnp.maximum(m_old, m_new)
        stat[old, row] = jnp.exp2(m_old - m_new)
        stat[cur, row] = m_new

    def stage_p(h, diag=False):
        row = one(h)
        m, alpha = stat[cur, row], stat[old, row]
        if diag:
            top = jnp.exp2(s_scr[h, :HB, :] - m)
            low = jnp.exp2(s_scr[h, HB:, HB:] - m[:, HB:])
            total = jnp.sum(top, axis=0, keepdims=True)
            right = total[:, HB:] + jnp.sum(low, axis=0, keepdims=True)
            total = jnp.concatenate([total[:, :HB], right], axis=1)
            top = top.astype(BF)
            p = (top[:, :HB], jnp.concatenate([top[:, HB:], low.astype(BF)], axis=0))
        else:
            p = jnp.exp2(s_scr[h] - m)
            total = jnp.sum(p, axis=0, keepdims=True)
            p = p.astype(BF)
        stat[den_row, row] = stat[den_row, row] * alpha + total
        return p, alpha

    def stage_v(h, j, held, diag=False):
        p, alpha = held
        if diag:
            acc[h, :, :HB] = acc[h, :, :HB] * alpha[:, :HB] + mm(vt[:, ds(j * BLK, HB)], p[0])
            acc[h, :, HB:] = acc[h, :, HB:] * alpha[:, HB:] + mm(vt[:, ds(j * BLK, BLK)], p[1])
        else:
            acc[h] = acc[h] * alpha + mm(vt[:, ds(j * BLK, BLK)], p)

    def finish(h, i, den, top):
        row = one(h)
        out = acc[h] / den
        o_ref[ds(i * BLK, BLK), head_cols(h)] = out.T.astype(BF)
        lse_ref[0, row, ds(i * BLK, BLK)] = top + jnp.log2(den)
        if kind == "local":
            rest[2][0, h, :, ds(i * BLK, BLK)] = out

    def pipeline(i, j, masked):
        for h in range(GROUP):
            held = stage_p(h)
            stage_a(h, i, j + 1, masked)
            stage_v(h, j, held)

    count = s_ref[HEADER - 1]
    i, steps, diag, init = task(0)
    for h in range(GROUP):
        stage_a(h, i, 0, jnp.logical_and(steps == 1, diag == 1), init)

    def row(t):
        i, steps, diag, _ = task(t)

        loop(steps - 2, lambda j: pipeline(i, j, False))

        pl.when(jnp.logical_and(steps > 1, diag == 1))(lambda: pipeline(i, steps - 2, True))
        if kind == "rest":
            pl.when(diag == 0)(lambda: pipeline(i, steps - 2, False))
        i2, _, _, init2 = task(jnp.minimum(t + 1, count - 1))

        def last_step(on_diag):
            for h in range(GROUP):
                held = stage_p(h, on_diag)
                final = (stat[den_row, one(h)], stat[cur, one(h)])
                stage_a(h, i2, 0, False, init2)
                stage_v(h, steps - 1, held, on_diag)
                finish(h, i, *final)

        if kind != "rest":
            last_step(True)
        else:
            pl.when(diag == 1)(lambda: last_step(True))
            pl.when(diag == 0)(lambda: last_step(False))

            @pl.when(init2 >= 0)
            def _():
                stat[den_row] = jnp.ones(stat.shape[1:], F32)
                for h in range(GROUP):
                    acc[h] = st_ref[0, h, :, ds(init2 * BLK, BLK)]

    loop(count, row)
    if kind == "rest":
        hi_ref[...] = o_ref[seq - hi_ref.shape[0]:, :]
        pair_ref[...] = o_ref[ds(s_ref[0] * pair_ref.shape[0], pair_ref.shape[0]), :]


def attn_fwd(kind, idx, q, k, v, extra=(), local=()):
    whole = q.shape[0]
    seq = whole if kind == "rest" else whole // 2
    nkv = k.shape[1] // HEAD

    def half_map(g, s):
        return (s[1], g)

    def head_map(g, s):
        return (g, 0, 0)

    def state_map(g, s):
        return (g, 0, 0, 0)

    at = half_map if kind == "local" else col_map
    lse_spec = pl.BlockSpec((1, 8, seq), head_map)
    outs, specs = [sds(seq, q.shape[1]), jax.ShapeDtypeStruct((nkv, 8, seq), F32)], []
    out_specs = [pl.BlockSpec((seq, GW), col_map), lse_spec]
    state = pl.BlockSpec((1, GROUP, HEAD, whole // 2), state_map)
    if kind == "local":
        outs.append(jax.ShapeDtypeStruct((nkv, GROUP, HEAD, seq), F32))
        out_specs.append(state)
    if kind == "rest":
        specs = [pl.BlockSpec((seq // 2, GW), col_map), pl.BlockSpec((1, 8, seq // 2), head_map), state]
        outs += [sds(r, q.shape[1]) for r in extra]
        out_specs += [pl.BlockSpec((r, GW), col_map) for r in extra]
    kspec = pl.BlockSpec((seq, HEAD), at)
    return call(lambda *refs: fwd_body(kind, *refs), (nkv,), [pl.BlockSpec((seq, GW), at), kspec, kspec] + specs,
                out_specs, outs, [idx, q, k, v, *local], nkv * GROUP * seq * seq * PAIR,
                scratch=[pltpu.VMEM((GROUP, PAIR, seq), BF), pltpu.VMEM((seq, PAIR), BF),
                         pltpu.VMEM((HEAD, seq), BF), pltpu.VMEM((GROUP, BLK, BLK), F32),
                         pltpu.VMEM((GROUP, HEAD, BLK), F32), pltpu.VMEM((GROUP, 8, BLK), F32)])


def bwd_body(s_ref, q_ref, do_ref, o_ref, lse_ref, qn_ref, don_ref, on_ref, lsen_ref, k_ref, v_ref, cos_hbm, sin_hbm,
             out_ref, pair_ref, ka, va, dkt, dvt, tab, tab_sem, *sets):
    i = pl.program_id(0)
    last = pl.num_programs(0) - 1
    seq = k_ref.shape[0]
    m3 = GROUP * HB
    cos_ref, sin_ref = tab.at[0], tab.at[1]

    def spots():
        for b in range(2):
            for h in range(GROUP):
                start = (b * GROUP + h) * HB
                yield h, slice(b * HB, b * HB + HB), head_cols(h), slice(start, start + HB)

    def pick(n):
        return [ref.at[n] for ref in sets]

    def prepare(q_src, do_src, o_src, lse_src, dst):
        qa, da, q3t, do3t, dq3 = dst
        srow = down((16, HB))
        blank = jnp.zeros((HEAD - 16, HB), BF)
        for h, src, cols, rows in spots():
            qh, doh = q_src[src, cols], do_src[src, cols]
            qa[rows, :HEAD] = qh
            da[rows, :HEAD] = doh
            q3t[:, rows] = qh.T
            dt = doh.T
            do3t[:, rows] = dt
            delta = jnp.sum(dt.astype(F32) * o_src[src, cols].T.astype(F32), axis=0, keepdims=True)
            parts = jnp.zeros((16, HB), F32)
            for n, part in enumerate(split3(lse_src[0, one(h), src] * (1.0 / SCALE2)) + split3(delta)):
                parts = jnp.where(srow == n, part, parts)
            block = jnp.concatenate([parts.astype(BF), blank], axis=0).T
            qa[rows, HEAD:] = block
            da[rows, HEAD:] = block
        dq3[...] = jnp.zeros_like(dq3)

    @pl.when(i == 0)
    def _():
        copies = [pltpu.make_async_copy(src, tab.at[n], tab_sem.at[n]) for n, src in enumerate((cos_hbm, sin_hbm))]
        for copy in copies:
            copy.start()
        dkt[...] = jnp.zeros_like(dkt)
        dvt[...] = jnp.zeros_like(dvt)

        def setup(c):
            sl = ds(c * BLK, BLK)
            third = across((BLK, HEAD)) // 3
            for n, (src, dst) in enumerate(((k_ref, ka), (v_ref, va))):
                dst[sl, :HEAD] = src[sl, :]
                dst[sl, HEAD:] = jnp.where(third == n, -1.0, 0.0).astype(BF)

        loop(seq // BLK, setup)
        prepare(q_ref, do_ref, o_ref, lse_ref, pick(0))
        for copy in copies:
            copy.wait()

    def scores(mine, rows, start, width):
        sl = pl.ds(pl.multiple_of(start, BLK), width)
        return rows, sl, width, mm_nt(mine[0][rows, :], ka[sl, :]), mm_nt(mine[1][rows, :], va[sl, :])

    def grads(mine, held, masked):
        _, _, q3t, do3t, dq3 = mine
        rows, sl, width, s, dp = held
        p = jnp.exp2(s * SCALE2)
        if masked:
            off = width - HB
            tail = p[:, off:]
            keep = down(tail.shape) % HB >= across(tail.shape)
            tail = jnp.where(keep, tail, 0.0)
            p = jnp.concatenate([p[:, :off], tail], axis=1) if off else tail
        dvt[:, sl] += mm(do3t[:, rows], p.astype(BF))
        dsv = (p * dp).astype(BF)
        dkt[:, sl] += mm(q3t[:, rows], dsv)
        dq3[rows, :] += mm(dsv, ka[sl, :HEAD])

    par, start = i % 2, (i // 2) * 2 * BLK

    def pair_step(t):
        mine = pick(par)
        grads(mine, scores(mine, slice(0, 2 * m3), t * 2 * BLK, 2 * BLK), False)

    loop(i // 2, pair_step)

    def finish(done, blk):
        for h, src, cols, rows in spots():
            rsl = ds(blk * BLK + src.start, HB)
            out_ref[rsl, cols] = rotate(done[-1][rows, :] * SCALE, cos_ref[rsl, :], -sin_ref[rsl, :]).astype(BF)

    def tail_steps(n):
        mine, width = pick(n), (n + 1) * BLK
        low = scores(mine, slice(0, m3), start, width - HB)
        high = scores(mine, slice(m3, 2 * m3), start, width)
        grads(mine, low, True)
        other = pick(1 - n)
        finish(other, jnp.maximum(i - 1, 0))
        prepare(qn_ref, don_ref, on_ref, lsen_ref, other)
        grads(mine, high, True)

    pl.when(par == 0)(lambda: tail_steps(0))
    pl.when(par == 1)(lambda: tail_steps(1))

    @pl.when(i == last)
    def _():
        finish(pick(par), i)

        def fin(c):
            sl = ds(c * 2 * BLK, 2 * BLK)
            out_ref[sl, GW:QK] = rotate(dkt[:, sl].T * SCALE, cos_ref[sl, :], -sin_ref[sl, :]).astype(BF)
            out_ref[sl, QK:] = dvt[:, sl].T.astype(BF)

        loop(seq // BLK // 2, fin)
        pair_ref[...] = out_ref[ds(s_ref[0] * pair_ref.shape[0], pair_ref.shape[0]), :]


def attn_bwd(idx, q, do, o, k, v, lse, tabs, rows):
    seq = k.shape[0]
    nq = seq // BLK
    m3 = GROUP * BLK
    kspec = pl.BlockSpec((seq, HEAD), lambda i, s: at_col(s[1]))
    row_specs = []
    for ahead in range(2):
        row_specs += [pl.BlockSpec((BLK, GW), lambda i, s, a=ahead: (jnp.minimum(i + a, nq - 1), s[1]))] * 3
        row_specs += [pl.BlockSpec((1, 8, BLK), lambda i, s, a=ahead: (s[1], 0, jnp.minimum(i + a, nq - 1)))]
    two_sets = [pltpu.VMEM((2, m3, PAIR), BF)] * 2 + [pltpu.VMEM((2, HEAD, m3), BF)] * 2 + [pltpu.VMEM((2, m3, HEAD), F32)]
    return call(bwd_body, (nq,),
                row_specs + [kspec] * 2 + [ANY] * 2,
                [pl.BlockSpec((r, PW), first_row) for r in (seq, rows)], [sds(r, PW) for r in (seq, rows)],
                [idx] + [q, do, o, lse] * 2 + [k, v, *tabs], GROUP * nq * (nq + 1) * BLK * BLK * PW,
                scratch=[pltpu.VMEM((seq, PAIR), BF)] * 2 + [pltpu.VMEM((HEAD, seq), F32)] * 2
                + [pltpu.VMEM((2, seq, HEAD), F32), pltpu.SemaphoreType.DMA((2,))] + two_sets)


def half(i, s, n):
    return s[n] * 2 + i


def pick_body(s_ref, oa, ra, ob, rb, own, pair):
    for n, (low, high, out) in enumerate(((oa, ra, own), (ob, rb, pair))):
        out[...] = jnp.where(half(pl.program_id(0), s_ref, n) < s_ref[2], low[...], high[...])


def pick_rows(idx, low, high, rows):
    w = low.shape[1]
    specs = []
    for n in range(2):
        specs.append(pl.BlockSpec((BLK, w), lambda i, s, n=n: at_row(jnp.minimum(half(i, s, n), s[2] - 1))))
        specs.append(pl.BlockSpec((BLK, w), lambda i, s, n=n: at_row(jnp.maximum(half(i, s, n) - s[2], 0))))
    return call(pick_body, (rows // BLK,), specs, [pl.BlockSpec((BLK, w), row_map)] * 2, [sds(rows, w)] * 2,
                [idx, low, high, low, high], rows * w)


def out_body(s_ref, x_ref, *rest):
    ops, out_ref = rest[:-1], rest[-1]
    lhs = jnp.concatenate([r[...] for r in ops[:4]], axis=1)
    rhs = jnp.concatenate([r[...] for r in ops[4:]], axis=0)
    out_ref[...] = (x_ref[...].astype(F32) + mm(lhs, rhs)).astype(BF)


def out_proj(idx, x, pieces, w_o):
    rows, d = x.shape
    hw = pieces[0].shape[1]
    return call(out_body, (d // BLK,),
                [pl.BlockSpec((rows, BLK), col_map)]
                + [pl.BlockSpec((rows, hw), m) for m in (own_map, first_row, first_row, first_row)]
                + [pl.BlockSpec((hw, BLK), lambda n, s, p=p: (s[p], n)) for p in range(4)],
                pl.BlockSpec((rows, BLK), col_map), sds(rows, d), [idx, x, *pieces] + [w_o] * 4,
                2 * rows * d * d)


def dwo_body(s_ref, oa_ref, ob_ref, oc_ref, dy_ref, fin, snd, ot):
    first, hw = ob_ref.shape

    @pl.when(jnp.logical_and(pl.program_id(0) == 0, pl.program_id(1) == 0))
    def _():
        for src, rows, base in ((oa_ref, slice(0, hw), 0), (ob_ref, slice(hw, 2 * hw), 0), (oc_ref, slice(hw, 2 * hw), first)):
            def tr(c):
                ot[rows, ds(c * BLK + base, BLK)] = src[ds(c * BLK, BLK), :].T

            loop(src.shape[0] // BLK, tr)

    val = mm(ot[ds(pl.program_id(1) * hw, hw), :], dy_ref[...])
    fin[...] = val
    snd[...] = val


def dw_o(idx, oa, ob, oc, dy):
    seq, d = dy.shape
    hw = oa.shape[1]
    o_specs = [pl.BlockSpec((r, hw), lambda i, p, s: first_row(i, s), pipeline_mode=pl.Buffered(1))
               for r in (seq, seq - oc.shape[0], oc.shape[0])]
    return call(dwo_body, (d // BLK, 2),
                o_specs + [pl.BlockSpec((seq, BLK), lambda i, p, s: at_col(i))],
                [pl.BlockSpec((hw, BLK), lambda i, p, s: (s[p], i)), pl.BlockSpec((hw, BLK), lambda i, p, s: (p, i))],
                [sds(4 * hw, d, F32), sds(2 * hw, d, F32)], [idx, oa, ob, oc, dy], 4 * seq * d * hw,
                scratch=[pltpu.VMEM((2 * hw, seq), BF)])


def dwown_body(s_ref, h_ref, ga_ref, gb_ref, gc_ref, wo_ref, _, fq, fk, fv, snd, wo_fin, g3, ht, sem, wsem):
    i, steps = pl.program_id(0), pl.num_programs(0)
    rows, per = wo_ref.shape[0], steps // 2
    start = jnp.where(i < per, s_ref[1] * per + i, s_ref[3] * per + i - per)
    wcopy = pltpu.make_async_copy(wo_ref, wo_fin.at[ds(start * rows, rows), :], wsem)
    wcopy.start()

    @pl.when(i > 1)
    def _():
        for copy in scatter(snd, (fq, fk, fv), s_ref[0], s_ref[2], sem.at[i % 2]):
            copy.wait()

    ht[...] = h_ref[...].T
    lhs = ht[...]
    for g, q_at, k_at in ((ga_ref, 0, 2 * GW), (gb_ref, GW, 2 * GW + HEAD), (gc_ref, 2 * PW, 2 * PW + GW)):
        val = mm(lhs, g[:, :QK])
        snd[:, q_at:q_at + GW] = val[:, :GW]
        snd[:, k_at:k_at + HEAD] = val[:, GW:]
    snd[:, 2 * QK:2 * PW] = mm(lhs, jnp.concatenate([ga_ref[:, QK:], gb_ref[:, QK:]], axis=1))
    for copy in scatter(snd, (fq, fk, fv), s_ref[0], s_ref[2], sem.at[i % 2]):
        copy.start()

    @pl.when(i == steps - 1)
    def _():
        g3[...] = gc_ref[ds(s_ref[1] * g3.shape[0], g3.shape[0]), :]
        for slot in range(2):
            for copy in scatter(snd, (fq, fk, fv), s_ref[0], s_ref[2], sem.at[slot]):
                copy.wait()

    wcopy.wait()


def scatter(rcv, outs, whole_dev, part_dev, sem):
    rows, src, copies = ds(pl.program_id(0) * rcv.shape[0], rcv.shape[0]), 0, []
    fq, fk, fv = outs
    for n, (out, col, w) in enumerate(((fq, whole_dev, 2 * GW), (fk, whole_dev, PAIR), (fv, whole_dev, PAIR),
                                       (fq, 2 * part_dev, GW), (fk, 2 * part_dev, HEAD))):
        copies.append(pltpu.make_async_copy(rcv.at[:, src:src + w], out.at[rows, ds(col * w, w)], sem.at[n]))
        src += w
    return copies


def dw_own(idx, h, ga, gb, gc, wo_rcv, wo_fin):
    seq, d = h.shape
    steps = d // HB
    gspec = pl.BlockSpec((seq, PW), first_row, pipeline_mode=pl.Buffered(1))
    widths = (2 * GW, PAIR, PAIR)
    sw = 2 * PW + QK
    return call(dwown_body, (steps,),
                [pl.BlockSpec((seq, HB), col_map)] + [gspec] * 3
                + [pl.BlockSpec((wo_rcv.shape[0] // steps, d), row_map), ANY],
                [ANY] * 3 + [pl.BlockSpec((HB, sw), row_map), ANY, pl.BlockSpec((seq // 4, PW), first_row)],
                [sds(d, 4 * w, F32) for w in widths] + [sds(d, sw, F32), sds(*wo_fin.shape, F32), sds(seq // 4, PW)],
                [idx, h, ga, gb, gc, wo_rcv, wo_fin], 2 * seq * d * sw,
                scratch=[pltpu.VMEM((HB, seq), BF), pltpu.SemaphoreType.DMA((2, 5)), pltpu.SemaphoreType.DMA],
                aliases={6: 4})


def dwgrp_body(s_ref, h_ref, ga_ref, gb_ref, *rest):
    fq, fk, fv, snd, g3, ht = rest[-6:]

    @pl.when(pl.program_id(0) == 0)
    def _():
        g3[...] = gb_ref[ds(s_ref[1] * g3.shape[0], g3.shape[0]), :]

    ht[...] = h_ref[...].T
    lhs = ht[...]
    val = mm(lhs, gb_ref[:, :QK])
    fq[...] = val[:, :GW]
    fk[...] = val[:, GW:]
    snd[:, :QK] = val
    val = mm(lhs, jnp.concatenate([ga_ref[...], gb_ref[:, QK:]], axis=1))
    fv[...] = val
    snd[:, QK:] = val


def group_specs(bm):
    return [pl.BlockSpec((bm, w), lambda i, s: (i, 2 * s[0] + 1)) for w in (GW, HEAD)] + \
        [pl.BlockSpec((bm, PAIR), lambda i, s: (i, s[0]))]


def dw_group(idx, h, ga, gb, bufs):
    seq, d = h.shape
    gspec = pl.BlockSpec((seq, PW), first_row, pipeline_mode=pl.Buffered(1))
    sw = QK + PAIR
    return call(dwgrp_body, (d // HB,),
                [pl.BlockSpec((seq, HB), col_map),
                 pl.BlockSpec((seq, HEAD), lambda i, s: at_col(QK // HEAD), pipeline_mode=pl.Buffered(1)), gspec] + [ANY] * 3,
                group_specs(HB) + [pl.BlockSpec((HB, sw), row_map), pl.BlockSpec((seq // 4, PW), first_row)],
                [sds(*b.shape, F32) for b in bufs] + [sds(d, sw, F32), sds(seq // 4, PW)],
                [idx, h, ga, gb, *bufs], 2 * seq * d * sw, scratch=[pltpu.VMEM((HB, seq), BF)],
                aliases={4 + n: n for n in range(3)})


def place_body(s_ref, rcv, *rest):
    q_out, k_out, v_out = rest[-3:]
    q_out[...] = rcv[:, :GW]
    k_out[...] = rcv[:, GW:QK]
    v_out[...] = rcv[:, QK:]


def place(idx, rcv, bufs):
    d, w = rcv.shape
    bm = BLK
    return call(place_body, (d // bm,), [pl.BlockSpec((bm, w), row_map)] + [ANY] * 3, group_specs(bm),
                [sds(*b.shape, F32) for b in bufs], [idx, rcv, *bufs], d * w, aliases={2 + n: n for n in range(3)})


def dx_body(s_ref, x_ref, dy_ref, gain_ref, inv_ref, *rest):
    pieces, weights, rcv = rest[:8], rest[8:20], rest[20]
    dx_hbm, dg_ref, fq, fk, fv, acc, xs, tot, dx_ref, dx_sem, sem = rest[-11:]
    n = pl.program_id(0)
    bn = x_ref.shape[1]
    rows, d = acc.shape
    copies = scatter(rcv, (fq, fk, fv), s_ref[1], s_ref[3], sem)
    for copy in copies:
        copy.start()

    @pl.when(n == 0)
    def _():
        tot[...] = jnp.zeros_like(tot)

    cuts = (slice(0, GW), slice(GW, QK), slice(QK, PW))
    lhs = jnp.concatenate([pieces[2 * p + g][:, c] for p in range(4) for c in cuts for g in range(2)], axis=1)
    rhs = jnp.concatenate([r[...] for r in weights], axis=1)
    dh = mm_nt(lhs, rhs)
    inv = inv_ref[...]
    for c in range(bn // HEAD):
        cols = head_cols(c)
        xb = x_ref[:, cols]
        xs[:, ds(n * bn + cols.start, HEAD)] = xb
        part, xf = dh[:, cols], xb.astype(F32)
        scaled = part * gain_ref[:, cols]
        tot[...] += scaled * xf
        acc[:, ds(n * bn + cols.start, HEAD)] = dy_ref[:, cols].astype(F32) + inv * scaled
        dg_ref[:, cols] = jnp.sum((part * (xf * inv)).reshape(rows // 8, 8, HEAD), axis=0)

    @pl.when(n == pl.num_programs(0) - 1)
    def _():
        step = HEAD // 2

        def stats(r):
            sl = ds(r * step, step)
            inv = inv_ref[sl, :]
            tot[sl, :] = jnp.broadcast_to(jnp.sum(tot[sl, :], axis=-1, keepdims=True) / d, (step, HEAD)) * inv * inv * inv

        loop(rows // step, stats)

        def epi(r):
            sl = ds(r * step, step)
            coef = tot[sl, :]
            for c in range(d // HEAD):
                cols = head_cols(c)
                dx_ref[sl, cols] = (acc[sl, cols] - xs[sl, cols].astype(F32) * coef).astype(BF)
            send(r).start()

        def send(r):
            sl = ds(r * step, step)
            return pltpu.make_async_copy(dx_ref.at[sl, :], dx_hbm.at[sl, :], dx_sem)

        loop(rows // step, epi)
        loop(rows // step, lambda r: send(r).wait())

    for copy in copies:
        copy.wait()


def dx_call(idx, x, dy, gain, inv, pieces, ws, rcv, bufs):
    rows, d = x.shape
    bn = HB
    once = pl.Buffered(1)
    maps = (own_map, own_map, first_row, first_row) * 2
    return call(dx_body, (d // bn,),
                [pl.BlockSpec((rows, bn), col_map)] * 2 + [pl.BlockSpec((1, bn), col_map), pl.BlockSpec((rows, HEAD), own_map)]
                + [pl.BlockSpec((rows, PW), m, pipeline_mode=once) for m in maps]
                + [pl.BlockSpec((bn, w.shape[1] // 4), lambda n, s, p=p: (n, s[p])) for p in range(4) for w in ws]
                + [pl.BlockSpec((bn, rcv.shape[1]), row_map)] + [ANY] * 3,
                [ANY, pl.BlockSpec((8, bn), col_map)] + [ANY] * 3,
                [sds(rows, d), sds(8, d, F32)] + [sds(*b.shape, F32) for b in bufs],
                [idx, x, dy, gain, inv, *pieces] + list(ws) * 4 + [rcv, *bufs], 16 * rows * d * PW,
                scratch=[pltpu.VMEM((rows, d), F32), pltpu.VMEM((rows, d), BF), pltpu.VMEM((rows, HEAD), F32),
                         pltpu.VMEM((rows, d), BF), pltpu.SemaphoreType.DMA, pltpu.SemaphoreType.DMA((5,))],
                aliases={26 + n: 2 + n for n in range(3)})


def solution(mesh):
    sp = mesh.shape['sp']
    cross = [(a, a ^ 2) for a in range(sp)]
    pair = [(a, a ^ 1) for a in range(sp)]

    def over(val):
        return lax.ppermute(val, 'sp', cross)

    def near(val):
        return lax.ppermute(val, 'sp', pair)

    def both(val):
        return lax.ppermute(val, 'sp', [(a, a ^ 3) for a in range(sp)])

    def after(val, *deps):
        return lax.optimization_barrier((val,) + deps)[0]

    def vec(*vals, dep=()):
        out = jnp.stack([jnp.asarray(v, jnp.int32) for v in vals])
        return after(out, *dep) if dep else out

    def step(x, dy, positions, gain, w_q, w_k, w_v, w_o):
        j = lax.axis_index('sp').astype(jnp.int32)
        rows, d = x.shape
        seq = rows * sp
        j1, j2, j3 = [j ^ n for n in (1, 2, 3)]
        dev = (j, j1, j2, j3)
        hpr = rows // HB
        ws = (w_q, w_k, w_v)

        gain_f = gain.astype(F32).reshape(1, d)

        cut = rows - HB
        xa = x[:cut]
        positions = after(positions, xa)
        pos2 = over(positions)
        pos1 = near(positions)
        x2a = over(xa)
        x2b = over(after(x, xa)[cut:])
        x1 = near(x)
        pos3 = near(pos2)
        dy1 = near(after(dy, x1))

        pos = jnp.zeros((seq,), jnp.int32)
        for blk, val in zip(dev, (positions, pos1, pos2, pos3)):
            pos = lax.dynamic_update_slice(pos, val, (blk * rows,))
        inv_freq = ROPE_THETA ** (-jnp.arange(0, HEAD, 2).astype(F32) / HEAD)
        angles = pos.astype(F32)[:, None] * inv_freq[None, :]
        cos_h, sin_h = jnp.cos(angles), jnp.sin(angles)
        tabs = (jnp.concatenate([cos_h, cos_h], axis=1), jnp.concatenate([-sin_h, sin_h], axis=1))

        dya, dyb = dy[:cut], dy[cut:]
        bufs = project(vec(j * hpr, j1 * hpr, j, dep=(dya, dyb)), x, x1, gain_f, ws, tabs, None, seq)
        dbufs = dout(vec(j * hpr, j1 * hpr, j, dep=bufs), dy, dy1, w_o, None, seq)

        chip, nh = j // 2, seq // BLK // 2
        tri = row_tasks(0, nh)
        first = seq // 2 - BLK
        square = [(i + nh, nh, 0, i) for i in range(nh)]

        def table(head, tasks):
            return jnp.concatenate([vec(*head, len(tasks)), jnp.asarray(tasks, jnp.int32).reshape(-1)])

        c_tasks = table((j1, 0), tri).at[HEADER - 1].set(nh - 1)
        local = attn_fwd("local", after(table((j1, chip), tri), *dbufs), *bufs[1:4])
        rest_tasks = jnp.where(chip == 0, table((j1, 0), row_tasks(nh, 2 * nh) * 2).at[HEADER - 1].set(nh),
                               table((j1, 1), tri + square))

        x2a = after(x2a, *local)
        dy2a = over(after(dya, x2a))
        x3a = near(x2a)
        bufs = project(vec(j2 * hpr, j3 * hpr, j), x2a, x3a, gain_f, ws, tabs, bufs, seq)
        x2b = after(x2b, *bufs)
        dy2b = over(after(dyb, x2b))
        x3b = near(x2b)
        bufs = project(vec((j2 + 1) * hpr - 1, (j3 + 1) * hpr - 1, j), x2b, x3b, gain_f, ws, tabs, bufs, seq)
        h_all, q, k, v, inv = bufs
        o, lse, o_hi, o_pair = attn_fwd("rest", rest_tasks, q, k, v, (seq - first, rows), local)
        orv = over(o_hi)
        o1 = near(o_pair)
        qc, kc, vc = project_first(vec(j2, dep=(o,)), h_all, ws, tabs, first)
        dy2a = after(dy2a, qc)
        dy3a = near(dy2a)
        oc = attn_fwd("local", c_tasks, qc, kc, vc)[0]

        dbufs = dout(vec(j2 * hpr, j3 * hpr, j, dep=(oc,)), dy2a, dy3a, w_o, dbufs, seq)
        dy2b = after(dy2b, *dbufs)
        dy3b = near(dy2b)
        dbufs = dout(vec((j2 + 1) * hpr - 1, (j3 + 1) * hpr - 1, j), dy2b, dy3b, w_o, dbufs, seq)
        dy_all, do = dbufs

        ga, ga_pair = attn_bwd(vec(j1, 0), q, do, o, k, v, lse, tabs, rows)
        ga2 = over(ga)
        ga1 = near(ga_pair)
        gb, gb_pair = attn_bwd(vec(j1, 1, dep=(ga,)), q, do, o, k, v, lse, tabs, rows)
        gb2 = over(gb)
        gb1 = near(gb_pair)

        orv = after(orv, gb)
        ox, ox_pair = pick_rows(vec(j, j1, nh - 1, dep=(gb,)), oc, orv, rows)
        o3 = near(ox_pair)
        wo_fin, wo_snd = dw_o(vec(j, j2, dep=(gb,)), o, oc, orv, dy_all)
        wo_rcv = near(wo_snd)
        result = out_proj(vec(*dev, dep=(wo_snd,)), x, (o, o1, ox, o3), w_o)
        ga2 = after(ga2, wo_snd)
        fq, fk, fv, snd, wo_fin, g3 = dw_own(vec(*dev, dep=(result,)), h_all, ga, gb, ga2, wo_rcv, wo_fin)
        rcv = near(snd)
        ga3 = near(g3)

        gb2 = after(gb2, snd)
        fq, fk, fv, snd_b, g3b = dw_group(vec(j2, j1), h_all, ga2, gb2, (fq, fk, fv))
        gb3 = near(g3b)
        rcv_b = near(snd_b)
        grad_x, dg, fq, fk, fv = dx_call(vec(*dev, dep=(snd_b,)), x, dy, gain_f, inv,
                                         (ga, gb, ga1, gb1, ga2, gb2, ga3, gb3), ws, rcv, (fq, fk, fv))
        dg = jnp.sum(dg, axis=0)
        dg = (dg + near(dg)) + (over(dg) + both(dg))
        fq, fk, fv = place(vec(j3), rcv_b, (fq, fk, fv))
        return result, grad_x, fq, fk, fv, wo_fin, dg

    seq_spec = P(('dp', 'sp'), None)
    whole = P(None, None)
    part_rows = P('dp', None)
    return jax.shard_map(step, mesh=mesh,
                         in_specs=(seq_spec, seq_spec, P(('dp', 'sp')), P(None), whole, whole, whole, whole),
                         out_specs=(seq_spec, seq_spec, part_rows, part_rows, part_rows, part_rows, P('dp')),
                         check_vma=False)
```

```python
import math

import jax
import jax.numpy as jnp
from jax import lax
from jax.experimental import pallas as pl
from jax.experimental.pallas import tpu as pltpu
from jax.sharding import PartitionSpec as P


HEAD = 128
GROUP = 3
GW = GROUP * HEAD
QK = GW + HEAD
PW = QK + HEAD
PAIR = 2 * HEAD
ROPE_THETA = 1000000.0
NORM_EPS = 1e-05
NEG_LARGE = -1e30
BF = jnp.bfloat16
F32 = jnp.float32
SCALE = HEAD ** -0.5
SCALE2 = SCALE * math.log2(math.e)
BLK = 512
HB = BLK // 2
VMEM_LIMIT = 65011712
ANY = pl.BlockSpec(memory_space=pl.ANY)


def first_row(i, s):
    return (0, 0)


def at_row(r):
    return (r, 0)


def at_col(c):
    return (0, c)


def row_map(i, s):
    return at_row(i)


def col_map(i, s):
    return at_col(i)


def own_map(i, s):
    return at_row(s[0])


def sds(rows, cols, dtype=BF):
    return jax.ShapeDtypeStruct((rows, cols), dtype)


def call(body, grid, in_specs, out_specs, out_shape, args, flops, scratch=(), aliases=None):
    return pl.pallas_call(
        body,
        grid_spec=pltpu.PrefetchScalarGridSpec(
            num_scalar_prefetch=1, grid=grid, in_specs=in_specs, out_specs=out_specs, scratch_shapes=list(scratch)),
        out_shape=out_shape, input_output_aliases=aliases or {},
        compiler_params=pltpu.CompilerParams(dimension_semantics=("arbitrary",) * len(grid),
                                             vmem_limit_bytes=VMEM_LIMIT),
        cost_estimate=pl.CostEstimate(flops=int(flops), bytes_accessed=int(flops) // BLK,
                                      transcendentals=0))(*args)


def down(shape):
    return lax.broadcasted_iota(jnp.int32, shape, 0)


def across(shape):
    return lax.broadcasted_iota(jnp.int32, shape, 1)


def loop(count, body):
    def run(c, _):
        body(c)
        return 0

    lax.fori_loop(0, count, run, 0)


def one(h):
    return slice(h, h + 1)


def head_cols(h):
    return slice(h * HEAD, h * HEAD + HEAD)


def mm(a, b):
    return jnp.dot(a, b, preferred_element_type=F32)


def mm_nt(a, b):
    return lax.dot_general(a, b, (((1,), (1,)), ((), ())), preferred_element_type=F32)


def rotate(val, cos_t, sin_t):
    return val * cos_t + pltpu.roll(val, HEAD // 2, 1) * sin_t


def ds(start, size):
    return pl.ds(pl.multiple_of(start, size), size)


def split3(val):
    hi = val.astype(BF).astype(F32)
    mid = (val - hi).astype(BF).astype(F32)
    return hi, mid, val - hi - mid


def qkv_of(h, wq_ref, wk_ref, wv_ref, cos_ref, sin_ref, q_ref, k_ref, v_ref):
    cos_t, sin_t = cos_ref[...], sin_ref[...]
    out = mm(h, wq_ref[...])
    for c in range(wq_ref.shape[1] // HEAD):
        sl = head_cols(c)
        q_ref[:, sl] = rotate(out[:, sl], cos_t, sin_t).astype(BF)
    out = mm(h, jnp.concatenate([wk_ref[...], wv_ref[...]], axis=1))
    for sl in (slice(0, HEAD), slice(HEAD, PAIR)):
        k_ref[:, sl] = rotate(out[:, sl], cos_t, sin_t).astype(BF)
    v_ref[...] = out[:, PAIR:].astype(BF)


def sources(arrays):
    steps = [arr.shape[0] // HB for arr in arrays]
    first = [sum(steps[:n]) for n in range(len(steps))]
    specs = []
    for at, count in zip(first, steps):
        specs.append(pl.BlockSpec((HB, arrays[0].shape[1]), lambda i, s, a=at, c=count: at_row(jnp.clip(i - a, 0, c - 1))))

    def out_map(i, s):
        row = s[0] + i
        for n, at in enumerate(first):
            row = jnp.where(i >= at, s[n] + i - at, row)
        return at_row(row)

    return first, steps, specs, out_map


def take(refs, first, steps, dst):
    for ref, at, count in zip(refs, first, steps):
        @pl.when(jnp.logical_and(pl.program_id(0) >= at, pl.program_id(0) < at + count))
        def _(ref=ref):
            dst[...] = ref[...]


def proj_body(first, steps, s_ref, *rest):
    n = len(first)
    gain_ref, wq_ref, wk_ref, wv_ref, cos_ref, sin_ref = rest[n:n + 6]
    h_ref, q_ref, k_ref, v_ref, inv_ref, src = rest[-6:]
    take(rest, first, steps, src)
    step = HEAD

    def stats(c):
        sl = ds(c * step, step)
        xf = src[sl, :].astype(F32)
        inv = lax.rsqrt(jnp.mean(xf * xf, axis=-1, keepdims=True) + NORM_EPS)
        inv_ref[sl, :] = jnp.broadcast_to(inv, (step, HEAD))

    def scale(c):
        sl = ds(c * step, step)
        inv, gain = inv_ref[sl, :], gain_ref[...]
        for m in range(src.shape[1] // HEAD):
            cols = head_cols(m)
            h_ref[sl, cols] = (src[sl, cols].astype(F32) * inv * gain[:, cols]).astype(BF)

    loop(src.shape[0] // step, stats)
    loop(src.shape[0] // step, scale)
    qkv_of(h_ref[...], wq_ref, wk_ref, wv_ref, cos_ref, sin_ref, q_ref, k_ref, v_ref)


def project(idx, xs, gain, ws, tabs, bufs, seq):
    d = xs[0].shape[1]
    first, steps, specs, out_map = sources(xs)
    widths = [w.shape[1] // 4 for w in ws]
    in_specs = specs + [pl.BlockSpec((1, d), first_row)]
    in_specs += [pl.BlockSpec((d, w), lambda i, s: at_col(s[len(xs)])) for w in widths]
    in_specs += [pl.BlockSpec((HB, HEAD), out_map)] * 2
    args = [idx, *xs, gain, *ws, *tabs]
    aliases = {}
    if bufs is not None:
        in_specs += [ANY] * len(bufs)
        aliases = {len(args) + n: n for n in range(len(bufs))}
        args += list(bufs)
    return call(lambda *refs: proj_body(first, steps, *refs), (sum(steps),), in_specs,
                [pl.BlockSpec((HB, w), out_map) for w in (d, *widths, HEAD)],
                [sds(seq, w) for w in (d, *widths)] + [sds(seq, HEAD, F32)], args, sum(steps) * BLK * d * sum(widths),
                scratch=[pltpu.VMEM((HB, d), BF)], aliases=aliases)


def projc_body(s_ref, h_ref, *rest):
    qkv_of(h_ref[...], *rest)


def project_first(idx, h, ws, tabs, rows):
    seq, d = h.shape
    widths = [w.shape[1] // 4 for w in ws]
    return call(projc_body, (rows // BLK,),
                [pl.BlockSpec((BLK, d), row_map)] + [pl.BlockSpec((d, w), lambda i, s: at_col(s[0])) for w in widths]
                + [pl.BlockSpec((BLK, HEAD), row_map)] * 2,
                [pl.BlockSpec((BLK, w), row_map) for w in widths], [sds(seq, w) for w in widths],
                [idx, h, *ws, *tabs], 2 * rows * d * sum(widths))


def dout_body(first, steps, s_ref, *rest):
    wo_ref, dy_out, do_out = rest[len(first)], *rest[-2:]
    take(rest, first, steps, dy_out)
    do_out[...] = mm_nt(dy_out[...], wo_ref[...]).astype(BF)


def dout(idx, dys, w_o, bufs, seq):
    d, oc = dys[0].shape[1], w_o.shape[0] // 4
    first, steps, specs, out_map = sources(dys)
    in_specs = specs + [pl.BlockSpec((oc, d), lambda i, s: at_row(s[len(dys)]))]
    args = [idx, *dys, w_o]
    aliases = {}
    if bufs is not None:
        in_specs += [ANY] * len(bufs)
        aliases = {len(args) + n: n for n in range(len(bufs))}
        args += list(bufs)
    return call(lambda *refs: dout_body(first, steps, *refs), (sum(steps),), in_specs,
                [pl.BlockSpec((HB, w), out_map) for w in (d, oc)],
                [sds(seq, w) for w in (d, oc)], args, sum(steps) * BLK * d * oc, aliases=aliases)


TASK = 4
HEADER = 3


def row_tasks(first, last):
    return [(i, i + 1, 1, -1) for i in range(first, last)]


def fwd_body(kind, s_ref, q_ref, k_ref, v_ref, *rest):
    qt, kk, vt, s_scr, acc, stat = rest[-6:]
    if kind == "rest":
        o1_ref, lse1_ref, st_ref, o_ref, lse_ref, hi_ref, pair_ref = rest[:7]
    else:
        o_ref, lse_ref = rest[:2]
    seq = k_ref.shape[0]

    def setup(c):
        sl = ds(c * BLK, BLK)
        vt[:, sl] = v_ref[sl, :].T
        kk[sl, :HEAD] = k_ref[sl, :]
        kk[sl, HEAD:] = k_ref[sl, :]
        for h in range(GROUP):
            qf = q_ref[sl, head_cols(h)].astype(F32) * SCALE2
            hi = qf.astype(BF)
            qt[h, :HEAD, sl] = hi.T
            qt[h, HEAD:, sl] = (qf - hi.astype(F32)).astype(BF).T

    loop(seq // BLK, setup)
    acc[...] = jnp.zeros_like(acc)
    stat[...] = jnp.zeros_like(stat)
    cur, old, den_row = 0, 1, 2
    lse_ref[...] = jnp.zeros_like(lse_ref)
    if kind == "rest":
        @pl.when(s_ref[1] == 0)
        def _():
            o_ref[:seq // 2, :] = o1_ref[...]
            lse_ref[0, :, :seq // 2] = lse1_ref[0]

    def task(t):
        return [s_ref[HEADER + t * TASK + n] for n in range(TASK)]

    def stage_a(h, i, j, masked, init=None):
        row = one(h)
        if masked is True:
            top = mm(kk[ds(j * BLK, HB), :], qt[h, :, ds(i * BLK, BLK)])
            low = mm(kk[ds(j * BLK + HB, HB), :], qt[h, :, ds(i * BLK + HB, HB)])
            top = jnp.where(down(top.shape) <= across(top.shape), top, NEG_LARGE)
            low = jnp.where(down(low.shape) <= across(low.shape), low, NEG_LARGE)
            s_scr[h, :HB, :] = top
            s_scr[h, HB:, HB:] = low
            m_new = jnp.max(top, axis=0, keepdims=True)
            right = jnp.maximum(m_new[:, HB:], jnp.max(low, axis=0, keepdims=True))
            m_new = jnp.concatenate([m_new[:, :HB], right], axis=1)
        else:
            s = mm(kk[ds(j * BLK, BLK), :], qt[h, :, ds(i * BLK, BLK)])
            if masked is not False:
                keep = down(s.shape) <= across(s.shape)
                s = jnp.where(jnp.logical_or(keep, jnp.logical_not(masked)), s, NEG_LARGE)
            s_scr[h] = s
            m_new = jnp.max(s, axis=0, keepdims=True)
        if init is None:
            m_old = stat[cur, row]
        elif kind == "rest":
            m_old = jnp.where(init >= 0, lse1_ref[0, row, ds(jnp.maximum(init, 0) * BLK, BLK)], NEG_LARGE)
        else:
            m_old = jnp.full(m_new.shape, NEG_LARGE, F32)
        m_new = jnp.maximum(m_old, m_new)
        stat[old, row] = jnp.exp2(m_old - m_new)
        stat[cur, row] = m_new

    def stage_p(h, diag=False):
        row = one(h)
        m, alpha = stat[cur, row], stat[old, row]
        if diag:
            top = jnp.exp2(s_scr[h, :HB, :] - m)
            low = jnp.exp2(s_scr[h, HB:, HB:] - m[:, HB:])
            total = jnp.sum(top, axis=0, keepdims=True)
            right = total[:, HB:] + jnp.sum(low, axis=0, keepdims=True)
            total = jnp.concatenate([total[:, :HB], right], axis=1)
            top = top.astype(BF)
            p = (top[:, :HB], jnp.concatenate([top[:, HB:], low.astype(BF)], axis=0))
        else:
            p = jnp.exp2(s_scr[h] - m)
            total = jnp.sum(p, axis=0, keepdims=True)
            p = p.astype(BF)
        stat[den_row, row] = stat[den_row, row] * alpha + total
        return p, alpha

    def stage_v(h, j, held, diag=False):
        p, alpha = held
        if diag:
            acc[h, :, :HB] = acc[h, :, :HB] * alpha[:, :HB] + mm(vt[:, ds(j * BLK, HB)], p[0])
            acc[h, :, HB:] = acc[h, :, HB:] * alpha[:, HB:] + mm(vt[:, ds(j * BLK, BLK)], p[1])
        else:
            acc[h] = acc[h] * alpha + mm(vt[:, ds(j * BLK, BLK)], p)

    def finish(h, i, den, top):
        row = one(h)
        out = acc[h] / den
        o_ref[ds(i * BLK, BLK), head_cols(h)] = out.T.astype(BF)
        lse_ref[0, row, ds(i * BLK, BLK)] = top + jnp.log2(den)
        if kind == "local":
            rest[2][0, h, :, ds(i * BLK, BLK)] = out

    def pipeline(i, j, masked):
        for h in range(GROUP):
            held = stage_p(h)
            stage_a(h, i, j + 1, masked)
            stage_v(h, j, held)

    count = s_ref[HEADER - 1]
    i, steps, diag, init = task(0)
    for h in range(GROUP):
        stage_a(h, i, 0, jnp.logical_and(steps == 1, diag == 1), init)

    def row(t):
        i, steps, diag, _ = task(t)

        loop(steps - 2, lambda j: pipeline(i, j, False))

        pl.when(jnp.logical_and(steps > 1, diag == 1))(lambda: pipeline(i, steps - 2, True))
        if kind == "rest":
            pl.when(diag == 0)(lambda: pipeline(i, steps - 2, False))
        i2, _, _, init2 = task(jnp.minimum(t + 1, count - 1))

        def last_step(on_diag):
            for h in range(GROUP):
                held = stage_p(h, on_diag)
                final = (stat[den_row, one(h)], stat[cur, one(h)])
                stage_a(h, i2, 0, False, init2)
                stage_v(h, steps - 1, held, on_diag)
                finish(h, i, *final)

        if kind != "rest":
            last_step(True)
        else:
            pl.when(diag == 1)(lambda: last_step(True))
            pl.when(diag == 0)(lambda: last_step(False))

            @pl.when(init2 >= 0)
            def _():
                stat[den_row] = jnp.ones(stat.shape[1:], F32)
                for h in range(GROUP):
                    acc[h] = st_ref[0, h, :, ds(init2 * BLK, BLK)]

    loop(count, row)
    if kind == "rest":
        hi_ref[...] = o_ref[seq - hi_ref.shape[0]:, :]
        pair_ref[...] = o_ref[ds(s_ref[0] * pair_ref.shape[0], pair_ref.shape[0]), :]


def attn_fwd(kind, idx, q, k, v, extra=(), local=()):
    whole = q.shape[0]
    seq = whole if kind == "rest" else whole // 2
    nkv = k.shape[1] // HEAD

    def half_map(g, s):
        return (s[1], g)

    def head_map(g, s):
        return (g, 0, 0)

    def state_map(g, s):
        return (g, 0, 0, 0)

    at = half_map if kind == "local" else col_map
    lse_spec = pl.BlockSpec((1, 8, seq), head_map)
    outs, specs = [sds(seq, q.shape[1]), jax.ShapeDtypeStruct((nkv, 8, seq), F32)], []
    out_specs = [pl.BlockSpec((seq, GW), col_map), lse_spec]
    state = pl.BlockSpec((1, GROUP, HEAD, whole // 2), state_map)
    if kind == "local":
        outs.append(jax.ShapeDtypeStruct((nkv, GROUP, HEAD, seq), F32))
        out_specs.append(state)
    if kind == "rest":
        specs = [pl.BlockSpec((seq // 2, GW), col_map), pl.BlockSpec((1, 8, seq // 2), head_map), state]
        outs += [sds(r, q.shape[1]) for r in extra]
        out_specs += [pl.BlockSpec((r, GW), col_map) for r in extra]
    kspec = pl.BlockSpec((seq, HEAD), at)
    return call(lambda *refs: fwd_body(kind, *refs), (nkv,), [pl.BlockSpec((seq, GW), at), kspec, kspec] + specs,
                out_specs, outs, [idx, q, k, v, *local], nkv * GROUP * seq * seq * PAIR,
                scratch=[pltpu.VMEM((GROUP, PAIR, seq), BF), pltpu.VMEM((seq, PAIR), BF),
                         pltpu.VMEM((HEAD, seq), BF), pltpu.VMEM((GROUP, BLK, BLK), F32),
                         pltpu.VMEM((GROUP, HEAD, BLK), F32), pltpu.VMEM((GROUP, 8, BLK), F32)])


def bwd_body(s_ref, q_ref, do_ref, o_ref, lse_ref, qn_ref, don_ref, on_ref, lsen_ref, k_ref, v_ref, cos_hbm, sin_hbm,
             out_ref, pair_ref, ka, va, dkt, dvt, tab, tab_sem, *sets):
    i = pl.program_id(0)
    last = pl.num_programs(0) - 1
    seq = k_ref.shape[0]
    m3 = GROUP * HB
    cos_ref, sin_ref = tab.at[0], tab.at[1]

    def spots():
        for b in range(2):
            for h in range(GROUP):
                start = (b * GROUP + h) * HB
                yield h, slice(b * HB, b * HB + HB), head_cols(h), slice(start, start + HB)

    def pick(n):
        return [ref.at[n] for ref in sets]

    def prepare(q_src, do_src, o_src, lse_src, dst):
        qa, da, q3t, do3t, dq3 = dst
        srow = down((16, HB))
        blank = jnp.zeros((HEAD - 16, HB), BF)
        for h, src, cols, rows in spots():
            qh, doh = q_src[src, cols], do_src[src, cols]
            qa[rows, :HEAD] = qh
            da[rows, :HEAD] = doh
            q3t[:, rows] = qh.T
            dt = doh.T
            do3t[:, rows] = dt
            delta = jnp.sum(dt.astype(F32) * o_src[src, cols].T.astype(F32), axis=0, keepdims=True)
            parts = jnp.zeros((16, HB), F32)
            for n, part in enumerate(split3(lse_src[0, one(h), src] * (1.0 / SCALE2)) + split3(delta)):
                parts = jnp.where(srow == n, part, parts)
            block = jnp.concatenate([parts.astype(BF), blank], axis=0).T
            qa[rows, HEAD:] = block
            da[rows, HEAD:] = block
        dq3[...] = jnp.zeros_like(dq3)

    @pl.when(i == 0)
    def _():
        copies = [pltpu.make_async_copy(src, tab.at[n], tab_sem.at[n]) for n, src in enumerate((cos_hbm, sin_hbm))]
        for copy in copies:
            copy.start()
        dkt[...] = jnp.zeros_like(dkt)
        dvt[...] = jnp.zeros_like(dvt)

        def setup(c):
            sl = ds(c * BLK, BLK)
            third = across((BLK, HEAD)) // 3
            for n, (src, dst) in enumerate(((k_ref, ka), (v_ref, va))):
                dst[sl, :HEAD] = src[sl, :]
                dst[sl, HEAD:] = jnp.where(third == n, -1.0, 0.0).astype(BF)

        loop(seq // BLK, setup)
        prepare(q_ref, do_ref, o_ref, lse_ref, pick(0))
        for copy in copies:
            copy.wait()

    def scores(mine, rows, start, width):
        sl = pl.ds(pl.multiple_of(start, BLK), width)
        return rows, sl, width, mm_nt(mine[0][rows, :], ka[sl, :]), mm_nt(mine[1][rows, :], va[sl, :])

    def grads(mine, held, masked):
        _, _, q3t, do3t, dq3 = mine
        rows, sl, width, s, dp = held
        p = jnp.exp2(s * SCALE2)
        if masked:
            off = width - HB
            tail = p[:, off:]
            keep = down(tail.shape) % HB >= across(tail.shape)
            tail = jnp.where(keep, tail, 0.0)
            p = jnp.concatenate([p[:, :off], tail], axis=1) if off else tail
        dvt[:, sl] += mm(do3t[:, rows], p.astype(BF))
        dsv = (p * dp).astype(BF)
        dkt[:, sl] += mm(q3t[:, rows], dsv)
        dq3[rows, :] += mm(dsv, ka[sl, :HEAD])

    par, start = i % 2, (i // 2) * 2 * BLK

    def pair_step(t):
        mine = pick(par)
        grads(mine, scores(mine, slice(0, 2 * m3), t * 2 * BLK, 2 * BLK), False)

    loop(i // 2, pair_step)

    def finish(done, blk):
        for h, src, cols, rows in spots():
            rsl = ds(blk * BLK + src.start, HB)
            out_ref[rsl, cols] = rotate(done[-1][rows, :] * SCALE, cos_ref[rsl, :], -sin_ref[rsl, :]).astype(BF)

    def tail_steps(n):
        mine, width = pick(n), (n + 1) * BLK
        low = scores(mine, slice(0, m3), start, width - HB)
        high = scores(mine, slice(m3, 2 * m3), start, width)
        grads(mine, low, True)
        other = pick(1 - n)
        finish(other, jnp.maximum(i - 1, 0))
        prepare(qn_ref, don_ref, on_ref, lsen_ref, other)
        grads(mine, high, True)

    pl.when(par == 0)(lambda: tail_steps(0))
    pl.when(par == 1)(lambda: tail_steps(1))

    @pl.when(i == last)
    def _():
        finish(pick(par), i)

        def fin(c):
            sl = ds(c * 2 * BLK, 2 * BLK)
            out_ref[sl, GW:QK] = rotate(dkt[:, sl].T * SCALE, cos_ref[sl, :], -sin_ref[sl, :]).astype(BF)
            out_ref[sl, QK:] = dvt[:, sl].T.astype(BF)

        loop(seq // BLK // 2, fin)
        pair_ref[...] = out_ref[ds(s_ref[0] * pair_ref.shape[0], pair_ref.shape[0]), :]


def attn_bwd(idx, q, do, o, k, v, lse, tabs, rows):
    seq = k.shape[0]
    nq = seq // BLK
    m3 = GROUP * BLK
    kspec = pl.BlockSpec((seq, HEAD), lambda i, s: at_col(s[1]))
    row_specs = []
    for ahead in range(2):
        row_specs += [pl.BlockSpec((BLK, GW), lambda i, s, a=ahead: (jnp.minimum(i + a, nq - 1), s[1]))] * 3
        row_specs += [pl.BlockSpec((1, 8, BLK), lambda i, s, a=ahead: (s[1], 0, jnp.minimum(i + a, nq - 1)))]
    two_sets = [pltpu.VMEM((2, m3, PAIR), BF)] * 2 + [pltpu.VMEM((2, HEAD, m3), BF)] * 2 + [pltpu.VMEM((2, m3, HEAD), F32)]
    return call(bwd_body, (nq,),
                row_specs + [kspec] * 2 + [ANY] * 2,
                [pl.BlockSpec((r, PW), first_row) for r in (seq, rows)], [sds(r, PW) for r in (seq, rows)],
                [idx] + [q, do, o, lse] * 2 + [k, v, *tabs], GROUP * nq * (nq + 1) * BLK * BLK * PW,
                scratch=[pltpu.VMEM((seq, PAIR), BF)] * 2 + [pltpu.VMEM((HEAD, seq), F32)] * 2
                + [pltpu.VMEM((2, seq, HEAD), F32), pltpu.SemaphoreType.DMA((2,))] + two_sets)


def half(i, s, n):
    return s[n] * 2 + i


def pick_body(s_ref, oa, ra, ob, rb, own, pair):
    for n, (low, high, out) in enumerate(((oa, ra, own), (ob, rb, pair))):
        out[...] = jnp.where(half(pl.program_id(0), s_ref, n) < s_ref[2], low[...], high[...])


def pick_rows(idx, low, high, rows):
    w = low.shape[1]
    specs = []
    for n in range(2):
        specs.append(pl.BlockSpec((BLK, w), lambda i, s, n=n: at_row(jnp.minimum(half(i, s, n), s[2] - 1))))
        specs.append(pl.BlockSpec((BLK, w), lambda i, s, n=n: at_row(jnp.maximum(half(i, s, n) - s[2], 0))))
    return call(pick_body, (rows // BLK,), specs, [pl.BlockSpec((BLK, w), row_map)] * 2, [sds(rows, w)] * 2,
                [idx, low, high, low, high], rows * w)


def out_body(s_ref, x_ref, *rest):
    ops, out_ref = rest[:-1], rest[-1]
    lhs = jnp.concatenate([r[...] for r in ops[:4]], axis=1)
    rhs = jnp.concatenate([r[...] for r in ops[4:]], axis=0)
    out_ref[...] = (x_ref[...].astype(F32) + mm(lhs, rhs)).astype(BF)


def out_proj(idx, x, pieces, w_o):
    rows, d = x.shape
    hw = pieces[0].shape[1]
    return call(out_body, (d // BLK,),
                [pl.BlockSpec((rows, BLK), col_map)]
                + [pl.BlockSpec((rows, hw), m) for m in (own_map, first_row, first_row, first_row)]
                + [pl.BlockSpec((hw, BLK), lambda n, s, p=p: (s[p], n)) for p in range(4)],
                pl.BlockSpec((rows, BLK), col_map), sds(rows, d), [idx, x, *pieces] + [w_o] * 4,
                2 * rows * d * d)


def dwo_body(s_ref, oa_ref, ob_ref, oc_ref, dy_ref, fin, snd, ot):
    first, hw = ob_ref.shape

    @pl.when(jnp.logical_and(pl.program_id(0) == 0, pl.program_id(1) == 0))
    def _():
        for src, rows, base in ((oa_ref, slice(0, hw), 0), (ob_ref, slice(hw, 2 * hw), 0), (oc_ref, slice(hw, 2 * hw), first)):
            def tr(c):
                ot[rows, ds(c * BLK + base, BLK)] = src[ds(c * BLK, BLK), :].T

            loop(src.shape[0] // BLK, tr)

    val = mm(ot[ds(pl.program_id(1) * hw, hw), :], dy_ref[...])
    fin[...] = val
    snd[...] = val


def dw_o(idx, oa, ob, oc, dy):
    seq, d = dy.shape
    hw = oa.shape[1]
    o_specs = [pl.BlockSpec((r, hw), lambda i, p, s: first_row(i, s), pipeline_mode=pl.Buffered(1))
               for r in (seq, seq - oc.shape[0], oc.shape[0])]
    return call(dwo_body, (d // BLK, 2),
                o_specs + [pl.BlockSpec((seq, BLK), lambda i, p, s: at_col(i))],
                [pl.BlockSpec((hw, BLK), lambda i, p, s: (s[p], i)), pl.BlockSpec((hw, BLK), lambda i, p, s: (p, i))],
                [sds(4 * hw, d, F32), sds(2 * hw, d, F32)], [idx, oa, ob, oc, dy], 4 * seq * d * hw,
                scratch=[pltpu.VMEM((2 * hw, seq), BF)])


def dwown_body(s_ref, h_ref, ga_ref, gb_ref, gc_ref, wo_ref, _, fq, fk, fv, snd, wo_fin, g3, ht, sem, wsem):
    i, steps = pl.program_id(0), pl.num_programs(0)
    rows, per = wo_ref.shape[0], steps // 2
    start = jnp.where(i < per, s_ref[1] * per + i, s_ref[3] * per + i - per)
    wcopy = pltpu.make_async_copy(wo_ref, wo_fin.at[ds(start * rows, rows), :], wsem)
    wcopy.start()

    @pl.when(i > 1)
    def _():
        for copy in scatter(snd, (fq, fk, fv), s_ref[0], s_ref[2], sem.at[i % 2]):
            copy.wait()

    ht[...] = h_ref[...].T
    lhs = ht[...]
    for g, q_at, k_at in ((ga_ref, 0, 2 * GW), (gb_ref, GW, 2 * GW + HEAD), (gc_ref, 2 * PW, 2 * PW + GW)):
        val = mm(lhs, g[:, :QK])
        snd[:, q_at:q_at + GW] = val[:, :GW]
        snd[:, k_at:k_at + HEAD] = val[:, GW:]
    snd[:, 2 * QK:2 * PW] = mm(lhs, jnp.concatenate([ga_ref[:, QK:], gb_ref[:, QK:]], axis=1))
    for copy in scatter(snd, (fq, fk, fv), s_ref[0], s_ref[2], sem.at[i % 2]):
        copy.start()

    @pl.when(i == steps - 1)
    def _():
        g3[...] = gc_ref[ds(s_ref[1] * g3.shape[0], g3.shape[0]), :]
        for slot in range(2):
            for copy in scatter(snd, (fq, fk, fv), s_ref[0], s_ref[2], sem.at[slot]):
                copy.wait()

    wcopy.wait()


def scatter(rcv, outs, whole_dev, part_dev, sem):
    rows, src, copies = ds(pl.program_id(0) * rcv.shape[0], rcv.shape[0]), 0, []
    fq, fk, fv = outs
    for n, (out, col, w) in enumerate(((fq, whole_dev, 2 * GW), (fk, whole_dev, PAIR), (fv, whole_dev, PAIR),
                                       (fq, 2 * part_dev, GW), (fk, 2 * part_dev, HEAD))):
        copies.append(pltpu.make_async_copy(rcv.at[:, src:src + w], out.at[rows, ds(col * w, w)], sem.at[n]))
        src += w
    return copies


def dw_own(idx, h, ga, gb, gc, wo_rcv, wo_fin):
    seq, d = h.shape
    steps = d // HB
    gspec = pl.BlockSpec((seq, PW), first_row, pipeline_mode=pl.Buffered(1))
    widths = (2 * GW, PAIR, PAIR)
    sw = 2 * PW + QK
    return call(dwown_body, (steps,),
                [pl.BlockSpec((seq, HB), col_map)] + [gspec] * 3
                + [pl.BlockSpec((wo_rcv.shape[0] // steps, d), row_map), ANY],
                [ANY] * 3 + [pl.BlockSpec((HB, sw), row_map), ANY, pl.BlockSpec((seq // 4, PW), first_row)],
                [sds(d, 4 * w, F32) for w in widths] + [sds(d, sw, F32), sds(*wo_fin.shape, F32), sds(seq // 4, PW)],
                [idx, h, ga, gb, gc, wo_rcv, wo_fin], 2 * seq * d * sw,
                scratch=[pltpu.VMEM((HB, seq), BF), pltpu.SemaphoreType.DMA((2, 5)), pltpu.SemaphoreType.DMA],
                aliases={6: 4})


def dwgrp_body(s_ref, h_ref, ga_ref, gb_ref, *rest):
    fq, fk, fv, snd, g3, ht = rest[-6:]

    @pl.when(pl.program_id(0) == 0)
    def _():
        g3[...] = gb_ref[ds(s_ref[1] * g3.shape[0], g3.shape[0]), :]

    ht[...] = h_ref[...].T
    lhs = ht[...]
    val = mm(lhs, gb_ref[:, :QK])
    fq[...] = val[:, :GW]
    fk[...] = val[:, GW:]
    snd[:, :QK] = val
    val = mm(lhs, jnp.concatenate([ga_ref[...], gb_ref[:, QK:]], axis=1))
    fv[...] = val
    snd[:, QK:] = val


def group_specs(bm):
    return [pl.BlockSpec((bm, w), lambda i, s: (i, 2 * s[0] + 1)) for w in (GW, HEAD)] + \
        [pl.BlockSpec((bm, PAIR), lambda i, s: (i, s[0]))]


def dw_group(idx, h, ga, gb, bufs):
    seq, d = h.shape
    gspec = pl.BlockSpec((seq, PW), first_row, pipeline_mode=pl.Buffered(1))
    sw = QK + PAIR
    return call(dwgrp_body, (d // HB,),
                [pl.BlockSpec((seq, HB), col_map),
                 pl.BlockSpec((seq, HEAD), lambda i, s: at_col(QK // HEAD), pipeline_mode=pl.Buffered(1)), gspec] + [ANY] * 3,
                group_specs(HB) + [pl.BlockSpec((HB, sw), row_map), pl.BlockSpec((seq // 4, PW), first_row)],
                [sds(*b.shape, F32) for b in bufs] + [sds(d, sw, F32), sds(seq // 4, PW)],
                [idx, h, ga, gb, *bufs], 2 * seq * d * sw, scratch=[pltpu.VMEM((HB, seq), BF)],
                aliases={4 + n: n for n in range(3)})


def place_body(s_ref, rcv, *rest):
    q_out, k_out, v_out = rest[-3:]
    q_out[...] = rcv[:, :GW]
    k_out[...] = rcv[:, GW:QK]
    v_out[...] = rcv[:, QK:]


def place(idx, rcv, bufs):
    d, w = rcv.shape
    bm = BLK
    return call(place_body, (d // bm,), [pl.BlockSpec((bm, w), row_map)] + [ANY] * 3, group_specs(bm),
                [sds(*b.shape, F32) for b in bufs], [idx, rcv, *bufs], d * w, aliases={2 + n: n for n in range(3)})


def dx_body(s_ref, x_ref, dy_ref, gain_ref, inv_ref, *rest):
    pieces, weights, rcv = rest[:8], rest[8:20], rest[20]
    dx_hbm, dg_ref, fq, fk, fv, acc, xs, tot, dx_ref, dx_sem, sem = rest[-11:]
    n = pl.program_id(0)
    bn = x_ref.shape[1]
    rows, d = acc.shape
    copies = scatter(rcv, (fq, fk, fv), s_ref[1], s_ref[3], sem)
    for copy in copies:
        copy.start()

    @pl.when(n == 0)
    def _():
        tot[...] = jnp.zeros_like(tot)

    cuts = (slice(0, GW), slice(GW, QK), slice(QK, PW))
    lhs = jnp.concatenate([pieces[2 * p + g][:, c] for p in range(4) for c in cuts for g in range(2)], axis=1)
    rhs = jnp.concatenate([r[...] for r in weights], axis=1)
    dh = mm_nt(lhs, rhs)
    inv = inv_ref[...]
    for c in range(bn // HEAD):
        cols = head_cols(c)
        xb = x_ref[:, cols]
        xs[:, ds(n * bn + cols.start, HEAD)] = xb
        part, xf = dh[:, cols], xb.astype(F32)
        scaled = part * gain_ref[:, cols]
        tot[...] += scaled * xf
        acc[:, ds(n * bn + cols.start, HEAD)] = dy_ref[:, cols].astype(F32) + inv * scaled
        dg_ref[:, cols] = jnp.sum((part * (xf * inv)).reshape(rows // 8, 8, HEAD), axis=0)

    @pl.when(n == pl.num_programs(0) - 1)
    def _():
        step = HEAD // 2

        def stats(r):
            sl = ds(r * step, step)
            inv = inv_ref[sl, :]
            tot[sl, :] = jnp.broadcast_to(jnp.sum(tot[sl, :], axis=-1, keepdims=True) / d, (step, HEAD)) * inv * inv * inv

        loop(rows // step, stats)

        def epi(r):
            sl = ds(r * step, step)
            coef = tot[sl, :]
            for c in range(d // HEAD):
                cols = head_cols(c)
                dx_ref[sl, cols] = (acc[sl, cols] - xs[sl, cols].astype(F32) * coef).astype(BF)
            send(r).start()

        def send(r):
            sl = ds(r * step, step)
            return pltpu.make_async_copy(dx_ref.at[sl, :], dx_hbm.at[sl, :], dx_sem)

        loop(rows // step, epi)
        loop(rows // step, lambda r: send(r).wait())

    for copy in copies:
        copy.wait()


def dx_call(idx, x, dy, gain, inv, pieces, ws, rcv, bufs):
    rows, d = x.shape
    bn = HB
    once = pl.Buffered(1)
    maps = (own_map, own_map, first_row, first_row) * 2
    return call(dx_body, (d // bn,),
                [pl.BlockSpec((rows, bn), col_map)] * 2 + [pl.BlockSpec((1, bn), col_map), pl.BlockSpec((rows, HEAD), own_map)]
                + [pl.BlockSpec((rows, PW), m, pipeline_mode=once) for m in maps]
                + [pl.BlockSpec((bn, w.shape[1] // 4), lambda n, s, p=p: (n, s[p])) for p in range(4) for w in ws]
                + [pl.BlockSpec((bn, rcv.shape[1]), row_map)] + [ANY] * 3,
                [ANY, pl.BlockSpec((8, bn), col_map)] + [ANY] * 3,
                [sds(rows, d), sds(8, d, F32)] + [sds(*b.shape, F32) for b in bufs],
                [idx, x, dy, gain, inv, *pieces] + list(ws) * 4 + [rcv, *bufs], 16 * rows * d * PW,
                scratch=[pltpu.VMEM((rows, d), F32), pltpu.VMEM((rows, d), BF), pltpu.VMEM((rows, HEAD), F32),
                         pltpu.VMEM((rows, d), BF), pltpu.SemaphoreType.DMA, pltpu.SemaphoreType.DMA((5,))],
                aliases={26 + n: 2 + n for n in range(3)})


def solution(mesh):
    sp = mesh.shape['sp']
    cross = [(a, a ^ 2) for a in range(sp)]
    pair = [(a, a ^ 1) for a in range(sp)]

    def over(val):
        return lax.ppermute(val, 'sp', cross)

    def near(val):
        return lax.ppermute(val, 'sp', pair)

    def both(val):
        return lax.ppermute(val, 'sp', [(a, a ^ 3) for a in range(sp)])

    def after(val, *deps):
        return lax.optimization_barrier((val,) + deps)[0]

    def vec(*vals, dep=()):
        out = jnp.stack([jnp.asarray(v, jnp.int32) for v in vals])
        return after(out, *dep) if dep else out

    def step(x, dy, positions, gain, w_q, w_k, w_v, w_o):
        j = lax.axis_index('sp').astype(jnp.int32)
        rows, d = x.shape
        seq = rows * sp
        j1, j2, j3 = [j ^ n for n in (1, 2, 3)]
        dev = (j, j1, j2, j3)
        hpr = rows // HB
        ws = (w_q, w_k, w_v)

        gain_f = gain.astype(F32).reshape(1, d)

        cut, mid = rows - HB, rows // 2
        xa = x[mid:cut]
        positions = after(positions, xa)
        pos2 = over(positions)
        pos1 = near(positions)
        x2a = over(xa)
        xb = after(x, xa)[:mid]
        x2b = over(xb)
        x2c = over(after(x, xb)[cut:])
        x1 = near(x)
        pos3 = near(pos2)
        dy1 = near(after(dy, x1))

        pos = jnp.zeros((seq,), jnp.int32)
        for blk, val in zip(dev, (positions, pos1, pos2, pos3)):
            pos = lax.dynamic_update_slice(pos, val, (blk * rows,))
        inv_freq = ROPE_THETA ** (-jnp.arange(0, HEAD, 2).astype(F32) / HEAD)
        angles = pos.astype(F32)[:, None] * inv_freq[None, :]
        cos_h, sin_h = jnp.cos(angles), jnp.sin(angles)
        tabs = (jnp.concatenate([cos_h, cos_h], axis=1), jnp.concatenate([-sin_h, sin_h], axis=1))

        dya, dyb = dy[:cut], dy[cut:]
        bufs = project(vec(j * hpr, j1 * hpr, j, dep=(dya, dyb)), (x, x1), gain_f, ws, tabs, None, seq)
        dbufs = dout(vec(j * hpr, j1 * hpr, j, dep=bufs), (dy, dy1), w_o, None, seq)

        chip, nh = j // 2, seq // BLK // 2
        tri = row_tasks(0, nh)
        first = seq // 2 - BLK
        square = [(i + nh, nh, 0, i) for i in range(nh)]

        def table(head, tasks):
            return jnp.concatenate([vec(*head, len(tasks)), jnp.asarray(tasks, jnp.int32).reshape(-1)])

        c_tasks = table((j1, 0), tri).at[HEADER - 1].set(nh - 1)
        local = attn_fwd("local", after(table((j1, chip), tri), *dbufs), *bufs[1:4])
        rest_tasks = jnp.where(chip == 0, table((j1, 0), row_tasks(nh, 2 * nh) * 2).at[HEADER - 1].set(nh),
                               table((j1, 1), tri + square))

        dy2a = over(after(dya, *bufs))
        dy2b = over(after(dyb, *bufs))
        x2a = after(x2a, *bufs)
        x3a = near(x2a)
        x2b = after(x2b, *local)
        x3b = near(x2b)
        idx = vec(*(dev * hpr + at // HB for dev in (j2, j3) for at in (mid, 0)), j, dep=local)
        bufs = project(idx, (x2a, x2b, x3a, x3b), gain_f, ws, tabs, bufs, seq)
        x2c = after(x2c, *bufs)
        x3c = near(x2c)
        bufs = project(vec((j2 + 1) * hpr - 1, (j3 + 1) * hpr - 1, j), (x2c, x3c), gain_f, ws, tabs, bufs, seq)
        h_all, q, k, v, inv = bufs
        o, lse, o_hi, o_pair = attn_fwd("rest", rest_tasks, q, k, v, (seq - first, rows), local)
        orv = over(o_hi)
        o1 = near(o_pair)
        qc, kc, vc = project_first(vec(j2, dep=(o,)), h_all, ws, tabs, first)
        dy2a = after(dy2a, qc)
        dy3a = near(dy2a)
        oc = attn_fwd("local", c_tasks, qc, kc, vc)[0]

        dbufs = dout(vec(j2 * hpr, j3 * hpr, j, dep=(oc,)), (dy2a, dy3a), w_o, dbufs, seq)
        dy2b = after(dy2b, *dbufs)
        dy3b = near(dy2b)
        dbufs = dout(vec((j2 + 1) * hpr - 1, (j3 + 1) * hpr - 1, j), (dy2b, dy3b), w_o, dbufs, seq)
        dy_all, do = dbufs

        ga, ga_pair = attn_bwd(vec(j1, 0), q, do, o, k, v, lse, tabs, rows)
        ga2 = over(ga)
        ga1 = near(ga_pair)
        gb, gb_pair = attn_bwd(vec(j1, 1, dep=(ga,)), q, do, o, k, v, lse, tabs, rows)
        gb2 = over(gb)
        gb1 = near(gb_pair)

        orv = after(orv, gb)
        ox, ox_pair = pick_rows(vec(j, j1, nh - 1, dep=(gb,)), oc, orv, rows)
        o3 = near(ox_pair)
        wo_fin, wo_snd = dw_o(vec(j, j2, dep=(gb,)), o, oc, orv, dy_all)
        wo_rcv = near(wo_snd)
        result = out_proj(vec(*dev, dep=(wo_snd,)), x, (o, o1, ox, o3), w_o)
        ga2 = after(ga2, wo_snd)
        fq, fk, fv, snd, wo_fin, g3 = dw_own(vec(*dev, dep=(result,)), h_all, ga, gb, ga2, wo_rcv, wo_fin)
        rcv = near(snd)
        ga3 = near(g3)

        gb2 = after(gb2, snd)
        fq, fk, fv, snd_b, g3b = dw_group(vec(j2, j1), h_all, ga2, gb2, (fq, fk, fv))
        gb3 = near(g3b)
        rcv_b = near(snd_b)
        grad_x, dg, fq, fk, fv = dx_call(vec(*dev, dep=(snd_b,)), x, dy, gain_f, inv,
                                         (ga, gb, ga1, gb1, ga2, gb2, ga3, gb3), ws, rcv, (fq, fk, fv))
        dg = jnp.sum(dg, axis=0)
        dg = (dg + near(dg)) + (over(dg) + both(dg))
        fq, fk, fv = place(vec(j3), rcv_b, (fq, fk, fv))
        return result, grad_x, fq, fk, fv, wo_fin, dg

    seq_spec = P(('dp', 'sp'), None)
    whole = P(None, None)
    part_rows = P('dp', None)
    return jax.shard_map(step, mesh=mesh,
                         in_specs=(seq_spec, seq_spec, P(('dp', 'sp')), P(None), whole, whole, whole, whole),
                         out_specs=(seq_spec, seq_spec, part_rows, part_rows, part_rows, part_rows, P('dp')),
                         check_vma=False)
```

```python
import math

import jax
import jax.numpy as jnp
from jax import lax
from jax.experimental import pallas as pl
from jax.experimental.pallas import tpu as pltpu
from jax.sharding import PartitionSpec as P


HEAD = 128
GROUP = 3
GW = GROUP * HEAD
QK = GW + HEAD
PW = QK + HEAD
PAIR = 2 * HEAD
ROPE_THETA = 1000000.0
NORM_EPS = 1e-05
NEG_LARGE = -1e30
BF = jnp.bfloat16
F32 = jnp.float32
SCALE = HEAD ** -0.5
SCALE2 = SCALE * math.log2(math.e)
BLK = 512
HB = BLK // 2
VMEM_LIMIT = 65011712
ANY = pl.BlockSpec(memory_space=pl.ANY)


def first_row(i, s):
    return (0, 0)


def at_row(r):
    return (r, 0)


def at_col(c):
    return (0, c)


def row_map(i, s):
    return at_row(i)


def col_map(i, s):
    return at_col(i)


def own_map(i, s):
    return at_row(s[0])


def sds(rows, cols, dtype=BF):
    return jax.ShapeDtypeStruct((rows, cols), dtype)


def call(body, grid, in_specs, out_specs, out_shape, args, flops, scratch=(), aliases=None):
    return pl.pallas_call(
        body,
        grid_spec=pltpu.PrefetchScalarGridSpec(
            num_scalar_prefetch=1, grid=grid, in_specs=in_specs, out_specs=out_specs, scratch_shapes=list(scratch)),
        out_shape=out_shape, input_output_aliases=aliases or {},
        compiler_params=pltpu.CompilerParams(dimension_semantics=("arbitrary",) * len(grid),
                                             vmem_limit_bytes=VMEM_LIMIT),
        cost_estimate=pl.CostEstimate(flops=int(flops), bytes_accessed=int(flops) // BLK,
                                      transcendentals=0))(*args)


def down(shape):
    return lax.broadcasted_iota(jnp.int32, shape, 0)


def across(shape):
    return lax.broadcasted_iota(jnp.int32, shape, 1)


def loop(count, body):
    def run(c, _):
        body(c)
        return 0

    lax.fori_loop(0, count, run, 0)


def one(h):
    return slice(h, h + 1)


def head_cols(h):
    return slice(h * HEAD, h * HEAD + HEAD)


def mm(a, b):
    return jnp.dot(a, b, preferred_element_type=F32)


def mm_nt(a, b):
    return lax.dot_general(a, b, (((1,), (1,)), ((), ())), preferred_element_type=F32)


def rotate(val, cos_t, sin_t):
    return val * cos_t + pltpu.roll(val, HEAD // 2, 1) * sin_t


def ds(start, size):
    return pl.ds(pl.multiple_of(start, size), size)


def split3(val):
    hi = val.astype(BF).astype(F32)
    mid = (val - hi).astype(BF).astype(F32)
    return hi, mid, val - hi - mid


def qkv_of(h, wq_ref, wk_ref, wv_ref, cos_ref, sin_ref, q_ref, k_ref, v_ref):
    cos_t, sin_t = cos_ref[...], sin_ref[...]
    out = mm(h, wq_ref[...])
    for c in range(wq_ref.shape[1] // HEAD):
        sl = head_cols(c)
        q_ref[:, sl] = rotate(out[:, sl], cos_t, sin_t).astype(BF)
    out = mm(h, jnp.concatenate([wk_ref[...], wv_ref[...]], axis=1))
    for sl in (slice(0, HEAD), slice(HEAD, PAIR)):
        k_ref[:, sl] = rotate(out[:, sl], cos_t, sin_t).astype(BF)
    v_ref[...] = out[:, PAIR:].astype(BF)


def sources(arrays):
    steps = [arr.shape[0] // HB for arr in arrays]
    first = [sum(steps[:n]) for n in range(len(steps))]
    specs = []
    for at, count in zip(first, steps):
        specs.append(pl.BlockSpec((HB, arrays[0].shape[1]), lambda i, s, a=at, c=count: at_row(jnp.clip(i - a, 0, c - 1))))

    def out_map(i, s):
        row = s[0] + i
        for n, at in enumerate(first):
            row = jnp.where(i >= at, s[n] + i - at, row)
        return at_row(row)

    return first, steps, specs, out_map


def take(refs, first, steps, dst):
    for ref, at, count in zip(refs, first, steps):
        @pl.when(jnp.logical_and(pl.program_id(0) >= at, pl.program_id(0) < at + count))
        def _(ref=ref):
            dst[...] = ref[...]


def proj_body(first, steps, s_ref, *rest):
    n = len(first)
    gain_ref, wq_ref, wk_ref, wv_ref, cos_ref, sin_ref = rest[n:n + 6]
    h_ref, q_ref, k_ref, v_ref, inv_ref, src = rest[-6:]
    take(rest, first, steps, src)
    step = HEAD

    def stats(c):
        sl = ds(c * step, step)
        xf = src[sl, :].astype(F32)
        inv = lax.rsqrt(jnp.mean(xf * xf, axis=-1, keepdims=True) + NORM_EPS)
        inv_ref[sl, :] = jnp.broadcast_to(inv, (step, HEAD))

    def scale(c):
        sl = ds(c * step, step)
        inv, gain = inv_ref[sl, :], gain_ref[...]
        for m in range(src.shape[1] // HEAD):
            cols = head_cols(m)
            h_ref[sl, cols] = (src[sl, cols].astype(F32) * inv * gain[:, cols]).astype(BF)

    loop(src.shape[0] // step, stats)
    loop(src.shape[0] // step, scale)
    qkv_of(h_ref[...], wq_ref, wk_ref, wv_ref, cos_ref, sin_ref, q_ref, k_ref, v_ref)


def project(idx, xs, gain, ws, tabs, bufs, seq):
    d = xs[0].shape[1]
    first, steps, specs, out_map = sources(xs)
    widths = [w.shape[1] // 4 for w in ws]
    in_specs = specs + [pl.BlockSpec((1, d), first_row)]
    in_specs += [pl.BlockSpec((d, w), lambda i, s: at_col(s[len(xs)])) for w in widths]
    in_specs += [pl.BlockSpec((HB, HEAD), out_map)] * 2
    args = [idx, *xs, gain, *ws, *tabs]
    aliases = {}
    if bufs is not None:
        in_specs += [ANY] * len(bufs)
        aliases = {len(args) + n: n for n in range(len(bufs))}
        args += list(bufs)
    return call(lambda *refs: proj_body(first, steps, *refs), (sum(steps),), in_specs,
                [pl.BlockSpec((HB, w), out_map) for w in (d, *widths, HEAD)],
                [sds(seq, w) for w in (d, *widths)] + [sds(seq, HEAD, F32)], args, sum(steps) * BLK * d * sum(widths),
                scratch=[pltpu.VMEM((HB, d), BF)], aliases=aliases)


def projc_body(s_ref, h_ref, *rest):
    qkv_of(h_ref[...], *rest)


def project_first(idx, h, ws, tabs, rows):
    seq, d = h.shape
    widths = [w.shape[1] // 4 for w in ws]
    return call(projc_body, (rows // BLK,),
                [pl.BlockSpec((BLK, d), row_map)] + [pl.BlockSpec((d, w), lambda i, s: at_col(s[0])) for w in widths]
                + [pl.BlockSpec((BLK, HEAD), row_map)] * 2,
                [pl.BlockSpec((BLK, w), row_map) for w in widths], [sds(seq, w) for w in widths],
                [idx, h, *ws, *tabs], 2 * rows * d * sum(widths))


def dout_body(first, steps, s_ref, *rest):
    wo_ref, dy_out, do_out = rest[len(first)], *rest[-2:]
    take(rest, first, steps, dy_out)
    do_out[...] = mm_nt(dy_out[...], wo_ref[...]).astype(BF)


def dout(idx, dys, w_o, bufs, seq):
    d, oc = dys[0].shape[1], w_o.shape[0] // 4
    first, steps, specs, out_map = sources(dys)
    in_specs = specs + [pl.BlockSpec((oc, d), lambda i, s: at_row(s[len(dys)]))]
    args = [idx, *dys, w_o]
    aliases = {}
    if bufs is not None:
        in_specs += [ANY] * len(bufs)
        aliases = {len(args) + n: n for n in range(len(bufs))}
        args += list(bufs)
    return call(lambda *refs: dout_body(first, steps, *refs), (sum(steps),), in_specs,
                [pl.BlockSpec((HB, w), out_map) for w in (d, oc)],
                [sds(seq, w) for w in (d, oc)], args, sum(steps) * BLK * d * oc, aliases=aliases)


TASK = 4
HEADER = 3


def row_tasks(first, last):
    return [(i, i + 1, 1, -1) for i in range(first, last)]


def fwd_body(kind, s_ref, q_ref, k_ref, v_ref, *rest):
    qt, kk, vt, s_scr, acc, stat = rest[-6:]
    if kind == "rest":
        o1_ref, lse1_ref, st_ref, o_ref, lse_ref, hi_ref, pair_ref = rest[:7]
    else:
        o_ref, lse_ref = rest[:2]
    seq = k_ref.shape[0]

    def setup(c):
        sl = ds(c * BLK, BLK)
        vt[:, sl] = v_ref[sl, :].T
        kk[sl, :HEAD] = k_ref[sl, :]
        kk[sl, HEAD:] = k_ref[sl, :]
        for h in range(GROUP):
            qf = q_ref[sl, head_cols(h)].astype(F32) * SCALE2
            hi = qf.astype(BF)
            qt[h, :HEAD, sl] = hi.T
            qt[h, HEAD:, sl] = (qf - hi.astype(F32)).astype(BF).T

    loop(seq // BLK, setup)
    acc[...] = jnp.zeros_like(acc)
    stat[...] = jnp.zeros_like(stat)
    cur, old, den_row = 0, 1, 2
    lse_ref[...] = jnp.zeros_like(lse_ref)
    if kind == "rest":
        @pl.when(s_ref[1] == 0)
        def _():
            o_ref[:seq // 2, :] = o1_ref[...]
            lse_ref[0, :, :seq // 2] = lse1_ref[0]

    def task(t):
        return [s_ref[HEADER + t * TASK + n] for n in range(TASK)]

    def stage_a(h, i, j, masked, init=None):
        row = one(h)
        if masked is True:
            top = mm(kk[ds(j * BLK, HB), :], qt[h, :, ds(i * BLK, BLK)])
            low = mm(kk[ds(j * BLK + HB, HB), :], qt[h, :, ds(i * BLK + HB, HB)])
            top = jnp.where(down(top.shape) <= across(top.shape), top, NEG_LARGE)
            low = jnp.where(down(low.shape) <= across(low.shape), low, NEG_LARGE)
            s_scr[h, :HB, :] = top
            s_scr[h, HB:, HB:] = low
            m_new = jnp.max(top, axis=0, keepdims=True)
            right = jnp.maximum(m_new[:, HB:], jnp.max(low, axis=0, keepdims=True))
            m_new = jnp.concatenate([m_new[:, :HB], right], axis=1)
        else:
            s = mm(kk[ds(j * BLK, BLK), :], qt[h, :, ds(i * BLK, BLK)])
            if masked is not False:
                keep = down(s.shape) <= across(s.shape)
                s = jnp.where(jnp.logical_or(keep, jnp.logical_not(masked)), s, NEG_LARGE)
            s_scr[h] = s
            m_new = jnp.max(s, axis=0, keepdims=True)
        if init is None:
            m_old = stat[cur, row]
        elif kind == "rest":
            m_old = jnp.where(init >= 0, lse1_ref[0, row, ds(jnp.maximum(init, 0) * BLK, BLK)], NEG_LARGE)
        else:
            m_old = jnp.full(m_new.shape, NEG_LARGE, F32)
        m_new = jnp.maximum(m_old, m_new)
        stat[old, row] = jnp.exp2(m_old - m_new)
        stat[cur, row] = m_new

    def stage_p(h, diag=False):
        row = one(h)
        m, alpha = stat[cur, row], stat[old, row]
        if diag:
            top = jnp.exp2(s_scr[h, :HB, :] - m)
            low = jnp.exp2(s_scr[h, HB:, HB:] - m[:, HB:])
            total = jnp.sum(top, axis=0, keepdims=True)
            right = total[:, HB:] + jnp.sum(low, axis=0, keepdims=True)
            total = jnp.concatenate([total[:, :HB], right], axis=1)
            top = top.astype(BF)
            p = (top[:, :HB], jnp.concatenate([top[:, HB:], low.astype(BF)], axis=0))
        else:
            p = jnp.exp2(s_scr[h] - m)
            total = jnp.sum(p, axis=0, keepdims=True)
            p = p.astype(BF)
        stat[den_row, row] = stat[den_row, row] * alpha + total
        return p, alpha

    def stage_v(h, j, held, diag=False):
        p, alpha = held
        if diag:
            acc[h, :, :HB] = acc[h, :, :HB] * alpha[:, :HB] + mm(vt[:, ds(j * BLK, HB)], p[0])
            acc[h, :, HB:] = acc[h, :, HB:] * alpha[:, HB:] + mm(vt[:, ds(j * BLK, BLK)], p[1])
        else:
            acc[h] = acc[h] * alpha + mm(vt[:, ds(j * BLK, BLK)], p)

    def finish(h, i, den, top):
        row = one(h)
        out = acc[h] / den
        o_ref[ds(i * BLK, BLK), head_cols(h)] = out.T.astype(BF)
        lse_ref[0, row, ds(i * BLK, BLK)] = top + jnp.log2(den)
        if kind == "local":
            rest[2][0, h, :, ds(i * BLK, BLK)] = out

    def pipeline(i, j, masked):
        for h in range(GROUP):
            held = stage_p(h)
            stage_a(h, i, j + 1, masked)
            stage_v(h, j, held)

    count = s_ref[HEADER - 1]
    i, steps, diag, init = task(0)
    for h in range(GROUP):
        stage_a(h, i, 0, jnp.logical_and(steps == 1, diag == 1), init)

    def row(t):
        i, steps, diag, _ = task(t)

        loop(steps - 2, lambda j: pipeline(i, j, False))

        pl.when(jnp.logical_and(steps > 1, diag == 1))(lambda: pipeline(i, steps - 2, True))
        if kind == "rest":
            pl.when(diag == 0)(lambda: pipeline(i, steps - 2, False))
        i2, _, _, init2 = task(jnp.minimum(t + 1, count - 1))

        def last_step(on_diag):
            for h in range(GROUP):
                held = stage_p(h, on_diag)
                final = (stat[den_row, one(h)], stat[cur, one(h)])
                stage_a(h, i2, 0, False, init2)
                stage_v(h, steps - 1, held, on_diag)
                finish(h, i, *final)

        if kind != "rest":
            last_step(True)
        else:
            pl.when(diag == 1)(lambda: last_step(True))
            pl.when(diag == 0)(lambda: last_step(False))

            @pl.when(init2 >= 0)
            def _():
                stat[den_row] = jnp.ones(stat.shape[1:], F32)
                for h in range(GROUP):
                    acc[h] = st_ref[0, h, :, ds(init2 * BLK, BLK)]

    loop(count, row)
    if kind == "rest":
        hi_ref[...] = o_ref[seq - hi_ref.shape[0]:, :]
        pair_ref[...] = o_ref[ds(s_ref[0] * pair_ref.shape[0], pair_ref.shape[0]), :]


def attn_fwd(kind, idx, q, k, v, extra=(), local=()):
    whole = q.shape[0]
    seq = whole if kind == "rest" else whole // 2
    nkv = k.shape[1] // HEAD

    def half_map(g, s):
        return (s[1], g)

    def head_map(g, s):
        return (g, 0, 0)

    def state_map(g, s):
        return (g, 0, 0, 0)

    at = half_map if kind == "local" else col_map
    lse_spec = pl.BlockSpec((1, 8, seq), head_map)
    outs, specs = [sds(seq, q.shape[1]), jax.ShapeDtypeStruct((nkv, 8, seq), F32)], []
    out_specs = [pl.BlockSpec((seq, GW), col_map), lse_spec]
    state = pl.BlockSpec((1, GROUP, HEAD, whole // 2), state_map)
    if kind == "local":
        outs.append(jax.ShapeDtypeStruct((nkv, GROUP, HEAD, seq), F32))
        out_specs.append(state)
    if kind == "rest":
        specs = [pl.BlockSpec((seq // 2, GW), col_map), pl.BlockSpec((1, 8, seq // 2), head_map), state]
        outs += [sds(r, q.shape[1]) for r in extra]
        out_specs += [pl.BlockSpec((r, GW), col_map) for r in extra]
    kspec = pl.BlockSpec((seq, HEAD), at)
    return call(lambda *refs: fwd_body(kind, *refs), (nkv,), [pl.BlockSpec((seq, GW), at), kspec, kspec] + specs,
                out_specs, outs, [idx, q, k, v, *local], nkv * GROUP * seq * seq * PAIR,
                scratch=[pltpu.VMEM((GROUP, PAIR, seq), BF), pltpu.VMEM((seq, PAIR), BF),
                         pltpu.VMEM((HEAD, seq), BF), pltpu.VMEM((GROUP, BLK, BLK), F32),
                         pltpu.VMEM((GROUP, HEAD, BLK), F32), pltpu.VMEM((GROUP, 8, BLK), F32)])


def bwd_body(s_ref, q_ref, do_ref, o_ref, lse_ref, qn_ref, don_ref, on_ref, lsen_ref, k_ref, v_ref, cos_hbm, sin_hbm,
             out_ref, pair_ref, ka, va, dkt, dvt, tab, tab_sem, *sets):
    i = pl.program_id(0)
    last = pl.num_programs(0) - 1
    seq = k_ref.shape[0]
    m3 = GROUP * HB
    cos_ref, sin_ref = tab.at[0], tab.at[1]

    def spots():
        for b in range(2):
            for h in range(GROUP):
                start = (b * GROUP + h) * HB
                yield h, slice(b * HB, b * HB + HB), head_cols(h), slice(start, start + HB)

    def pick(n):
        return [ref.at[n] for ref in sets]

    def prepare(q_src, do_src, o_src, lse_src, dst):
        qa, da, q3t, do3t, dq3 = dst
        srow = down((16, HB))
        blank = jnp.zeros((HEAD - 16, HB), BF)
        for h, src, cols, rows in spots():
            qh, doh = q_src[src, cols], do_src[src, cols]
            qa[rows, :HEAD] = qh
            da[rows, :HEAD] = doh
            q3t[:, rows] = qh.T
            dt = doh.T
            do3t[:, rows] = dt
            delta = jnp.sum(dt.astype(F32) * o_src[src, cols].T.astype(F32), axis=0, keepdims=True)
            parts = jnp.zeros((16, HB), F32)
            for n, part in enumerate(split3(lse_src[0, one(h), src] * (1.0 / SCALE2)) + split3(delta)):
                parts = jnp.where(srow == n, part, parts)
            block = jnp.concatenate([parts.astype(BF), blank], axis=0).T
            qa[rows, HEAD:] = block
            da[rows, HEAD:] = block
        dq3[...] = jnp.zeros_like(dq3)

    @pl.when(i == 0)
    def _():
        copies = [pltpu.make_async_copy(src, tab.at[n], tab_sem.at[n]) for n, src in enumerate((cos_hbm, sin_hbm))]
        for copy in copies:
            copy.start()
        dkt[...] = jnp.zeros_like(dkt)
        dvt[...] = jnp.zeros_like(dvt)

        def setup(c):
            sl = ds(c * BLK, BLK)
            third = across((BLK, HEAD)) // 3
            for n, (src, dst) in enumerate(((k_ref, ka), (v_ref, va))):
                dst[sl, :HEAD] = src[sl, :]
                dst[sl, HEAD:] = jnp.where(third == n, -1.0, 0.0).astype(BF)

        loop(seq // BLK, setup)
        prepare(q_ref, do_ref, o_ref, lse_ref, pick(0))
        for copy in copies:
            copy.wait()

    def scores(mine, rows, start, width):
        sl = pl.ds(pl.multiple_of(start, BLK), width)
        return rows, sl, width, mm_nt(mine[0][rows, :], ka[sl, :]), mm_nt(mine[1][rows, :], va[sl, :])

    def grads(mine, held, masked):
        _, _, q3t, do3t, dq3 = mine
        rows, sl, width, s, dp = held
        p = jnp.exp2(s * SCALE2)
        if masked:
            off = width - HB
            tail = p[:, off:]
            keep = down(tail.shape) % HB >= across(tail.shape)
            tail = jnp.where(keep, tail, 0.0)
            p = jnp.concatenate([p[:, :off], tail], axis=1) if off else tail
        dvt[:, sl] += mm(do3t[:, rows], p.astype(BF))
        dsv = (p * dp).astype(BF)
        dkt[:, sl] += mm(q3t[:, rows], dsv)
        dq3[rows, :] += mm(dsv, ka[sl, :HEAD])

    par, start = i % 2, (i // 2) * 2 * BLK

    def pair_step(t):
        mine = pick(par)
        grads(mine, scores(mine, slice(0, 2 * m3), t * 2 * BLK, 2 * BLK), False)

    loop(i // 2, pair_step)

    def finish(done, blk):
        for h, src, cols, rows in spots():
            rsl = ds(blk * BLK + src.start, HB)
            out_ref[rsl, cols] = rotate(done[-1][rows, :] * SCALE, cos_ref[rsl, :], -sin_ref[rsl, :]).astype(BF)

    def tail_steps(n):
        mine, width = pick(n), (n + 1) * BLK
        low = scores(mine, slice(0, m3), start, width - HB)
        high = scores(mine, slice(m3, 2 * m3), start, width)
        grads(mine, low, True)
        other = pick(1 - n)
        finish(other, jnp.maximum(i - 1, 0))
        prepare(qn_ref, don_ref, on_ref, lsen_ref, other)
        grads(mine, high, True)

    pl.when(par == 0)(lambda: tail_steps(0))
    pl.when(par == 1)(lambda: tail_steps(1))

    @pl.when(i == last)
    def _():
        finish(pick(par), i)

        def fin(c):
            sl = ds(c * 2 * BLK, 2 * BLK)
            out_ref[sl, GW:QK] = rotate(dkt[:, sl].T * SCALE, cos_ref[sl, :], -sin_ref[sl, :]).astype(BF)
            out_ref[sl, QK:] = dvt[:, sl].T.astype(BF)

        loop(seq // BLK // 2, fin)
        pair_ref[...] = out_ref[ds(s_ref[0] * pair_ref.shape[0], pair_ref.shape[0]), :]


def attn_bwd(idx, q, do, o, k, v, lse, tabs, rows):
    seq = k.shape[0]
    nq = seq // BLK
    m3 = GROUP * BLK
    kspec = pl.BlockSpec((seq, HEAD), lambda i, s: at_col(s[1]))
    row_specs = []
    for ahead in range(2):
        row_specs += [pl.BlockSpec((BLK, GW), lambda i, s, a=ahead: (jnp.minimum(i + a, nq - 1), s[1]))] * 3
        row_specs += [pl.BlockSpec((1, 8, BLK), lambda i, s, a=ahead: (s[1], 0, jnp.minimum(i + a, nq - 1)))]
    two_sets = [pltpu.VMEM((2, m3, PAIR), BF)] * 2 + [pltpu.VMEM((2, HEAD, m3), BF)] * 2 + [pltpu.VMEM((2, m3, HEAD), F32)]
    return call(bwd_body, (nq,),
                row_specs + [kspec] * 2 + [ANY] * 2,
                [pl.BlockSpec((r, PW), first_row) for r in (seq, rows)], [sds(r, PW) for r in (seq, rows)],
                [idx] + [q, do, o, lse] * 2 + [k, v, *tabs], GROUP * nq * (nq + 1) * BLK * BLK * PW,
                scratch=[pltpu.VMEM((seq, PAIR), BF)] * 2 + [pltpu.VMEM((HEAD, seq), F32)] * 2
                + [pltpu.VMEM((2, seq, HEAD), F32), pltpu.SemaphoreType.DMA((2,))] + two_sets)


def half(i, s, n):
    return s[n] * 2 + i


def pick_body(s_ref, oa, ra, ob, rb, own, pair):
    for n, (low, high, out) in enumerate(((oa, ra, own), (ob, rb, pair))):
        out[...] = jnp.where(half(pl.program_id(0), s_ref, n) < s_ref[2], low[...], high[...])


def pick_rows(idx, low, high, rows):
    w = low.shape[1]
    specs = []
    for n in range(2):
        specs.append(pl.BlockSpec((BLK, w), lambda i, s, n=n: at_row(jnp.minimum(half(i, s, n), s[2] - 1))))
        specs.append(pl.BlockSpec((BLK, w), lambda i, s, n=n: at_row(jnp.maximum(half(i, s, n) - s[2], 0))))
    return call(pick_body, (rows // BLK,), specs, [pl.BlockSpec((BLK, w), row_map)] * 2, [sds(rows, w)] * 2,
                [idx, low, high, low, high], rows * w)


def out_body(s_ref, x_ref, *rest):
    ops, out_ref = rest[:-1], rest[-1]
    lhs = jnp.concatenate([r[...] for r in ops[:4]], axis=1)
    rhs = jnp.concatenate([r[...] for r in ops[4:]], axis=0)
    out_ref[...] = (x_ref[...].astype(F32) + mm(lhs, rhs)).astype(BF)


def out_proj(idx, x, pieces, w_o):
    rows, d = x.shape
    hw = pieces[0].shape[1]
    return call(out_body, (d // BLK,),
                [pl.BlockSpec((rows, BLK), col_map)]
                + [pl.BlockSpec((rows, hw), m) for m in (own_map, first_row, first_row, first_row)]
                + [pl.BlockSpec((hw, BLK), lambda n, s, p=p: (s[p], n)) for p in range(4)],
                pl.BlockSpec((rows, BLK), col_map), sds(rows, d), [idx, x, *pieces] + [w_o] * 4,
                2 * rows * d * d)


def dwo_body(s_ref, oa_ref, ob_ref, oc_ref, dy_ref, fin, snd, ot):
    first, hw = ob_ref.shape

    @pl.when(jnp.logical_and(pl.program_id(0) == 0, pl.program_id(1) == 0))
    def _():
        for src, rows, base in ((oa_ref, slice(0, hw), 0), (ob_ref, slice(hw, 2 * hw), 0), (oc_ref, slice(hw, 2 * hw), first)):
            def tr(c):
                ot[rows, ds(c * BLK + base, BLK)] = src[ds(c * BLK, BLK), :].T

            loop(src.shape[0] // BLK, tr)

    val = mm(ot[ds(pl.program_id(1) * hw, hw), :], dy_ref[...])
    fin[...] = val
    snd[...] = val


def dw_o(idx, oa, ob, oc, dy):
    seq, d = dy.shape
    hw = oa.shape[1]
    o_specs = [pl.BlockSpec((r, hw), lambda i, p, s: first_row(i, s), pipeline_mode=pl.Buffered(1))
               for r in (seq, seq - oc.shape[0], oc.shape[0])]
    return call(dwo_body, (d // BLK, 2),
                o_specs + [pl.BlockSpec((seq, BLK), lambda i, p, s: at_col(i))],
                [pl.BlockSpec((hw, BLK), lambda i, p, s: (s[p], i)), pl.BlockSpec((hw, BLK), lambda i, p, s: (p, i))],
                [sds(4 * hw, d, F32), sds(2 * hw, d, F32)], [idx, oa, ob, oc, dy], 4 * seq * d * hw,
                scratch=[pltpu.VMEM((2 * hw, seq), BF)])


def dwown_body(s_ref, h_ref, ga_ref, gb_ref, gc_ref, wo_ref, _, fq, fk, fv, snd, wo_fin, g3, ht, sem, wsem):
    i, steps = pl.program_id(0), pl.num_programs(0)
    rows, per = wo_ref.shape[0], steps // 2
    start = jnp.where(i < per, s_ref[1] * per + i, s_ref[3] * per + i - per)
    wcopy = pltpu.make_async_copy(wo_ref, wo_fin.at[ds(start * rows, rows), :], wsem)
    wcopy.start()

    @pl.when(i > 1)
    def _():
        for copy in scatter(snd, (fq, fk, fv), s_ref[0], s_ref[2], sem.at[i % 2]):
            copy.wait()

    ht[...] = h_ref[...].T
    lhs = ht[...]
    for g, q_at, k_at in ((ga_ref, 0, 2 * GW), (gb_ref, GW, 2 * GW + HEAD), (gc_ref, 2 * PW, 2 * PW + GW)):
        val = mm(lhs, g[:, :QK])
        snd[:, q_at:q_at + GW] = val[:, :GW]
        snd[:, k_at:k_at + HEAD] = val[:, GW:]
    snd[:, 2 * QK:2 * PW] = mm(lhs, jnp.concatenate([ga_ref[:, QK:], gb_ref[:, QK:]], axis=1))
    for copy in scatter(snd, (fq, fk, fv), s_ref[0], s_ref[2], sem.at[i % 2]):
        copy.start()

    @pl.when(i == steps - 1)
    def _():
        g3[...] = gc_ref[ds(s_ref[1] * g3.shape[0], g3.shape[0]), :]
        for slot in range(2):
            for copy in scatter(snd, (fq, fk, fv), s_ref[0], s_ref[2], sem.at[slot]):
                copy.wait()

    wcopy.wait()


def scatter(rcv, outs, whole_dev, part_dev, sem):
    rows, src, copies = ds(pl.program_id(0) * rcv.shape[0], rcv.shape[0]), 0, []
    fq, fk, fv = outs
    for n, (out, col, w) in enumerate(((fq, whole_dev, 2 * GW), (fk, whole_dev, PAIR), (fv, whole_dev, PAIR),
                                       (fq, 2 * part_dev, GW), (fk, 2 * part_dev, HEAD))):
        copies.append(pltpu.make_async_copy(rcv.at[:, src:src + w], out.at[rows, ds(col * w, w)], sem.at[n]))
        src += w
    return copies


def dw_own(idx, h, ga, gb, gc, wo_rcv, wo_fin):
    seq, d = h.shape
    steps = d // HB
    gspec = pl.BlockSpec((seq, PW), first_row, pipeline_mode=pl.Buffered(1))
    widths = (2 * GW, PAIR, PAIR)
    sw = 2 * PW + QK
    return call(dwown_body, (steps,),
                [pl.BlockSpec((seq, HB), col_map)] + [gspec] * 3
                + [pl.BlockSpec((wo_rcv.shape[0] // steps, d), row_map), ANY],
                [ANY] * 3 + [pl.BlockSpec((HB, sw), row_map), ANY, pl.BlockSpec((seq // 4, PW), first_row)],
                [sds(d, 4 * w, F32) for w in widths] + [sds(d, sw, F32), sds(*wo_fin.shape, F32), sds(seq // 4, PW)],
                [idx, h, ga, gb, gc, wo_rcv, wo_fin], 2 * seq * d * sw,
                scratch=[pltpu.VMEM((HB, seq), BF), pltpu.SemaphoreType.DMA((2, 5)), pltpu.SemaphoreType.DMA],
                aliases={6: 4})


def dwgrp_body(s_ref, h_ref, ga_ref, gb_ref, *rest):
    fq, fk, fv, snd, g3, ht = rest[-6:]

    @pl.when(pl.program_id(0) == 0)
    def _():
        g3[...] = gb_ref[ds(s_ref[1] * g3.shape[0], g3.shape[0]), :]

    ht[...] = h_ref[...].T
    lhs = ht[...]
    val = mm(lhs, gb_ref[:, :QK])
    fq[...] = val[:, :GW]
    fk[...] = val[:, GW:]
    snd[:, :QK] = val
    val = mm(lhs, jnp.concatenate([ga_ref[...], gb_ref[:, QK:]], axis=1))
    fv[...] = val
    snd[:, QK:] = val


def group_specs(bm):
    return [pl.BlockSpec((bm, w), lambda i, s: (i, 2 * s[0] + 1)) for w in (GW, HEAD)] + \
        [pl.BlockSpec((bm, PAIR), lambda i, s: (i, s[0]))]


def dw_group(idx, h, ga, gb, bufs):
    seq, d = h.shape
    gspec = pl.BlockSpec((seq, PW), first_row, pipeline_mode=pl.Buffered(1))
    sw = QK + PAIR
    return call(dwgrp_body, (d // HB,),
                [pl.BlockSpec((seq, HB), col_map),
                 pl.BlockSpec((seq, HEAD), lambda i, s: at_col(QK // HEAD), pipeline_mode=pl.Buffered(1)), gspec] + [ANY] * 3,
                group_specs(HB) + [pl.BlockSpec((HB, sw), row_map), pl.BlockSpec((seq // 4, PW), first_row)],
                [sds(*b.shape, F32) for b in bufs] + [sds(d, sw, F32), sds(seq // 4, PW)],
                [idx, h, ga, gb, *bufs], 2 * seq * d * sw, scratch=[pltpu.VMEM((HB, seq), BF)],
                aliases={4 + n: n for n in range(3)})


def place_body(s_ref, rcv, *rest):
    q_out, k_out, v_out = rest[-3:]
    q_out[...] = rcv[:, :GW]
    k_out[...] = rcv[:, GW:QK]
    v_out[...] = rcv[:, QK:]


def place(idx, rcv, bufs):
    d, w = rcv.shape
    bm = 2 * BLK
    return call(place_body, (d // bm,), [pl.BlockSpec((bm, w), row_map)] + [ANY] * 3, group_specs(bm),
                [sds(*b.shape, F32) for b in bufs], [idx, rcv, *bufs], d * w, aliases={2 + n: n for n in range(3)})


def dx_body(s_ref, x_ref, dy_ref, gain_ref, inv_ref, *rest):
    pieces, weights, rcv = rest[:8], rest[8:20], rest[20]
    dx_hbm, dg_ref, fq, fk, fv, acc, xs, tot, dx_ref, dx_sem, sem = rest[-11:]
    n = pl.program_id(0)
    bn = x_ref.shape[1]
    rows, d = acc.shape
    copies = scatter(rcv, (fq, fk, fv), s_ref[1], s_ref[3], sem)
    for copy in copies:
        copy.start()

    @pl.when(n == 0)
    def _():
        tot[...] = jnp.zeros_like(tot)

    cuts = (slice(0, GW), slice(GW, QK), slice(QK, PW))
    lhs = jnp.concatenate([pieces[2 * p + g][:, c] for p in range(4) for c in cuts for g in range(2)], axis=1)
    rhs = jnp.concatenate([r[...] for r in weights], axis=1)
    dh = mm_nt(lhs, rhs)
    inv = inv_ref[...]
    for c in range(bn // HEAD):
        cols = head_cols(c)
        xb = x_ref[:, cols]
        xs[:, ds(n * bn + cols.start, HEAD)] = xb
        part, xf = dh[:, cols], xb.astype(F32)
        scaled = part * gain_ref[:, cols]
        tot[...] += scaled * xf
        acc[:, ds(n * bn + cols.start, HEAD)] = dy_ref[:, cols].astype(F32) + inv * scaled
        dg_ref[:, cols] = jnp.sum((part * (xf * inv)).reshape(rows // 8, 8, HEAD), axis=0)

    @pl.when(n == pl.num_programs(0) - 1)
    def _():
        step = HEAD // 2

        def stats(r):
            sl = ds(r * step, step)
            inv = inv_ref[sl, :]
            tot[sl, :] = jnp.broadcast_to(jnp.sum(tot[sl, :], axis=-1, keepdims=True) / d, (step, HEAD)) * inv * inv * inv

        loop(rows // step, stats)

        def epi(r):
            sl = ds(r * step, step)
            coef = tot[sl, :]
            for c in range(d // HEAD):
                cols = head_cols(c)
                dx_ref[sl, cols] = (acc[sl, cols] - xs[sl, cols].astype(F32) * coef).astype(BF)
            send(r).start()

        def send(r):
            sl = ds(r * step, step)
            return pltpu.make_async_copy(dx_ref.at[sl, :], dx_hbm.at[sl, :], dx_sem)

        loop(rows // step, epi)
        loop(rows // step, lambda r: send(r).wait())

    for copy in copies:
        copy.wait()


def dx_call(idx, x, dy, gain, inv, pieces, ws, rcv, bufs):
    rows, d = x.shape
    bn = HB
    once = pl.Buffered(1)
    maps = (own_map, own_map, first_row, first_row) * 2
    return call(dx_body, (d // bn,),
                [pl.BlockSpec((rows, bn), col_map)] * 2 + [pl.BlockSpec((1, bn), col_map), pl.BlockSpec((rows, HEAD), own_map)]
                + [pl.BlockSpec((rows, PW), m, pipeline_mode=once) for m in maps]
                + [pl.BlockSpec((bn, w.shape[1] // 4), lambda n, s, p=p: (n, s[p])) for p in range(4) for w in ws]
                + [pl.BlockSpec((bn, rcv.shape[1]), row_map)] + [ANY] * 3,
                [ANY, pl.BlockSpec((8, bn), col_map)] + [ANY] * 3,
                [sds(rows, d), sds(8, d, F32)] + [sds(*b.shape, F32) for b in bufs],
                [idx, x, dy, gain, inv, *pieces] + list(ws) * 4 + [rcv, *bufs], 16 * rows * d * PW,
                scratch=[pltpu.VMEM((rows, d), F32), pltpu.VMEM((rows, d), BF), pltpu.VMEM((rows, HEAD), F32),
                         pltpu.VMEM((rows, d), BF), pltpu.SemaphoreType.DMA, pltpu.SemaphoreType.DMA((5,))],
                aliases={26 + n: 2 + n for n in range(3)})


def solution(mesh):
    sp = mesh.shape['sp']
    cross = [(a, a ^ 2) for a in range(sp)]
    pair = [(a, a ^ 1) for a in range(sp)]

    def over(val):
        return lax.ppermute(val, 'sp', cross)

    def near(val):
        return lax.ppermute(val, 'sp', pair)

    def both(val):
        return lax.ppermute(val, 'sp', [(a, a ^ 3) for a in range(sp)])

    def after(val, *deps):
        return lax.optimization_barrier((val,) + deps)[0]

    def vec(*vals, dep=()):
        out = jnp.stack([jnp.asarray(v, jnp.int32) for v in vals])
        return after(out, *dep) if dep else out

    def step(x, dy, positions, gain, w_q, w_k, w_v, w_o):
        j = lax.axis_index('sp').astype(jnp.int32)
        rows, d = x.shape
        seq = rows * sp
        j1, j2, j3 = [j ^ n for n in (1, 2, 3)]
        dev = (j, j1, j2, j3)
        hpr = rows // HB
        ws = (w_q, w_k, w_v)

        gain_f = gain.astype(F32).reshape(1, d)

        cut, mid = rows - HB, rows // 2
        xa = x[mid:cut]
        positions = after(positions, xa)
        pos2 = over(positions)
        pos1 = near(positions)
        x2a = over(xa)
        xb = after(x, xa)[:mid]
        x2b = over(xb)
        x2c = over(after(x, xb)[cut:])
        x1 = near(x)
        pos3 = near(pos2)
        dy1 = near(after(dy, x1))

        pos = jnp.zeros((seq,), jnp.int32)
        for blk, val in zip(dev, (positions, pos1, pos2, pos3)):
            pos = lax.dynamic_update_slice(pos, val, (blk * rows,))
        inv_freq = ROPE_THETA ** (-jnp.arange(0, HEAD, 2).astype(F32) / HEAD)
        angles = pos.astype(F32)[:, None] * inv_freq[None, :]
        cos_h, sin_h = jnp.cos(angles), jnp.sin(angles)
        tabs = (jnp.concatenate([cos_h, cos_h], axis=1), jnp.concatenate([-sin_h, sin_h], axis=1))

        bufs = project(vec(j * hpr, j1 * hpr, j), (x, x1), gain_f, ws, tabs, None, seq)
        dbufs = dout(vec(j * hpr, j1 * hpr, j, dep=bufs), (dy, dy1), w_o, None, seq)

        chip, nh = j // 2, seq // BLK // 2
        tri = row_tasks(0, nh)
        first = seq // 2 - BLK
        square = [(i + nh, nh, 0, i) for i in range(nh)]

        def table(head, tasks):
            return jnp.concatenate([vec(*head, len(tasks)), jnp.asarray(tasks, jnp.int32).reshape(-1)])

        c_tasks = table((j1, 0), tri).at[HEADER - 1].set(nh - 1)
        local = attn_fwd("local", after(table((j1, chip), tri), *dbufs), *bufs[1:4])
        rest_tasks = jnp.where(chip == 0, table((j1, 0), row_tasks(nh, 2 * nh) * 2).at[HEADER - 1].set(nh),
                               table((j1, 1), tri + square))

        x2a = after(x2a, *bufs)
        x3a = near(x2a)
        x2b = after(x2b, *local)
        x3b = near(x2b)
        dyl = after(dy, *local)
        dya, dyb = dyl[:cut], dyl[cut:]
        dy2a, dy2b = over(dya), over(dyb)
        idx = vec(*(dev * hpr + at // HB for dev in (j2, j3) for at in (mid, 0)), j, dep=local)
        bufs = project(idx, (x2a, x2b, x3a, x3b), gain_f, ws, tabs, bufs, seq)
        x2c = after(x2c, *bufs)
        x3c = near(x2c)
        bufs = project(vec((j2 + 1) * hpr - 1, (j3 + 1) * hpr - 1, j), (x2c, x3c), gain_f, ws, tabs, bufs, seq)
        h_all, q, k, v, inv = bufs
        o, lse, o_hi, o_pair = attn_fwd("rest", rest_tasks, q, k, v, (seq - first, rows), local)
        orv = over(o_hi)
        o1 = near(o_pair)
        qc, kc, vc = project_first(vec(j2, dep=(o,)), h_all, ws, tabs, first)
        dy2a = after(dy2a, qc)
        dy3a = near(dy2a)
        oc = attn_fwd("local", c_tasks, qc, kc, vc)[0]

        dbufs = dout(vec(j2 * hpr, j3 * hpr, j, dep=(oc,)), (dy2a, dy3a), w_o, dbufs, seq)
        dy2b = after(dy2b, *dbufs)
        dy3b = near(dy2b)
        dbufs = dout(vec((j2 + 1) * hpr - 1, (j3 + 1) * hpr - 1, j), (dy2b, dy3b), w_o, dbufs, seq)
        dy_all, do = dbufs

        ga, ga_pair = attn_bwd(vec(j1, 0), q, do, o, k, v, lse, tabs, rows)
        ga2 = over(ga)
        ga1 = near(ga_pair)
        gb, gb_pair = attn_bwd(vec(j1, 1, dep=(ga,)), q, do, o, k, v, lse, tabs, rows)
        gb2 = over(gb)
        gb1 = near(gb_pair)

        orv = after(orv, gb)
        ox, ox_pair = pick_rows(vec(j, j1, nh - 1, dep=(gb,)), oc, orv, rows)
        o3 = near(ox_pair)
        wo_fin, wo_snd = dw_o(vec(j, j2, dep=(gb,)), o, oc, orv, dy_all)
        wo_rcv = near(wo_snd)
        result = out_proj(vec(*dev, dep=(wo_snd,)), x, (o, o1, ox, o3), w_o)
        ga2 = after(ga2, wo_snd)
        fq, fk, fv, snd, wo_fin, g3 = dw_own(vec(*dev, dep=(result,)), h_all, ga, gb, ga2, wo_rcv, wo_fin)
        rcv = near(snd)
        ga3 = near(g3)

        gb2 = after(gb2, snd)
        fq, fk, fv, snd_b, g3b = dw_group(vec(j2, j1), h_all, ga2, gb2, (fq, fk, fv))
        gb3 = near(g3b)
        rcv_b = near(snd_b)
        grad_x, dg, fq, fk, fv = dx_call(vec(*dev, dep=(snd_b,)), x, dy, gain_f, inv,
                                         (ga, gb, ga1, gb1, ga2, gb2, ga3, gb3), ws, rcv, (fq, fk, fv))
        dg = jnp.sum(dg, axis=0)
        dg = (dg + near(dg)) + (over(dg) + both(dg))
        fq, fk, fv = place(vec(j3), rcv_b, (fq, fk, fv))
        return result, grad_x, fq, fk, fv, wo_fin, dg

    seq_spec = P(('dp', 'sp'), None)
    whole = P(None, None)
    part_rows = P('dp', None)
    return jax.shard_map(step, mesh=mesh,
                         in_specs=(seq_spec, seq_spec, P(('dp', 'sp')), P(None), whole, whole, whole, whole),
                         out_specs=(seq_spec, seq_spec, part_rows, part_rows, part_rows, part_rows, P('dp')),
                         check_vma=False)
```
